256 devices in a mesh: groups: 2 (over z), seq: 128 (over y, x, core).
Axes of the slice: x: 8, y: 8, z: 2, core: 2. Of those that a mesh axis runs over, the one named last changes fastest.
The devices are a block of a 8x8x16 slice.
Arguments:
- queries: bfloat16 [256, 8192], P(('groups', 'seq')), parts along dimension 0, may hold values from -320 to 320, as said below
- span_keys: bfloat16 [256, 1024], P(('groups', 'seq')), parts along dimension 0, may hold values from -6 to 6
- span_values: bfloat16 [256, 1024], P(('groups', 'seq')), parts along dimension 0, may hold values from -6 to 6
- cache_keys: bfloat16 [65536, 1024], P(('groups', 'seq')), parts along dimension 0, may hold values from -6 to 6
- cache_values: bfloat16 [65536, 1024], P(('groups', 'seq')), parts along dimension 0, may hold values from -6 to 6
- page_table: int32 [4096], P(('groups', 'seq')), parts along dimension 0, may hold values from 0 to 2047, each once
- page_counts: int32 [256], P(('groups', 'seq')), parts along dimension 0, may hold values from 1 to 16, 1024 in all
- span_start: int32 [2], P('groups'), parts along dimension 0, may hold values from 16384 to 32767
Outputs:
- attended: bfloat16 [256, 8192], P(('groups', 'seq')), parts along dimension 0
The draws below stay inside these ranges and needn't reach their ends.
There are 2 independent parts, one for each index of `groups`. The reference program is written for one: setup_inputs(seed, part) draws one part's arguments, and reference() takes and returns one part's arrays. A program takes and returns all parts, laid end to end along the dimension named above; each array names one. Nothing has to cross between parts.
Inputs may be any that keep to these rules, and one draw needn't show every extreme that they name: `queries`: queries of every row; in some draws rows differ in scale by a large factor. `page_table`: A permutation of the 2048 logical pages. `page_counts`: counts of the shards sum to 1024; slots at or beyond a shard's count hold no page; some shard holds 16.
All inputs are finite; a program needn't handle non-finite values.
Results may differ from the reference program's by a relative error of at most 0.02.
The reference program's roundings to bfloat16 on the way count: a program that leaves them out, or rounds other values in their place, can miss the bound.
Values may be sent and summed in bfloat16 or wider, within the bound.
A program may use at most 64 MiB of HBM per device.

```python
import math
import jax
import jax.numpy as jnp
import numpy as np
from jax import lax

H = 64
KVH = 8
HD = 128
PAGE = 16
PAGES_DEV = 16
Q_TOK = 128
N_PAGES = 2048
LIVE_PAGES = 1024
N_SEQ = 128


def draw_queries(key, part):
    first_key = jax.random.fold_in(jax.random.fold_in(key, 11), 0)
    values = jnp.clip(jax.random.normal(first_key, (Q_TOK, H * HD), jnp.float32), -6.0, 6.0)
    return values.astype(jnp.bfloat16)


def shard_levels(rng, dims, shards, least, high):
    loudness = 1.0
    for dim, blocks in shards:
        draws = jax.random.uniform(jax.random.fold_in(jax.random.fold_in(rng, 6), dim), (blocks,), jnp.float32, least / len(shards), high / len(shards))
        loudness = loudness * jnp.repeat(jnp.exp(draws), dims[dim] // blocks).reshape((-1,) + (1,) * (len(dims) - 1 - dim))
    return loudness


def profile(count, total, reach, lean):
    portions = [(1 << 20) // math.isqrt(standing ** lean) + 1 for standing in range(2, count + 1)]
    rest, counts = total - reach - (count - 1), [1] * (count - 1)
    while rest > 0:
        candidates = [i for i in range(count - 1) if counts[i] < reach]
        whole, budget = sum([portions[i] for i in candidates]), rest
        for i in candidates:
            more = min(reach - counts[i], max(1, budget * portions[i] // whole), rest)
            counts[i] = counts[i] + more
            rest = rest - more
    return np.array([reach] + counts)


def uneven(stream_key, amount, total, bound, lean):
    if amount == 2:
        one = jax.random.randint(stream_key, (), max(1, total - bound), min(bound, total - 1) + 1)
        return jnp.stack([one, total - one])
    sizes = jnp.asarray(profile(amount, total, bound, lean), jnp.int32)
    couples = (amount - 1) // 2
    source_of, receiver = sizes[1:1 + 2 * couples:2], sizes[2:2 + 2 * couples:2]
    slack = jnp.minimum(source_of - 1, bound - receiver)
    moved = jax.random.randint(jax.random.fold_in(stream_key, 1), (couples,), 0, 1 << 20) % (slack + 1)
    sizes = sizes.at[1:1 + 2 * couples:2].set(source_of - moved).at[2:2 + 2 * couples:2].set(receiver + moved)
    return sizes[jax.random.permutation(jax.random.fold_in(stream_key, 2), amount)]


def gaussian(rng, dims, deviation, most, pieces=(), kind=jnp.bfloat16):
    values = deviation * jax.random.normal(rng, dims, jnp.float32)
    if pieces:
        values = values * shard_levels(rng, dims, pieces, -0.22, 0.18)
    return jnp.clip(values, -most, most).astype(kind)


def setup_inputs(seed: int = 0, part: int = 0) -> dict:
    splits = jax.random.split(jax.random.key(seed), 9)
    part_splits = jax.random.split(jax.random.fold_in(splits[8], part), 9)
    queries = draw_queries(jax.random.fold_in(jax.random.fold_in(splits[8], part), 71), part)
    span_keys = gaussian(part_splits[1], (Q_TOK, KVH * HD), 1.0, 6.0, ((0, 128),))
    span_values = gaussian(part_splits[2], (Q_TOK, KVH * HD), 1.0, 6.0, ((0, 128),))
    cache_keys = gaussian(part_splits[3], (N_PAGES * PAGE, KVH * HD), 1.0, 6.0, ((0, 128),))
    cache_values = gaussian(part_splits[4], (N_PAGES * PAGE, KVH * HD), 1.0, 6.0, ((0, 128),))
    page_table = jax.random.permutation(part_splits[5], N_PAGES).astype(jnp.int32)
    page_counts = uneven(part_splits[6], N_SEQ, LIVE_PAGES, PAGES_DEV, 2).astype(jnp.int32)
    span_start = jax.random.randint(part_splits[7], (1,), N_PAGES * PAGE // 2, N_PAGES * PAGE).astype(jnp.int32)
    return dict(queries=queries, span_keys=span_keys, span_values=span_values, cache_keys=cache_keys, cache_values=cache_values, page_table=page_table, page_counts=page_counts, span_start=span_start)


rope_base = 1000000.0
masked_low = -1e30


def rotate(values, positions, heads):
    count_rows = values.shape[0]
    width = values.shape[1] // heads
    half_width = width // 2
    frequency = rope_base ** (-(jnp.arange(half_width, dtype=jnp.float32) * 2.0 / width))
    angles = positions.astype(jnp.float32)[:, None] * frequency[None, :]
    cosine = jnp.cos(angles)[:, None, :]
    sine_part = jnp.sin(angles)[:, None, :]
    headed = values.astype(jnp.float32).reshape(count_rows, heads, width)
    first_half = headed[..., :half_width]
    second_half = headed[..., half_width:]
    turned = jnp.concatenate([first_half * cosine - second_half * sine_part, second_half * cosine + first_half * sine_part], axis=-1)
    return turned.reshape(count_rows, heads * width)


def rounded(values):
    return lax.optimization_barrier(values.astype(jnp.bfloat16)).astype(jnp.float32)


def reference(queries, span_keys, span_values, cache_keys, cache_values, page_table, page_counts, span_start):
    start = span_start[0]
    group = H // KVH
    factor = HD ** -0.5
    key_rows = PAGES_DEV * PAGE
    query_positions = start + jnp.arange(Q_TOK, dtype=jnp.int32)
    query_heads = rounded(rotate(queries, query_positions, H)).reshape(Q_TOK, KVH, group, HD)
    span_heads = rounded(rotate(span_keys, query_positions, KVH)).reshape(Q_TOK, KVH, HD)
    span_vals = span_values.astype(jnp.float32).reshape(Q_TOK, KVH, HD)

    def one_shard(carry, shard_id):
        run_max, run_num, run_den = carry
        keys = lax.dynamic_slice_in_dim(cache_keys, (shard_id * key_rows).astype(jnp.int32), key_rows, 0)
        vals = lax.dynamic_slice_in_dim(cache_values, (shard_id * key_rows).astype(jnp.int32), key_rows, 0)
        table = lax.dynamic_slice_in_dim(page_table, (shard_id * PAGES_DEV).astype(jnp.int32), PAGES_DEV, 0)
        row_ids = jnp.arange(key_rows, dtype=jnp.int32)
        slot_ids = row_ids // PAGE
        positions = jnp.repeat(table, PAGE) * PAGE + row_ids % PAGE
        usable = (slot_ids < page_counts[shard_id]) & (positions < start)
        key_heads = rounded(rotate(keys, positions, KVH)).reshape(key_rows, KVH, HD)
        scores = jnp.einsum('tkgd,skd->ktgs', query_heads, key_heads) * factor
        live = usable[None, None, None, :]
        best = jnp.max(jnp.where(live, scores, masked_low), axis=-1)
        weights = jnp.where(live, jnp.exp(scores - best[..., None]), 0.0)
        denom = jnp.sum(weights, axis=-1)
        numer = jnp.einsum('ktgs,skd->ktgd', rounded(weights), vals.astype(jnp.float32).reshape(key_rows, KVH, HD))
        newest = jnp.maximum(run_max, best)
        old_part = jnp.exp(run_max - newest)
        new_part = jnp.exp(best - newest)
        run_num = run_num * old_part[..., None] + numer * new_part[..., None]
        run_den = run_den * old_part + denom * new_part
        return (newest, run_num, run_den), None

    start_max = jnp.full((KVH, Q_TOK, group), masked_low, jnp.float32)
    start_num = jnp.zeros((KVH, Q_TOK, group, HD), jnp.float32)
    start_den = jnp.zeros((KVH, Q_TOK, group), jnp.float32)
    (pre_max, pre_num, pre_den), unused = lax.scan(one_shard, (start_max, start_num, start_den), jnp.arange(N_SEQ, dtype=jnp.int32))

    self_scores = jnp.einsum('tkgd,skd->ktgs', query_heads, span_heads) * factor
    causal = (jnp.arange(Q_TOK, dtype=jnp.int32)[None, :] <= jnp.arange(Q_TOK, dtype=jnp.int32)[:, None])[None, :, None, :]
    self_max = jnp.max(jnp.where(causal, self_scores, masked_low), axis=-1)
    self_weights = jnp.where(causal, jnp.exp(self_scores - self_max[..., None]), 0.0)
    self_den = jnp.sum(self_weights, axis=-1)
    self_num = jnp.einsum('ktgs,skd->ktgd', rounded(self_weights), span_vals)

    both = jnp.maximum(pre_max, self_max)
    first_weight = jnp.exp(pre_max - both)
    second_weight = jnp.exp(self_max - both)
    total_num = pre_num * first_weight[..., None] + self_num * second_weight[..., None]
    total_den = pre_den * first_weight + self_den * second_weight
    result = total_num / total_den[..., None]
    return result.transpose(1, 0, 2, 3).reshape(Q_TOK, H * HD).astype(jnp.bfloat16)
```

```python
import functools
import math

import jax
import jax.numpy as jnp
import numpy as np
from jax import lax
from jax.experimental import pallas as pl
from jax.experimental.pallas import tpu as pltpu
from jax.sharding import PartitionSpec as P

H = 64
KVH = 8
PAGE = 16
GROUP = H // KVH
ROPE_BASE = 1000000.0
DEAD = -1e30
FLOOR = -1e29
CLASSES = 4
MESH = pl.DeviceIdType.MESH
F32 = jnp.float32
BF16 = jnp.bfloat16


def rope_table(width, rows):
    half = width // 2
    freq = ROPE_BASE ** (-(np.arange(half, dtype=np.float64) * 2.0 / width))
    turns = np.concatenate([freq, freq]) / (2.0 * np.pi)
    pieces, rest = [], turns
    for _ in range(2):
        scale = 2.0 ** (np.floor(np.log2(rest)) - 7.0)
        part = np.floor(rest / scale) * scale
        pieces.append(part)
        rest = rest - part
    pieces.append(rest)
    sign = np.concatenate([-np.ones(half), np.ones(half)])
    angle = np.arange(rows, dtype=np.float64)[:, None] * np.concatenate([freq, freq])[None, :]
    pad = np.zeros((8 - len(pieces) - 1, width))
    return np.concatenate(
        [np.stack(pieces), sign[None], pad, np.cos(angle), np.sin(angle) * sign[None]]
    ).astype(np.float32)


def cos_sin(position, table_ref):
    def part(k):
        turn = position * table_ref[k : k + 1, :]
        return turn - jnp.floor(turn)

    turn = part(0) + part(1) + part(2)
    turn = turn - jnp.floor(turn + 0.5)
    angle = turn * (2.0 * math.pi)
    return jnp.cos(angle), jnp.sin(angle) * table_ref[3:4, :]


def kernel(
    side,
    start_ref,
    count_ref,
    pages_ref,
    table_ref,
    q_hbm,
    sk_hbm,
    sv_hbm,
    k_hbm,
    v_hbm,
    out_ref,
    q_raw,
    sk_raw,
    sv_raw,
    k_raw,
    q_rows,
    cos_ref,
    sin_ref,
    kx,
    vx,
    kall,
    vall,
    kspan,
    vspan,
    span_f32,
    bias_ref,
    qsrc,
    q1,
    q2,
    scores,
    o1src,
    s1src,
    o1,
    s1,
    o2src,
    s2src,
    o2,
    s2,
    wts,
    local_sem,
    kv_send,
    kv_recv,
    q1_send,
    q1_recv,
    q2_send,
    q2_recv,
    o1_send,
    o1_recv,
    o2_send,
    o2_recv,
):
    width = out_ref.shape[1]
    rows = k_hbm.shape[0]
    half_rows = rows // 2
    units = kall.shape[0]
    row_toks = 2 * side
    piece = row_toks * GROUP
    me = lax.axis_index("seq")
    core = me % 2
    x = (me // 2) % side
    y = me // (2 * side)

    def at(px, py, pc):
        return ((py % side) * side + (px % side)) * 2 + pc

    copies = [
        pltpu.make_async_copy(q_hbm, q_raw, local_sem.at[0]),
        pltpu.make_async_copy(sk_hbm, sk_raw, local_sem.at[1]),
        pltpu.make_async_copy(sv_hbm, sv_raw, local_sem.at[2]),
        pltpu.make_async_copy(k_hbm, k_raw, local_sem.at[3]),
    ]
    v_copies = []
    for h in range(KVH):
        for hf in range(2):
            v_copies.append(
                pltpu.make_async_copy(
                    v_hbm.at[pl.ds(hf * half_rows, half_rows), pl.ds(h * width, width)],
                    vx.at[h, hf, pl.ds(0, half_rows), :],
                    local_sem.at[4 + 2 * h + hf],
                )
            )
    for copy in copies + v_copies:
        copy.start()

    barrier = pltpu.get_barrier_semaphore()

    def greet(device):
        pl.semaphore_signal(barrier, inc=1, device_id={"seq": device}, device_id_type=MESH)

    for dx in range(1, side):
        for pc in range(2):
            greet(at(x + dx, y, pc))
    greet(at(x, y, 1 - core))
    for dy in range(1, side):
        greet(at(x, y + dy, core))
    greet(at(x, y + 1, 1 - core))
    greet(at(x, y + side - 1, 1 - core))
    partners = 2 * (side - 1) + 1 + (side - 1) + 2

    start = start_ref[0]
    count = count_ref[0]

    own_pos = (start + me).astype(F32)
    own_cos, own_sin = cos_sin(jnp.full((8, width), own_pos, F32), table_ref)
    copies[0].wait()
    q_all = q_raw[...].astype(F32)
    for r in range(H):
        q_rows[r : r + 1, :] = q_all[:, r * width : (r + 1) * width]
    for e in range(2):
        for pc in range(2):
            for b in range(2):
                head = 2 * (e + 2 * b) + pc
                part = q_rows[head * GROUP : (head + 1) * GROUP, :]
                turned = part * own_cos + pltpu.roll(part, width // 2, 1) * own_sin
                qsrc[e, pc, b] = turned.astype(BF16)

    pl.semaphore_wait(barrier, partners)

    def q1_copy(px, pc):
        return pltpu.make_async_remote_copy(
            src_ref=qsrc.at[px % 2, pc],
            dst_ref=q1.at[:, 2 * x + core],
            send_sem=q1_send.at[2 * px + pc],
            recv_sem=q1_recv.at[2 * x + core],
            device_id={"seq": at(px, y, pc)},
            device_id_type=MESH,
        )

    def q1_arrival(px, pc):
        return pltpu.make_async_remote_copy(
            src_ref=qsrc.at[0, 0],
            dst_ref=q1.at[:, 2 * px + pc],
            send_sem=q1_send.at[2 * px + pc],
            recv_sem=q1_recv.at[2 * px + pc],
            device_id={"seq": at(px, y, pc)},
            device_id_type=MESH,
        )

    far_first = [side // 2]
    for step in range(side // 2 - 1, 0, -1):
        far_first += [step, side - step]
    near_first = far_first[::-1]
    row_partners = [((x + dx) % side, pc) for dx in far_first for pc in range(2)]
    row_partners.append((x, 1 - core))
    for px, pc in row_partners:
        q1_copy(px, pc).start()
    for b in range(2):
        q1[b, 2 * x + core] = qsrc[x % 2, core, b]

    f_me = (x + 2 * y) % CLASSES
    tile_row = lax.broadcasted_iota(jnp.int32, (16, width), 0)
    lane = lax.broadcasted_iota(jnp.int32, (1, width), 1)
    biases = []
    for hf in range(2):
        page = jnp.zeros((1, width), jnp.int32)
        for j in range(half_rows // PAGE):
            page = jnp.where(lane // PAGE == j, pages_ref[hf * (half_rows // PAGE) + j], page)
        slot = hf * (half_rows // PAGE) + lane // PAGE
        usable = (slot < count) & (page * PAGE + lane % PAGE < start)
        biases.append(jnp.where(usable, 0.0, DEAD).astype(F32))

    copies[2].wait()
    sv_all = sv_raw[...].astype(F32)
    for h in range(KVH):
        own_v = jnp.broadcast_to(sv_all[:, h * width : (h + 1) * width], (16, width))
        vx[h, 0, half_rows : half_rows + 16, :] = jnp.where(tile_row == 0, own_v, 0.0).astype(BF16)
        vx[h, 1, half_rows : half_rows + 16, :] = jnp.zeros((16, width), BF16)

    def kv_copies(which, buf, landing):
        out = []

        def add(index, head, halves, slot, device):
            src = buf.at[head] if halves is None else buf.at[head, halves]
            dst = landing.at[pl.ds(slot, 2)] if halves is None else landing.at[slot]
            out.append(
                pltpu.make_async_remote_copy(
                    src_ref=src,
                    dst_ref=dst,
                    send_sem=kv_send.at[which, index[0]],
                    recv_sem=kv_recv.at[which, index[1]],
                    device_id={"seq": device},
                    device_id_type=MESH,
                )
            )

        for pc in range(2):
            head = 2 * ((f_me + 1) % CLASSES) + pc
            add((1 + pc, 1 + core), head, None, 4 + 2 * core, at(x + 1, y, pc))
            head = 2 * ((f_me + 3) % CLASSES) + pc
            add((3 + pc, 3 + core), head, None, 8 + 2 * core, at(x + side - 1, y, pc))
            head = 2 * ((f_me + 2) % CLASSES) + pc
            add((5 + pc, 5 + core), head, 0, 12 + core, at(x, y + 1, pc))
            add((7 + pc, 7 + core), head, 1, 14 + core, at(x, y + side - 1, pc))
        head = 2 * f_me + (1 - core)
        add((0, 0), head, None, 2 * core, at(x, y, 1 - core))
        return out

    def kv_arrivals(which, buf, landing):
        out = []

        def add(index, double, slot, device):
            out.append(
                pltpu.make_async_remote_copy(
                    src_ref=buf.at[0] if double else buf.at[0, 0],
                    dst_ref=landing.at[pl.ds(slot, 2)] if double else landing.at[slot],
                    send_sem=kv_send.at[which, index],
                    recv_sem=kv_recv.at[which, index],
                    device_id={"seq": device},
                    device_id_type=MESH,
                )
            )

        add(0, True, 2 * (1 - core), at(x, y, 1 - core))
        for pc in range(2):
            add(1 + pc, True, 4 + 2 * pc, at(x + side - 1, y, pc))
            add(3 + pc, True, 8 + 2 * pc, at(x + 1, y, pc))
            add(5 + pc, False, 12 + pc, at(x, y + side - 1, pc))
            add(7 + pc, False, 14 + pc, at(x, y + 1, pc))
        return out

    for copy in v_copies:
        copy.wait()
    v_sends = kv_copies(1, vx, vall)
    for copy in v_sends:
        copy.start()
    my_head = 2 * f_me + core
    for hf in range(2):
        vall[2 * core + hf] = vx[my_head, hf]

    page_row = lax.broadcasted_iota(jnp.int32, (16, width), 0)
    page_pos = jnp.zeros((16, width), jnp.int32)
    for j in range(rows // PAGE):
        page_pos = jnp.where(page_row == j, pages_ref[j] * PAGE, page_pos)
    page_cos, page_sin = cos_sin(page_pos.astype(F32), table_ref)
    row_cos = table_ref[8 : 8 + PAGE, :]
    row_sin = table_ref[8 + PAGE : 8 + 2 * PAGE, :]
    for j in range(rows // PAGE):
        pc_, ps_ = page_cos[j : j + 1, :], page_sin[j : j + 1, :]
        cos_ref[j * PAGE : (j + 1) * PAGE, :] = pc_ * row_cos - ps_ * row_sin
        sin_ref[j * PAGE : (j + 1) * PAGE, :] = ps_ * row_cos + pc_ * row_sin
    copies[1].wait()
    sk_all = sk_raw[...].astype(F32)
    copies[3].wait()
    for h in range(KVH):
        span = jnp.broadcast_to(sk_all[:, h * width : (h + 1) * width], (8, width))
        span = span * own_cos + pltpu.roll(span, width // 2, 1) * own_sin
        span = jnp.broadcast_to(span[0:1, :], (16, width))
        for hf in range(2):
            first = span if hf == 0 else jnp.zeros((16, width), F32)
            tile = jnp.where(tile_row == 0, first, jnp.where(tile_row == 1, biases[hf], 0.0))
            kx[h, hf, half_rows : half_rows + 16, :] = tile.astype(BF16)

    @pl.loop(0, KVH)
    def _(h):
        cols = pl.ds(pl.multiple_of(h * width, width), width)
        for hf in range(2):
            span_rows = slice(hf * half_rows, (hf + 1) * half_rows)
            part = k_raw[span_rows, cols].astype(F32)
            turned = part * cos_ref[span_rows, :]
            turned = turned + pltpu.roll(part, width // 2, 1) * sin_ref[span_rows, :]
            kx[h, hf, 0:half_rows, :] = turned.astype(BF16)

    k_sends = kv_copies(0, kx, kall)
    for copy in k_sends:
        copy.start()
    for hf in range(2):
        kall[2 * core + hf] = kx[my_head, hf]

    for px, pc in row_partners:
        q1_arrival(px, pc).wait_recv()

    def bit(py):
        return (x // 2 + py) % 2

    def q2_copy(py):
        return pltpu.make_async_remote_copy(
            src_ref=q1.at[bit(py)],
            dst_ref=q2.at[y],
            send_sem=q2_send.at[py],
            recv_sem=q2_recv.at[y],
            device_id={"seq": at(x, py, core)},
            device_id_type=MESH,
        )

    def q2_arrival(py):
        return pltpu.make_async_remote_copy(
            src_ref=q1.at[0],
            dst_ref=q2.at[py],
            send_sem=q2_send.at[py],
            recv_sem=q2_recv.at[py],
            device_id={"seq": at(x, py, core)},
            device_id_type=MESH,
        )

    for dy in far_first:
        q2_copy((y + dy) % side).start()
    q2[y] = q1[bit(y)]

    for arrival in kv_arrivals(1, vx, vall) + kv_arrivals(0, kx, kall):
        arrival.wait_recv()
    span_units = [0, 2, 4, 6, 8, 10, 12, 13]
    span_toks = [
        at(x, y, 0),
        at(x, y, 1),
        at(x + side - 1, y, 0),
        at(x + side - 1, y, 1),
        at(x + 1, y, 0),
        at(x + 1, y, 1),
        at(x, y + side - 1, 0),
        at(x, y + side - 1, 1),
    ]
    for u in range(units):
        tile = kall[u, half_rows : half_rows + 16, :].astype(F32)
        bias_ref[:, u * half_rows : (u + 1) * half_rows] = tile[1:2, :]
        if u in span_units:
            k = span_units.index(u)
            span_f32[0, k : k + 1, :] = tile[0:1, :]
            tile = vall[u, half_rows : half_rows + 16, :].astype(F32)
            span_f32[1, k : k + 1, :] = tile[0:1, :]
    kspan[...] = jnp.zeros_like(kspan)
    vspan[...] = jnp.zeros_like(vspan)
    zero8 = jnp.zeros((8, width), F32)
    kspan[0:16, :] = jnp.concatenate([span_f32[0], zero8]).astype(BF16)
    vspan[0:16, :] = jnp.concatenate([span_f32[1], zero8]).astype(BF16)
    span_tok = jnp.full((1, width), 1 << 20, jnp.int32)
    for k, tok in enumerate(span_toks):
        span_tok = jnp.where(lane == k, tok, span_tok)

    exponent = width**-0.5 / math.log(2.0)
    contract = (((1,), (1,)), ((), ()))
    chunk = 2 * half_rows

    def o1_copies(py):
        return [
            pltpu.make_async_remote_copy(
                src_ref=src.at[py],
                dst_ref=dst.at[y],
                send_sem=o1_send.at[k, py],
                recv_sem=o1_recv.at[k, y],
                device_id={"seq": at(x, py, core)},
                device_id_type=MESH,
            )
            for k, (src, dst) in enumerate(((o1src, o1), (s1src, s1)))
        ]

    def o1_arrivals(py):
        return [
            pltpu.make_async_remote_copy(
                src_ref=src.at[py],
                dst_ref=dst.at[py],
                send_sem=o1_send.at[k, py],
                recv_sem=o1_recv.at[k, py],
                device_id={"seq": at(x, py, core)},
                device_id_type=MESH,
            )
            for k, (src, dst) in enumerate(((o1src, o1), (s1src, s1)))
        ]

    def attend(py):
        query = q2[py].astype(F32).reshape(piece, width).astype(BF16)
        best = None
        for u in range(0, units, 2):
            keys = kall[u : u + 2, 0:half_rows, :].reshape(chunk, width)
            s = lax.dot_general(query, keys, contract, preferred_element_type=F32)
            s = s + bias_ref[:, u * half_rows : (u + 2) * half_rows]
            scores[:, u * half_rows : (u + 2) * half_rows] = s
            for k in range(chunk // width):
                part = s[:, k * width : (k + 1) * width]
                best = part if best is None else jnp.maximum(best, part)
        s = lax.dot_general(query, kspan[...], contract, preferred_element_type=F32)
        q_tok = py * row_toks + lax.broadcasted_iota(jnp.int32, (piece, width), 0) // GROUP
        s_span = jnp.where(span_tok <= q_tok, s, DEAD)
        best = jnp.maximum(best, s_span)
        top = jnp.maximum(jnp.max(best, axis=1, keepdims=True), FLOOR)
        w = jnp.exp2((s_span - top) * exponent)
        total = w
        num = jnp.dot(w.astype(BF16), vspan[...], preferred_element_type=F32)
        for u in range(0, units, 2):
            s = scores[:, u * half_rows : (u + 2) * half_rows]
            w = jnp.exp2((s - top) * exponent)
            for k in range(chunk // width):
                total = total + w[:, k * width : (k + 1) * width]
            vals = vall[u : u + 2, 0:half_rows, :].reshape(chunk, width)
            num = num + jnp.dot(w.astype(BF16), vals, preferred_element_type=F32)
        den = jnp.sum(total, axis=1, keepdims=True)
        cols = lax.broadcasted_iota(jnp.int32, (piece, width), 1)
        stat = jnp.where(cols == 0, top, jnp.where(cols == 1, den, 0.0))
        return num.astype(BF16), stat.T[0:8, :]

    num, stat = attend(y)
    o1[y] = num
    s1[y] = stat

    @pl.loop(1, side)
    def _(k):
        dy = jnp.where(k % 2 == 1, (k + 1) // 2, side - k // 2)
        py = (y + dy) % side
        q2_arrival(py).wait_recv()
        num, stat = attend(py)
        o1src[py] = num
        s1src[py] = stat
        for copy in o1_copies(py):
            copy.start()

    for dy in near_first:
        for arrival in o1_arrivals((y + dy) % side):
            arrival.wait_recv()
    tops, dens = [], []
    weight_rows = []
    srcs = []
    for b in range(2):
        ys = [(x // 2 + b) % 2 + 2 * k for k in range(side // 2)]
        stats = [s1[py] for py in ys]
        top = functools.reduce(jnp.maximum, [s[0:1, :] for s in stats])
        ws = [jnp.exp2((s[0:1, :] - top) * exponent) for s in stats]
        den = sum(w * s[1:2, :] for w, s in zip(ws, stats))
        tops.append(top)
        dens.append(den)
        weight_rows += ws
        srcs.append(ys)
    stacked = jnp.concatenate(weight_rows, axis=0)
    wide = jnp.concatenate([stacked, jnp.zeros((width - 8, width), F32)], axis=0)
    columns = wide.T
    row_id = lax.broadcasted_iota(jnp.int32, (8, width), 0)
    merged_stat = jnp.zeros((8, width), F32)
    for b in range(2):
        total = None
        for k, py in enumerate(srcs[b]):
            part = o1[py].astype(F32) * columns[:, 4 * b + k : 4 * b + k + 1]
            total = part if total is None else total + part
        o2src[b] = total.reshape(row_toks, GROUP, width).astype(BF16)
        merged_stat = jnp.where(row_id == 2 * b, tops[b], merged_stat)
        merged_stat = jnp.where(row_id == 2 * b + 1, dens[b], merged_stat)
    s2src[...] = merged_stat

    def o2_copies(px, pc):
        tok = 2 * px + pc
        return [
            pltpu.make_async_remote_copy(
                src_ref=src,
                dst_ref=dst.at[2 * x + core],
                send_sem=o2_send.at[k, tok],
                recv_sem=o2_recv.at[k, 2 * x + core],
                device_id={"seq": at(px, y, pc)},
                device_id_type=MESH,
            )
            for k, (src, dst) in enumerate(((o2src.at[:, tok], o2), (s2src, s2)))
        ]

    def o2_arrivals(px, pc):
        tok = 2 * px + pc
        return [
            pltpu.make_async_remote_copy(
                src_ref=src,
                dst_ref=dst.at[tok],
                send_sem=o2_send.at[k, tok],
                recv_sem=o2_recv.at[k, tok],
                device_id={"seq": at(px, y, pc)},
                device_id_type=MESH,
            )
            for k, (src, dst) in enumerate(((o2src.at[:, 0], o2), (s2src, s2)))
        ]

    for px, pc in row_partners:
        for copy in o2_copies(px, pc):
            copy.start()
    o2[2 * x + core] = o2src[:, 2 * x + core]
    s2[2 * x + core] = merged_stat
    for px, pc in row_partners:
        for arrival in o2_arrivals(px, pc):
            arrival.wait_recv()

    normal = []
    for e in range(2):
        for pc in range(2):
            for b in range(2):
                stats = [s2[2 * (e + 2 * k) + pc] for k in range(side // 2)]
                top = functools.reduce(jnp.maximum, [s[2 * b : 2 * b + 1, :] for s in stats])
                ws = [jnp.exp2((s[2 * b : 2 * b + 1, :] - top) * exponent) for s in stats]
                den = sum(w * s[2 * b + 1 : 2 * b + 2, :] for w, s in zip(ws, stats))
                normal += [w / den for w in ws]
    wts[...] = jnp.zeros_like(wts)
    for k, w in enumerate(normal):
        wts[k : k + 1, :] = w
    wts[...] = wts[...].T
    mine = wts[pl.ds(pl.multiple_of((2 * x + core) * GROUP, GROUP), GROUP), :]
    for e in range(2):
        for pc in range(2):
            for b in range(2):
                total = None
                for k in range(side // 2):
                    col = ((e * 2 + pc) * 2 + b) * (side // 2) + k
                    part = o2[2 * (e + 2 * k) + pc, b].astype(F32) * mine[:, col : col + 1]
                    total = part if total is None else total + part
                head = 2 * (e + 2 * b) + pc
                out_ref[head * GROUP : (head + 1) * GROUP, :] = total

    for px, pc in row_partners:
        q1_copy(px, pc).wait_send()
        for copy in o2_copies(px, pc):
            copy.wait_send()
    for dy in near_first:
        q2_copy((y + dy) % side).wait_send()
        for copy in o1_copies((y + dy) % side):
            copy.wait_send()
    for copy in v_sends + k_sends:
        copy.wait_send()


def solution(mesh):
    seq = mesh.shape["seq"]
    side = math.isqrt(seq // 2)

    def body(
        queries, span_keys, span_values, cache_keys, cache_values, page_table, page_counts, span_start
    ):
        width = queries.shape[1] // H
        rows = cache_keys.shape[0]
        half = rows // 2
        row_toks = 2 * side
        piece = row_toks * GROUP
        table = jnp.asarray(rope_table(width, PAGE))
        units = 16
        vm = pltpu.VMEM
        dma = pltpu.SemaphoreType.DMA
        smem = pl.BlockSpec(memory_space=pltpu.SMEM)
        vmem = pl.BlockSpec(memory_space=pltpu.VMEM)
        hbm = pl.BlockSpec(memory_space=pl.ANY)
        scratch = [
            vm((1, H * width), BF16),
            vm((1, KVH * width), BF16),
            vm((1, KVH * width), BF16),
            vm((rows, KVH * width), BF16),
            vm((H, width), F32),
            vm((rows, width), F32),
            vm((rows, width), F32),
            vm((KVH, 2, half + 16, width), BF16),
            vm((KVH, 2, half + 16, width), BF16),
            vm((units, half + 16, width), BF16),
            vm((units, half + 16, width), BF16),
            vm((width, width), BF16),
            vm((width, width), BF16),
            vm((2, 8, width), F32),
            vm((1, units * half), F32),
            vm((2, 2, 2, GROUP, width), BF16),
            vm((2, row_toks, GROUP, width), BF16),
            vm((side, row_toks, GROUP, width), BF16),
            vm((piece, units * half), F32),
            vm((side, piece, width), BF16),
            vm((side, 8, width), F32),
            vm((side, piece, width), BF16),
            vm((side, 8, width), F32),
            vm((2, row_toks, GROUP, width), BF16),
            vm((8, width), F32),
            vm((row_toks, 2, GROUP, width), BF16),
            vm((row_toks, 8, width), F32),
            vm((width, width), F32),
            dma((4 + 2 * KVH,)),
            dma((2, 9)),
            dma((2, 9)),
            dma((row_toks,)),
            dma((row_toks,)),
            dma((side,)),
            dma((side,)),
            dma((2, side)),
            dma((2, side)),
            dma((2, row_toks)),
            dma((2, row_toks)),
        ]
        out = pl.pallas_call(
            functools.partial(kernel, side),
            out_shape=jax.ShapeDtypeStruct((H, width), F32),
            in_specs=[smem, smem, smem, vmem, hbm, hbm, hbm, hbm, hbm],
            out_specs=vmem,
            scratch_shapes=scratch,
            compiler_params=pltpu.CompilerParams(collective_id=0, has_side_effects=True),
            name="paged_prefix",
        )(
            span_start,
            page_counts,
            page_table,
            table,
            queries,
            span_keys,
            span_values,
            cache_keys,
            cache_values,
        )
        return out.astype(BF16).reshape(queries.shape)

    in_specs = (
        P(("groups", "seq"), None),
        P(("groups", "seq"), None),
        P(("groups", "seq"), None),
        P(("groups", "seq"), None),
        P(("groups", "seq"), None),
        P(("groups", "seq")),
        P(("groups", "seq")),
        P("groups"),
    )
    out_specs = P(("groups", "seq"), None)
    return jax.shard_map(body, mesh=mesh, in_specs=in_specs, out_specs=out_specs, check_vma=False)
```

```python
import functools
import math

import jax
import jax.numpy as jnp
import numpy as np
from jax import lax
from jax.experimental import pallas as pl
from jax.experimental.pallas import tpu as pltpu
from jax.sharding import PartitionSpec as P

H = 64
KVH = 8
PAGE = 16
GROUP = H // KVH
ROPE_BASE = 1000000.0
DEAD = -1e30
FLOOR = -1e29
CLASSES = 4
MESH = pl.DeviceIdType.MESH
F32 = jnp.float32
BF16 = jnp.bfloat16


def rope_table(width, rows):
    half = width // 2
    freq = ROPE_BASE ** (-(np.arange(half, dtype=np.float64) * 2.0 / width))
    turns = np.concatenate([freq, freq]) / (2.0 * np.pi)
    pieces, rest = [], turns
    for _ in range(2):
        scale = 2.0 ** (np.floor(np.log2(rest)) - 7.0)
        part = np.floor(rest / scale) * scale
        pieces.append(part)
        rest = rest - part
    pieces.append(rest)
    sign = np.concatenate([-np.ones(half), np.ones(half)])
    angle = np.arange(rows, dtype=np.float64)[:, None] * np.concatenate([freq, freq])[None, :]
    pad = np.zeros((8 - len(pieces) - 1, width))
    return np.concatenate(
        [np.stack(pieces), sign[None], pad, np.cos(angle), np.sin(angle) * sign[None]]
    ).astype(np.float32)


def cos_sin(position, table_ref):
    def part(k):
        turn = position * table_ref[k : k + 1, :]
        return turn - jnp.floor(turn)

    turn = part(0) + part(1) + part(2)
    turn = turn - jnp.floor(turn + 0.5)
    angle = turn * (2.0 * math.pi)
    return jnp.cos(angle), jnp.sin(angle) * table_ref[3:4, :]


def kernel(
    side,
    start_ref,
    count_ref,
    pages_ref,
    table_ref,
    q_hbm,
    sk_hbm,
    sv_hbm,
    k_hbm,
    v_hbm,
    out_ref,
    q_raw,
    sk_raw,
    sv_raw,
    k_raw,
    q_rows,
    cos_ref,
    sin_ref,
    kx,
    vx,
    kall,
    vall,
    kspan,
    vspan,
    span_f32,
    bias_ref,
    qsrc,
    q1,
    q2,
    scores,
    o1src,
    s1src,
    o1,
    s1,
    o2src,
    s2src,
    o2,
    s2,
    wts,
    local_sem,
    kv_send,
    kv_recv,
    q1_send,
    q1_recv,
    q2_send,
    q2_recv,
    o1_send,
    o1_recv,
    o2_send,
    o2_recv,
):
    width = q_rows.shape[1]
    rows = k_hbm.shape[0]
    half_rows = rows // 2
    units = kall.shape[0]
    row_toks = 2 * side
    piece = row_toks * GROUP
    me = lax.axis_index("seq")
    core = me % 2
    x = (me // 2) % side
    y = me // (2 * side)
    u = jnp.where(core == 0, x, y)
    v = jnp.where(core == 0, y, x)
    other = 1 - core

    def dev(pu, pv, pc):
        pu, pv = pu % side, pv % side
        px = jnp.where(core == 0, pu, pv)
        py = jnp.where(core == 0, pv, pu)
        return (py * side + px) * 2 + pc

    def remote(src, dst, send, recv, device):
        return pltpu.make_async_remote_copy(
            src_ref=src,
            dst_ref=dst,
            send_sem=send,
            recv_sem=recv,
            device_id={"seq": device},
            device_id_type=MESH,
        )

    copies = [
        pltpu.make_async_copy(q_hbm, q_raw, local_sem.at[0]),
        pltpu.make_async_copy(sk_hbm, sk_raw, local_sem.at[1]),
        pltpu.make_async_copy(sv_hbm, sv_raw, local_sem.at[2]),
        pltpu.make_async_copy(k_hbm, k_raw, local_sem.at[3]),
    ]
    v_copies = []
    for h in range(KVH):
        for hf in range(2):
            v_copies.append(
                pltpu.make_async_copy(
                    v_hbm.at[pl.ds(hf * half_rows, half_rows), pl.ds(h * width, width)],
                    vx.at[h, hf, pl.ds(0, half_rows), :],
                    local_sem.at[4 + 2 * h + hf],
                )
            )
    for copy in copies + v_copies:
        copy.start()

    barrier = pltpu.get_barrier_semaphore()

    def greet(device):
        pl.semaphore_signal(barrier, inc=1, device_id={"seq": device}, device_id_type=MESH)

    for d in range(1, side):
        for pc in range(2):
            greet(dev(u + d, v, pc))
            greet(dev(u, v + d, pc))
    greet(dev(u, v, other))
    partners = 4 * (side - 1) + 1

    start = start_ref[0]
    count = count_ref[0]

    own_pos = (start + me).astype(F32)
    own_cos, own_sin = cos_sin(jnp.full((8, width), own_pos, F32), table_ref)
    copies[0].wait()
    q_all = q_raw[...].astype(F32)
    for r in range(H):
        q_rows[r : r + 1, :] = q_all[:, r * width : (r + 1) * width]
    for net in range(2):
        for e in range(2):
            for b in range(2):
                head = CLASSES * net + e + 2 * b
                part = q_rows[head * GROUP : (head + 1) * GROUP, :]
                turned = part * own_cos + pltpu.roll(part, width // 2, 1) * own_sin
                qsrc[net, e, b] = turned.astype(BF16)

    pl.semaphore_wait(barrier, partners)

    far_first = [side // 2]
    for step in range(side // 2 - 1, 0, -1):
        far_first += [step, side - step]
    near_first = far_first[::-1]
    q1_copies = []
    for d in far_first + [0]:
        if d:
            pu = (u + d) % side
            q1_copies.append(
                remote(
                    qsrc.at[core, pu % 2],
                    q1.at[:, 2 * u + core],
                    q1_send.at[2 * d],
                    q1_recv.at[2 * u + core],
                    dev(pu, v, core),
                )
            )
        pv = (v + d) % side
        q1_copies.append(
            remote(
                qsrc.at[other, pv % 2],
                q1.at[:, 2 * v + core],
                q1_send.at[2 * d + 1],
                q1_recv.at[2 * v + core],
                dev(u, pv, other),
            )
        )
    for copy in q1_copies:
        copy.start()
    for b in range(2):
        q1[b, 2 * u + core] = qsrc[core, u % 2, b]

    line_slots = [2 * ((u + d) % side) + pc for d in near_first for pc in range(2)]
    line_slots.append(2 * u + other)

    tile_row = lax.broadcasted_iota(jnp.int32, (16, width), 0)
    lane = lax.broadcasted_iota(jnp.int32, (1, width), 1)
    half_pages = half_rows // PAGE
    biases = []
    for hf in range(2):
        page = jnp.zeros((1, width), jnp.int32)
        for j in range(half_pages):
            page = jnp.where(lane // PAGE == j, pages_ref[hf * half_pages + j], page)
        slot = hf * half_pages + lane // PAGE
        usable = (slot < count) & (page * PAGE + lane % PAGE < start)
        biases.append(jnp.where(usable, 0.0, DEAD).astype(F32))

    copies[2].wait()
    sv_all = sv_raw[...].astype(F32)
    for h in range(KVH):
        own_v = jnp.broadcast_to(sv_all[:, h * width : (h + 1) * width], (16, width))
        vx[h, 0, half_rows : half_rows + 16, :] = jnp.where(tile_row == 0, own_v, 0.0).astype(BF16)
        vx[h, 1, half_rows : half_rows + 16, :] = jnp.zeros((16, width), BF16)

    def kv_copies(which, buf, landing):
        out = []

        def add(there, here, head, half, slot, device):
            src = buf.at[head] if half is None else buf.at[head, half]
            dst = landing.at[pl.ds(slot, 2)] if half is None else landing.at[slot]
            out.append(remote(src, dst, kv_send.at[which, here], kv_recv.at[which, there], device))

        for own in (True, False):
            net = core if own else other
            nu, nv = (u, v) if own else (v, u)
            here = 0 if own else 1

            def at(pu, pv, own=own, net=net):
                return dev(pu, pv, net) if own else dev(pv, pu, net)

            base = nu + 2 * nv
            head = CLASSES * net + (base + 1) % CLASSES
            add(1 + core, 1 + here, head, None, 4 + 2 * core, at(nu + 1, nv))
            head = CLASSES * net + (base + 3) % CLASSES
            add(3 + core, 3 + here, head, None, 8 + 2 * core, at(nu + side - 1, nv))
            head = CLASSES * net + (base + 2) % CLASSES
            add(5 + core, 5 + here, head, 0, 12 + core, at(nu, nv + 1))
            add(7 + core, 7 + here, head, 1, 14 + core, at(nu, nv + side - 1))
            if not own:
                add(0, 0, CLASSES * net + base % CLASSES, None, 2 * core, at(nu, nv))
        return out

    def kv_arrivals(which, buf, landing):
        out = []

        def add(index, double, slot):
            out.append(
                remote(
                    buf.at[0] if double else buf.at[0, 0],
                    landing.at[pl.ds(slot, 2)] if double else landing.at[slot],
                    kv_send.at[which, index],
                    kv_recv.at[which, index],
                    dev(u, v, other),
                )
            )

        add(0, True, 2 * other)
        for pc in range(2):
            add(1 + pc, True, 4 + 2 * pc)
            add(3 + pc, True, 8 + 2 * pc)
            add(5 + pc, False, 12 + pc)
            add(7 + pc, False, 14 + pc)
        return out

    for copy in v_copies:
        copy.wait()
    v_sends = kv_copies(1, vx, vall)
    for copy in v_sends:
        copy.start()
    my_head = CLASSES * core + (u + 2 * v) % CLASSES
    for hf in range(2):
        vall[2 * core + hf] = vx[my_head, hf]

    page_pos = jnp.zeros((16, width), jnp.int32)
    for j in range(rows // PAGE):
        page_pos = jnp.where(tile_row == j, pages_ref[j] * PAGE, page_pos)
    page_cos, page_sin = cos_sin(page_pos.astype(F32), table_ref)
    row_cos = table_ref[8 : 8 + PAGE, :]
    row_sin = table_ref[8 + PAGE : 8 + 2 * PAGE, :]
    for j in range(rows // PAGE):
        pc_, ps_ = page_cos[j : j + 1, :], page_sin[j : j + 1, :]
        cos_ref[j * PAGE : (j + 1) * PAGE, :] = pc_ * row_cos - ps_ * row_sin
        sin_ref[j * PAGE : (j + 1) * PAGE, :] = ps_ * row_cos + pc_ * row_sin
    copies[1].wait()
    sk_all = sk_raw[...].astype(F32)
    copies[3].wait()
    for h in range(KVH):
        span = jnp.broadcast_to(sk_all[:, h * width : (h + 1) * width], (8, width))
        span = span * own_cos + pltpu.roll(span, width // 2, 1) * own_sin
        span = jnp.broadcast_to(span[0:1, :], (16, width))
        for hf in range(2):
            first = span if hf == 0 else jnp.zeros((16, width), F32)
            tile = jnp.where(tile_row == 0, first, jnp.where(tile_row == 1, biases[hf], 0.0))
            kx[h, hf, half_rows : half_rows + 16, :] = tile.astype(BF16)

    @pl.loop(0, KVH)
    def _(h):
        cols = pl.ds(pl.multiple_of(h * width, width), width)
        for hf in range(2):
            span_rows = slice(hf * half_rows, (hf + 1) * half_rows)
            part = k_raw[span_rows, cols].astype(F32)
            turned = part * cos_ref[span_rows, :]
            turned = turned + pltpu.roll(part, width // 2, 1) * sin_ref[span_rows, :]
            kx[h, hf, 0:half_rows, :] = turned.astype(BF16)

    k_sends = kv_copies(0, kx, kall)
    for copy in k_sends:
        copy.start()
    for hf in range(2):
        kall[2 * core + hf] = kx[my_head, hf]

    for slot in line_slots:
        remote(
            qsrc.at[0, 0], q1.at[:, slot], q1_send.at[slot], q1_recv.at[slot], dev(u, v, other)
        ).wait_recv()

    def bit(pv):
        return (u // 2 + pv) % 2

    q2_sends = []
    for d in far_first:
        pv = (v + d) % side
        q2_sends.append(
            remote(q1.at[bit(pv)], q2.at[v], q2_send.at[pv], q2_recv.at[v], dev(u, pv, core))
        )
    for copy in q2_sends:
        copy.start()
    q2[v] = q1[bit(v)]

    def q2_arrival(pv):
        return remote(q1.at[0], q2.at[pv], q2_send.at[pv], q2_recv.at[pv], dev(u, pv, core))

    for copy in q1_copies:
        copy.wait_send()
    for arrival in kv_arrivals(1, vx, vall) + kv_arrivals(0, kx, kall):
        arrival.wait_recv()
    span_units = [0, 2, 4, 6, 8, 10, 12, 13]
    span_toks = [
        dev(pu, pv, pc)
        for pu, pv in ((u, v), (u + side - 1, v), (u + 1, v), (u, v + side - 1))
        for pc in range(2)
    ]
    for unit in range(units):
        tile = kall[unit, half_rows : half_rows + 16, :].astype(F32)
        bias_ref[:, unit * half_rows : (unit + 1) * half_rows] = tile[1:2, :]
        if unit in span_units:
            k = span_units.index(unit)
            span_f32[0, k : k + 1, :] = tile[0:1, :]
            tile = vall[unit, half_rows : half_rows + 16, :].astype(F32)
            span_f32[1, k : k + 1, :] = tile[0:1, :]
    kspan[...] = jnp.zeros_like(kspan)
    vspan[...] = jnp.zeros_like(vspan)
    zero8 = jnp.zeros((8, width), F32)
    kspan[0:16, :] = jnp.concatenate([span_f32[0], zero8]).astype(BF16)
    vspan[0:16, :] = jnp.concatenate([span_f32[1], zero8]).astype(BF16)
    span_tok = jnp.full((1, width), 1 << 20, jnp.int32)
    for k, tok in enumerate(span_toks):
        span_tok = jnp.where(lane == k, tok, span_tok)

    exponent = width**-0.5 / math.log(2.0)
    contract = (((1,), (1,)), ((), ()))
    chunk = 2 * half_rows
    pair = 2 * piece

    def o1_copies(pv):
        return [
            remote(src.at[pv], dst.at[v], o1_send.at[k, pv], o1_recv.at[k, v], dev(u, pv, core))
            for k, (src, dst) in enumerate(((o1src, o1), (s1src, s1)))
        ]

    def o1_arrivals(pv):
        return [
            remote(src.at[pv], dst.at[pv], o1_send.at[k, pv], o1_recv.at[k, pv], dev(u, pv, core))
            for k, (src, dst) in enumerate(((o1src, o1), (s1src, s1)))
        ]

    slot_of = lax.broadcasted_iota(jnp.int32, (piece, 1), 0) // GROUP

    def token_of(pv):
        along = jnp.where(core == 0, 2, 2 * side)
        across = jnp.where(core == 0, 2 * side, 2)
        return (slot_of // 2) * along + pv * across + slot_of % 2

    def attend(pvs):
        query = jnp.concatenate(
            [q2[pv].astype(F32).reshape(piece, width).astype(BF16) for pv in pvs]
        )
        best = None
        for unit in range(0, units, 2):
            keys = kall[unit : unit + 2, 0:half_rows, :].reshape(chunk, width)
            s = lax.dot_general(query, keys, contract, preferred_element_type=F32)
            s = s + bias_ref[:, unit * half_rows : (unit + 2) * half_rows]
            scores[:, unit * half_rows : (unit + 2) * half_rows] = s
            for k in range(chunk // width):
                part = s[:, k * width : (k + 1) * width]
                best = part if best is None else jnp.maximum(best, part)
        s = lax.dot_general(query, kspan[...], contract, preferred_element_type=F32)
        q_tok = jnp.concatenate([token_of(pv) for pv in pvs])
        s_span = jnp.where(span_tok <= q_tok, s, DEAD)
        best = jnp.maximum(best, s_span)
        top = jnp.maximum(jnp.max(best, axis=1, keepdims=True), FLOOR)
        w = jnp.exp2((s_span - top) * exponent)
        total = w
        num = jnp.dot(w.astype(BF16), vspan[...], preferred_element_type=F32)
        for unit in range(0, units, 2):
            s = scores[:, unit * half_rows : (unit + 2) * half_rows]
            w = jnp.exp2((s - top) * exponent)
            for k in range(chunk // width):
                total = total + w[:, k * width : (k + 1) * width]
            vals = vall[unit : unit + 2, 0:half_rows, :].reshape(chunk, width)
            num = num + jnp.dot(w.astype(BF16), vals, preferred_element_type=F32)
        den = jnp.sum(total, axis=1, keepdims=True)
        cols = lax.broadcasted_iota(jnp.int32, (pair, width), 1)
        stat = jnp.where(cols == 0, top, jnp.where(cols == 1, den, 0.0))
        for k, pv in enumerate(pvs):
            part = num[k * piece : (k + 1) * piece].astype(BF16)
            part_stat = stat[k * piece : (k + 1) * piece].T[0:2, :]
            o1src[pv] = part
            s1src[pv] = part_stat

            @pl.when(pv != v)
            def _(pv=pv):
                for copy in o1_copies(pv):
                    copy.start()

            @pl.when(pv == v)
            def _(pv=pv, part=part, part_stat=part_stat):
                o1[pv] = part
                s1[pv] = part_stat

    @pl.loop(0, side // 2)
    def _(k):
        pvs = [k + 1, jnp.where(k == side // 2 - 1, 0, side - 1 - k)]
        for pv in pvs:

            @pl.when(pv != v)
            def _(pv=pv):
                q2_arrival(pv).wait_recv()

        attend(pvs)

    for copy in v_sends + k_sends + q2_sends:
        copy.wait_send()
    for d in near_first:
        for arrival in o1_arrivals((v + d) % side):
            arrival.wait_recv()
    tops, dens, weight_rows, srcs = [], [], [], []
    for b in range(2):
        vs = [(u // 2 + b) % 2 + 2 * k for k in range(side // 2)]
        stats = [s1[pv] for pv in vs]
        top = functools.reduce(jnp.maximum, [s[0:1, :] for s in stats])
        ws = [jnp.exp2((s[0:1, :] - top) * exponent) for s in stats]
        den = sum(w * s[1:2, :] for w, s in zip(ws, stats))
        tops.append(top)
        dens.append(den)
        weight_rows += ws
        srcs.append(vs)
    stacked = jnp.concatenate(weight_rows, axis=0)
    wide = jnp.concatenate([stacked, jnp.zeros((width - 8, width), F32)], axis=0)
    columns = wide.T
    for b in range(2):
        total = None
        for k, pv in enumerate(srcs[b]):
            part = o1[pv].astype(F32) * columns[:, 4 * b + k : 4 * b + k + 1]
            total = part if total is None else total + part
        o2src[b] = total.reshape(row_toks, GROUP, width).astype(BF16)
        s2src[2 * b : 2 * b + 1, :] = tops[b]
        s2src[2 * b + 1 : 2 * b + 2, :] = dens[b]

    line = core * side + u
    o2_sends = []
    for d in far_first + [0]:
        for own in (True, False):
            if d == 0 and own:
                continue
            pu = (u + d) % side
            pc = core if own else other
            slot = 2 * pu + pc
            for k, (src, dst) in enumerate(((o2src.at[:, slot], o2), (s2src, s2))):
                o2_sends.append(
                    remote(
                        src, dst.at[line], o2_send.at[k, slot], o2_recv.at[k, line], dev(pu, v, pc)
                    )
                )
    for copy in o2_sends:
        copy.start()
    o2[line] = o2src[:, 2 * u + core]
    s2[line] = s2src[...]
    for d in near_first:
        for copy in o1_copies((v + d) % side):
            copy.wait_send()
    o2_lines = [core * side + (u + d) % side for d in near_first]
    o2_lines += [other * side + (v + d) % side for d in near_first + [0]]
    for src_line in o2_lines:
        for k, (src, dst) in enumerate(((o2src.at[:, 0], o2), (s2src, s2))):
            remote(
                src,
                dst.at[src_line],
                o2_send.at[k, src_line],
                o2_recv.at[k, src_line],
                dev(u, v, other),
            ).wait_recv()

    normal = []
    for net in range(2):
        for e in range(2):
            for b in range(2):
                stats = [s2[net * side + e + 2 * k] for k in range(side // 2)]
                top = functools.reduce(jnp.maximum, [s[2 * b : 2 * b + 1, :] for s in stats])
                ws = [jnp.exp2((s[2 * b : 2 * b + 1, :] - top) * exponent) for s in stats]
                den = sum(w * s[2 * b + 1 : 2 * b + 2, :] for w, s in zip(ws, stats))
                normal += [w / den for w in ws]
    wts[...] = jnp.zeros_like(wts)
    for k, w in enumerate(normal):
        wts[k : k + 1, :] = w
    wts[...] = wts[...].T
    slots = (2 * x + core, 2 * y + core)
    for net in range(2):
        mine = wts[pl.ds(pl.multiple_of(slots[net] * GROUP, GROUP), GROUP), :]
        for e in range(2):
            for b in range(2):
                total = None
                for k in range(side // 2):
                    col = ((net * 2 + e) * 2 + b) * (side // 2) + k
                    part = o2[net * side + e + 2 * k, b].astype(F32) * mine[:, col : col + 1]
                    total = part if total is None else total + part
                head = CLASSES * net + e + 2 * b
                for g in range(GROUP):
                    at = (head * GROUP + g) * width
                    out_ref[:, at : at + width] = total[g : g + 1, :]
    for copy in o2_sends:
        copy.wait_send()


def solution(mesh):
    seq = mesh.shape["seq"]
    side = math.isqrt(seq // 2)

    def body(
        queries, span_keys, span_values, cache_keys, cache_values, page_table, page_counts, span_start
    ):
        width = queries.shape[1] // H
        rows = cache_keys.shape[0]
        half = rows // 2
        row_toks = 2 * side
        piece = row_toks * GROUP
        table = jnp.asarray(rope_table(width, PAGE))
        units = 16
        vm = pltpu.VMEM
        dma = pltpu.SemaphoreType.DMA
        smem = pl.BlockSpec(memory_space=pltpu.SMEM)
        vmem = pl.BlockSpec(memory_space=pltpu.VMEM)
        hbm = pl.BlockSpec(memory_space=pl.ANY)
        scratch = [
            vm((1, H * width), BF16),
            vm((1, KVH * width), BF16),
            vm((1, KVH * width), BF16),
            vm((rows, KVH * width), BF16),
            vm((H, width), F32),
            vm((rows, width), F32),
            vm((rows, width), F32),
            vm((KVH, 2, half + 16, width), BF16),
            vm((KVH, 2, half + 16, width), BF16),
            vm((units, half + 16, width), BF16),
            vm((units, half + 16, width), BF16),
            vm((width, width), BF16),
            vm((width, width), BF16),
            vm((2, 8, width), F32),
            vm((1, units * half), F32),
            vm((2, 2, 2, GROUP, width), BF16),
            vm((2, row_toks, GROUP, width), BF16),
            vm((side, row_toks, GROUP, width), BF16),
            vm((2 * piece, units * half), F32),
            vm((side, piece, width), BF16),
            vm((side, 2, width), F32),
            vm((side, piece, width), BF16),
            vm((side, 2, width), F32),
            vm((2, row_toks, GROUP, width), BF16),
            vm((4, width), F32),
            vm((row_toks, 2, GROUP, width), BF16),
            vm((row_toks, 4, width), F32),
            vm((width, width), F32),
            dma((4 + 2 * KVH,)),
            dma((2, 9)),
            dma((2, 9)),
            dma((row_toks,)),
            dma((row_toks,)),
            dma((side,)),
            dma((side,)),
            dma((2, side)),
            dma((2, side)),
            dma((2, row_toks)),
            dma((2, row_toks)),
        ]
        out = pl.pallas_call(
            functools.partial(kernel, side),
            out_shape=jax.ShapeDtypeStruct(queries.shape, F32),
            in_specs=[smem, smem, smem, vmem, hbm, hbm, hbm, hbm, hbm],
            out_specs=vmem,
            scratch_shapes=scratch,
            compiler_params=pltpu.CompilerParams(collective_id=0, has_side_effects=True),
            name="paged_prefix",
        )(
            span_start,
            page_counts,
            page_table,
            table,
            queries,
            span_keys,
            span_values,
            cache_keys,
            cache_values,
        )
        return out.astype(BF16)

    in_specs = (
        P(("groups", "seq"), None),
        P(("groups", "seq"), None),
        P(("groups", "seq"), None),
        P(("groups", "seq"), None),
        P(("groups", "seq"), None),
        P(("groups", "seq")),
        P(("groups", "seq")),
        P("groups"),
    )
    out_specs = P(("groups", "seq"), None)
    return jax.shard_map(body, mesh=mesh, in_specs=in_specs, out_specs=out_specs, check_vma=False)
```

```python
import functools
import math

import jax
import jax.numpy as jnp
import numpy as np
from jax import lax
from jax.experimental import pallas as pl
from jax.experimental.pallas import tpu as pltpu
from jax.sharding import PartitionSpec as P

H = 64
KVH = 8
PAGE = 16
GROUP = H // KVH
ROPE_BASE = 1000000.0
DEAD = -1e30
FLOOR = -1e29
CLASSES = 4
MESH = pl.DeviceIdType.MESH
F32 = jnp.float32
BF16 = jnp.bfloat16
EXTRA = 16


def rope_table(width, rows):
    half = width // 2
    freq = ROPE_BASE ** (-(np.arange(half, dtype=np.float64) * 2.0 / width))
    turns = np.concatenate([freq, freq]) / (2.0 * np.pi)
    pieces, rest = [], turns
    for _ in range(2):
        scale = 2.0 ** (np.floor(np.log2(rest)) - 7.0)
        part = np.floor(rest / scale) * scale
        pieces.append(part)
        rest = rest - part
    pieces.append(rest)
    sign = np.concatenate([-np.ones(half), np.ones(half)])
    angle = np.arange(rows, dtype=np.float64)[:, None] * np.concatenate([freq, freq])[None, :]
    pad = np.zeros((8 - len(pieces) - 1, width))
    return np.concatenate(
        [np.stack(pieces), sign[None], pad, np.cos(angle), np.sin(angle) * sign[None]]
    ).astype(np.float32)


def cos_sin(position, table_ref):
    def part(k):
        turn = position * table_ref[k : k + 1, :]
        return turn - jnp.floor(turn)

    turn = part(0) + part(1) + part(2)
    turn = turn - jnp.floor(turn + 0.5)
    angle = turn * (2.0 * math.pi)
    return jnp.cos(angle), jnp.sin(angle) * table_ref[3:4, :]


def in_three(value):
    high = value.astype(BF16).astype(F32)
    middle = (value - high).astype(BF16).astype(F32)
    return [high, middle, value - high - middle]


def kernel(
    side,
    start_hbm,
    count_hbm,
    pages_hbm,
    table_hbm,
    q_hbm,
    sk_hbm,
    sv_hbm,
    k_hbm,
    v_hbm,
    out_ref,
    start_ref,
    count_ref,
    pages_ref,
    table_ref,
    q_raw,
    sk_raw,
    sv_raw,
    k_raw,
    q_rows,
    cos_ref,
    sin_ref,
    kx,
    vx,
    kall,
    vall,
    vturned,
    kbias,
    rows16,
    kspan,
    vspan,
    qsrc,
    q1,
    q2,
    scores,
    o1src,
    o1,
    o2src,
    o2,
    local_sem,
    kv_send,
    kv_recv,
    q1_send,
    q1_recv,
    q2_send,
    q2_recv,
    o1_send,
    o1_recv,
    o2_send,
    o2_recv,
    told,
    side_in,
):
    width = q_rows.shape[1]
    rows = k_hbm.shape[0]
    half_rows = rows // 2
    units = kall.shape[0]
    toks = 2 * side
    piece = toks * GROUP
    me = lax.axis_index("seq")
    core = me % 2
    x = (me // 2) % side
    y = me // (2 * side)
    u = jnp.where(core == 0, x, y)
    v = jnp.where(core == 0, y, x)
    other = 1 - core

    def chip(px, py, pc):
        return ((py % side) * side + px % side) * 2 + pc

    def dev(pu, pv, pc):
        return chip(jnp.where(core == 0, pu, pv), jnp.where(core == 0, pv, pu), pc)

    def remote(src, dst, send, recv, device):
        return pltpu.make_async_remote_copy(
            src_ref=src,
            dst_ref=dst,
            send_sem=send,
            recv_sem=recv,
            device_id={"seq": device},
            device_id_type=MESH,
        )

    def sent(ref, sem):
        remote(ref, ref, sem, sem, chip(x, y, other)).wait_send()

    def landed(ref, sem):
        remote(ref, ref, sem, sem, chip(x, y, other)).wait_recv()

    local = {
        name: pltpu.make_async_copy(src, dst, local_sem.at[k])
        for k, (name, src, dst) in enumerate(
            (
                ("start", start_hbm, start_ref),
                ("count", count_hbm, count_ref),
                ("pages", pages_hbm, pages_ref),
                ("table", table_hbm, table_ref),
                ("q", q_hbm, q_raw),
                ("sk", sk_hbm, sk_raw),
                ("sv", sv_hbm, sv_raw),
                ("k", k_hbm, k_raw),
            )
        )
    }
    for copy in local.values():
        copy.start()
    for h in range(KVH):
        for hf in range(2):
            pltpu.make_async_copy(
                v_hbm.at[pl.ds(hf * half_rows, half_rows), pl.ds(h * width, width)],
                vx.at[h, hf],
                local_sem.at[len(local)],
            ).start()

    barrier = pltpu.get_barrier_semaphore()

    def signal(sem, device):
        pl.semaphore_signal(sem, inc=1, device_id={"seq": device}, device_id_type=MESH)

    for d in (1, side - 1):
        signal(barrier, chip(x + d, y, 0))
        signal(barrier, chip(x, y + d, 0))

    @pl.when(core == 1)
    def _():
        signal(barrier, chip(x, y, 0))
        for d in range(1, side):
            signal(barrier, chip(x + d, y, 1))
            signal(barrier, chip(x, y + d, 1))

    for name in ("start", "count", "pages", "table", "q"):
        local[name].wait()
    start = start_ref[0]
    count = count_ref[0]
    own_pos = (start + me).astype(F32)
    own_cos, own_sin = cos_sin(jnp.full((8, width), own_pos, F32), table_ref)
    q_all = q_raw[...].astype(F32)
    for r in range(H):
        q_rows[r : r + 1, :] = q_all[:, r * width : (r + 1) * width]
    for net in range(2):
        for e in range(2):
            for b in range(2):
                head = CLASSES * net + e + 2 * b
                part = q_rows[head * GROUP : (head + 1) * GROUP, :]
                turned = part * own_cos + pltpu.roll(part, width // 2, 1) * own_sin
                qsrc[net, e, b] = turned.astype(BF16)

    @pl.when(core == 0)
    def _():
        pl.semaphore_wait(barrier, 2 * 4 + 1)
        signal(told, chip(x, y, 1))

    @pl.when(core == 1)
    def _():
        pl.semaphore_wait(told, 1)

    def send_cache(which, buf, landing):
        def send(head, half, slot, device):
            src = buf.at[head] if half is None else buf.at[head, half]
            dst = landing.at[pl.ds(slot, 2)] if half is None else landing.at[slot]
            remote(src, dst, kv_send.at[which], kv_recv.at[which], device).start()

        for own in (True, False):
            net = core if own else other
            nu, nv = (u, v) if own else (v, u)

            def at(pu, pv, own=own, net=net):
                return dev(pu, pv, net) if own else dev(pv, pu, net)

            base = nu + 2 * nv
            head = CLASSES * net + (base + 1) % CLASSES
            send(head, None, 4 + 2 * core, at(nu + 1, nv))
            head = CLASSES * net + (base + 3) % CLASSES
            send(head, None, 8 + 2 * core, at(nu + side - 1, nv))
            head = CLASSES * net + (base + 2) % CLASSES
            send(head, 0, 12 + core, at(nu, nv + 1))
            send(head, 1, 14 + core, at(nu, nv + side - 1))
            if not own:
                send(CLASSES * net + base % CLASSES, None, 2 * core, at(nu, nv))

    my_head = CLASSES * core + (u + 2 * v) % CLASSES

    pltpu.make_async_copy(vx, vx, local_sem.at[len(local)]).wait()
    send_cache(1, vx, vall)
    for hf in range(2):
        vall[2 * core + hf] = vx[my_head, hf]

    tile_row = lax.broadcasted_iota(jnp.int32, (EXTRA, width), 0)
    lane = lax.broadcasted_iota(jnp.int32, (1, width), 1)
    half_pages = half_rows // PAGE
    biases = []
    for hf in range(2):
        page = jnp.zeros((1, width), jnp.int32)
        for j in range(half_pages):
            page = jnp.where(lane // PAGE == j, pages_ref[hf * half_pages + j], page)
        slot = hf * half_pages + lane // PAGE
        usable = (slot < count) & (page * PAGE + lane % PAGE < start)
        biases.append(jnp.where(usable, 0.0, DEAD).astype(F32))
    page_pos = jnp.zeros((16, width), jnp.int32)
    for j in range(rows // PAGE):
        page_pos = jnp.where(tile_row == j, pages_ref[j] * PAGE, page_pos)
    page_cos, page_sin = cos_sin(page_pos.astype(F32), table_ref)
    row_cos = table_ref[8 : 8 + PAGE, :]
    row_sin = table_ref[8 + PAGE : 8 + 2 * PAGE, :]
    for j in range(rows // PAGE):
        pc_, ps_ = page_cos[j : j + 1, :], page_sin[j : j + 1, :]
        cos_ref[j * PAGE : (j + 1) * PAGE, :] = pc_ * row_cos - ps_ * row_sin
        sin_ref[j * PAGE : (j + 1) * PAGE, :] = ps_ * row_cos + pc_ * row_sin
    for name in ("sk", "sv", "k"):
        local[name].wait()
    sk_all = sk_raw[...].astype(F32)
    sv_all = sv_raw[...].astype(F32)
    for h in range(KVH):
        span = jnp.broadcast_to(sk_all[:, h * width : (h + 1) * width], (8, width))
        span = span * own_cos + pltpu.roll(span, width // 2, 1) * own_sin
        span = jnp.broadcast_to(span[0:1, :], (EXTRA, width))
        value = jnp.broadcast_to(sv_all[:, h * width : (h + 1) * width], (EXTRA, width))
        for hf in range(2):
            tile = jnp.where(tile_row == 0, span, jnp.where(tile_row == 2, value, 0.0))
            tile = jnp.where(tile_row == 1, biases[hf], tile)
            kx[h, hf, half_rows : half_rows + EXTRA, :] = tile.astype(BF16)

    @pl.loop(0, KVH)
    def _(h):
        cols = pl.ds(pl.multiple_of(h * width, width), width)
        for hf in range(2):
            span_rows = slice(hf * half_rows, (hf + 1) * half_rows)
            part = k_raw[span_rows, cols].astype(F32)
            turned = part * cos_ref[span_rows, :]
            turned = turned + pltpu.roll(part, width // 2, 1) * sin_ref[span_rows, :]
            kx[h, hf, 0:half_rows, :] = turned.astype(BF16)

    far_first = [side // 2]
    for step in range(side // 2 - 1, 0, -1):
        far_first += [step, side - step]

    @pl.when(core == 1)
    def _():
        pl.semaphore_wait(barrier, 2 * (side - 1))
        signal(told, chip(x, y, 0))

    @pl.when(core == 0)
    def _():
        pl.semaphore_wait(told, 1)
        for d in far_first:
            signal(side_in, chip(x + d, y, 1))
            signal(side_in, chip(x, y + d, 1))

    def send_q1(net, along, device):
        spot = 2 * (x if net == 0 else y) + core
        remote(
            qsrc.at[net, along % 2], q1.at[net, :, spot], q1_send, q1_recv.at[net], device
        ).start()

    for d in far_first:
        send_q1(0, (x + d) % side, chip(x + d, y, 1))
        send_q1(1, (y + d) % side, chip(x, y + d, 1))

    @pl.when(core == 0)
    def _():
        send_q1(0, x, chip(x, y, 1))
        send_q1(1, y, chip(x, y, 1))

    send_cache(0, kx, kall)
    for hf in range(2):
        kall[2 * core + hf] = kx[my_head, hf]

    @pl.when(core == 1)
    def _():
        for net, spot in ((0, 2 * x + 1), (1, 2 * y + 1)):
            for b in range(2):
                q1[net, b, spot] = qsrc[net, (x if net == 0 else y) % 2, b]
        pl.semaphore_wait(side_in, 2 * (side - 1))
        for net in range(2):
            landed(q1.at[net, :, pl.ds(0, toks - 1)], q1_recv.at[net])
            nu, nv = (x, y) if net == 0 else (y, x)

            def send_q2(pv, device, net=net, nu=nu, nv=nv):
                remote(
                    q1.at[net, (nu // 2 + pv) % 2],
                    q2.at[nv],
                    q2_send.at[net],
                    q2_recv.at[nv],
                    device,
                ).start()

            for d in far_first:
                pv = (nv + d) % side
                send_q2(pv, chip(x, pv, 0) if net == 0 else chip(pv, y, 1))
            if net == 0:
                send_q2(y, chip(x, y, 0))
            else:
                q2[x] = q1[1, (y // 2 + x) % 2]

    landed(vall.at[pl.ds(0, units - 2)], kv_recv.at[1])
    for unit in range(units):
        vturned[:, unit * half_rows : (unit + 1) * half_rows] = vall[unit].T

    landed(kall.at[pl.ds(0, units - 2)], kv_recv.at[0])
    span_units = [0, 2, 4, 6, 8, 10, 12, 13]
    span_toks = [
        dev(pu, pv, pc)
        for pu, pv in ((u, v), (u + side - 1, v), (u + 1, v), (u, v + side - 1))
        for pc in range(2)
    ]
    rows16[...] = jnp.zeros_like(rows16)
    for unit in range(units):
        tile = kall[unit, half_rows : half_rows + EXTRA, :].astype(F32)
        rows16[0, unit : unit + 1, :] = tile[1:2, :]
        if unit in span_units:
            k = span_units.index(unit)
            rows16[1, k : k + 1, :] = tile[0:1, :]
            rows16[2, k : k + 1, :] = tile[2:3, :]
    zeros = jnp.zeros((width - 16, width), F32)
    bias_cols = jnp.concatenate([rows16[0], zeros]).T
    for unit in range(units):
        turned = bias_cols if unit == 0 else pltpu.roll(bias_cols, width - unit, 1)
        kbias[unit * half_rows : (unit + 1) * half_rows, :] = turned.astype(BF16)
    kspan[...] = rows16[1].astype(BF16)
    vspan[...] = jnp.concatenate([rows16[2], zeros]).T.astype(BF16)
    span_tok = jnp.full((16, piece), 1 << 20, jnp.int32)
    for k, tok in enumerate(span_toks):
        span_tok = jnp.where(tile_row == k, tok, span_tok)

    exponent = width**-0.5 / math.log(2.0)
    contract = (((1,), (1,)), ((), ()))
    chunk = 2 * half_rows
    cols = 2 * piece

    def send_o1(pv):
        remote(
            o1src.at[pv], o1.at[core, v], o1_send, o1_recv.at[core], dev(u, pv, 1)
        ).start()

    col_slot = lax.broadcasted_iota(jnp.int32, (1, piece), 1) // GROUP
    tok_along = jnp.where(core == 0, 2, 2 * side)
    tok_across = jnp.where(core == 0, 2 * side, 2)
    col_tok = (col_slot // 2) * tok_along + col_slot % 2
    one_hot = jnp.where(lax.broadcasted_iota(jnp.int32, (cols, width), 1) == 0, 1.0, 0.0).astype(BF16)

    def attend(pvs):
        query = jnp.concatenate(
            [q2[pv].astype(F32).reshape(piece, width).astype(BF16) for pv in pvs]
        )
        query = jnp.concatenate([query, one_hot], axis=1)
        s = lax.dot_general(kspan[...], query[:, :width], contract, preferred_element_type=F32)
        live = jnp.concatenate([span_tok <= col_tok + pv * tok_across for pv in pvs], axis=1)
        s_span = jnp.where(live, s, DEAD)
        best = jnp.maximum(s_span[0:8], s_span[8:16])
        for k in range(units // 2):
            keys = kall[2 * k : 2 * k + 2, 0:half_rows, :].reshape(chunk, width)
            keys = jnp.concatenate([keys, kbias[k * chunk : (k + 1) * chunk, :]], axis=1)
            s = lax.dot_general(keys, query, contract, preferred_element_type=F32)
            scores[k * chunk : (k + 1) * chunk, :] = s
            best = jnp.maximum(best, jnp.max(s.reshape(chunk // 8, 8, cols), axis=0))
        top = jnp.maximum(jnp.max(best, axis=0, keepdims=True), FLOOR)
        w = jnp.exp2((s_span - top) * exponent)
        total = w[0:8] + w[8:16]
        w = jnp.concatenate([w, jnp.zeros((width - 16, cols), F32)])
        num = jnp.dot(vspan[...], w.astype(BF16), preferred_element_type=F32)
        for k in range(units // 2):
            w = jnp.exp2((scores[k * chunk : (k + 1) * chunk, :] - top) * exponent)
            total = total + jnp.sum(w.reshape(chunk // 8, 8, cols), axis=0)
            num = num + jnp.dot(
                vturned[:, k * chunk : (k + 1) * chunk],
                w.astype(BF16),
                preferred_element_type=F32,
            )
        den = jnp.sum(total, axis=0, keepdims=True)
        stat = jnp.concatenate(in_three(top) + in_three(den) + [jnp.zeros((EXTRA - 6, cols), F32)])
        for k, pv in enumerate(pvs):
            lanes = slice(k * piece, (k + 1) * piece)
            o1src[pv, 0:width, :] = num[:, lanes].astype(BF16)
            o1src[pv, width : width + EXTRA, :] = stat[:, lanes].astype(BF16)

            @pl.when((pv != v) | (core == 0))
            def _(pv=pv):
                send_o1(pv)

            @pl.when((pv == v) & (core == 1))
            def _(pv=pv):
                o1[1, pv] = o1src[pv]

    @pl.loop(0, side // 2)
    def _(k):
        pvs = [k + 1, (k + 1 + side // 2) % side]
        for pv in pvs:

            @pl.when((pv != v) | (core == 0))
            def _(pv=pv):
                landed(q2.at[pv], q2_recv.at[pv])

        attend(pvs)

    sent(vall.at[pl.ds(0, units - 2)], kv_send.at[1])
    sent(kall.at[pl.ds(0, units - 2)], kv_send.at[0])

    @pl.when(core == 0)
    def _():
        sent(q1.at[0], q1_send)
        sent(o1.at[0], o1_send)

    @pl.when(core == 1)
    def _():
        sent(q1.at[0, :, pl.ds(0, toks - 2)], q1_send)
        sent(q2, q2_send.at[0])
        sent(q2.at[pl.ds(0, side - 1)], q2_send.at[1])
        for net in range(2):
            landed(o1.at[net] if net == 0 else o1.at[net, pl.ds(0, side - 1)], o1_recv.at[net])
            nu = x if net == 0 else y
            stats = []
            for b in range(2):
                vs = [(nu // 2 + b) % 2 + 2 * k for k in range(side // 2)]
                tiles = [o1[net, pv, width : width + EXTRA, :].astype(F32) for pv in vs]
                tops = [t[0:1] + t[1:2] + t[2:3] for t in tiles]
                dens = [t[3:4] + t[4:5] + t[5:6] for t in tiles]
                top = functools.reduce(jnp.maximum, tops)
                ws = [jnp.exp2((t - top) * exponent) for t in tops]
                stats += in_three(top) + in_three(sum(w * d for w, d in zip(ws, dens)))
                total = None
                for w, pv in zip(ws, vs):
                    part = o1[net, pv, 0:width, :].astype(F32) * w
                    total = part if total is None else total + part
                o2src[net, :, b] = total.T.reshape(toks, GROUP, width).astype(BF16)
            stat = jnp.concatenate(stats + [jnp.zeros((width - len(stats), piece), F32)]).T
            o2src[net, :, 2] = stat.reshape(toks, GROUP, width).astype(BF16)
            line = x if net == 0 else side + y

            def send_o2(slot, device, net=net, line=line):
                remote(o2src.at[net, slot], o2.at[line], o2_send, o2_recv, device).start()

            for d in far_first:
                for pc in range(2):
                    if net == 0:
                        px = (x + d) % side
                        send_o2(2 * px + pc, chip(px, y, pc))
                    else:
                        py = (y + d) % side
                        send_o2(2 * py + pc, chip(x, py, pc))
            send_o2(2 * nu, chip(x, y, 0))
            o2[line] = o2src[net, 2 * nu + 1]
        sent(o1.at[0, pl.ds(0, side - 1)], o1_send)
        landed(o2.at[pl.ds(0, toks - 2)], o2_recv)
        sent(o2src.at[:, pl.ds(0, toks - 1)], o2_send)

    @pl.when(core == 0)
    def _():
        landed(o2, o2_recv)

    tops, dens = [[], []], [[], []]
    for src in range(toks):
        tile = o2[src, 2].astype(F32)
        tile = tile + pltpu.roll(tile, width - 1, 1) + pltpu.roll(tile, width - 2, 1)
        for b in range(2):
            tops[b].append(jnp.broadcast_to(tile[:, 6 * b : 6 * b + 1], (GROUP, width)))
            dens[b].append(jnp.broadcast_to(tile[:, 6 * b + 3 : 6 * b + 4], (GROUP, width)))
    for net in range(2):
        for e in range(2):
            srcs = [net * side + e + 2 * k for k in range(side // 2)]
            for b in range(2):
                top = functools.reduce(jnp.maximum, [tops[b][s] for s in srcs])
                ws = [jnp.exp2((tops[b][s] - top) * exponent) for s in srcs]
                den = sum(w * dens[b][s] for w, s in zip(ws, srcs))
                num = sum(w * o2[s, b].astype(F32) for w, s in zip(ws, srcs))
                head = CLASSES * net + e + 2 * b
                out_ref[head * GROUP : (head + 1) * GROUP, :] = num / den


def solution(mesh):
    seq = mesh.shape["seq"]
    side = math.isqrt(seq // 2)

    def body(
        queries, span_keys, span_values, cache_keys, cache_values, page_table, page_counts, span_start
    ):
        width = queries.shape[1] // H
        rows = cache_keys.shape[0]
        half = rows // 2
        toks = 2 * side
        piece = toks * GROUP
        table = jnp.asarray(rope_table(width, PAGE))
        units = 16
        vm = pltpu.VMEM
        dma = pltpu.SemaphoreType.DMA
        hbm = pl.BlockSpec(memory_space=pl.ANY)
        scratch = [
            pltpu.SMEM(span_start.shape, jnp.int32),
            pltpu.SMEM(page_counts.shape, jnp.int32),
            pltpu.SMEM(page_table.shape, jnp.int32),
            vm(table.shape, F32),
            vm((1, H * width), BF16),
            vm((1, KVH * width), BF16),
            vm((1, KVH * width), BF16),
            vm((rows, KVH * width), BF16),
            vm((H, width), F32),
            vm((rows, width), F32),
            vm((rows, width), F32),
            vm((KVH, 2, half + EXTRA, width), BF16),
            vm((KVH, 2, half, width), BF16),
            vm((units, half + EXTRA, width), BF16),
            vm((units, half, width), BF16),
            vm((width, units * half), BF16),
            vm((units * half, width), BF16),
            vm((3, 16, width), F32),
            vm((16, width), BF16),
            vm((width, width), BF16),
            vm((2, 2, 2, GROUP, width), BF16),
            vm((2, 2, toks, GROUP, width), BF16),
            vm((side, toks, GROUP, width), BF16),
            vm((units * half, 2 * piece), F32),
            vm((side, width + EXTRA, piece), BF16),
            vm((2, side, width + EXTRA, piece), BF16),
            vm((2, toks, 3, GROUP, width), BF16),
            vm((toks, 3, GROUP, width), BF16),
            dma((9,)),
            dma((2,)),
            dma((2,)),
            dma(()),
            dma((2,)),
            dma((2,)),
            dma((side,)),
            dma(()),
            dma((2,)),
            dma(()),
            dma(()),
            pltpu.SemaphoreType.REGULAR,
            pltpu.SemaphoreType.REGULAR,
        ]
        out = pl.pallas_call(
            functools.partial(kernel, side),
            out_shape=pltpu.VMEM((H, width), F32),
            in_specs=[hbm] * 9,
            out_specs=pl.BlockSpec(memory_space=pltpu.VMEM),
            scratch_shapes=scratch,
            compiler_params=pltpu.CompilerParams(collective_id=0, has_side_effects=True),
            name="paged_prefix",
        )(
            span_start,
            page_counts,
            page_table,
            table,
            queries,
            span_keys,
            span_values,
            cache_keys,
            cache_values,
        )
        return out.reshape(queries.shape).astype(BF16)

    in_specs = (
        P(("groups", "seq"), None),
        P(("groups", "seq"), None),
        P(("groups", "seq"), None),
        P(("groups", "seq"), None),
        P(("groups", "seq"), None),
        P(("groups", "seq")),
        P(("groups", "seq")),
        P("groups"),
    )
    out_specs = P(("groups", "seq"), None)
    return jax.shard_map(body, mesh=mesh, in_specs=in_specs, out_specs=out_specs, check_vma=False)
```

```python
import functools
import math

import jax
import jax.numpy as jnp
import numpy as np
from jax import lax
from jax.experimental import pallas as pl
from jax.experimental.pallas import tpu as pltpu
from jax.sharding import PartitionSpec as P

H = 64
KVH = 8
PAGE = 16
GROUP = H // KVH
ROPE_BASE = 1000000.0
DEAD = -1e30
FLOOR = -1e29
CLASSES = 4
MESH = pl.DeviceIdType.MESH
F32 = jnp.float32
BF16 = jnp.bfloat16
EXTRA = 16


def rope_table(width, rows):
    half = width // 2
    freq = ROPE_BASE ** (-(np.arange(half, dtype=np.float64) * 2.0 / width))
    turns = np.concatenate([freq, freq]) / (2.0 * np.pi)
    pieces, rest = [], turns
    for _ in range(2):
        scale = 2.0 ** (np.floor(np.log2(rest)) - 7.0)
        part = np.floor(rest / scale) * scale
        pieces.append(part)
        rest = rest - part
    pieces.append(rest)
    sign = np.concatenate([-np.ones(half), np.ones(half)])
    angle = np.arange(rows, dtype=np.float64)[:, None] * np.concatenate([freq, freq])[None, :]
    pad = np.zeros((8 - len(pieces) - 1, width))
    return np.concatenate(
        [np.stack(pieces), sign[None], pad, np.cos(angle), np.sin(angle) * sign[None]]
    ).astype(np.float32)


def cos_sin(position, table_ref):
    def part(k):
        turn = position * table_ref[k : k + 1, :]
        return turn - jnp.floor(turn)

    turn = part(0) + part(1) + part(2)
    turn = turn - jnp.floor(turn + 0.5)
    angle = turn * (2.0 * math.pi)
    return jnp.cos(angle), jnp.sin(angle) * table_ref[3:4, :]


def in_three(value):
    high = value.astype(BF16).astype(F32)
    middle = (value - high).astype(BF16).astype(F32)
    return [high, middle, value - high - middle]


def kernel(
    side,
    start_hbm,
    count_hbm,
    pages_hbm,
    table_hbm,
    q_hbm,
    sk_hbm,
    sv_hbm,
    k_hbm,
    v_hbm,
    out_ref,
    start_ref,
    count_ref,
    pages_ref,
    table_ref,
    q_raw,
    sk_raw,
    sv_raw,
    k_raw,
    q_rows,
    cos_ref,
    sin_ref,
    kx,
    vx,
    kall,
    vall,
    vturned,
    kbias,
    rows16,
    kspan,
    vspan,
    qsrc,
    q1,
    q2,
    scores,
    o1src,
    o1,
    o2src,
    o2,
    local_sem,
    kv_send,
    kv_recv,
    q0_sem,
    q1_send,
    q1_recv,
    q2_send,
    q2_recv,
    o1_send,
    o1_recv,
    o2_send,
    o2_recv,
    told,
    told_far,
    near_side,
    side_in,
    span_scores,
    tops,
):
    width = q_rows.shape[1]
    rows = k_hbm.shape[0]
    half_rows = rows // 2
    units = kall.shape[0]
    toks = 2 * side
    piece = toks * GROUP
    me = lax.axis_index("seq")
    core = me % 2
    x = (me // 2) % side
    y = me // (2 * side)
    u = jnp.where(core == 0, x, y)
    v = jnp.where(core == 0, y, x)
    other = 1 - core

    def chip(px, py, pc):
        return ((py % side) * side + px % side) * 2 + pc

    def dev(pu, pv, pc):
        return chip(jnp.where(core == 0, pu, pv), jnp.where(core == 0, pv, pu), pc)

    def remote(src, dst, send, recv, device):
        return pltpu.make_async_remote_copy(
            src_ref=src,
            dst_ref=dst,
            send_sem=send,
            recv_sem=recv,
            device_id={"seq": device},
            device_id_type=MESH,
        )

    def sent(ref, sem):
        remote(ref, ref, sem, sem, chip(x, y, other)).wait_send()

    def landed(ref, sem):
        remote(ref, ref, sem, sem, chip(x, y, other)).wait_recv()

    local = {
        name: pltpu.make_async_copy(src, dst, local_sem.at[k])
        for k, (name, src, dst) in enumerate(
            (
                ("start", start_hbm, start_ref),
                ("count", count_hbm, count_ref),
                ("pages", pages_hbm, pages_ref),
                ("table", table_hbm, table_ref),
                ("q", q_hbm, q_raw),
                ("sk", sk_hbm, sk_raw),
                ("sv", sv_hbm, sv_raw),
                ("k", k_hbm, k_raw),
            )
        )
    }
    for copy in local.values():
        copy.start()
    for h in range(KVH):
        for hf in range(2):
            pltpu.make_async_copy(
                v_hbm.at[pl.ds(hf * half_rows, half_rows), pl.ds(h * width, width)],
                vx.at[h, hf],
                local_sem.at[len(local)],
            ).start()

    barrier = pltpu.get_barrier_semaphore()

    def signal(sem, device):
        pl.semaphore_signal(sem, inc=1, device_id={"seq": device}, device_id_type=MESH)

    neighbours = ((1, 0), (side - 1, 0), (0, 1), (0, side - 1))

    @pl.when(core == 1)
    def _():
        signal(barrier, chip(x, y, 0))
        for dx, dy in neighbours:
            signal(barrier, chip(x + dx, y + dy, 0))
        for d in range(1, side):
            signal(barrier, chip(x + d, y, 1))
            signal(barrier, chip(x, y + d, 1))

    for name in ("start", "count", "pages", "table", "q"):
        local[name].wait()
    start = start_ref[0]
    count = count_ref[0]
    own_pos = (start + me).astype(F32)
    own_cos, own_sin = cos_sin(jnp.full((8, width), own_pos, F32), table_ref)
    q_all = q_raw[...].astype(F32)
    for r in range(H):
        q_rows[r : r + 1, :] = q_all[:, r * width : (r + 1) * width]
    for net in range(2):
        for e in range(2):
            for b in range(2):
                head = CLASSES * net + e + 2 * b
                part = q_rows[head * GROUP : (head + 1) * GROUP, :]
                turned = part * own_cos + pltpu.roll(part, width // 2, 1) * own_sin
                qsrc[net, e, b, core] = turned.astype(BF16)

    @pl.when(core == 0)
    def _():
        pl.semaphore_wait(barrier, 4 + 1)
        signal(told, chip(x, y, 1))
        for dx, dy in neighbours:
            signal(near_side, chip(x + dx, y + dy, 1))
        remote(qsrc.at[:, :, :, 0], qsrc.at[:, :, :, 0], q0_sem, q0_sem, chip(x, y, 1)).start()

    @pl.when(core == 1)
    def _():
        pl.semaphore_wait(told, 1)

    def send_cache(which, net):
        buf, landing = (kx, kall) if which == 0 else (vx, vall)

        def send(head, half, slot, device):
            src = buf.at[head] if half is None else buf.at[head, half]
            dst = landing.at[pl.ds(slot, 2)] if half is None else landing.at[slot]
            remote(src, dst, kv_send.at[which], kv_recv.at[which], device).start()

        nu, nv = (x, y) if net == 0 else (y, x)

        def at(pu, pv):
            return chip(pu, pv, 0) if net == 0 else chip(pv, pu, 1)

        base = nu + 2 * nv
        head = CLASSES * net + (base + 1) % CLASSES
        send(head, None, 4 + 2 * core, at(nu + 1, nv))
        head = CLASSES * net + (base + 3) % CLASSES
        send(head, None, 8 + 2 * core, at(nu + side - 1, nv))
        head = CLASSES * net + (base + 2) % CLASSES
        send(head, 0, 12 + core, at(nu, nv + 1))
        send(head, 1, 14 + core, at(nu, nv + side - 1))
        head = CLASSES * net + base % CLASSES

        @pl.when(core == net)
        def _():
            for hf in range(2):
                landing[2 * core + hf] = buf[head, hf]

        @pl.when(core != net)
        def _():
            send(head, None, 2 * core, at(nu, nv))

    pltpu.make_async_copy(vx, vx, local_sem.at[len(local)]).wait()
    send_cache(1, 1)

    tile_row = lax.broadcasted_iota(jnp.int32, (EXTRA, width), 0)
    lane = lax.broadcasted_iota(jnp.int32, (1, width), 1)
    half_pages = half_rows // PAGE
    biases = []
    for hf in range(2):
        page = jnp.zeros((1, width), jnp.int32)
        for j in range(half_pages):
            page = jnp.where(lane // PAGE == j, pages_ref[hf * half_pages + j], page)
        slot = hf * half_pages + lane // PAGE
        usable = (slot < count) & (page * PAGE + lane % PAGE < start)
        biases.append(jnp.where(usable, 0.0, DEAD).astype(F32))
    page_pos = jnp.zeros((16, width), jnp.int32)
    for j in range(rows // PAGE):
        page_pos = jnp.where(tile_row == j, pages_ref[j] * PAGE, page_pos)
    page_cos, page_sin = cos_sin(page_pos.astype(F32), table_ref)
    row_cos = table_ref[8 : 8 + PAGE, :]
    row_sin = table_ref[8 + PAGE : 8 + 2 * PAGE, :]
    for j in range(rows // PAGE):
        pc_, ps_ = page_cos[j : j + 1, :], page_sin[j : j + 1, :]
        cos_ref[j * PAGE : (j + 1) * PAGE, :] = pc_ * row_cos - ps_ * row_sin
        sin_ref[j * PAGE : (j + 1) * PAGE, :] = ps_ * row_cos + pc_ * row_sin
    for name in ("sk", "sv", "k"):
        local[name].wait()
    sk_all = sk_raw[...].astype(F32)
    sv_all = sv_raw[...].astype(F32)
    for h in range(KVH):
        span = jnp.broadcast_to(sk_all[:, h * width : (h + 1) * width], (8, width))
        span = span * own_cos + pltpu.roll(span, width // 2, 1) * own_sin
        span = jnp.broadcast_to(span[0:1, :], (EXTRA, width))
        value = jnp.broadcast_to(sv_all[:, h * width : (h + 1) * width], (EXTRA, width))
        for hf in range(2):
            tile = jnp.where(tile_row == 0, span, jnp.where(tile_row == 2, value, 0.0))
            tile = jnp.where(tile_row == 1, biases[hf], tile)
            kx[h, hf, half_rows : half_rows + EXTRA, :] = tile.astype(BF16)

    @pl.loop(0, KVH // 2)
    def _(step):
        for h in (2 * step, 2 * step + 1):
            cols = pl.ds(pl.multiple_of(h * width, width), width)
            for hf in range(2):
                span_rows = slice(hf * half_rows, (hf + 1) * half_rows)
                part = k_raw[span_rows, cols].astype(F32)
                turned = part * cos_ref[span_rows, :]
                turned = turned + pltpu.roll(part, width // 2, 1) * sin_ref[span_rows, :]
                kx[h, hf, 0:half_rows, :] = turned.astype(BF16)

    far_first = [side // 2]
    for step in range(side // 2 - 1, 0, -1):
        far_first += [step, side - step]

    @pl.when(core == 0)
    def _():
        send_cache(0, 1)
        pl.semaphore_wait(told, 1)
        send_cache(1, 0)
        send_cache(0, 0)
        pl.semaphore_wait(told_far, 1)
        for d in far_first:
            signal(side_in, chip(x + d, y, 1))
            signal(side_in, chip(x, y + d, 1))

    @pl.when(core == 1)
    def _():
        pl.semaphore_wait(near_side, 4)
        signal(told, chip(x, y, 0))
        send_cache(1, 0)
        pl.semaphore_wait(barrier, 2 * (side - 1))
        signal(told_far, chip(x, y, 0))
        landed(qsrc.at[:, :, :, 0], q0_sem)
        for d in far_first:
            for net in range(2):
                place = x if net == 0 else y
                along = (place + d) % side
                remote(
                    qsrc.at[net, along % 2],
                    q1.at[net, :, pl.ds(2 * place, 2)],
                    q1_send,
                    q1_recv.at[net],
                    chip(along, y, 1) if net == 0 else chip(x, along, 1),
                ).start()
        send_cache(0, 1)
        send_cache(0, 0)

    @pl.when(core == 1)
    def _():
        for net, place in ((0, x), (1, y)):
            for b in range(2):
                for pc in range(2):
                    q1[net, b, 2 * place + pc] = qsrc[net, place % 2, b, pc]
        pl.semaphore_wait(side_in, 2 * (side - 1))
        for net in range(2):
            landed(q1.at[net, :, pl.ds(0, toks - 2)], q1_recv.at[net])
            nu, nv = (x, y) if net == 0 else (y, x)

            def send_q2(pv, device, net=net, nu=nu, nv=nv):
                remote(
                    q1.at[net, (nu // 2 + pv) % 2],
                    q2.at[nv],
                    q2_send.at[net],
                    q2_recv.at[nv],
                    device,
                ).start()

            for d in far_first:
                pv = (nv + d) % side
                send_q2(pv, chip(x, pv, 0) if net == 0 else chip(pv, y, 1))
            if net == 0:
                send_q2(y, chip(x, y, 0))
            else:
                q2[x] = q1[1, (y // 2 + x) % 2]

    landed(vall.at[pl.ds(0, units - 2)], kv_recv.at[1])
    for unit in range(units):
        vturned[:, unit * half_rows : (unit + 1) * half_rows] = vall[unit].T

    landed(kall.at[pl.ds(0, units - 2)], kv_recv.at[0])
    span_units = [0, 2, 4, 6, 8, 10, 12, 13]
    span_toks = [
        dev(pu, pv, pc)
        for pu, pv in ((u, v), (u + side - 1, v), (u + 1, v), (u, v + side - 1))
        for pc in range(2)
    ]
    rows16[...] = jnp.zeros_like(rows16)
    for unit in range(units):
        tile = kall[unit, half_rows : half_rows + EXTRA, :].astype(F32)
        rows16[0, unit : unit + 1, :] = tile[1:2, :]
        if unit in span_units:
            k = span_units.index(unit)
            rows16[1, k : k + 1, :] = tile[0:1, :]
            rows16[2, k : k + 1, :] = tile[2:3, :]
    zeros = jnp.zeros((width - 16, width), F32)
    bias_cols = jnp.concatenate([rows16[0], zeros]).T
    for unit in range(units):
        turned = bias_cols if unit == 0 else pltpu.roll(bias_cols, width - unit, 1)
        kbias[unit * half_rows : (unit + 1) * half_rows, :] = turned.astype(BF16)
    kspan[...] = rows16[1].astype(BF16)
    vspan[...] = jnp.concatenate([rows16[2], zeros]).T.astype(BF16)
    span_tok = jnp.full((16, piece), 1 << 20, jnp.int32)
    for k, tok in enumerate(span_toks):
        span_tok = jnp.where(tile_row == k, tok, span_tok)

    exponent = width**-0.5 / math.log(2.0)
    contract = (((1,), (1,)), ((), ()))
    chunk = 2 * half_rows
    cols = 2 * piece

    def send_o1(pv):
        remote(
            o1src.at[pv], o1.at[core, v], o1_send, o1_recv.at[core], dev(u, pv, 1)
        ).start()

    col_slot = lax.broadcasted_iota(jnp.int32, (1, piece), 1) // GROUP
    tok_along = jnp.where(core == 0, 2, 2 * side)
    tok_across = jnp.where(core == 0, 2 * side, 2)
    col_tok = (col_slot // 2) * tok_along + col_slot % 2
    one_hot = jnp.where(lax.broadcasted_iota(jnp.int32, (cols, width), 1) == 0, 1.0, 0.0).astype(BF16)

    half_units = units // 2
    half_cache = half_units * half_rows
    always = me < 4 * side * side

    def attend(pvs):
        query = jnp.concatenate(
            [q2[pv].astype(F32).reshape(piece, width).astype(BF16) for pv in pvs]
        )
        query = jnp.concatenate([query, one_hot], axis=1)
        s = lax.dot_general(kspan[...], query[:, :width], contract, preferred_element_type=F32)
        live = jnp.concatenate([span_tok <= col_tok + pv * tok_across for pv in pvs], axis=1)
        s_span = jnp.where(live, s, DEAD)
        span_scores[...] = s_span
        best = jnp.maximum(s_span[0:8], s_span[8:16])
        for p in range(2):
            span = slice(p * half_cache, (p + 1) * half_cache)
            keys = kall[p * half_units : (p + 1) * half_units, 0:half_rows, :]
            keys = jnp.concatenate([keys.reshape(half_cache, width), kbias[span, :]], axis=1)
            s = lax.dot_general(keys, query, contract, preferred_element_type=F32)
            scores[span, :] = s
            best = jnp.maximum(best, jnp.max(s.reshape(-1, 8, cols), axis=0))
        tops[...] = jnp.maximum(jnp.max(best, axis=0, keepdims=True), FLOOR)

        @pl.when(always)
        def _():
            top = tops[...]
            w = jnp.exp2((span_scores[...] - top) * exponent)
            total = w[0:8] + w[8:16]
            w = jnp.concatenate([w, jnp.zeros((width - 16, cols), F32)])
            nums = [jnp.dot(vspan[...], w.astype(BF16), preferred_element_type=F32), None]
            for k in range(units // 2):
                w = jnp.exp2((scores[k * chunk : (k + 1) * chunk, :] - top) * exponent)
                total = total + jnp.sum(w.reshape(chunk // 8, 8, cols), axis=0)
                part = jnp.dot(
                    vturned[:, k * chunk : (k + 1) * chunk],
                    w.astype(BF16),
                    preferred_element_type=F32,
                )
                nums[k % 2] = part if nums[k % 2] is None else nums[k % 2] + part
            num = nums[0] + nums[1]
            den = jnp.sum(total, axis=0, keepdims=True)
            stat = jnp.concatenate(
                in_three(top) + in_three(den) + [jnp.zeros((EXTRA - 6, cols), F32)]
            )
            for k, pv in enumerate(pvs):
                lanes = slice(k * piece, (k + 1) * piece)
                o1src[pv, 0:width, :] = num[:, lanes].astype(BF16)
                o1src[pv, width : width + EXTRA, :] = stat[:, lanes].astype(BF16)

        for pv in pvs:

            @pl.when((pv != v) | (core == 0))
            def _(pv=pv):
                send_o1(pv)

            @pl.when((pv == v) & (core == 1))
            def _(pv=pv):
                o1[1, pv] = o1src[pv]

    @pl.loop(0, side // 2)
    def _(k):
        pvs = [(v + jnp.where(k == 0, 0, side // 2 - k)) % side, (v + side // 2 + k) % side]
        for pv in pvs:

            @pl.when((pv != v) | (core == 0))
            def _(pv=pv):
                landed(q2.at[pv], q2_recv.at[pv])

        attend(pvs)

    sent(vall.at[pl.ds(0, units - 2)], kv_send.at[1])
    sent(kall.at[pl.ds(0, units - 2)], kv_send.at[0])

    @pl.when(core == 0)
    def _():
        sent(qsrc.at[:, :, :, 0], q0_sem)
        sent(o1.at[0], o1_send)

    @pl.when(core == 1)
    def _():
        sent(q1.at[:, :, pl.ds(0, toks - 2)], q1_send)
        sent(q2, q2_send.at[0])
        sent(q2.at[pl.ds(0, side - 1)], q2_send.at[1])
        for net in range(2):
            landed(o1.at[net] if net == 0 else o1.at[net, pl.ds(0, side - 1)], o1_recv.at[net])
            nu = x if net == 0 else y
            stats = []
            for b in range(2):
                vs = [(nu // 2 + b) % 2 + 2 * k for k in range(side // 2)]
                tiles = [o1[net, pv, width : width + EXTRA, :].astype(F32) for pv in vs]
                tops = [t[0:1] + t[1:2] + t[2:3] for t in tiles]
                dens = [t[3:4] + t[4:5] + t[5:6] for t in tiles]
                top = functools.reduce(jnp.maximum, tops)
                ws = [jnp.exp2((t - top) * exponent) for t in tops]
                stats += in_three(top) + in_three(sum(w * d for w, d in zip(ws, dens)))
                total = None
                for w, pv in zip(ws, vs):
                    part = o1[net, pv, 0:width, :].astype(F32) * w
                    total = part if total is None else total + part
                o2src[net, :, b] = total.T.reshape(toks, GROUP, width).astype(BF16)
            stat = jnp.concatenate(stats + [jnp.zeros((width - len(stats), piece), F32)]).T
            o2src[net, :, 2] = stat.reshape(toks, GROUP, width).astype(BF16)
            line = x if net == 0 else side + y

            def send_o2(slot, device, net=net, line=line):
                remote(o2src.at[net, slot], o2.at[line], o2_send, o2_recv, device).start()

            for d in far_first:
                for pc in range(2):
                    if net == 0:
                        px = (x + d) % side
                        send_o2(2 * px + pc, chip(px, y, pc))
                    else:
                        py = (y + d) % side
                        send_o2(2 * py + pc, chip(x, py, pc))
            send_o2(2 * nu, chip(x, y, 0))
            o2[line] = o2src[net, 2 * nu + 1]
        sent(o1.at[0, pl.ds(0, side - 1)], o1_send)
        landed(o2.at[pl.ds(0, toks - 2)], o2_recv)
        sent(o2src.at[:, pl.ds(0, toks - 1)], o2_send)

    @pl.when(core == 0)
    def _():
        landed(o2, o2_recv)

    tops, dens = [[], []], [[], []]
    for src in range(toks):
        tile = o2[src, 2].astype(F32)
        tile = tile + pltpu.roll(tile, width - 1, 1) + pltpu.roll(tile, width - 2, 1)
        for b in range(2):
            tops[b].append(jnp.broadcast_to(tile[:, 6 * b : 6 * b + 1], (GROUP, width)))
            dens[b].append(jnp.broadcast_to(tile[:, 6 * b + 3 : 6 * b + 4], (GROUP, width)))
    for net in range(2):
        for e in range(2):
            srcs = [net * side + e + 2 * k for k in range(side // 2)]
            for b in range(2):
                top = functools.reduce(jnp.maximum, [tops[b][s] for s in srcs])
                ws = [jnp.exp2((tops[b][s] - top) * exponent) for s in srcs]
                den = sum(w * dens[b][s] for w, s in zip(ws, srcs))
                num = sum(w * o2[s, b].astype(F32) for w, s in zip(ws, srcs))
                head = CLASSES * net + e + 2 * b
                out_ref[head * GROUP : (head + 1) * GROUP, :] = num / den


def solution(mesh):
    seq = mesh.shape["seq"]
    side = math.isqrt(seq // 2)

    def body(
        queries, span_keys, span_values, cache_keys, cache_values, page_table, page_counts, span_start
    ):
        width = queries.shape[1] // H
        rows = cache_keys.shape[0]
        half = rows // 2
        toks = 2 * side
        piece = toks * GROUP
        table = jnp.asarray(rope_table(width, PAGE))
        units = 16
        vm = pltpu.VMEM
        dma = pltpu.SemaphoreType.DMA
        hbm = pl.BlockSpec(memory_space=pl.ANY)
        scratch = [
            pltpu.SMEM(span_start.shape, jnp.int32),
            pltpu.SMEM(page_counts.shape, jnp.int32),
            pltpu.SMEM(page_table.shape, jnp.int32),
            vm(table.shape, F32),
            vm((1, H * width), BF16),
            vm((1, KVH * width), BF16),
            vm((1, KVH * width), BF16),
            vm((rows, KVH * width), BF16),
            vm((H, width), F32),
            vm((rows, width), F32),
            vm((rows, width), F32),
            vm((KVH, 2, half + EXTRA, width), BF16),
            vm((KVH, 2, half, width), BF16),
            vm((units, half + EXTRA, width), BF16),
            vm((units, half, width), BF16),
            vm((width, units * half), BF16),
            vm((units * half, width), BF16),
            vm((3, 16, width), F32),
            vm((16, width), BF16),
            vm((width, width), BF16),
            vm((2, 2, 2, 2, GROUP, width), BF16),
            vm((2, 2, toks, GROUP, width), BF16),
            vm((side, toks, GROUP, width), BF16),
            vm((units * half, 2 * piece), F32),
            vm((side, width + EXTRA, piece), BF16),
            vm((2, side, width + EXTRA, piece), BF16),
            vm((2, toks, 3, GROUP, width), BF16),
            vm((toks, 3, GROUP, width), BF16),
            dma((9,)),
            dma((2,)),
            dma((2,)),
            dma(()),
            dma(()),
            dma((2,)),
            dma((2,)),
            dma((side,)),
            dma(()),
            dma((2,)),
            dma(()),
            dma(()),
            pltpu.SemaphoreType.REGULAR,
            pltpu.SemaphoreType.REGULAR,
            pltpu.SemaphoreType.REGULAR,
            pltpu.SemaphoreType.REGULAR,
            vm((16, 2 * piece), F32),
            vm((1, 2 * piece), F32),
        ]
        out = pl.pallas_call(
            functools.partial(kernel, side),
            out_shape=pltpu.VMEM((H, width), F32),
            in_specs=[hbm] * 9,
            out_specs=pl.BlockSpec(memory_space=pltpu.VMEM),
            scratch_shapes=scratch,
            compiler_params=pltpu.CompilerParams(collective_id=0, has_side_effects=True),
            name="paged_prefix",
        )(
            span_start,
            page_counts,
            page_table,
            table,
            queries,
            span_keys,
            span_values,
            cache_keys,
            cache_values,
        )
        return out.reshape(queries.shape).astype(BF16)

    in_specs = (
        P(("groups", "seq"), None),
        P(("groups", "seq"), None),
        P(("groups", "seq"), None),
        P(("groups", "seq"), None),
        P(("groups", "seq"), None),
        P(("groups", "seq")),
        P(("groups", "seq")),
        P("groups"),
    )
    out_specs = P(("groups", "seq"), None)
    return jax.shard_map(body, mesh=mesh, in_specs=in_specs, out_specs=out_specs, check_vma=False)
```

```python
import functools
import math

import jax
import jax.numpy as jnp
import numpy as np
from jax import lax
from jax.experimental import pallas as pl
from jax.experimental.pallas import tpu as pltpu
from jax.sharding import PartitionSpec as P

H = 64
KVH = 8
PAGE = 16
GROUP = H // KVH
ROPE_BASE = 1000000.0
DEAD = -1e30
FLOOR = -1e29
CLASSES = 4
MESH = pl.DeviceIdType.MESH
F32 = jnp.float32
BF16 = jnp.bfloat16
EXTRA = 16


def rope_table(width, rows):
    half = width // 2
    freq = ROPE_BASE ** (-(np.arange(half, dtype=np.float64) * 2.0 / width))
    turns = np.concatenate([freq, freq]) / (2.0 * np.pi)
    pieces, rest = [], turns
    for _ in range(2):
        scale = 2.0 ** (np.floor(np.log2(rest)) - 7.0)
        part = np.floor(rest / scale) * scale
        pieces.append(part)
        rest = rest - part
    pieces.append(rest)
    sign = np.concatenate([-np.ones(half), np.ones(half)])
    angle = np.arange(rows, dtype=np.float64)[:, None] * np.concatenate([freq, freq])[None, :]
    pad = np.zeros((8 - len(pieces) - 1, width))
    return np.concatenate(
        [np.stack(pieces), sign[None], pad, np.cos(angle), np.sin(angle) * sign[None]]
    ).astype(np.float32)


def cos_sin(position, table_ref):
    def part(k):
        turn = position * table_ref[k : k + 1, :]
        return turn - jnp.floor(turn)

    turn = part(0) + part(1) + part(2)
    turn = turn - jnp.floor(turn + 0.5)
    angle = turn * (2.0 * math.pi)
    return jnp.cos(angle), jnp.sin(angle) * table_ref[3:4, :]


def in_three(value):
    high = value.astype(BF16).astype(F32)
    middle = (value - high).astype(BF16).astype(F32)
    return [high, middle, value - high - middle]


def kernel(
    side,
    start_hbm,
    count_hbm,
    pages_hbm,
    table_hbm,
    q_hbm,
    sk_hbm,
    sv_hbm,
    k_hbm,
    v_hbm,
    out_ref,
    start_ref,
    count_ref,
    pages_ref,
    table_ref,
    q_raw,
    sk_raw,
    sv_raw,
    k_raw,
    q_rows,
    cos_ref,
    sin_ref,
    kx,
    vx,
    kall,
    vall,
    kall0,
    vall0,
    vturned,
    kbias,
    rows16,
    kspan,
    vspan,
    qsrc,
    q1,
    q2,
    scores_a,
    scores_b,
    o1src,
    o1,
    o2src,
    o2,
    local_sem,
    kv_send,
    kv_recv,
    on_send,
    q0_sem,
    q1_send,
    q1_recv,
    q2_send,
    q2_recv,
    o1_send,
    o1_recv,
    o2_send,
    o2_recv,
    told,
    told_far,
    side_row,
    side_col,
    side_col0,
    span_a,
    span_b,
    top_a,
    top_b,
):
    width = q_rows.shape[1]
    rows = k_hbm.shape[0]
    half_rows = rows // 2
    units = kall.shape[0]
    toks = 2 * side
    piece = toks * GROUP
    me = lax.axis_index("seq")
    core = me % 2
    x = (me // 2) % side
    y = me // (2 * side)
    u = jnp.where(core == 0, x, y)
    v = jnp.where(core == 0, y, x)
    other = 1 - core

    def chip(px, py, pc):
        return ((py % side) * side + px % side) * 2 + pc

    def dev(pu, pv, pc):
        return chip(jnp.where(core == 0, pu, pv), jnp.where(core == 0, pv, pu), pc)

    def remote(src, dst, send, recv, device):
        return pltpu.make_async_remote_copy(
            src_ref=src,
            dst_ref=dst,
            send_sem=send,
            recv_sem=recv,
            device_id={"seq": device},
            device_id_type=MESH,
        )

    def sent(ref, sem):
        remote(ref, ref, sem, sem, chip(x, y, other)).wait_send()

    def landed(ref, sem):
        remote(ref, ref, sem, sem, chip(x, y, other)).wait_recv()

    local = {
        name: pltpu.make_async_copy(src, dst, local_sem.at[k])
        for k, (name, src, dst) in enumerate(
            (
                ("start", start_hbm, start_ref),
                ("count", count_hbm, count_ref),
                ("pages", pages_hbm, pages_ref),
                ("table", table_hbm, table_ref),
                ("q", q_hbm, q_raw),
                ("sk", sk_hbm, sk_raw),
                ("sv", sv_hbm, sv_raw),
                ("k", k_hbm, k_raw),
            )
        )
    }
    for copy in local.values():
        copy.start()
    for h in range(KVH):
        for hf in range(2):
            pltpu.make_async_copy(
                v_hbm.at[pl.ds(hf * half_rows, half_rows), pl.ds(h * width, width)],
                vx.at[h, hf],
                local_sem.at[len(local)],
            ).start()

    barrier = pltpu.get_barrier_semaphore()

    def signal(sem, device):
        pl.semaphore_signal(sem, inc=1, device_id={"seq": device}, device_id_type=MESH)

    neighbours = ((1, 0), (side - 1, 0), (0, 1), (0, side - 1))

    @pl.when(core == 1)
    def _():
        signal(barrier, chip(x, y, 0))
        for dx, dy in neighbours:
            signal(barrier, chip(x + dx, y + dy, 0))
        for d in range(1, side):
            signal(barrier, chip(x + d, y, 1))
            signal(barrier, chip(x, y + d, 1))

    for name in ("start", "count", "pages", "table", "q"):
        local[name].wait()
    start = start_ref[0]
    count = count_ref[0]
    own_pos = (start + me).astype(F32)
    own_cos, own_sin = cos_sin(jnp.full((8, width), own_pos, F32), table_ref)
    q_all = q_raw[...].astype(F32)
    for r in range(H):
        q_rows[r : r + 1, :] = q_all[:, r * width : (r + 1) * width]
    for net in range(2):
        for e in range(2):
            for b in range(2):
                head = CLASSES * net + e + 2 * b
                part = q_rows[head * GROUP : (head + 1) * GROUP, :]
                turned = part * own_cos + pltpu.roll(part, width // 2, 1) * own_sin
                qsrc[net, e, b, core] = turned.astype(BF16)

    far_first = [side // 2]
    for step in range(side // 2 - 1, 0, -1):
        far_first += [step, side - step]

    def send_q1(toks_sent, slot, sem):
        for d in far_first:
            for net in range(2):
                place = x if net == 0 else y
                along = (place + d) % side
                remote(
                    qsrc.at[net, along % 2, :, toks_sent],
                    q1.at[net, :, slot(place)],
                    sem,
                    q1_recv.at[net],
                    chip(along, y, 1) if net == 0 else chip(x, along, 1),
                ).start()

    @pl.when(core == 0)
    def _():
        pl.semaphore_wait(barrier, 4 + 1)
        signal(told, chip(x, y, 1))
        remote(qsrc.at[:, :, :, 0], qsrc.at[:, :, :, 0], q0_sem, q0_sem, chip(x, y, 1)).start()

        @pl.when(me == 0)
        def _():
            pl.semaphore_wait(told_far, 1)
            send_q1(0, lambda place: 2 * place, q1_send)

    def send_cache(which):
        buf = (kx, vx)[which]
        for net in range(2):
            landing = ((kall0, vall0), (kall, vall))[net][which]

            def send(head, half, slot, device, net=net, landing=landing):
                src = buf.at[head] if half is None else buf.at[head, half]
                dst = landing.at[pl.ds(slot, 2)] if half is None else landing.at[slot]
                remote(src, dst, kv_send.at[which, net], kv_recv.at[which, net], device).start()

            nu, nv = (x, y) if net == 0 else (y, x)

            def at(pu, pv, net=net):
                return chip(pu, pv, 1) if net == 0 else chip(pv, pu, 1)

            base = nu + 2 * nv
            head = CLASSES * net + (base + 1) % CLASSES
            send(head, None, 4 + 2 * core, at(nu + 1, nv))
            head = CLASSES * net + (base + 3) % CLASSES
            send(head, None, 8 + 2 * core, at(nu + side - 1, nv))
            head = CLASSES * net + (base + 2) % CLASSES
            send(head, 0, 12 + core, at(nu, nv + 1))
            send(head, 1, 14 + core, at(nu, nv + side - 1))
        own = ((kall, vall)[which], (kall0, vall0)[which])
        head0 = (x + 2 * y) % CLASSES
        head1 = CLASSES + (y + 2 * x) % CLASSES

        @pl.when(core == 0)
        def _():
            own[0][0:2] = buf[head0]
            remote(
                buf.at[head1],
                own[0].at[pl.ds(0, 2)],
                kv_send.at[which, 1],
                kv_recv.at[which, 1],
                chip(x, y, 1),
            ).start()

        @pl.when(core == 1)
        def _():
            own[0][2:4] = buf[head1]
            own[1][2:4] = buf[head0]

    pltpu.make_async_copy(vx, vx, local_sem.at[len(local)]).wait()

    @pl.when(core == 0)
    def _():
        send_cache(1)

    tile_row = lax.broadcasted_iota(jnp.int32, (EXTRA, width), 0)
    lane = lax.broadcasted_iota(jnp.int32, (1, width), 1)
    half_pages = half_rows // PAGE
    biases = []
    for hf in range(2):
        page = jnp.zeros((1, width), jnp.int32)
        for j in range(half_pages):
            page = jnp.where(lane // PAGE == j, pages_ref[hf * half_pages + j], page)
        slot = hf * half_pages + lane // PAGE
        usable = (slot < count) & (page * PAGE + lane % PAGE < start)
        biases.append(jnp.where(usable, 0.0, DEAD).astype(F32))
    page_pos = jnp.zeros((16, width), jnp.int32)
    for j in range(rows // PAGE):
        page_pos = jnp.where(tile_row == j, pages_ref[j] * PAGE, page_pos)
    page_cos, page_sin = cos_sin(page_pos.astype(F32), table_ref)
    row_cos = table_ref[8 : 8 + PAGE, :]
    row_sin = table_ref[8 + PAGE : 8 + 2 * PAGE, :]
    for j in range(rows // PAGE):
        pc_, ps_ = page_cos[j : j + 1, :], page_sin[j : j + 1, :]
        cos_ref[j * PAGE : (j + 1) * PAGE, :] = pc_ * row_cos - ps_ * row_sin
        sin_ref[j * PAGE : (j + 1) * PAGE, :] = ps_ * row_cos + pc_ * row_sin
    for name in ("sk", "sv", "k"):
        local[name].wait()
    sk_all = sk_raw[...].astype(F32)
    sv_all = sv_raw[...].astype(F32)
    for h in range(KVH):
        span = jnp.broadcast_to(sk_all[:, h * width : (h + 1) * width], (8, width))
        span = span * own_cos + pltpu.roll(span, width // 2, 1) * own_sin
        span = jnp.broadcast_to(span[0:1, :], (EXTRA, width))
        value = jnp.broadcast_to(sv_all[:, h * width : (h + 1) * width], (EXTRA, width))
        for hf in range(2):
            tile = jnp.where(tile_row == 0, span, jnp.where(tile_row == 2, value, 0.0))
            tile = jnp.where(tile_row == 1, biases[hf], tile)
            kx[h, hf, half_rows : half_rows + EXTRA, :] = tile.astype(BF16)

    @pl.loop(0, KVH // 2)
    def _(step):
        for h in (2 * step, 2 * step + 1):
            cols = pl.ds(pl.multiple_of(h * width, width), width)
            for hf in range(2):
                span_rows = slice(hf * half_rows, (hf + 1) * half_rows)
                part = k_raw[span_rows, cols].astype(F32)
                turned = part * cos_ref[span_rows, :]
                turned = turned + pltpu.roll(part, width // 2, 1) * sin_ref[span_rows, :]
                kx[h, hf, 0:half_rows, :] = turned.astype(BF16)

    @pl.when(core == 0)
    def _():
        send_cache(0)
        @pl.when(me > 1)
        def _():
            pl.semaphore_wait(told_far, 1)

        for d in far_first:
            signal(side_row, chip(x + d, y, 1))

        @pl.when(y == 0)
        def _():
            for d in far_first:
                signal(side_col0, chip(x, y + d, 1))

        @pl.when(y != 0)
        def _():
            for d in far_first:
                signal(side_col, chip(x, y + d, 1))

    @pl.when(core == 1)
    def _():
        @pl.when(me <= 1)
        def _():
            pl.semaphore_wait(barrier, 2 * (side - 1))
            send_q1(1, lambda place: 2 * place + 1, q1_send)
            send_cache(1)
            send_cache(0)
            pl.semaphore_wait(told, 1)

        @pl.when(me > 1)
        def _():
            pl.semaphore_wait(told, 1)
            send_cache(1)
            pl.semaphore_wait(barrier, 2 * (side - 1))

        signal(told_far, chip(x, y, 0))

        @pl.when(me > 1)
        def _():
            landed(qsrc.at[:, :, :, 0], q0_sem)
            send_q1(pl.ds(0, 2), lambda place: pl.ds(2 * place, 2), q1_send)

        @pl.when(me > 1)
        def _():
            send_cache(0)

    remote_units = units - 2
    near_units = units - 4

    @pl.when(core == 1)
    def _():
        @pl.when(me <= 1)
        def _():
            landed(qsrc.at[:, :, :, 0], q0_sem)

        for net, place in ((0, x), (1, y)):
            for b in range(2):
                for pc in range(2):
                    q1[net, b, 2 * place + pc] = qsrc[net, place % 2, b, pc]
        pl.semaphore_wait(side_col, jnp.where(y == 0, side - 1, side - 2))

        def send_q2(net, pv):
            nu, nv = (x, y) if net == 0 else (y, x)
            remote(
                q1.at[net, (nu // 2 + pv) % 2],
                q2.at[nv],
                q2_send.at[net],
                q2_recv.at[nv],
                chip(x, pv, 0) if net == 0 else chip(pv, y, 1),
            ).start()

        def relay0():
            landed(q1.at[0, :, pl.ds(0, toks - 2)], q1_recv.at[0])
            for d in far_first:
                pv = (y + d) % side

                @pl.when(pv != 0)
                def _(pv=pv):
                    send_q2(0, pv)

            send_q2(0, y)

        def relay1():
            landed(q1.at[1, :, pl.ds(0, toks - 2)], q1_recv.at[1])
            for d in far_first:
                send_q2(1, (x + d) % side)
            q2[x] = q1[1, (y // 2 + x) % 2]

        def hand_on():
            for which, (src, dst) in ((1, (vall0, vall)), (0, (kall0, kall))):
                landed(src.at[pl.ds(0, near_units)], kv_recv.at[which, 0])
                span = pl.ds(2, remote_units)
                remote(
                    src.at[span],
                    dst.at[span],
                    on_send.at[which],
                    kv_recv.at[which, 0],
                    chip(x, y, 0),
                ).start()

        @pl.when(y != 0)
        def _():
            relay0()

        @pl.when((y == 0) & (x != 0))
        def _():
            relay1()

        line0 = jnp.where(y == 0, x, jnp.where(x == 0, y, 0))
        far_line0 = (line0 > 1) & (line0 < side - 1)

        @pl.when(far_line0)
        def _():
            hand_on()

        def relay_top():
            pl.semaphore_wait(side_col0, 1)
            send_q2(0, 0)

        @pl.when((x == 0) & (y != 0))
        def _():
            relay_top()

        @pl.when((y != 0) | (x == 0))
        def _():
            relay1()

        @pl.when(y == 0)
        def _():
            relay0()

        @pl.when((x != 0) & (y != 0))
        def _():
            relay_top()

        @pl.when(jnp.logical_not(far_line0))
        def _():
            hand_on()

        landed(vall.at[pl.ds(0, remote_units)], kv_recv.at[1, 1])

    @pl.when(core == 0)
    def _():
        landed(vall.at[pl.ds(0, remote_units)], kv_recv.at[1, 0])

    for unit in range(units):
        vturned[:, unit * half_rows : (unit + 1) * half_rows] = vall[unit].T

    @pl.when(core == 1)
    def _():
        landed(kall.at[pl.ds(0, remote_units)], kv_recv.at[0, 1])

    @pl.when(core == 0)
    def _():
        landed(kall.at[pl.ds(0, remote_units)], kv_recv.at[0, 0])

    span_units = [0, 2, 4, 6, 8, 10, 12, 13]
    span_toks = [
        dev(pu, pv, pc)
        for pu, pv in ((u, v), (u + side - 1, v), (u + 1, v), (u, v + side - 1))
        for pc in range(2)
    ]
    rows16[...] = jnp.zeros_like(rows16)
    for unit in range(units):
        tile = kall[unit, half_rows : half_rows + EXTRA, :].astype(F32)
        rows16[0, unit : unit + 1, :] = tile[1:2, :]
        if unit in span_units:
            k = span_units.index(unit)
            rows16[1, k : k + 1, :] = tile[0:1, :]
            rows16[2, k : k + 1, :] = tile[2:3, :]
    zeros = jnp.zeros((width - 16, width), F32)
    bias_cols = jnp.concatenate([rows16[0], zeros]).T
    for unit in range(units):
        turned = bias_cols if unit == 0 else pltpu.roll(bias_cols, width - unit, 1)
        kbias[unit * half_rows : (unit + 1) * half_rows, :] = turned.astype(BF16)
    kspan[...] = rows16[1].astype(BF16)
    vspan[...] = jnp.concatenate([rows16[2], zeros]).T.astype(BF16)
    span_tok = jnp.full((16, piece), 1 << 20, jnp.int32)
    for k, tok in enumerate(span_toks):
        span_tok = jnp.where(tile_row == k, tok, span_tok)

    exponent = width**-0.5 / math.log(2.0)
    contract = (((1,), (1,)), ((), ()))
    chunk = 2 * half_rows
    cols = 2 * piece

    def send_o1(pv):
        remote(
            o1src.at[pv], o1.at[core, v], o1_send, o1_recv.at[core], dev(u, pv, 1)
        ).start()

    col_slot = lax.broadcasted_iota(jnp.int32, (1, piece), 1) // GROUP
    tok_along = jnp.where(core == 0, 2, 2 * side)
    tok_across = jnp.where(core == 0, 2 * side, 2)
    col_tok = (col_slot // 2) * tok_along + col_slot % 2
    one_hot = jnp.where(lax.broadcasted_iota(jnp.int32, (cols, width), 1) == 0, 1.0, 0.0).astype(BF16)

    scores, span_scores, tops = (scores_a, scores_b), (span_a, span_b), (top_a, top_b)
    half_units = units // 2
    half_cache = half_units * half_rows
    always = me < 4 * side * side

    def score(pvs, buf):
        query = jnp.concatenate(
            [q2[pv].astype(F32).reshape(piece, width).astype(BF16) for pv in pvs]
        )
        query = jnp.concatenate([query, one_hot], axis=1)
        s = lax.dot_general(kspan[...], query[:, :width], contract, preferred_element_type=F32)
        live = jnp.concatenate([span_tok <= col_tok + pv * tok_across for pv in pvs], axis=1)
        s_span = jnp.where(live, s, DEAD)
        span_scores[buf][...] = s_span
        best = jnp.maximum(s_span[0:8], s_span[8:16])
        for p in range(2):
            span = slice(p * half_cache, (p + 1) * half_cache)
            keys = kall[p * half_units : (p + 1) * half_units, 0:half_rows, :]
            keys = jnp.concatenate([keys.reshape(half_cache, width), kbias[span, :]], axis=1)
            s = lax.dot_general(keys, query, contract, preferred_element_type=F32)
            scores[buf][span, :] = s
            best = jnp.maximum(best, jnp.max(s.reshape(-1, 8, cols), axis=0))
        tops[buf][...] = jnp.maximum(jnp.max(best, axis=0, keepdims=True), FLOOR)

    def weigh(pvs, buf):
        top = tops[buf][...]
        w = jnp.exp2((span_scores[buf][...] - top) * exponent)
        total = w[0:8] + w[8:16]
        w = jnp.concatenate([w, jnp.zeros((width - 16, cols), F32)])
        nums = [jnp.dot(vspan[...], w.astype(BF16), preferred_element_type=F32), None]
        for k in range(units // 2):
            w = jnp.exp2((scores[buf][k * chunk : (k + 1) * chunk, :] - top) * exponent)
            total = total + jnp.sum(w.reshape(chunk // 8, 8, cols), axis=0)
            part = jnp.dot(
                vturned[:, k * chunk : (k + 1) * chunk],
                w.astype(BF16),
                preferred_element_type=F32,
            )
            nums[k % 2] = part if nums[k % 2] is None else nums[k % 2] + part
        num = nums[0] + nums[1]
        den = jnp.sum(total, axis=0, keepdims=True)
        stat = jnp.concatenate(in_three(top) + in_three(den) + [jnp.zeros((EXTRA - 6, cols), F32)])
        for k, pv in enumerate(pvs):
            lanes = slice(k * piece, (k + 1) * piece)
            o1src[pv, 0:width, :] = num[:, lanes].astype(BF16)
            o1src[pv, width : width + EXTRA, :] = stat[:, lanes].astype(BF16)

    def pair(k):
        last = (v + side - 1) % side
        near = (v + jnp.where(k == 0, 0, side // 2 - k)) % side
        far = (v + side // 2 + k) % side
        near, far = [jnp.where(p == 0, last, p) for p in (near, far)]
        return [near, jnp.where(k == side // 2 - 1, 0, far)]

    def queries_in(pvs):
        for pv in pvs:

            @pl.when((pv != v) | (core == 0))
            def _(pv=pv):
                landed(q2.at[pv], q2_recv.at[pv])

    def results_out(pvs):
        for pv in pvs:

            @pl.when((pv != v) | (core == 0))
            def _(pv=pv):
                send_o1(pv)

            @pl.when((pv == v) & (core == 1))
            def _(pv=pv):
                o1[1, pv] = o1src[pv]

    pairs = side // 2
    queries_in(pair(0))
    score(pair(0), 0)

    for k in range(pairs - 2):
        queries_in(pair(k + 1))

        @pl.when(always)
        def _(k=k):
            score(pair(k + 1), (k + 1) % 2)
            weigh(pair(k), k % 2)

        results_out(pair(k))

    @pl.when(always)
    def _():
        weigh(pair(pairs - 2), pairs % 2)

    results_out(pair(pairs - 2))
    queries_in(pair(pairs - 1))

    @pl.when(always)
    def _():
        score(pair(pairs - 1), (pairs - 1) % 2)

    @pl.when(always)
    def _():
        weigh(pair(pairs - 1), (pairs - 1) % 2)

    results_out(pair(pairs - 1))

    for which, buf in enumerate((kall, vall)):
        sent(buf.at[pl.ds(0, near_units // 2)], kv_send.at[which, 0])

        @pl.when(core == 0)
        def _(which=which, buf=buf):
            sent(buf.at[pl.ds(0, near_units // 2 + 2)], kv_send.at[which, 1])

        @pl.when(core == 1)
        def _(which=which, buf=buf):
            sent(buf.at[pl.ds(0, near_units // 2)], kv_send.at[which, 1])
            sent(buf.at[pl.ds(0, remote_units)], on_send.at[which])

    @pl.when(core == 0)
    def _():
        sent(qsrc.at[:, :, :, 0], q0_sem)

        @pl.when(me == 0)
        def _():
            sent(q1.at[:, :, pl.ds(0, side - 1)], q1_send)

        sent(o1.at[0], o1_send)

    @pl.when(core == 1)
    def _():
        @pl.when(me <= 1)
        def _():
            sent(q1.at[:, :, pl.ds(0, side - 1)], q1_send)

        @pl.when(me > 1)
        def _():
            sent(q1.at[:, :, pl.ds(0, toks - 2)], q1_send)

        sent(q2, q2_send.at[0])
        sent(q2.at[pl.ds(0, side - 1)], q2_send.at[1])
        pl.semaphore_wait(side_row, side - 1)
        for net in range(2):
            landed(o1.at[net] if net == 0 else o1.at[net, pl.ds(0, side - 1)], o1_recv.at[net])
            nu = x if net == 0 else y
            stats = []
            for b in range(2):
                vs = [(nu // 2 + b) % 2 + 2 * k for k in range(side // 2)]
                tiles = [o1[net, pv, width : width + EXTRA, :].astype(F32) for pv in vs]
                tops = [t[0:1] + t[1:2] + t[2:3] for t in tiles]
                dens = [t[3:4] + t[4:5] + t[5:6] for t in tiles]
                top = functools.reduce(jnp.maximum, tops)
                ws = [jnp.exp2((t - top) * exponent) for t in tops]
                stats += in_three(top) + in_three(sum(w * d for w, d in zip(ws, dens)))
                total = None
                for w, pv in zip(ws, vs):
                    part = o1[net, pv, 0:width, :].astype(F32) * w
                    total = part if total is None else total + part
                o2src[net, :, b] = total.T.reshape(toks, GROUP, width).astype(BF16)
            stat = jnp.concatenate(stats + [jnp.zeros((width - len(stats), piece), F32)]).T
            o2src[net, :, 2] = stat.reshape(toks, GROUP, width).astype(BF16)
            line = x if net == 0 else side + y

            def send_o2(slot, device, net=net, line=line):
                remote(o2src.at[net, slot], o2.at[line], o2_send, o2_recv, device).start()

            for d in far_first:
                for pc in range(2):
                    if net == 0:
                        px = (x + d) % side
                        send_o2(2 * px + pc, chip(px, y, pc))
                    else:
                        py = (y + d) % side
                        send_o2(2 * py + pc, chip(x, py, pc))
            send_o2(2 * nu, chip(x, y, 0))
            o2[line] = o2src[net, 2 * nu + 1]
        sent(o1.at[0, pl.ds(0, side - 1)], o1_send)
        landed(o2.at[pl.ds(0, toks - 2)], o2_recv)
        sent(o2src.at[:, pl.ds(0, toks - 1)], o2_send)

    @pl.when(core == 0)
    def _():
        landed(o2, o2_recv)

    tops, dens = [[], []], [[], []]
    for src in range(toks):
        tile = o2[src, 2].astype(F32)
        tile = tile + pltpu.roll(tile, width - 1, 1) + pltpu.roll(tile, width - 2, 1)
        for b in range(2):
            tops[b].append(jnp.broadcast_to(tile[:, 6 * b : 6 * b + 1], (GROUP, width)))
            dens[b].append(jnp.broadcast_to(tile[:, 6 * b + 3 : 6 * b + 4], (GROUP, width)))
    for net in range(2):
        for e in range(2):
            srcs = [net * side + e + 2 * k for k in range(side // 2)]
            for b in range(2):
                top = functools.reduce(jnp.maximum, [tops[b][s] for s in srcs])
                ws = [jnp.exp2((tops[b][s] - top) * exponent) for s in srcs]
                den = sum(w * dens[b][s] for w, s in zip(ws, srcs))
                num = sum(w * o2[s, b].astype(F32) for w, s in zip(ws, srcs))
                head = CLASSES * net + e + 2 * b
                out_ref[head * GROUP : (head + 1) * GROUP, :] = num / den


def solution(mesh):
    seq = mesh.shape["seq"]
    side = math.isqrt(seq // 2)

    def body(
        queries, span_keys, span_values, cache_keys, cache_values, page_table, page_counts, span_start
    ):
        width = queries.shape[1] // H
        rows = cache_keys.shape[0]
        half = rows // 2
        toks = 2 * side
        piece = toks * GROUP
        table = jnp.asarray(rope_table(width, PAGE))
        units = 16
        vm = pltpu.VMEM
        dma = pltpu.SemaphoreType.DMA
        hbm = pl.BlockSpec(memory_space=pl.ANY)
        scratch = [
            pltpu.SMEM(span_start.shape, jnp.int32),
            pltpu.SMEM(page_counts.shape, jnp.int32),
            pltpu.SMEM(page_table.shape, jnp.int32),
            vm(table.shape, F32),
            vm((1, H * width), BF16),
            vm((1, KVH * width), BF16),
            vm((1, KVH * width), BF16),
            vm((rows, KVH * width), BF16),
            vm((H, width), F32),
            vm((rows, width), F32),
            vm((rows, width), F32),
            vm((KVH, 2, half + EXTRA, width), BF16),
            vm((KVH, 2, half, width), BF16),
            vm((units, half + EXTRA, width), BF16),
            vm((units, half, width), BF16),
            vm((units, half + EXTRA, width), BF16),
            vm((units, half, width), BF16),
            vm((width, units * half), BF16),
            vm((units * half, width), BF16),
            vm((3, 16, width), F32),
            vm((16, width), BF16),
            vm((width, width), BF16),
            vm((2, 2, 2, 2, GROUP, width), BF16),
            vm((2, 2, toks, GROUP, width), BF16),
            vm((side, toks, GROUP, width), BF16),
            vm((units * half, 2 * piece), F32),
            vm((units * half, 2 * piece), F32),
            vm((side, width + EXTRA, piece), BF16),
            vm((2, side, width + EXTRA, piece), BF16),
            vm((2, toks, 3, GROUP, width), BF16),
            vm((toks, 3, GROUP, width), BF16),
            dma((9,)),
            dma((2, 2)),
            dma((2, 2)),
            dma((2,)),
            dma(()),
            dma(()),
            dma((2,)),
            dma((2,)),
            dma((side,)),
            dma(()),
            dma((2,)),
            dma(()),
            dma(()),
            pltpu.SemaphoreType.REGULAR,
            pltpu.SemaphoreType.REGULAR,
            pltpu.SemaphoreType.REGULAR,
            pltpu.SemaphoreType.REGULAR,
            pltpu.SemaphoreType.REGULAR,
            vm((16, 2 * piece), F32),
            vm((16, 2 * piece), F32),
            vm((1, 2 * piece), F32),
            vm((1, 2 * piece), F32),
        ]
        out = pl.pallas_call(
            functools.partial(kernel, side),
            out_shape=pltpu.VMEM((H, width), F32),
            in_specs=[hbm] * 9,
            out_specs=pl.BlockSpec(memory_space=pltpu.VMEM),
            scratch_shapes=scratch,
            compiler_params=pltpu.CompilerParams(collective_id=0, has_side_effects=True),
            name="paged_prefix",
        )(
            span_start,
            page_counts,
            page_table,
            table,
            queries,
            span_keys,
            span_values,
            cache_keys,
            cache_values,
        )
        return out.reshape(queries.shape).astype(BF16)

    in_specs = (
        P(("groups", "seq"), None),
        P(("groups", "seq"), None),
        P(("groups", "seq"), None),
        P(("groups", "seq"), None),
        P(("groups", "seq"), None),
        P(("groups", "seq")),
        P(("groups", "seq")),
        P("groups"),
    )
    out_specs = P(("groups", "seq"), None)
    return jax.shard_map(body, mesh=mesh, in_specs=in_specs, out_specs=out_specs, check_vma=False)
```

```python
import functools
import math

import jax
import jax.numpy as jnp
import numpy as np
from jax import lax
from jax.experimental import pallas as pl
from jax.experimental.pallas import tpu as pltpu
from jax.sharding import PartitionSpec as P

H = 64
KVH = 8
PAGE = 16
GROUP = H // KVH
ROPE_BASE = 1000000.0
DEAD = -1e30
FLOOR = -1e29
CLASSES = 4
MESH = pl.DeviceIdType.MESH
F32 = jnp.float32
BF16 = jnp.bfloat16
EXTRA = 16


def rope_table(width, rows):
    half = width // 2
    freq = ROPE_BASE ** (-(np.arange(half, dtype=np.float64) * 2.0 / width))
    turns = np.concatenate([freq, freq]) / (2.0 * np.pi)
    pieces, rest = [], turns
    for _ in range(2):
        scale = 2.0 ** (np.floor(np.log2(rest)) - 7.0)
        part = np.floor(rest / scale) * scale
        pieces.append(part)
        rest = rest - part
    pieces.append(rest)
    sign = np.concatenate([-np.ones(half), np.ones(half)])
    angle = np.arange(rows, dtype=np.float64)[:, None] * np.concatenate([freq, freq])[None, :]
    pad = np.zeros((8 - len(pieces) - 1, width))
    return np.concatenate(
        [np.stack(pieces), sign[None], pad, np.cos(angle), np.sin(angle) * sign[None]]
    ).astype(np.float32)


def cos_sin(position, table_ref):
    def part(k):
        turn = position * table_ref[k : k + 1, :]
        return turn - jnp.floor(turn)

    turn = part(0) + part(1) + part(2)
    turn = turn - jnp.floor(turn + 0.5)
    angle = turn * (2.0 * math.pi)
    return jnp.cos(angle), jnp.sin(angle) * table_ref[3:4, :]


def in_three(value):
    high = value.astype(BF16).astype(F32)
    middle = (value - high).astype(BF16).astype(F32)
    return [high, middle, value - high - middle]


def kernel(
    side,
    start_hbm,
    count_hbm,
    pages_hbm,
    table_hbm,
    q_hbm,
    sk_hbm,
    sv_hbm,
    k_hbm,
    v_hbm,
    out_ref,
    start_ref,
    count_ref,
    pages_ref,
    table_ref,
    q_raw,
    sk_raw,
    sv_raw,
    k_raw,
    q_rows,
    cos_ref,
    sin_ref,
    kx,
    vx,
    kall,
    vall,
    kall0,
    vall0,
    vturned,
    kbias,
    rows16,
    kspan,
    vspan,
    qsrc,
    q1,
    q2,
    scores_a,
    scores_b,
    o1src,
    o1,
    o2src,
    o2,
    qlate,
    q2l,
    late_src,
    o1l,
    o2l,
    local_sem,
    kv_send,
    kv_recv,
    on_send,
    q0_sem,
    q1_send,
    q1_recv,
    q2_send,
    q2_recv,
    o1_send,
    o1_recv,
    o2_send,
    o2_recv,
    ql_recv,
    q2l_send,
    q2l_recv,
    o1l_send,
    o1l_recv,
    told,
    told_far,
    side_row,
    side_col,
    side_col0,
    span_a,
    span_b,
    top_a,
    top_b,
):
    width = q_rows.shape[1]
    rows = k_hbm.shape[0]
    half_rows = rows // 2
    units = kall.shape[0]
    toks = 2 * side
    piece = toks * GROUP
    me = lax.axis_index("seq")
    core = me % 2
    x = (me // 2) % side
    y = me // (2 * side)
    u = jnp.where(core == 0, x, y)
    v = jnp.where(core == 0, y, x)
    other = 1 - core

    def chip(px, py, pc):
        return ((py % side) * side + px % side) * 2 + pc

    def dev(pu, pv, pc):
        return chip(jnp.where(core == 0, pu, pv), jnp.where(core == 0, pv, pu), pc)

    def remote(src, dst, send, recv, device):
        return pltpu.make_async_remote_copy(
            src_ref=src,
            dst_ref=dst,
            send_sem=send,
            recv_sem=recv,
            device_id={"seq": device},
            device_id_type=MESH,
        )

    def sent(ref, sem):
        remote(ref, ref, sem, sem, chip(x, y, other)).wait_send()

    def landed(ref, sem):
        remote(ref, ref, sem, sem, chip(x, y, other)).wait_recv()

    local = {
        name: pltpu.make_async_copy(src, dst, local_sem.at[k])
        for k, (name, src, dst) in enumerate(
            (
                ("start", start_hbm, start_ref),
                ("count", count_hbm, count_ref),
                ("pages", pages_hbm, pages_ref),
                ("table", table_hbm, table_ref),
                ("q", q_hbm, q_raw),
                ("sk", sk_hbm, sk_raw),
                ("sv", sv_hbm, sv_raw),
                ("k", k_hbm, k_raw),
            )
        )
    }
    for copy in local.values():
        copy.start()
    for h in range(KVH):
        for hf in range(2):
            pltpu.make_async_copy(
                v_hbm.at[pl.ds(hf * half_rows, half_rows), pl.ds(h * width, width)],
                vx.at[h, hf],
                local_sem.at[len(local)],
            ).start()

    barrier = pltpu.get_barrier_semaphore()

    def signal(sem, device):
        pl.semaphore_signal(sem, inc=1, device_id={"seq": device}, device_id_type=MESH)

    neighbours = ((1, 0), (side - 1, 0), (0, 1), (0, side - 1))

    @pl.when(core == 1)
    def _():
        signal(barrier, chip(x, y, 0))
        for dx, dy in neighbours:
            signal(barrier, chip(x + dx, y + dy, 0))
        for d in range(1, side):
            signal(barrier, chip(x + d, y, 1))
            signal(barrier, chip(x, y + d, 1))

    for name in ("start", "count", "pages", "table", "q"):
        local[name].wait()
    start = start_ref[0]
    count = count_ref[0]
    own_pos = (start + me).astype(F32)
    own_cos, own_sin = cos_sin(jnp.full((8, width), own_pos, F32), table_ref)
    q_all = q_raw[...].astype(F32)
    for r in range(H):
        q_rows[r : r + 1, :] = q_all[:, r * width : (r + 1) * width]
    for net in range(2):
        for e in range(2):
            for b in range(2):
                head = CLASSES * net + e + 2 * b
                part = q_rows[head * GROUP : (head + 1) * GROUP, :]
                turned = part * own_cos + pltpu.roll(part, width // 2, 1) * own_sin
                qsrc[net, e, b, core] = turned.astype(BF16)

    far_first = [side // 2]
    for step in range(side // 2 - 1, 0, -1):
        far_first += [step, side - step]

    def send_q1(toks_sent, landing, recv):
        for d in far_first:
            for net in range(2):
                place = x if net == 0 else y
                along = (place + d) % side
                remote(
                    qsrc.at[net, along % 2, :, toks_sent],
                    landing(net, place),
                    q1_send,
                    recv.at[net],
                    chip(along, y, 1) if net == 0 else chip(x, along, 1),
                ).start()

    @pl.when(core == 0)
    def _():
        pl.semaphore_wait(barrier, 4 + 1)
        signal(told, chip(x, y, 1))
        remote(qsrc.at[:, :, :, 0], qsrc.at[:, :, :, 0], q0_sem, q0_sem, chip(x, y, 1)).start()


    def send_cache(which):
        buf = (kx, vx)[which]
        for net in range(2):
            landing = ((kall0, vall0), (kall, vall))[net][which]

            def send(head, half, slot, device, net=net, landing=landing):
                src = buf.at[head] if half is None else buf.at[head, half]
                dst = landing.at[pl.ds(slot, 2)] if half is None else landing.at[slot]
                remote(src, dst, kv_send.at[which, net], kv_recv.at[which, net], device).start()

            nu, nv = (x, y) if net == 0 else (y, x)

            def at(pu, pv, net=net):
                return chip(pu, pv, 1) if net == 0 else chip(pv, pu, 1)

            base = nu + 2 * nv
            head = CLASSES * net + (base + 1) % CLASSES
            send(head, None, 4 + 2 * core, at(nu + 1, nv))
            head = CLASSES * net + (base + 3) % CLASSES
            send(head, None, 8 + 2 * core, at(nu + side - 1, nv))
            head = CLASSES * net + (base + 2) % CLASSES
            send(head, 0, 12 + core, at(nu, nv + 1))
            send(head, 1, 14 + core, at(nu, nv + side - 1))
        own = ((kall, vall)[which], (kall0, vall0)[which])
        head0 = (x + 2 * y) % CLASSES
        head1 = CLASSES + (y + 2 * x) % CLASSES

        @pl.when(core == 0)
        def _():
            own[0][0:2] = buf[head0]
            remote(
                buf.at[head1],
                own[0].at[pl.ds(0, 2)],
                kv_send.at[which, 1],
                kv_recv.at[which, 1],
                chip(x, y, 1),
            ).start()

        @pl.when(core == 1)
        def _():
            own[0][2:4] = buf[head1]
            own[1][2:4] = buf[head0]

    pltpu.make_async_copy(vx, vx, local_sem.at[len(local)]).wait()

    @pl.when(core == 0)
    def _():
        send_cache(1)

    tile_row = lax.broadcasted_iota(jnp.int32, (EXTRA, width), 0)
    lane = lax.broadcasted_iota(jnp.int32, (1, width), 1)
    half_pages = half_rows // PAGE
    biases = []
    for hf in range(2):
        page = jnp.zeros((1, width), jnp.int32)
        for j in range(half_pages):
            page = jnp.where(lane // PAGE == j, pages_ref[hf * half_pages + j], page)
        slot = hf * half_pages + lane // PAGE
        usable = (slot < count) & (page * PAGE + lane % PAGE < start)
        biases.append(jnp.where(usable, 0.0, DEAD).astype(F32))
    page_pos = jnp.zeros((16, width), jnp.int32)
    for j in range(rows // PAGE):
        page_pos = jnp.where(tile_row == j, pages_ref[j] * PAGE, page_pos)
    page_cos, page_sin = cos_sin(page_pos.astype(F32), table_ref)
    row_cos = table_ref[8 : 8 + PAGE, :]
    row_sin = table_ref[8 + PAGE : 8 + 2 * PAGE, :]
    for j in range(rows // PAGE):
        pc_, ps_ = page_cos[j : j + 1, :], page_sin[j : j + 1, :]
        cos_ref[j * PAGE : (j + 1) * PAGE, :] = pc_ * row_cos - ps_ * row_sin
        sin_ref[j * PAGE : (j + 1) * PAGE, :] = ps_ * row_cos + pc_ * row_sin
    for name in ("sk", "sv", "k"):
        local[name].wait()
    sk_all = sk_raw[...].astype(F32)
    sv_all = sv_raw[...].astype(F32)
    for h in range(KVH):
        span = jnp.broadcast_to(sk_all[:, h * width : (h + 1) * width], (8, width))
        span = span * own_cos + pltpu.roll(span, width // 2, 1) * own_sin
        span = jnp.broadcast_to(span[0:1, :], (EXTRA, width))
        value = jnp.broadcast_to(sv_all[:, h * width : (h + 1) * width], (EXTRA, width))
        for hf in range(2):
            tile = jnp.where(tile_row == 0, span, jnp.where(tile_row == 2, value, 0.0))
            tile = jnp.where(tile_row == 1, biases[hf], tile)
            kx[h, hf, half_rows : half_rows + EXTRA, :] = tile.astype(BF16)

    @pl.loop(0, KVH // 2)
    def _(step):
        for h in (2 * step, 2 * step + 1):
            cols = pl.ds(pl.multiple_of(h * width, width), width)
            for hf in range(2):
                span_rows = slice(hf * half_rows, (hf + 1) * half_rows)
                part = k_raw[span_rows, cols].astype(F32)
                turned = part * cos_ref[span_rows, :]
                turned = turned + pltpu.roll(part, width // 2, 1) * sin_ref[span_rows, :]
                kx[h, hf, 0:half_rows, :] = turned.astype(BF16)

    @pl.when(core == 0)
    def _():
        send_cache(0)
        pl.semaphore_wait(told_far, 1)
        for d in far_first:
            signal(side_row, chip(x + d, y, 1))

        @pl.when(y == 0)
        def _():
            for d in far_first:
                signal(side_col0, chip(x, y + d, 1))

        @pl.when(y != 0)
        def _():
            for d in far_first:
                signal(side_col, chip(x, y + d, 1))

    @pl.when(core == 1)
    def _():
        @pl.when(me == 1)
        def _():
            pl.semaphore_wait(barrier, 2 * (side - 1))
            send_q1(1, lambda net, place: q1.at[net, :, 2 * place + 1], q1_recv)
            send_cache(1)
            send_cache(0)
            pl.semaphore_wait(told, 1)
            signal(told_far, chip(x, y, 0))
            landed(qsrc.at[:, :, :, 0], q0_sem)
            send_q1(0, lambda net, place: qlate.at[net], ql_recv)
            qlate[0] = qsrc[0, 0, :, 0]
            qlate[1] = qsrc[1, 0, :, 0]

        @pl.when(me > 1)
        def _():
            pl.semaphore_wait(told, 1)
            send_cache(1)
            pl.semaphore_wait(barrier, 2 * (side - 1))
            signal(told_far, chip(x, y, 0))
            landed(qsrc.at[:, :, :, 0], q0_sem)
            send_q1(pl.ds(0, 2), lambda net, place: q1.at[net, :, pl.ds(2 * place, 2)], q1_recv)
            send_cache(0)

    remote_units = units - 2
    near_units = units - 4

    @pl.when(core == 1)
    def _():
        for net, place in ((0, x), (1, y)):
            for b in range(2):
                q1[net, b, 2 * place + 1] = qsrc[net, place % 2, b, 1]

        @pl.when(me > 1)
        def _():
            for net, place in ((0, x), (1, y)):
                for b in range(2):
                    q1[net, b, 2 * place] = qsrc[net, place % 2, b, 0]

        for net, across in ((0, y), (1, x)):

            @pl.when(across == 0)
            def _(net=net):
                for b in range(2):
                    q1[net, b, 0] = jnp.zeros((GROUP, width), BF16)

        pl.semaphore_wait(side_col, jnp.where(y == 0, side - 1, side - 2))

        def send_q2(net, pv):
            nu, nv = (x, y) if net == 0 else (y, x)
            remote(
                q1.at[net, (nu // 2 + pv) % 2],
                q2.at[nv],
                q2_send.at[net],
                q2_recv.at[nv],
                chip(x, pv, 0) if net == 0 else chip(pv, y, 1),
            ).start()

        def all_in(net, along, across):
            short = (across == 0) & (along != 0)

            @pl.when(short)
            def _():
                landed(q1.at[net, :, pl.ds(0, toks - 3)], q1_recv.at[net])

            @pl.when(jnp.logical_not(short))
            def _():
                landed(q1.at[net, :, pl.ds(0, toks - 2)], q1_recv.at[net])

        all_in(0, x, y)
        for d in far_first:
            pv = (y + d) % side

            @pl.when(pv != 0)
            def _(pv=pv):
                send_q2(0, pv)

        send_q2(0, y)
        all_in(1, y, x)
        for d in far_first:
            send_q2(1, (x + d) % side)
        q2[x] = q1[1, (y // 2 + x) % 2]

        def hand_on():
            for which, (src, dst) in ((1, (vall0, vall)), (0, (kall0, kall))):
                landed(src.at[pl.ds(0, near_units)], kv_recv.at[which, 0])
                span = pl.ds(2, remote_units)
                remote(
                    src.at[span],
                    dst.at[span],
                    on_send.at[which],
                    kv_recv.at[which, 0],
                    chip(x, y, 0),
                ).start()

        line0 = jnp.where(y == 0, x, jnp.where(x == 0, y, 0))
        by_chip0 = (line0 == 1) | (line0 == side - 1)

        @pl.when(jnp.logical_not(by_chip0))
        def _():
            hand_on()

        @pl.when(y != 0)
        def _():
            pl.semaphore_wait(side_col0, 1)
            send_q2(0, 0)

        @pl.when(y == 0)
        def _():
            @pl.when(x != 0)
            def _():
                landed(qlate.at[0], ql_recv.at[0])

            for d in far_first + [0]:
                remote(
                    qlate.at[0, (x // 2 + d) % 2], q2l, q2l_send, q2l_recv, chip(x, d, 0)
                ).start()

        @pl.when(x == 0)
        def _():
            @pl.when(y != 0)
            def _():
                landed(qlate.at[1], ql_recv.at[1])

            for d in far_first:
                remote(
                    qlate.at[1, (y // 2 + d) % 2], q2l, q2l_send, q2l_recv, chip(d, y, 1)
                ).start()
            q2l[...] = qlate[1, (y // 2) % 2]

        @pl.when(by_chip0)
        def _():
            hand_on()

        landed(vall.at[pl.ds(0, remote_units)], kv_recv.at[1, 1])

    @pl.when(core == 0)
    def _():
        landed(vall.at[pl.ds(0, remote_units)], kv_recv.at[1, 0])

    for unit in range(units):
        vturned[:, unit * half_rows : (unit + 1) * half_rows] = vall[unit].T

    @pl.when(core == 1)
    def _():
        landed(kall.at[pl.ds(0, remote_units)], kv_recv.at[0, 1])

    @pl.when(core == 0)
    def _():
        landed(kall.at[pl.ds(0, remote_units)], kv_recv.at[0, 0])

    span_units = [0, 2, 4, 6, 8, 10, 12, 13]
    span_toks = [
        dev(pu, pv, pc)
        for pu, pv in ((u, v), (u + side - 1, v), (u + 1, v), (u, v + side - 1))
        for pc in range(2)
    ]
    rows16[...] = jnp.zeros_like(rows16)
    for unit in range(units):
        tile = kall[unit, half_rows : half_rows + EXTRA, :].astype(F32)
        rows16[0, unit : unit + 1, :] = tile[1:2, :]
        if unit in span_units:
            k = span_units.index(unit)
            rows16[1, k : k + 1, :] = tile[0:1, :]
            rows16[2, k : k + 1, :] = tile[2:3, :]
    zeros = jnp.zeros((width - 16, width), F32)
    bias_cols = jnp.concatenate([rows16[0], zeros]).T
    for unit in range(units):
        turned = bias_cols if unit == 0 else pltpu.roll(bias_cols, width - unit, 1)
        kbias[unit * half_rows : (unit + 1) * half_rows, :] = turned.astype(BF16)
    kspan[...] = rows16[1].astype(BF16)
    vspan[...] = jnp.concatenate([rows16[2], zeros]).T.astype(BF16)
    span_tok = jnp.full((16, piece), 1 << 20, jnp.int32)
    for k, tok in enumerate(span_toks):
        span_tok = jnp.where(tile_row == k, tok, span_tok)

    exponent = width**-0.5 / math.log(2.0)
    contract = (((1,), (1,)), ((), ()))
    chunk = 2 * half_rows
    cols = 2 * piece

    def send_o1(pv):
        remote(
            o1src.at[pv], o1.at[core, v], o1_send, o1_recv.at[core], dev(u, pv, 1)
        ).start()

    col_slot = lax.broadcasted_iota(jnp.int32, (1, piece), 1) // GROUP
    tok_along = jnp.where(core == 0, 2, 2 * side)
    tok_across = jnp.where(core == 0, 2 * side, 2)
    col_tok = (col_slot // 2) * tok_along + col_slot % 2
    one_hot = jnp.where(lax.broadcasted_iota(jnp.int32, (cols, width), 1) == 0, 1.0, 0.0).astype(BF16)

    scores, span_scores, tops = (scores_a, scores_b), (span_a, span_b), (top_a, top_b)
    half_units = units // 2
    half_cache = half_units * half_rows
    always = me < 4 * side * side

    def score(query, live, buf):
        n = query.shape[0]
        query = jnp.concatenate([query, one_hot[:n]], axis=1)
        s = lax.dot_general(kspan[...], query[:, :width], contract, preferred_element_type=F32)
        s_span = jnp.where(live, s, DEAD)
        span_scores[buf][:, :n] = s_span
        best = jnp.maximum(s_span[0:8], s_span[8:16])
        for p in range(2):
            span = slice(p * half_cache, (p + 1) * half_cache)
            keys = kall[p * half_units : (p + 1) * half_units, 0:half_rows, :]
            keys = jnp.concatenate([keys.reshape(half_cache, width), kbias[span, :]], axis=1)
            s = lax.dot_general(keys, query, contract, preferred_element_type=F32)
            scores[buf][span, :n] = s
            best = jnp.maximum(best, jnp.max(s.reshape(-1, 8, n), axis=0))
        tops[buf][:, :n] = jnp.maximum(jnp.max(best, axis=0, keepdims=True), FLOOR)

    def weigh(buf, n):
        top = tops[buf][:, :n]
        w = jnp.exp2((span_scores[buf][:, :n] - top) * exponent)
        total = w[0:8] + w[8:16]
        w = jnp.concatenate([w, jnp.zeros((width - 16, n), F32)])
        nums = [jnp.dot(vspan[...], w.astype(BF16), preferred_element_type=F32), None]
        for k in range(units // 2):
            w = jnp.exp2((scores[buf][k * chunk : (k + 1) * chunk, :n] - top) * exponent)
            total = total + jnp.sum(w.reshape(chunk // 8, 8, n), axis=0)
            part = jnp.dot(
                vturned[:, k * chunk : (k + 1) * chunk],
                w.astype(BF16),
                preferred_element_type=F32,
            )
            nums[k % 2] = part if nums[k % 2] is None else nums[k % 2] + part
        den = jnp.sum(total, axis=0, keepdims=True)
        stat = jnp.concatenate(in_three(top) + in_three(den) + [jnp.zeros((EXTRA - 6, n), F32)])
        return nums[0] + nums[1], stat

    def score_pair(pvs, buf):
        query = jnp.concatenate(
            [q2[pv].astype(F32).reshape(piece, width).astype(BF16) for pv in pvs]
        )
        live = jnp.concatenate([span_tok <= col_tok + pv * tok_across for pv in pvs], axis=1)
        score(query, live, buf)

    def weigh_pair(pvs, buf):
        num, stat = weigh(buf, cols)
        for k, pv in enumerate(pvs):
            lanes = slice(k * piece, (k + 1) * piece)
            o1src[pv, 0:width, :] = num[:, lanes].astype(BF16)
            o1src[pv, width : width + EXTRA, :] = stat[:, lanes].astype(BF16)

    def pair(k):
        return [
            (v + jnp.where(k == 0, 0, side // 2 - k)) % side,
            (v + side // 2 + k) % side,
        ]

    def queries_in(pvs):
        for pv in pvs:

            @pl.when((pv != v) | (core == 0))
            def _(pv=pv):
                landed(q2.at[pv], q2_recv.at[pv])

    def results_out(pvs):
        for pv in pvs:

            @pl.when((pv != v) | (core == 0))
            def _(pv=pv):
                send_o1(pv)

            @pl.when((pv == v) & (core == 1))
            def _(pv=pv):
                o1[1, pv] = o1src[pv]

    pairs = side // 2
    queries_in(pair(0))
    score_pair(pair(0), 0)

    for k in range(pairs - 1):
        queries_in(pair(k + 1))

        @pl.when(always)
        def _(k=k):
            score_pair(pair(k + 1), (k + 1) % 2)
            weigh_pair(pair(k), k % 2)

        results_out(pair(k))

    @pl.when(always)
    def _():
        weigh_pair(pair(pairs - 1), (pairs - 1) % 2)

    results_out(pair(pairs - 1))

    @pl.when((core == 0) | (x != 0))
    def _():
        landed(q2l, q2l_recv)

    @pl.when(always)
    def _():
        query = jnp.concatenate([q2l[...].astype(F32), jnp.zeros((piece - GROUP, width), F32)])
        score(query.astype(BF16), span_tok <= 0, 0)

    @pl.when(always)
    def _():
        num, stat = weigh(0, piece)
        late_src[0] = num.T[0:GROUP].astype(BF16)
        wide = jnp.concatenate([stat, jnp.zeros((width - EXTRA, piece), F32)])
        late_src[1] = wide.T[0:GROUP].astype(BF16)

    @pl.when(core == 0)
    def _():
        remote(late_src, o1l.at[0, y], o1l_send, o1l_recv.at[0], chip(x, 0, 1)).start()

    @pl.when((core == 1) & (x != 0))
    def _():
        remote(late_src, o1l.at[1, x], o1l_send, o1l_recv.at[1], chip(0, y, 1)).start()

    @pl.when((core == 1) & (x == 0))
    def _():
        o1l[1, 0] = late_src[...]

    for which, buf in enumerate((kall, vall)):
        sent(buf.at[pl.ds(0, near_units // 2)], kv_send.at[which, 0])

        @pl.when(core == 0)
        def _(which=which, buf=buf):
            sent(buf.at[pl.ds(0, near_units // 2 + 2)], kv_send.at[which, 1])

        @pl.when(core == 1)
        def _(which=which, buf=buf):
            sent(buf.at[pl.ds(0, near_units // 2)], kv_send.at[which, 1])
            sent(buf.at[pl.ds(0, remote_units)], on_send.at[which])

    @pl.when((core == 0) | (x != 0))
    def _():
        sent(late_src, o1l_send)

    @pl.when(core == 0)
    def _():
        sent(qsrc.at[:, :, :, 0], q0_sem)

        sent(o1.at[0], o1_send)

    @pl.when(core == 1)
    def _():
        @pl.when(me == 1)
        def _():
            sent(q1.at[:, :, pl.ds(0, toks - 2)], q1_send)
            sent(q2.at[0, pl.ds(0, toks - 1)], q2l_send)

        @pl.when((me != 1) & (y == 0))
        def _():
            sent(q2.at[0, pl.ds(0, side)], q2l_send)

        @pl.when((me != 1) & (x == 0))
        def _():
            sent(q2.at[0, pl.ds(0, side - 1)], q2l_send)

        @pl.when(me > 1)
        def _():
            sent(q1.at[:, :, pl.ds(0, toks - 2)], q1_send)

        sent(q2, q2_send.at[0])
        sent(q2.at[pl.ds(0, side - 1)], q2_send.at[1])
        pl.semaphore_wait(side_row, side - 1)
        for step in range(2):
            net = jnp.where(y == 0, step, 1 - step)
            nu = jnp.where(net == 0, x, y)
            across = jnp.where(net == 0, y, x)
            line = net * side + nu

            def owner(along, pc, net=net):
                return chip(jnp.where(net == 0, along, x), jnp.where(net == 0, y, along), pc)

            def send_o2(src, device, line=line):
                remote(src, o2.at[line], o2_send, o2_recv, device).start()

            @pl.when(net == 0)
            def _():
                landed(o1.at[0], o1_recv.at[0])

            @pl.when(net == 1)
            def _():
                landed(o1.at[1, pl.ds(0, side - 1)], o1_recv.at[1])

            stats = []
            for b in range(2):
                vs = [(nu // 2 + b) % 2 + 2 * k for k in range(side // 2)]
                tiles = [o1[net, pv, width : width + EXTRA, :].astype(F32) for pv in vs]
                tops = [t[0:1] + t[1:2] + t[2:3] for t in tiles]
                dens = [t[3:4] + t[4:5] + t[5:6] for t in tiles]
                top = functools.reduce(jnp.maximum, tops)
                ws = [jnp.exp2((t - top) * exponent) for t in tops]
                stats += in_three(top) + in_three(sum(w * d for w, d in zip(ws, dens)))
                total = None
                for w, pv in zip(ws, vs):
                    part = o1[net, pv, 0:width, :].astype(F32) * w
                    total = part if total is None else total + part
                o2src[net, :, b] = total.T.reshape(toks, GROUP, width).astype(BF16)
            stat = jnp.concatenate(stats + [jnp.zeros((width - len(stats), piece), F32)]).T
            o2src[net, :, 2] = stat.reshape(toks, GROUP, width).astype(BF16)
            for d in far_first + [0]:
                along = (nu + d) % side

                @pl.when((along != 0) | (across != 0))
                def _(along=along):
                    send_o2(o2src.at[net, 2 * along], owner(along, 0))

                if d:
                    send_o2(o2src.at[net, 2 * along + 1], owner(along, 1))
            o2[line] = o2src[net, 2 * nu + 1]

            def late_parts(net):
                nu = jnp.where(net == 0, x, y)

                @pl.when(net == 0)
                def _():
                    landed(o1l.at[0], o1l_recv.at[0])

                @pl.when(net == 1)
                def _():
                    landed(o1l.at[1, pl.ds(0, side - 1)], o1l_recv.at[1])

                stat = jnp.zeros((GROUP, width), F32)
                for b in range(2):
                    vs = [(nu // 2 + b) % 2 + 2 * k for k in range(side // 2)]
                    tops, dens = [], []
                    for pv in vs:
                        tile = o1l[net, pv, 1].astype(F32)
                        tile = tile + pltpu.roll(tile, width - 1, 1) + pltpu.roll(tile, width - 2, 1)
                        tops.append(jnp.broadcast_to(tile[:, 0:1], (GROUP, width)))
                        dens.append(jnp.broadcast_to(tile[:, 3:4], (GROUP, width)))
                    top = functools.reduce(jnp.maximum, tops)
                    ws = [jnp.exp2((t - top) * exponent) for t in tops]
                    den = sum(w * d for w, d in zip(ws, dens))
                    num = sum(w * o1l[net, pv, 0].astype(F32) for w, pv in zip(ws, vs))
                    o2l[net, b] = num.astype(BF16)
                    for k, value in enumerate(in_three(top) + in_three(den)):
                        stat = jnp.where(lane == 6 * b + k, value, stat)
                o2l[net, 2] = stat.astype(BF16)
                remote(
                    o2l.at[net], o2.at[net * side + nu], o2_send, o2_recv, chip(0, 0, 0)
                ).start()

            @pl.when((across == 0) & (me != 1))
            def _(net=net):
                late_parts(net)

        @pl.when(me == 1)
        def _():
            @pl.loop(0, 2)
            def _(net):
                late_parts(net)

        sent(o1.at[0, pl.ds(0, side - 1)], o1_send)
        landed(o2.at[pl.ds(0, toks - 2)], o2_recv)
        sent(o2src.at[:, pl.ds(0, toks - 1)], o2_send)

    @pl.when(core == 0)
    def _():
        landed(o2, o2_recv)

    tops, dens = [[], []], [[], []]
    for src in range(toks):
        tile = o2[src, 2].astype(F32)
        tile = tile + pltpu.roll(tile, width - 1, 1) + pltpu.roll(tile, width - 2, 1)
        for b in range(2):
            tops[b].append(jnp.broadcast_to(tile[:, 6 * b : 6 * b + 1], (GROUP, width)))
            dens[b].append(jnp.broadcast_to(tile[:, 6 * b + 3 : 6 * b + 4], (GROUP, width)))
    for net in range(2):
        for e in range(2):
            srcs = [net * side + e + 2 * k for k in range(side // 2)]
            for b in range(2):
                top = functools.reduce(jnp.maximum, [tops[b][s] for s in srcs])
                ws = [jnp.exp2((tops[b][s] - top) * exponent) for s in srcs]
                den = sum(w * dens[b][s] for w, s in zip(ws, srcs))
                num = sum(w * o2[s, b].astype(F32) for w, s in zip(ws, srcs))
                head = CLASSES * net + e + 2 * b
                out_ref[head * GROUP : (head + 1) * GROUP, :] = num / den


def solution(mesh):
    seq = mesh.shape["seq"]
    side = math.isqrt(seq // 2)

    def body(
        queries, span_keys, span_values, cache_keys, cache_values, page_table, page_counts, span_start
    ):
        width = queries.shape[1] // H
        rows = cache_keys.shape[0]
        half = rows // 2
        toks = 2 * side
        piece = toks * GROUP
        table = jnp.asarray(rope_table(width, PAGE))
        units = 16
        vm = pltpu.VMEM
        dma = pltpu.SemaphoreType.DMA
        hbm = pl.BlockSpec(memory_space=pl.ANY)
        scratch = [
            pltpu.SMEM(span_start.shape, jnp.int32),
            pltpu.SMEM(page_counts.shape, jnp.int32),
            pltpu.SMEM(page_table.shape, jnp.int32),
            vm(table.shape, F32),
            vm((1, H * width), BF16),
            vm((1, KVH * width), BF16),
            vm((1, KVH * width), BF16),
            vm((rows, KVH * width), BF16),
            vm((H, width), F32),
            vm((rows, width), F32),
            vm((rows, width), F32),
            vm((KVH, 2, half + EXTRA, width), BF16),
            vm((KVH, 2, half, width), BF16),
            vm((units, half + EXTRA, width), BF16),
            vm((units, half, width), BF16),
            vm((units, half + EXTRA, width), BF16),
            vm((units, half, width), BF16),
            vm((width, units * half), BF16),
            vm((units * half, width), BF16),
            vm((3, 16, width), F32),
            vm((16, width), BF16),
            vm((width, width), BF16),
            vm((2, 2, 2, 2, GROUP, width), BF16),
            vm((2, 2, toks, GROUP, width), BF16),
            vm((side, toks, GROUP, width), BF16),
            vm((units * half, 2 * piece), F32),
            vm((units * half, 2 * piece), F32),
            vm((side, width + EXTRA, piece), BF16),
            vm((2, side, width + EXTRA, piece), BF16),
            vm((2, toks, 3, GROUP, width), BF16),
            vm((toks, 3, GROUP, width), BF16),
            vm((2, 2, GROUP, width), BF16),
            vm((GROUP, width), BF16),
            vm((2, GROUP, width), BF16),
            vm((2, side, 2, GROUP, width), BF16),
            vm((2, 3, GROUP, width), BF16),
            dma((9,)),
            dma((2, 2)),
            dma((2, 2)),
            dma((2,)),
            dma(()),
            dma(()),
            dma((2,)),
            dma((2,)),
            dma((side,)),
            dma(()),
            dma((2,)),
            dma(()),
            dma(()),
            dma((2,)),
            dma(()),
            dma(()),
            dma(()),
            dma((2,)),
            pltpu.SemaphoreType.REGULAR,
            pltpu.SemaphoreType.REGULAR,
            pltpu.SemaphoreType.REGULAR,
            pltpu.SemaphoreType.REGULAR,
            pltpu.SemaphoreType.REGULAR,
            vm((16, 2 * piece), F32),
            vm((16, 2 * piece), F32),
            vm((1, 2 * piece), F32),
            vm((1, 2 * piece), F32),
        ]
        out = pl.pallas_call(
            functools.partial(kernel, side),
            out_shape=pltpu.VMEM((H, width), F32),
            in_specs=[hbm] * 9,
            out_specs=pl.BlockSpec(memory_space=pltpu.VMEM),
            scratch_shapes=scratch,
            compiler_params=pltpu.CompilerParams(collective_id=0, has_side_effects=True),
            name="paged_prefix",
        )(
            span_start,
            page_counts,
            page_table,
            table,
            queries,
            span_keys,
            span_values,
            cache_keys,
            cache_values,
        )
        return out.reshape(queries.shape).astype(BF16)

    in_specs = (
        P(("groups", "seq"), None),
        P(("groups", "seq"), None),
        P(("groups", "seq"), None),
        P(("groups", "seq"), None),
        P(("groups", "seq"), None),
        P(("groups", "seq")),
        P(("groups", "seq")),
        P("groups"),
    )
    out_specs = P(("groups", "seq"), None)
    return jax.shard_map(body, mesh=mesh, in_specs=in_specs, out_specs=out_specs, check_vma=False)
```

```python
import functools
import math

import jax
import jax.numpy as jnp
import numpy as np
from jax import lax
from jax.experimental import pallas as pl
from jax.experimental.pallas import tpu as pltpu
from jax.sharding import PartitionSpec as P

H = 64
KVH = 8
PAGE = 16
GROUP = H // KVH
ROPE_BASE = 1000000.0
DEAD = -1e30
FLOOR = -1e29
CLASSES = 4
MESH = pl.DeviceIdType.MESH
F32 = jnp.float32
BF16 = jnp.bfloat16
EXTRA = 16


def rope_table(width, rows):
    half = width // 2
    freq = ROPE_BASE ** (-(np.arange(half, dtype=np.float64) * 2.0 / width))
    turns = np.concatenate([freq, freq]) / (2.0 * np.pi)
    pieces, rest = [], turns
    for _ in range(2):
        scale = 2.0 ** (np.floor(np.log2(rest)) - 7.0)
        part = np.floor(rest / scale) * scale
        pieces.append(part)
        rest = rest - part
    pieces.append(rest)
    sign = np.concatenate([-np.ones(half), np.ones(half)])
    angle = np.arange(rows, dtype=np.float64)[:, None] * np.concatenate([freq, freq])[None, :]
    pad = np.zeros((8 - len(pieces) - 1, width))
    return np.concatenate(
        [np.stack(pieces), sign[None], pad, np.cos(angle), np.sin(angle) * sign[None]]
    ).astype(np.float32)


def cos_sin(position, table_ref):
    def part(k):
        turn = position * table_ref[k : k + 1, :]
        return turn - jnp.floor(turn)

    turn = part(0) + part(1) + part(2)
    turn = turn - jnp.floor(turn + 0.5)
    angle = turn * (2.0 * math.pi)
    return jnp.cos(angle), jnp.sin(angle) * table_ref[3:4, :]


def in_three(value):
    high = value.astype(BF16).astype(F32)
    middle = (value - high).astype(BF16).astype(F32)
    return [high, middle, value - high - middle]


def kernel(
    side,
    start_hbm,
    count_hbm,
    pages_hbm,
    table_hbm,
    q_hbm,
    sk_hbm,
    sv_hbm,
    k_hbm,
    v_hbm,
    out_ref,
    start_ref,
    count_ref,
    pages_ref,
    table_ref,
    q_raw,
    sk_raw,
    sv_raw,
    k_raw,
    q_rows,
    cos_ref,
    sin_ref,
    kx,
    vx,
    kall,
    vall,
    kall0,
    vall0,
    vturned,
    kbias,
    rows16,
    kspan,
    vspan,
    qsrc,
    q1,
    q2,
    scores_a,
    scores_b,
    o1src,
    o1,
    o2src,
    o2,
    qlate,
    q2l,
    q2x,
    late_src,
    o1l,
    o2l,
    local_sem,
    kv_send,
    kv_recv,
    on_send,
    q0_sem,
    q1_send,
    q1_recv,
    q2_send,
    q2_recv,
    o1_send,
    o1_recv,
    o2_send,
    o2_recv,
    ql_recv,
    q2l_send,
    q2l_recv,
    q2x_send,
    q2x_recv,
    o1l_send,
    o1l_recv,
    told,
    told_far,
    side_row,
    side_col,
    span_a,
    span_b,
    top_a,
    top_b,
):
    width = q_rows.shape[1]
    rows = k_hbm.shape[0]
    half_rows = rows // 2
    units = kall.shape[0]
    toks = 2 * side
    piece = toks * GROUP
    me = lax.axis_index("seq")
    core = me % 2
    x = (me // 2) % side
    y = me // (2 * side)
    u = jnp.where(core == 0, x, y)
    v = jnp.where(core == 0, y, x)
    other = 1 - core

    def chip(px, py, pc):
        return ((py % side) * side + px % side) * 2 + pc

    def dev(pu, pv, pc):
        return chip(jnp.where(core == 0, pu, pv), jnp.where(core == 0, pv, pu), pc)

    def remote(src, dst, send, recv, device):
        return pltpu.make_async_remote_copy(
            src_ref=src,
            dst_ref=dst,
            send_sem=send,
            recv_sem=recv,
            device_id={"seq": device},
            device_id_type=MESH,
        )

    def sent(ref, sem):
        remote(ref, ref, sem, sem, chip(x, y, other)).wait_send()

    def landed(ref, sem):
        remote(ref, ref, sem, sem, chip(x, y, other)).wait_recv()

    local = {
        name: pltpu.make_async_copy(src, dst, local_sem.at[k])
        for k, (name, src, dst) in enumerate(
            (
                ("start", start_hbm, start_ref),
                ("count", count_hbm, count_ref),
                ("pages", pages_hbm, pages_ref),
                ("table", table_hbm, table_ref),
                ("q", q_hbm, q_raw),
                ("sk", sk_hbm, sk_raw),
                ("sv", sv_hbm, sv_raw),
                ("k", k_hbm, k_raw),
            )
        )
    }
    for copy in local.values():
        copy.start()
    for h in range(KVH):
        for hf in range(2):
            pltpu.make_async_copy(
                v_hbm.at[pl.ds(hf * half_rows, half_rows), pl.ds(h * width, width)],
                vx.at[h, hf],
                local_sem.at[len(local)],
            ).start()

    barrier = pltpu.get_barrier_semaphore()

    def signal(sem, device):
        pl.semaphore_signal(sem, inc=1, device_id={"seq": device}, device_id_type=MESH)

    neighbours = ((1, 0), (side - 1, 0), (0, 1), (0, side - 1))
    line0 = jnp.where(y == 0, x, jnp.where(x == 0, y, 0))
    by_chip0 = (line0 == 1) | (line0 == side - 1)

    @pl.when((core == 0) & by_chip0)
    def _():
        signal(barrier, chip(0, 0, 0))

    @pl.when(core == 1)
    def _():
        signal(barrier, chip(x, y, 0))
        for dx, dy in neighbours:
            signal(barrier, chip(x + dx, y + dy, 0))
        for d in range(1, side):
            signal(barrier, chip(x + d, y, 1))
            signal(barrier, chip(x, y + d, 1))

    for name in ("start", "count", "pages", "table", "q"):
        local[name].wait()
    start = start_ref[0]
    count = count_ref[0]
    own_pos = (start + me).astype(F32)
    own_cos, own_sin = cos_sin(jnp.full((8, width), own_pos, F32), table_ref)
    q_all = q_raw[...].astype(F32)
    for r in range(H):
        q_rows[r : r + 1, :] = q_all[:, r * width : (r + 1) * width]
    for net in range(2):
        for e in range(2):
            for b in range(2):
                head = CLASSES * net + e + 2 * b
                part = q_rows[head * GROUP : (head + 1) * GROUP, :]
                turned = part * own_cos + pltpu.roll(part, width // 2, 1) * own_sin
                qsrc[net, e, b, core] = turned.astype(BF16)

    far_first = [side // 2]
    for step in range(side // 2 - 1, 0, -1):
        far_first += [step, side - step]

    def send_q1(toks_sent, landing, recv):
        for d in far_first:
            for net in range(2):
                place = x if net == 0 else y
                along = (place + d) % side
                remote(
                    qsrc.at[net, along % 2, :, toks_sent],
                    landing(net, place),
                    q1_send,
                    recv.at[net],
                    chip(along, y, 1) if net == 0 else chip(x, along, 1),
                ).start()

    @pl.when(core == 0)
    def _():
        pl.semaphore_wait(barrier, jnp.where(me == 0, 4 + 4 + 1, 4 + 1))
        signal(told, chip(x, y, 1))
        remote(qsrc.at[:, :, :, 0], qsrc.at[:, :, :, 0], q0_sem, q0_sem, chip(x, y, 1)).start()


    def send_cache(which):
        buf = (kx, vx)[which]

        def send_all(net, landing, target):
            def send(head, half, slot, device):
                src = buf.at[head] if half is None else buf.at[head, half]
                dst = landing.at[pl.ds(slot, 2)] if half is None else landing.at[slot]
                remote(src, dst, kv_send.at[which, net], kv_recv.at[which, net], device).start()

            nu, nv = (x, y) if net == 0 else (y, x)

            def at(pu, pv):
                return chip(pu, pv, target) if net == 0 else chip(pv, pu, target)

            base = nu + 2 * nv
            head = CLASSES * net + (base + 1) % CLASSES
            send(head, None, 4 + 2 * core, at(nu + 1, nv))
            head = CLASSES * net + (base + 3) % CLASSES
            send(head, None, 8 + 2 * core, at(nu + side - 1, nv))
            head = CLASSES * net + (base + 2) % CLASSES
            send(head, 0, 12 + core, at(nu, nv + 1))
            send(head, 1, 14 + core, at(nu, nv + side - 1))

        @pl.when(me != 0)
        def _():
            send_all(0, (kall0, vall0)[which], 1)

        @pl.when(me == 0)
        def _():
            send_all(0, (kall, vall)[which], 0)

        send_all(1, (kall, vall)[which], 1)
        own = ((kall, vall)[which], (kall0, vall0)[which])
        head0 = (x + 2 * y) % CLASSES
        head1 = CLASSES + (y + 2 * x) % CLASSES

        @pl.when(core == 0)
        def _():
            own[0][0:2] = buf[head0]
            remote(
                buf.at[head1],
                own[0].at[pl.ds(0, 2)],
                kv_send.at[which, 1],
                kv_recv.at[which, 1],
                chip(x, y, 1),
            ).start()

        @pl.when(core == 1)
        def _():
            own[0][2:4] = buf[head1]
            own[1][2:4] = buf[head0]

    pltpu.make_async_copy(vx, vx, local_sem.at[len(local)]).wait()

    @pl.when(core == 0)
    def _():
        send_cache(1)

    tile_row = lax.broadcasted_iota(jnp.int32, (EXTRA, width), 0)
    lane = lax.broadcasted_iota(jnp.int32, (1, width), 1)
    half_pages = half_rows // PAGE
    biases = []
    for hf in range(2):
        page = jnp.zeros((1, width), jnp.int32)
        for j in range(half_pages):
            page = jnp.where(lane // PAGE == j, pages_ref[hf * half_pages + j], page)
        slot = hf * half_pages + lane // PAGE
        usable = (slot < count) & (page * PAGE + lane % PAGE < start)
        biases.append(jnp.where(usable, 0.0, DEAD).astype(F32))
    page_pos = jnp.zeros((16, width), jnp.int32)
    for j in range(rows // PAGE):
        page_pos = jnp.where(tile_row == j, pages_ref[j] * PAGE, page_pos)
    page_cos, page_sin = cos_sin(page_pos.astype(F32), table_ref)
    row_cos = table_ref[8 : 8 + PAGE, :]
    row_sin = table_ref[8 + PAGE : 8 + 2 * PAGE, :]
    for j in range(rows // PAGE):
        pc_, ps_ = page_cos[j : j + 1, :], page_sin[j : j + 1, :]
        cos_ref[j * PAGE : (j + 1) * PAGE, :] = pc_ * row_cos - ps_ * row_sin
        sin_ref[j * PAGE : (j + 1) * PAGE, :] = ps_ * row_cos + pc_ * row_sin
    for name in ("sk", "sv", "k"):
        local[name].wait()
    sk_all = sk_raw[...].astype(F32)
    sv_all = sv_raw[...].astype(F32)
    for h in range(KVH):
        span = jnp.broadcast_to(sk_all[:, h * width : (h + 1) * width], (8, width))
        span = span * own_cos + pltpu.roll(span, width // 2, 1) * own_sin
        span = jnp.broadcast_to(span[0:1, :], (EXTRA, width))
        value = jnp.broadcast_to(sv_all[:, h * width : (h + 1) * width], (EXTRA, width))
        for hf in range(2):
            tile = jnp.where(tile_row == 0, span, jnp.where(tile_row == 2, value, 0.0))
            tile = jnp.where(tile_row == 1, biases[hf], tile)
            kx[h, hf, half_rows : half_rows + EXTRA, :] = tile.astype(BF16)

    @pl.loop(0, KVH // 2)
    def _(step):
        for h in (2 * step, 2 * step + 1):
            cols = pl.ds(pl.multiple_of(h * width, width), width)
            for hf in range(2):
                span_rows = slice(hf * half_rows, (hf + 1) * half_rows)
                part = k_raw[span_rows, cols].astype(F32)
                turned = part * cos_ref[span_rows, :]
                turned = turned + pltpu.roll(part, width // 2, 1) * sin_ref[span_rows, :]
                kx[h, hf, 0:half_rows, :] = turned.astype(BF16)

    @pl.when(core == 0)
    def _():
        send_cache(0)
        pl.semaphore_wait(told_far, 1)

        @pl.when(me != 0)
        def _():
            for d in far_first:
                signal(side_row, chip(x + d, y, 1))
                signal(side_col, chip(x, y + d, 1))

    @pl.when(core == 1)
    def _():
        @pl.when(me == 1)
        def _():
            pl.semaphore_wait(barrier, 2 * (side - 1))
            send_q1(1, lambda net, place: q1.at[net, :, 2 * place + 1], q1_recv)
            send_cache(1)
            send_cache(0)
            pl.semaphore_wait(told, 1)
            signal(told_far, chip(x, y, 0))
            landed(qsrc.at[:, :, :, 0], q0_sem)
            send_q1(0, lambda net, place: qlate.at[net], ql_recv)
            qlate[0] = qsrc[0, 0, :, 0]
            qlate[1] = qsrc[1, 0, :, 0]

        @pl.when(me > 1)
        def _():
            pl.semaphore_wait(told, 1)
            send_cache(1)
            pl.semaphore_wait(barrier, 2 * (side - 1))
            signal(told_far, chip(x, y, 0))
            landed(qsrc.at[:, :, :, 0], q0_sem)
            send_q1(pl.ds(0, 2), lambda net, place: q1.at[net, :, pl.ds(2 * place, 2)], q1_recv)
            send_cache(0)

    remote_units = units - 2
    near_units = units - 4

    @pl.when(core == 1)
    def _():
        for net, place in ((0, x), (1, y)):
            for b in range(2):
                q1[net, b, 2 * place + 1] = qsrc[net, place % 2, b, 1]

        @pl.when(me > 1)
        def _():
            for net, place in ((0, x), (1, y)):
                for b in range(2):
                    q1[net, b, 2 * place] = qsrc[net, place % 2, b, 0]

        for net, across in ((0, y), (1, x)):

            @pl.when(across == 0)
            def _(net=net):
                for b in range(2):
                    q1[net, b, 0] = jnp.zeros((GROUP, width), BF16)

        pl.semaphore_wait(side_col, jnp.where((x == 0) & (y != 0), side - 2, side - 1))

        def send_q2(net, pv):
            nu, nv = (x, y) if net == 0 else (y, x)
            remote(
                q1.at[net, (nu // 2 + pv) % 2],
                q2.at[nv],
                q2_send.at[net],
                q2_recv.at[nv],
                chip(x, pv, 0) if net == 0 else chip(pv, y, 1),
            ).start()

        def all_in(net, along, across):
            short = (across == 0) & (along != 0)

            @pl.when(short)
            def _():
                landed(q1.at[net, :, pl.ds(0, toks - 3)], q1_recv.at[net])

            @pl.when(jnp.logical_not(short))
            def _():
                landed(q1.at[net, :, pl.ds(0, toks - 2)], q1_recv.at[net])

        all_in(0, x, y)
        for d in far_first:
            pv = (y + d) % side

            @pl.when((x != 0) | (pv != 0))
            def _(pv=pv):
                send_q2(0, pv)

            @pl.when((x == 0) & (pv == 0))
            def _():
                remote(q1.at[0, 0], q2x.at[y], q2_send.at[0], q2x_recv, chip(0, 0, 1)).start()

        @pl.when(me != 1)
        def _():
            send_q2(0, y)

        @pl.when(me == 1)
        def _():
            q2x[0] = q1[0, 0]

        all_in(1, y, x)
        for d in far_first:
            send_q2(1, (x + d) % side)
        q2[x] = q1[1, (y // 2 + x) % 2]

        def hand_on():
            cases = [(jnp.logical_not(by_chip0), near_units, ((2, units),))]
            for here, slots in (
                ((y == 0) & (x == 1), (4, 6)),
                ((y == 0) & (x == side - 1), (8, 10)),
                ((x == 0) & (y == 1), (12, 13)),
                ((x == 0) & (y == side - 1), (14, 15)),
            ):
                spans = ((2, slots[0]), (slots[1], units))
                cases.append((here, near_units - slots[1] + slots[0], spans))
            for which, (src, dst) in ((1, (vall0, vall)), (0, (kall0, kall))):
                for here, amount, spans in cases:

                    @pl.when(here)
                    def _(which=which, src=src, dst=dst, amount=amount, spans=spans):
                        landed(src.at[pl.ds(0, amount)], kv_recv.at[which, 0])
                        for first, end in spans:
                            span = pl.ds(first, end - first)
                            remote(
                                src.at[span],
                                dst.at[span],
                                on_send.at[which],
                                kv_recv.at[which, 0],
                                chip(x, y, 0),
                            ).start()

        hand_on()

        @pl.when(y == 0)
        def _():
            @pl.when(x != 0)
            def _():
                landed(qlate.at[0], ql_recv.at[0])

            for d in far_first + [0]:
                remote(
                    qlate.at[0, (x // 2 + d) % 2], q2l, q2l_send, q2l_recv, chip(x, d, 0)
                ).start()

        @pl.when(x == 0)
        def _():
            @pl.when(y != 0)
            def _():
                landed(qlate.at[1], ql_recv.at[1])

            for d in far_first:
                remote(
                    qlate.at[1, (y // 2 + d) % 2], q2l, q2l_send, q2l_recv, chip(d, y, 1)
                ).start()
            q2l[...] = qlate[1, (y // 2) % 2]

        landed(vall.at[pl.ds(0, remote_units)], kv_recv.at[1, 1])

    @pl.when(core == 0)
    def _():
        landed(vall.at[pl.ds(0, remote_units)], kv_recv.at[1, 0])

    for unit in range(units):
        vturned[:, unit * half_rows : (unit + 1) * half_rows] = vall[unit].T

    @pl.when(core == 1)
    def _():
        landed(kall.at[pl.ds(0, remote_units)], kv_recv.at[0, 1])

    @pl.when(core == 0)
    def _():
        landed(kall.at[pl.ds(0, remote_units)], kv_recv.at[0, 0])

    span_units = [0, 2, 4, 6, 8, 10, 12, 13]
    span_toks = [
        dev(pu, pv, pc)
        for pu, pv in ((u, v), (u + side - 1, v), (u + 1, v), (u, v + side - 1))
        for pc in range(2)
    ]
    rows16[...] = jnp.zeros_like(rows16)
    for unit in range(units):
        tile = kall[unit, half_rows : half_rows + EXTRA, :].astype(F32)
        rows16[0, unit : unit + 1, :] = tile[1:2, :]
        if unit in span_units:
            k = span_units.index(unit)
            rows16[1, k : k + 1, :] = tile[0:1, :]
            rows16[2, k : k + 1, :] = tile[2:3, :]
    zeros = jnp.zeros((width - 16, width), F32)
    bias_cols = jnp.concatenate([rows16[0], zeros]).T
    for unit in range(units):
        turned = bias_cols if unit == 0 else pltpu.roll(bias_cols, width - unit, 1)
        kbias[unit * half_rows : (unit + 1) * half_rows, :] = turned.astype(BF16)
    kspan[...] = rows16[1].astype(BF16)
    vspan[...] = jnp.concatenate([rows16[2], zeros]).T.astype(BF16)
    span_tok = jnp.full((16, piece), 1 << 20, jnp.int32)
    for k, tok in enumerate(span_toks):
        span_tok = jnp.where(tile_row == k, tok, span_tok)

    exponent = width**-0.5 / math.log(2.0)
    contract = (((1,), (1,)), ((), ()))
    chunk = 2 * half_rows
    cols = 2 * piece

    def send_o1(pv):
        remote(
            o1src.at[pv], o1.at[core, v], o1_send, o1_recv.at[core], dev(u, pv, 1)
        ).start()

    col_slot = lax.broadcasted_iota(jnp.int32, (1, piece), 1) // GROUP
    tok_along = jnp.where(core == 0, 2, 2 * side)
    tok_across = jnp.where(core == 0, 2 * side, 2)
    col_tok = (col_slot // 2) * tok_along + col_slot % 2
    one_hot = jnp.where(lax.broadcasted_iota(jnp.int32, (cols, width), 1) == 0, 1.0, 0.0).astype(BF16)

    scores, span_scores, tops = (scores_a, scores_b), (span_a, span_b), (top_a, top_b)
    half_units = units // 2
    half_cache = half_units * half_rows
    always = me < 4 * side * side

    def score(query, live, buf):
        n = query.shape[0]
        query = jnp.concatenate([query, one_hot[:n]], axis=1)
        s = lax.dot_general(kspan[...], query[:, :width], contract, preferred_element_type=F32)
        s_span = jnp.where(live, s, DEAD)
        span_scores[buf][:, :n] = s_span
        best = jnp.maximum(s_span[0:8], s_span[8:16])
        for p in range(2):
            span = slice(p * half_cache, (p + 1) * half_cache)
            keys = kall[p * half_units : (p + 1) * half_units, 0:half_rows, :]
            keys = jnp.concatenate([keys.reshape(half_cache, width), kbias[span, :]], axis=1)
            s = lax.dot_general(keys, query, contract, preferred_element_type=F32)
            scores[buf][span, :n] = s
            best = jnp.maximum(best, jnp.max(s.reshape(-1, 8, n), axis=0))
        tops[buf][:, :n] = jnp.maximum(jnp.max(best, axis=0, keepdims=True), FLOOR)

    def weigh(buf, n):
        top = tops[buf][:, :n]
        w = jnp.exp2((span_scores[buf][:, :n] - top) * exponent)
        total = w[0:8] + w[8:16]
        w = jnp.concatenate([w, jnp.zeros((width - 16, n), F32)])
        nums = [jnp.dot(vspan[...], w.astype(BF16), preferred_element_type=F32), None]
        for k in range(units // 2):
            w = jnp.exp2((scores[buf][k * chunk : (k + 1) * chunk, :n] - top) * exponent)
            total = total + jnp.sum(w.reshape(chunk // 8, 8, n), axis=0)
            part = jnp.dot(
                vturned[:, k * chunk : (k + 1) * chunk],
                w.astype(BF16),
                preferred_element_type=F32,
            )
            nums[k % 2] = part if nums[k % 2] is None else nums[k % 2] + part
        den = jnp.sum(total, axis=0, keepdims=True)
        stat = jnp.concatenate(in_three(top) + in_three(den) + [jnp.zeros((EXTRA - 6, n), F32)])
        return nums[0] + nums[1], stat

    def score_pair(pvs, buf):
        query = jnp.concatenate(
            [q2[pv].astype(F32).reshape(piece, width).astype(BF16) for pv in pvs]
        )
        live = jnp.concatenate([span_tok <= col_tok + pv * tok_across for pv in pvs], axis=1)
        score(query, live, buf)

    def weigh_pair(pvs, buf):
        num, stat = weigh(buf, cols)
        for k, pv in enumerate(pvs):
            lanes = slice(k * piece, (k + 1) * piece)
            o1src[pv, 0:width, :] = num[:, lanes].astype(BF16)
            o1src[pv, width : width + EXTRA, :] = stat[:, lanes].astype(BF16)

    def pair(k):
        late = (me <= 1) | by_chip0
        near = (v + jnp.where(k == 0, 0, side // 2 - k)) % side
        far = (v + side // 2 + k) % side
        return [jnp.where(late, (side - k) % side, near), jnp.where(late, k + 1, far)]

    def queries_in(pvs):
        for pv in pvs:

            @pl.when(((pv != v) | (core == 0)) & (me != 0))
            def _(pv=pv):
                landed(q2.at[pv], q2_recv.at[pv])

    def results_out(pvs):
        for pv in pvs:

            @pl.when((pv != v) | (core == 0))
            def _(pv=pv):
                send_o1(pv)

            @pl.when((pv == v) & (core == 1))
            def _(pv=pv):
                o1[1, pv] = o1src[pv]

    pairs = side // 2
    @pl.when(me == 0)
    def _():
        landed(q2, q2_recv.at[0])

    queries_in(pair(0))
    score_pair(pair(0), 0)

    for k in range(pairs - 1):
        queries_in(pair(k + 1))

        @pl.when(always)
        def _(k=k):
            score_pair(pair(k + 1), (k + 1) % 2)
            weigh_pair(pair(k), k % 2)

        results_out(pair(k))
        if k == 0:

            @pl.when(me == 1)
            def _():
                landed(q2x.at[pl.ds(0, side - 1)], q2x_recv)
                remote(q2x, q2, q2x_send, q2_recv.at[0], chip(0, 0, 0)).start()

    @pl.when(always)
    def _():
        weigh_pair(pair(pairs - 1), (pairs - 1) % 2)

    results_out(pair(pairs - 1))

    @pl.when((core == 0) | (x != 0))
    def _():
        landed(q2l, q2l_recv)

    @pl.when(always)
    def _():
        query = jnp.concatenate([q2l[...].astype(F32), jnp.zeros((piece - GROUP, width), F32)])
        score(query.astype(BF16), span_tok <= 0, 0)

    @pl.when(always)
    def _():
        num, stat = weigh(0, piece)
        late_src[0] = num.T[0:GROUP].astype(BF16)
        wide = jnp.concatenate([stat, jnp.zeros((width - EXTRA, piece), F32)])
        late_src[1] = wide.T[0:GROUP].astype(BF16)

    late_slot = jnp.where(core == 0, y, x)
    late_to = jnp.where(
        core == 0,
        jnp.where(x == 0, 0, chip(x, 0, 1)),
        jnp.where(y == 0, 0, chip(0, y, 1)),
    )
    late_stays = (me == 0) | ((core == 1) & (x == 0) & (y != 0))

    @pl.when(jnp.logical_not(late_stays))
    def _():
        remote(late_src, o1l.at[core, late_slot], o1l_send, o1l_recv.at[core], late_to).start()

    @pl.when(late_stays)
    def _():
        o1l[core, late_slot] = late_src[...]

    def merge_late(net, nu, out):
        stat = jnp.zeros((GROUP, width), F32)
        for b in range(2):
            vs = [(nu // 2 + b) % 2 + 2 * k for k in range(side // 2)]
            tops, dens = [], []
            for pv in vs:
                tile = o1l[net, pv, 1].astype(F32)
                tile = tile + pltpu.roll(tile, width - 1, 1) + pltpu.roll(tile, width - 2, 1)
                tops.append(jnp.broadcast_to(tile[:, 0:1], (GROUP, width)))
                dens.append(jnp.broadcast_to(tile[:, 3:4], (GROUP, width)))
            top = functools.reduce(jnp.maximum, tops)
            ws = [jnp.exp2((t - top) * exponent) for t in tops]
            den = sum(w * d for w, d in zip(ws, dens))
            num = sum(w * o1l[net, pv, 0].astype(F32) for w, pv in zip(ws, vs))
            out[b] = num.astype(BF16)
            for k, value in enumerate(in_three(top) + in_three(den)):
                stat = jnp.where(lane == 6 * b + k, value, stat)
        out[2] = stat.astype(BF16)

    for which, buf in enumerate((kall, vall)):
        sent(buf.at[pl.ds(0, near_units // 2)], kv_send.at[which, 0])

        @pl.when(core == 0)
        def _(which=which, buf=buf):
            sent(buf.at[pl.ds(0, near_units // 2 + 2)], kv_send.at[which, 1])

        @pl.when(core == 1)
        def _(which=which, buf=buf):
            sent(buf.at[pl.ds(0, near_units // 2)], kv_send.at[which, 1])
            for here, amount in (
                (line0 * by_chip0 == 0, remote_units),
                ((y == 0) & by_chip0, remote_units - 2),
                ((x == 0) & by_chip0, remote_units - 1),
            ):

                @pl.when(here)
                def _(which=which, buf=buf, amount=amount):
                    sent(buf.at[pl.ds(0, amount)], on_send.at[which])


    @pl.when(jnp.logical_not(late_stays))
    def _():
        sent(late_src, o1l_send)

    @pl.when(core == 0)
    def _():
        sent(qsrc.at[:, :, :, 0], q0_sem)

        sent(o1.at[0], o1_send)

    @pl.when(core == 1)
    def _():
        @pl.when(me == 1)
        def _():
            sent(q1.at[:, :, pl.ds(0, toks - 2)], q1_send)
            sent(q2.at[0, pl.ds(0, toks - 1)], q2l_send)

        @pl.when((me != 1) & (y == 0))
        def _():
            sent(q2.at[0, pl.ds(0, side)], q2l_send)

        @pl.when((me != 1) & (x == 0))
        def _():
            sent(q2.at[0, pl.ds(0, side - 1)], q2l_send)

        @pl.when(me > 1)
        def _():
            sent(q1.at[:, :, pl.ds(0, toks - 2)], q1_send)

        @pl.when(me == 1)
        def _():
            sent(q2.at[pl.ds(0, side - 1)], q2_send.at[0])
            sent(q2x, q2x_send)

        @pl.when(me != 1)
        def _():
            sent(q2, q2_send.at[0])

        sent(q2.at[pl.ds(0, side - 1)], q2_send.at[1])
        pl.semaphore_wait(side_row, jnp.where((y == 0) & (x != 0), side - 2, side - 1))
        for step in range(2):
            net = jnp.where(jnp.minimum(y, side - y) <= jnp.minimum(x, side - x), step, 1 - step)
            nu = jnp.where(net == 0, x, y)
            across = jnp.where(net == 0, y, x)
            line = net * side + nu

            def owner(along, pc, net=net):
                return chip(jnp.where(net == 0, along, x), jnp.where(net == 0, y, along), pc)

            def send_o2(src, device, line=line):
                remote(src, o2.at[line], o2_send, o2_recv, device).start()

            @pl.when(net == 0)
            def _():
                landed(o1.at[0], o1_recv.at[0])

            @pl.when(net == 1)
            def _():
                landed(o1.at[1, pl.ds(0, side - 1)], o1_recv.at[1])

            stats = []
            for b in range(2):
                vs = [(nu // 2 + b) % 2 + 2 * k for k in range(side // 2)]
                tiles = [o1[net, pv, width : width + EXTRA, :].astype(F32) for pv in vs]
                tops = [t[0:1] + t[1:2] + t[2:3] for t in tiles]
                dens = [t[3:4] + t[4:5] + t[5:6] for t in tiles]
                top = functools.reduce(jnp.maximum, tops)
                ws = [jnp.exp2((t - top) * exponent) for t in tops]
                stats += in_three(top) + in_three(sum(w * d for w, d in zip(ws, dens)))
                total = None
                for w, pv in zip(ws, vs):
                    part = o1[net, pv, 0:width, :].astype(F32) * w
                    total = part if total is None else total + part
                o2src[net, :, b] = total.T.reshape(toks, GROUP, width).astype(BF16)
            stat = jnp.concatenate(stats + [jnp.zeros((width - len(stats), piece), F32)]).T
            o2src[net, :, 2] = stat.reshape(toks, GROUP, width).astype(BF16)
            for d in far_first + [0]:
                along = (nu + d) % side

                @pl.when((along != 0) | (across != 0))
                def _(along=along):
                    send_o2(o2src.at[net, 2 * along], owner(along, 0))

                if d:
                    send_o2(o2src.at[net, 2 * along + 1], owner(along, 1))
            o2[line] = o2src[net, 2 * nu + 1]

            @pl.when((across == 0) & (me != 1))
            def _(net=net, nu=nu, line=line):
                @pl.when(net == 0)
                def _():
                    landed(o1l.at[0], o1l_recv.at[0])

                @pl.when(net == 1)
                def _():
                    landed(o1l.at[1, pl.ds(0, side - 1)], o1l_recv.at[1])

                merge_late(net, nu, o2l)
                send_o2(o2l, 0)

        sent(o1.at[0, pl.ds(0, side - 1)], o1_send)
        landed(o2.at[pl.ds(0, toks - 2)], o2_recv)

    @pl.when(core == 0)
    def _():
        @pl.when(me != 0)
        def _():
            landed(o2, o2_recv)

        @pl.when(me == 0)
        def _():
            landed(o1l.at[0, pl.ds(0, side - 1)], o1l_recv.at[0])
            landed(o1l.at[1], o1l_recv.at[1])
            merge_late(0, 0, o2.at[0])
            merge_late(1, 0, o2.at[side])
            landed(o2.at[pl.ds(0, toks - 2)], o2_recv)

    tops, dens = [[], []], [[], []]
    for src in range(toks):
        tile = o2[src, 2].astype(F32)
        tile = tile + pltpu.roll(tile, width - 1, 1) + pltpu.roll(tile, width - 2, 1)
        for b in range(2):
            tops[b].append(jnp.broadcast_to(tile[:, 6 * b : 6 * b + 1], (GROUP, width)))
            dens[b].append(jnp.broadcast_to(tile[:, 6 * b + 3 : 6 * b + 4], (GROUP, width)))
    for net in range(2):
        for e in range(2):
            srcs = [net * side + e + 2 * k for k in range(side // 2)]
            for b in range(2):
                top = functools.reduce(jnp.maximum, [tops[b][s] for s in srcs])
                ws = [jnp.exp2((tops[b][s] - top) * exponent) for s in srcs]
                den = sum(w * dens[b][s] for w, s in zip(ws, srcs))
                num = sum(w * o2[s, b].astype(F32) for w, s in zip(ws, srcs))
                head = CLASSES * net + e + 2 * b
                out_ref[head * GROUP : (head + 1) * GROUP, :] = num / den

    @pl.when(me == 1)
    def _():
        sent(o2src.at[:, pl.ds(0, toks - 2)], o2_send)

    @pl.when((core == 1) & (me != 1))
    def _():
        sent(o2src.at[:, pl.ds(0, toks - 1)], o2_send)


def solution(mesh):
    seq = mesh.shape["seq"]
    side = math.isqrt(seq // 2)

    def body(
        queries, span_keys, span_values, cache_keys, cache_values, page_table, page_counts, span_start
    ):
        width = queries.shape[1] // H
        rows = cache_keys.shape[0]
        half = rows // 2
        toks = 2 * side
        piece = toks * GROUP
        table = jnp.asarray(rope_table(width, PAGE))
        units = 16
        vm = pltpu.VMEM
        dma = pltpu.SemaphoreType.DMA
        hbm = pl.BlockSpec(memory_space=pl.ANY)
        scratch = [
            pltpu.SMEM(span_start.shape, jnp.int32),
            pltpu.SMEM(page_counts.shape, jnp.int32),
            pltpu.SMEM(page_table.shape, jnp.int32),
            vm(table.shape, F32),
            vm((1, H * width), BF16),
            vm((1, KVH * width), BF16),
            vm((1, KVH * width), BF16),
            vm((rows, KVH * width), BF16),
            vm((H, width), F32),
            vm((rows, width), F32),
            vm((rows, width), F32),
            vm((KVH, 2, half + EXTRA, width), BF16),
            vm((KVH, 2, half, width), BF16),
            vm((units, half + EXTRA, width), BF16),
            vm((units, half, width), BF16),
            vm((units, half + EXTRA, width), BF16),
            vm((units, half, width), BF16),
            vm((width, units * half), BF16),
            vm((units * half, width), BF16),
            vm((3, 16, width), F32),
            vm((16, width), BF16),
            vm((width, width), BF16),
            vm((2, 2, 2, 2, GROUP, width), BF16),
            vm((2, 2, toks, GROUP, width), BF16),
            vm((side, toks, GROUP, width), BF16),
            vm((units * half, 2 * piece), F32),
            vm((units * half, 2 * piece), F32),
            vm((side, width + EXTRA, piece), BF16),
            vm((2, side, width + EXTRA, piece), BF16),
            vm((2, toks, 3, GROUP, width), BF16),
            vm((toks, 3, GROUP, width), BF16),
            vm((2, 2, GROUP, width), BF16),
            vm((GROUP, width), BF16),
            vm((side, toks, GROUP, width), BF16),
            vm((2, GROUP, width), BF16),
            vm((2, side, 2, GROUP, width), BF16),
            vm((3, GROUP, width), BF16),
            dma((9,)),
            dma((2, 2)),
            dma((2, 2)),
            dma((2,)),
            dma(()),
            dma(()),
            dma((2,)),
            dma((2,)),
            dma((side,)),
            dma(()),
            dma((2,)),
            dma(()),
            dma(()),
            dma((2,)),
            dma(()),
            dma(()),
            dma(()),
            dma(()),
            dma(()),
            dma((2,)),
            pltpu.SemaphoreType.REGULAR,
            pltpu.SemaphoreType.REGULAR,
            pltpu.SemaphoreType.REGULAR,
            pltpu.SemaphoreType.REGULAR,
            vm((16, 2 * piece), F32),
            vm((16, 2 * piece), F32),
            vm((1, 2 * piece), F32),
            vm((1, 2 * piece), F32),
        ]
        out = pl.pallas_call(
            functools.partial(kernel, side),
            out_shape=pltpu.VMEM((H, width), F32),
            in_specs=[hbm] * 9,
            out_specs=pl.BlockSpec(memory_space=pltpu.VMEM),
            scratch_shapes=scratch,
            compiler_params=pltpu.CompilerParams(collective_id=0, has_side_effects=True),
            name="paged_prefix",
        )(
            span_start,
            page_counts,
            page_table,
            table,
            queries,
            span_keys,
            span_values,
            cache_keys,
            cache_values,
        )
        return out.reshape(queries.shape).astype(BF16)

    in_specs = (
        P(("groups", "seq"), None),
        P(("groups", "seq"), None),
        P(("groups", "seq"), None),
        P(("groups", "seq"), None),
        P(("groups", "seq"), None),
        P(("groups", "seq")),
        P(("groups", "seq")),
        P("groups"),
    )
    out_specs = P(("groups", "seq"), None)
    return jax.shard_map(body, mesh=mesh, in_specs=in_specs, out_specs=out_specs, check_vma=False)
```

```python
import functools
import math

import jax
import jax.numpy as jnp
import numpy as np
from jax import lax
from jax.experimental import pallas as pl
from jax.experimental.pallas import tpu as pltpu
from jax.sharding import PartitionSpec as P

H = 64
KVH = 8
PAGE = 16
GROUP = H // KVH
ROPE_BASE = 1000000.0
DEAD = -1e30
FLOOR = -1e29
CLASSES = 4
MESH = pl.DeviceIdType.MESH
F32 = jnp.float32
BF16 = jnp.bfloat16
EXTRA = 8


def rope_table(width, rows):
    half = width // 2
    freq = ROPE_BASE ** (-(np.arange(half, dtype=np.float64) * 2.0 / width))
    turns = np.concatenate([freq, freq]) / (2.0 * np.pi)
    pieces, rest = [], turns
    for _ in range(2):
        scale = 2.0 ** (np.floor(np.log2(rest)) - 7.0)
        part = np.floor(rest / scale) * scale
        pieces.append(part)
        rest = rest - part
    pieces.append(rest)
    sign = np.concatenate([-np.ones(half), np.ones(half)])
    angle = np.arange(rows, dtype=np.float64)[:, None] * np.concatenate([freq, freq])[None, :]
    pad = np.zeros((8 - len(pieces) - 1, width))
    return np.concatenate(
        [np.stack(pieces), sign[None], pad, np.cos(angle), np.sin(angle) * sign[None]]
    ).astype(np.float32)


def cos_sin(position, table_ref):
    def part(k):
        turn = position * table_ref[k : k + 1, :]
        return turn - jnp.floor(turn)

    turn = part(0) + part(1) + part(2)
    turn = turn - jnp.floor(turn + 0.5)
    angle = turn * (2.0 * math.pi)
    return jnp.cos(angle), jnp.sin(angle) * table_ref[3:4, :]


def in_three(value):
    high = value.astype(BF16).astype(F32)
    middle = (value - high).astype(BF16).astype(F32)
    return [high, middle, value - high - middle]


def kernel(
    side,
    start_ref,
    count_ref,
    pages_hbm,
    table_hbm,
    q_hbm,
    sk_hbm,
    sv_hbm,
    k_hbm,
    v_hbm,
    out_ref,
    pages_ref,
    table_ref,
    q_raw,
    sk_raw,
    sv_raw,
    k_raw,
    q_rows,
    cos_ref,
    sin_ref,
    kx,
    vx,
    kall,
    vall,
    kall0,
    vall0,
    vturned,
    kbias,
    rows16,
    kspan,
    vspan,
    qsrc,
    q1,
    q2,
    scores_a,
    scores_b,
    o1src,
    o1,
    o2src,
    o2,
    qlate,
    q2l,
    late_src,
    o1l,
    o2l,
    local_sem,
    kv_send,
    kv_recv,
    on_send,
    q0_sem,
    q1_send,
    q1_recv,
    q2_send,
    q2_recv,
    o1_send,
    o1_recv,
    o2_send,
    o2_recv,
    ql_recv,
    q2l_send,
    q2l_recv,
    o1l_send,
    o1l_recv,
    told,
    told_far,
    side_row,
    side_col,
    span_a,
    span_b,
    top_a,
    top_b,
):
    width = q_rows.shape[1]
    rows = k_hbm.shape[0]
    half_rows = rows // 2
    units = kall.shape[0]
    toks = 2 * side
    piece = toks * GROUP
    me = lax.axis_index("seq")
    core = me % 2
    x = (me // 2) % side
    y = me // (2 * side)
    u = jnp.where(core == 0, x, y)
    v = jnp.where(core == 0, y, x)
    other = 1 - core

    def chip(px, py, pc):
        return ((py % side) * side + px % side) * 2 + pc

    def dev(pu, pv, pc):
        return chip(jnp.where(core == 0, pu, pv), jnp.where(core == 0, pv, pu), pc)

    def remote(src, dst, send, recv, device):
        return pltpu.make_async_remote_copy(
            src_ref=src,
            dst_ref=dst,
            send_sem=send,
            recv_sem=recv,
            device_id={"seq": device},
            device_id_type=MESH,
        )

    def sent(ref, sem):
        remote(ref, ref, sem, sem, chip(x, y, other)).wait_send()

    def landed(ref, sem):
        remote(ref, ref, sem, sem, chip(x, y, other)).wait_recv()

    local = {
        name: pltpu.make_async_copy(src, dst, local_sem.at[k])
        for k, (name, src, dst) in enumerate(
            (
                ("pages", pages_hbm, pages_ref),
                ("table", table_hbm, table_ref),
                ("q", q_hbm, q_raw),
                ("sk", sk_hbm, sk_raw),
                ("sv", sv_hbm, sv_raw),
                ("k", k_hbm, k_raw),
            )
        )
    }
    for copy in local.values():
        copy.start()
    for h in range(KVH):
        for hf in range(2):
            pltpu.make_async_copy(
                v_hbm.at[pl.ds(hf * half_rows, half_rows), pl.ds(h * width, width)],
                vx.at[h, hf],
                local_sem.at[len(local)],
            ).start()

    barrier = pltpu.get_barrier_semaphore()

    def signal(sem, device):
        pl.semaphore_signal(sem, inc=1, device_id={"seq": device}, device_id_type=MESH)

    neighbours = ((1, 0), (side - 1, 0), (0, 1), (0, side - 1))
    line0 = jnp.where(y == 0, x, jnp.where(x == 0, y, 0))
    by_chip0 = (line0 == 1) | (line0 == side - 1)

    @pl.when((core == 0) & by_chip0)
    def _():
        signal(barrier, chip(0, 0, 0))

    @pl.when(core == 1)
    def _():
        signal(barrier, chip(x, y, 0))
        for dx, dy in neighbours:
            signal(barrier, chip(x + dx, y + dy, 0))
        for d in range(1, side):
            signal(barrier, chip(x + d, y, 1))
            signal(barrier, chip(x, y + d, 1))

    for name in ("pages", "table", "q"):
        local[name].wait()
    start = start_ref[0]
    count = count_ref[0]
    own_pos = (start + me).astype(F32)
    own_cos, own_sin = cos_sin(jnp.full((8, width), own_pos, F32), table_ref)
    q_all = q_raw[...].astype(F32)
    for r in range(H):
        q_rows[r : r + 1, :] = q_all[:, r * width : (r + 1) * width]
    for net in range(2):
        for e in range(2):
            for b in range(2):
                head = CLASSES * net + e + 2 * b
                part = q_rows[head * GROUP : (head + 1) * GROUP, :]
                turned = part * own_cos + pltpu.roll(part, width // 2, 1) * own_sin
                qsrc[net, e, b, core] = turned.astype(BF16)

    far_first = [side // 2]
    for step in range(side // 2 - 1, 0, -1):
        far_first += [step, side - step]

    def send_q1(toks_sent, landing, recv):
        for d in far_first:
            for net in range(2):
                place = x if net == 0 else y
                along = (place + d) % side
                remote(
                    qsrc.at[net, along % 2, :, toks_sent],
                    landing(net, place),
                    q1_send,
                    recv.at[net],
                    chip(along, y, 1) if net == 0 else chip(x, along, 1),
                ).start()

    @pl.when(core == 0)
    def _():
        pl.semaphore_wait(barrier, jnp.where(me == 0, 4 + 4 + 1, 4 + 1))
        signal(told, chip(x, y, 1))
        remote(qsrc.at[:, :, :, 0], qsrc.at[:, :, :, 0], q0_sem, q0_sem, chip(x, y, 1)).start()


    def send_cache(which):
        buf = (kx, vx)[which]

        def send_all(net, landing, target):
            def send(head, half, slot, device):
                src = buf.at[head] if half is None else buf.at[head, half]
                dst = landing.at[pl.ds(slot, 2)] if half is None else landing.at[slot]
                remote(src, dst, kv_send.at[which, net], kv_recv.at[which, net], device).start()

            nu, nv = (x, y) if net == 0 else (y, x)

            def at(pu, pv):
                return chip(pu, pv, target) if net == 0 else chip(pv, pu, target)

            base = nu + 2 * nv
            head = CLASSES * net + (base + 1) % CLASSES
            send(head, None, 4 + 2 * core, at(nu + 1, nv))
            head = CLASSES * net + (base + 3) % CLASSES
            send(head, None, 8 + 2 * core, at(nu + side - 1, nv))
            head = CLASSES * net + (base + 2) % CLASSES
            send(head, 0, 12 + core, at(nu, nv + 1))
            send(head, 1, 14 + core, at(nu, nv + side - 1))

        @pl.when(me != 0)
        def _():
            send_all(0, (kall0, vall0)[which], 1)

        @pl.when(me == 0)
        def _():
            send_all(0, (kall, vall)[which], 0)

        send_all(1, (kall, vall)[which], 1)
        own = ((kall, vall)[which], (kall0, vall0)[which])
        head0 = (x + 2 * y) % CLASSES
        head1 = CLASSES + (y + 2 * x) % CLASSES

        @pl.when(core == 0)
        def _():
            own[0][0:2] = buf[head0]
            remote(
                buf.at[head1],
                own[0].at[pl.ds(0, 2)],
                kv_send.at[which, 1],
                kv_recv.at[which, 1],
                chip(x, y, 1),
            ).start()

        @pl.when(core == 1)
        def _():
            own[0][2:4] = buf[head1]
            own[1][2:4] = buf[head0]

    pltpu.make_async_copy(vx, vx, local_sem.at[len(local)]).wait()

    @pl.when(core == 0)
    def _():
        send_cache(1)

    tile_row = lax.broadcasted_iota(jnp.int32, (EXTRA, width), 0)
    row16 = lax.broadcasted_iota(jnp.int32, (16, width), 0)
    lane = lax.broadcasted_iota(jnp.int32, (1, width), 1)
    half_pages = half_rows // PAGE
    biases = []
    for hf in range(2):
        page = jnp.zeros((1, width), jnp.int32)
        for j in range(half_pages):
            page = jnp.where(lane // PAGE == j, pages_ref[hf * half_pages + j], page)
        slot = hf * half_pages + lane // PAGE
        usable = (slot < count) & (page * PAGE + lane % PAGE < start)
        biases.append(jnp.where(usable, 0.0, DEAD).astype(F32))
    page_pos = jnp.zeros((16, width), jnp.int32)
    for j in range(rows // PAGE):
        page_pos = jnp.where(row16 == j, pages_ref[j] * PAGE, page_pos)
    page_cos, page_sin = cos_sin(page_pos.astype(F32), table_ref)
    row_cos = table_ref[8 : 8 + PAGE, :]
    row_sin = table_ref[8 + PAGE : 8 + 2 * PAGE, :]
    for j in range(rows // PAGE):
        pc_, ps_ = page_cos[j : j + 1, :], page_sin[j : j + 1, :]
        cos_ref[j * PAGE : (j + 1) * PAGE, :] = pc_ * row_cos - ps_ * row_sin
        sin_ref[j * PAGE : (j + 1) * PAGE, :] = ps_ * row_cos + pc_ * row_sin
    for name in ("sk", "sv", "k"):
        local[name].wait()
    sk_all = sk_raw[...].astype(F32)
    sv_all = sv_raw[...].astype(F32)
    for h in range(KVH):
        span = jnp.broadcast_to(sk_all[:, h * width : (h + 1) * width], (8, width))
        span = span * own_cos + pltpu.roll(span, width // 2, 1) * own_sin
        span = jnp.broadcast_to(span[0:1, :], (EXTRA, width))
        value = jnp.broadcast_to(sv_all[:, h * width : (h + 1) * width], (EXTRA, width))
        for hf in range(2):
            tile = jnp.where(tile_row == 0, span, jnp.where(tile_row == 2, value, 0.0))
            tile = jnp.where(tile_row == 1, biases[hf], tile)
            kx[h, hf, half_rows : half_rows + EXTRA, :] = tile.astype(BF16)

    @pl.loop(0, KVH // 2)
    def _(step):
        for h in (2 * step, 2 * step + 1):
            cols = pl.ds(pl.multiple_of(h * width, width), width)
            for hf in range(2):
                span_rows = slice(hf * half_rows, (hf + 1) * half_rows)
                part = k_raw[span_rows, cols].astype(F32)
                turned = part * cos_ref[span_rows, :]
                turned = turned + pltpu.roll(part, width // 2, 1) * sin_ref[span_rows, :]
                kx[h, hf, 0:half_rows, :] = turned.astype(BF16)

    @pl.when(core == 0)
    def _():
        send_cache(0)
        pl.semaphore_wait(told_far, 1)

        @pl.when(me != 0)
        def _():
            for d in far_first:
                signal(side_row, chip(x + d, y, 1))
                signal(side_col, chip(x, y + d, 1))

    @pl.when(core == 1)
    def _():
        @pl.when(me == 1)
        def _():
            pl.semaphore_wait(barrier, 2 * (side - 1))
            send_q1(1, lambda net, place: q1.at[net, :, 2 * place + 1], q1_recv)
            send_cache(1)
            send_cache(0)
            pl.semaphore_wait(told, 1)
            signal(told_far, chip(x, y, 0))
            landed(qsrc.at[:, :, :, 0], q0_sem)
            send_q1(0, lambda net, place: qlate.at[net], ql_recv)
            qlate[0] = qsrc[0, 0, :, 0]
            qlate[1] = qsrc[1, 0, :, 0]

        @pl.when(me > 1)
        def _():
            pl.semaphore_wait(told, 1)
            send_cache(1)
            pl.semaphore_wait(barrier, 2 * (side - 1))
            signal(told_far, chip(x, y, 0))
            landed(qsrc.at[:, :, :, 0], q0_sem)
            send_q1(pl.ds(0, 2), lambda net, place: q1.at[net, :, pl.ds(2 * place, 2)], q1_recv)
            send_cache(0)

    remote_units = units - 2
    near_units = units - 4

    @pl.when(core == 1)
    def _():
        for net, place in ((0, x), (1, y)):
            for b in range(2):
                q1[net, b, 2 * place + 1] = qsrc[net, place % 2, b, 1]

        @pl.when(me > 1)
        def _():
            for net, place in ((0, x), (1, y)):
                for b in range(2):
                    q1[net, b, 2 * place] = qsrc[net, place % 2, b, 0]

        for net, across in ((0, y), (1, x)):

            @pl.when(across == 0)
            def _(net=net):
                for b in range(2):
                    q1[net, b, 0] = jnp.zeros((GROUP, width), BF16)

        pl.semaphore_wait(side_col, jnp.where((x == 0) & (y != 0), side - 2, side - 1))

        def send_q2(net, pv):
            nu, nv = (x, y) if net == 0 else (y, x)
            remote(
                q1.at[net, (nu // 2 + pv) % 2],
                q2.at[nv],
                q2_send.at[net],
                q2_recv.at[nv],
                chip(x, pv, 0) if net == 0 else chip(pv, y, 1),
            ).start()

        def all_in(net, along, across):
            short = (across == 0) & (along != 0)

            @pl.when(short)
            def _():
                landed(q1.at[net, :, pl.ds(0, toks - 3)], q1_recv.at[net])

            @pl.when(jnp.logical_not(short))
            def _():
                landed(q1.at[net, :, pl.ds(0, toks - 2)], q1_recv.at[net])

        all_in(0, x, y)
        for d in far_first:
            pv = (y + d) % side

            @pl.when((x != 0) | (pv != 0))
            def _(pv=pv):
                send_q2(0, pv)

        send_q2(0, y)
        all_in(1, y, x)
        for d in far_first:
            send_q2(1, (x + d) % side)
        q2[x] = q1[1, (y // 2 + x) % 2]

        def hand_on():
            cases = [(jnp.logical_not(by_chip0), near_units, ((2, units),))]
            for here, slots in (
                ((y == 0) & (x == 1), (4, 6)),
                ((y == 0) & (x == side - 1), (8, 10)),
                ((x == 0) & (y == 1), (12, 13)),
                ((x == 0) & (y == side - 1), (14, 15)),
            ):
                spans = ((2, slots[0]), (slots[1], units))
                cases.append((here, near_units - slots[1] + slots[0], spans))
            for which, (src, dst) in ((1, (vall0, vall)), (0, (kall0, kall))):
                for here, amount, spans in cases:

                    @pl.when(here)
                    def _(which=which, src=src, dst=dst, amount=amount, spans=spans):
                        landed(src.at[pl.ds(0, amount)], kv_recv.at[which, 0])
                        for first, end in spans:
                            span = pl.ds(first, end - first)
                            remote(
                                src.at[span],
                                dst.at[span],
                                on_send.at[which],
                                kv_recv.at[which, 0],
                                chip(x, y, 0),
                            ).start()

        hand_on()

        @pl.when(y == 0)
        def _():
            @pl.when(x != 0)
            def _():
                landed(qlate.at[0], ql_recv.at[0])

            for d in far_first + [0]:
                remote(
                    qlate.at[0, (x // 2 + d) % 2], q2l, q2l_send, q2l_recv, chip(x, d, 0)
                ).start()

        @pl.when(x == 0)
        def _():
            @pl.when(y != 0)
            def _():
                landed(qlate.at[1], ql_recv.at[1])
                send_q2(0, 0)

            for d in far_first:
                remote(
                    qlate.at[1, (y // 2 + d) % 2], q2l, q2l_send, q2l_recv, chip(d, y, 1)
                ).start()
            q2l[...] = qlate[1, (y // 2) % 2]

        landed(vall.at[pl.ds(0, remote_units)], kv_recv.at[1, 1])

    @pl.when(core == 0)
    def _():
        landed(vall.at[pl.ds(0, remote_units)], kv_recv.at[1, 0])

    for unit in range(units):
        vturned[:, unit * half_rows : (unit + 1) * half_rows] = vall[unit].T

    @pl.when(core == 1)
    def _():
        landed(kall.at[pl.ds(0, remote_units)], kv_recv.at[0, 1])

    @pl.when(core == 0)
    def _():
        landed(kall.at[pl.ds(0, remote_units)], kv_recv.at[0, 0])

    span_units = [0, 2, 4, 6, 8, 10, 12, 13]
    span_toks = [
        dev(pu, pv, pc)
        for pu, pv in ((u, v), (u + side - 1, v), (u + 1, v), (u, v + side - 1))
        for pc in range(2)
    ]
    rows16[...] = jnp.zeros_like(rows16)
    for unit in range(units):
        tile = kall[unit, half_rows : half_rows + EXTRA, :].astype(F32)
        rows16[0, unit : unit + 1, :] = tile[1:2, :]
        if unit in span_units:
            k = span_units.index(unit)
            rows16[1, k : k + 1, :] = tile[0:1, :]
            rows16[2, k : k + 1, :] = tile[2:3, :]
    zeros = jnp.zeros((width - 16, width), F32)
    bias_cols = jnp.concatenate([rows16[0], zeros]).T
    for unit in range(units):
        turned = bias_cols if unit == 0 else pltpu.roll(bias_cols, width - unit, 1)
        kbias[unit * half_rows : (unit + 1) * half_rows, :] = turned.astype(BF16)
    kspan[...] = rows16[1].astype(BF16)
    vspan[...] = jnp.concatenate([rows16[2], zeros]).T.astype(BF16)
    span_tok = jnp.full((16, piece), 1 << 20, jnp.int32)
    for k, tok in enumerate(span_toks):
        span_tok = jnp.where(row16 == k, tok, span_tok)

    exponent = width**-0.5 / math.log(2.0)
    contract = (((1,), (1,)), ((), ()))
    chunk = 2 * half_rows
    cols = 2 * piece

    def send_o1(pv):
        remote(
            o1src.at[pv], o1.at[core, v], o1_send, o1_recv.at[core], dev(u, pv, 1)
        ).start()

    col_slot = lax.broadcasted_iota(jnp.int32, (1, piece), 1) // GROUP
    tok_along = jnp.where(core == 0, 2, 2 * side)
    tok_across = jnp.where(core == 0, 2 * side, 2)
    col_tok = (col_slot // 2) * tok_along + col_slot % 2
    one_hot = jnp.where(lax.broadcasted_iota(jnp.int32, (cols, width), 1) == 0, 1.0, 0.0).astype(BF16)

    scores, span_scores, tops = (scores_a, scores_b), (span_a, span_b), (top_a, top_b)
    half_units = units // 2
    half_cache = half_units * half_rows
    always = me < 4 * side * side

    def score(query, live, buf):
        n = query.shape[0]
        query = jnp.concatenate([query, one_hot[:n]], axis=1)
        s = lax.dot_general(kspan[...], query[:, :width], contract, preferred_element_type=F32)
        s_span = jnp.where(live, s, DEAD)
        span_scores[buf][:, :n] = s_span
        best = jnp.maximum(s_span[0:8], s_span[8:16])
        for p in range(2):
            span = slice(p * half_cache, (p + 1) * half_cache)
            keys = kall[p * half_units : (p + 1) * half_units, 0:half_rows, :]
            keys = jnp.concatenate([keys.reshape(half_cache, width), kbias[span, :]], axis=1)
            s = lax.dot_general(keys, query, contract, preferred_element_type=F32)
            scores[buf][span, :n] = s
            best = jnp.maximum(best, jnp.max(s.reshape(-1, 8, n), axis=0))
        tops[buf][:, :n] = jnp.maximum(jnp.max(best, axis=0, keepdims=True), FLOOR)

    def weigh(buf, n):
        top = tops[buf][:, :n]
        w = jnp.exp2((span_scores[buf][:, :n] - top) * exponent)
        total = w[0:8] + w[8:16]
        w = jnp.concatenate([w, jnp.zeros((width - 16, n), F32)])
        nums = [jnp.dot(vspan[...], w.astype(BF16), preferred_element_type=F32), None]
        for k in range(units // 2):
            w = jnp.exp2((scores[buf][k * chunk : (k + 1) * chunk, :n] - top) * exponent)
            total = total + jnp.sum(w.reshape(chunk // 8, 8, n), axis=0)
            part = jnp.dot(
                vturned[:, k * chunk : (k + 1) * chunk],
                w.astype(BF16),
                preferred_element_type=F32,
            )
            nums[k % 2] = part if nums[k % 2] is None else nums[k % 2] + part
        den = jnp.sum(total, axis=0, keepdims=True)
        stat = jnp.concatenate(in_three(top) + in_three(den) + [jnp.zeros((EXTRA - 6, n), F32)])
        return nums[0] + nums[1], stat

    def score_pair(pvs, buf):
        query = jnp.concatenate(
            [q2[pv].astype(F32).reshape(piece, width).astype(BF16) for pv in pvs]
        )
        live = jnp.concatenate([span_tok <= col_tok + pv * tok_across for pv in pvs], axis=1)
        score(query, live, buf)

    def weigh_pair(pvs, buf):
        num, stat = weigh(buf, cols)
        for k, pv in enumerate(pvs):
            lanes = slice(k * piece, (k + 1) * piece)
            o1src[pv, 0:width, :] = num[:, lanes].astype(BF16)
            o1src[pv, width : width + EXTRA, :] = stat[:, lanes].astype(BF16)

    def pair(k):
        late, away, half = (me <= 1) | by_chip0, jnp.where(v < side // 2, -1, 1), side // 2
        a, b = [(0, 1), (half, half - 1), (1 - half, half - 2), (2 - half, -1)][k]
        return [
            jnp.where(late, (side - k) % side, (v + away * a + side) % side),
            jnp.where(late, k + 1, (v + away * b + side) % side),
        ]

    def queries_in(pvs):
        for pv in pvs:

            @pl.when((pv != v) | (core == 0))
            def _(pv=pv):
                landed(q2.at[pv], q2_recv.at[pv])

    def results_out(pvs):
        for pv in pvs:

            @pl.when((pv != v) | (core == 0))
            def _(pv=pv):
                send_o1(pv)

            @pl.when((pv == v) & (core == 1))
            def _(pv=pv):
                o1[1, pv] = o1src[pv]

    pairs = side // 2
    queries_in(pair(0))
    score_pair(pair(0), 0)

    for k in range(pairs - 1):
        queries_in(pair(k + 1))

        @pl.when(always)
        def _(k=k):
            score_pair(pair(k + 1), (k + 1) % 2)
            weigh_pair(pair(k), k % 2)

        results_out(pair(k))

    @pl.when((core == 0) | (x != 0))
    def _():
        landed(q2l, q2l_recv)

    @pl.when(always)
    def _():
        query = jnp.concatenate([q2l[...].astype(F32), jnp.zeros((piece - GROUP, width), F32)])
        score(query.astype(BF16), span_tok <= 0, pairs % 2)
        weigh_pair(pair(pairs - 1), (pairs - 1) % 2)

    results_out(pair(pairs - 1))

    @pl.when(always)
    def _():
        num, stat = weigh(pairs % 2, piece)
        late_src[0] = num.T[0:GROUP].astype(BF16)
        wide = jnp.concatenate([stat, jnp.zeros((width - EXTRA, piece), F32)])
        late_src[1] = wide.T[0:GROUP].astype(BF16)

    late_slot = jnp.where(core == 0, y, x)
    late_to = jnp.where(
        core == 0,
        jnp.where(x == 0, 0, chip(x, 0, 1)),
        jnp.where(y == 0, 0, chip(0, y, 1)),
    )
    late_stays = (me == 0) | ((core == 1) & (x == 0) & (y != 0))

    @pl.when(jnp.logical_not(late_stays))
    def _():
        remote(late_src, o1l.at[core, late_slot], o1l_send, o1l_recv.at[core], late_to).start()

    @pl.when(late_stays)
    def _():
        o1l[core, late_slot] = late_src[...]

    def merge_late(net, nu, out):
        stat = jnp.zeros((GROUP, width), F32)
        for b in range(2):
            vs = [(nu // 2 + b) % 2 + 2 * k for k in range(side // 2)]
            tops, dens = [], []
            for pv in vs:
                tile = o1l[net, pv, 1].astype(F32)
                tile = tile + pltpu.roll(tile, width - 1, 1) + pltpu.roll(tile, width - 2, 1)
                tops.append(jnp.broadcast_to(tile[:, 0:1], (GROUP, width)))
                dens.append(jnp.broadcast_to(tile[:, 3:4], (GROUP, width)))
            top = functools.reduce(jnp.maximum, tops)
            ws = [jnp.exp2((t - top) * exponent) for t in tops]
            den = sum(w * d for w, d in zip(ws, dens))
            num = sum(w * o1l[net, pv, 0].astype(F32) for w, pv in zip(ws, vs))
            out[b] = num.astype(BF16)
            for k, value in enumerate(in_three(top) + in_three(den)):
                stat = jnp.where(lane == 6 * b + k, value, stat)
        out[2] = stat.astype(BF16)

    def cache_gone():
        for which, buf in enumerate((kall, vall)):
            sent(buf.at[pl.ds(0, near_units // 2)], kv_send.at[which, 0])

            @pl.when(core == 0)
            def _(which=which, buf=buf):
                sent(buf.at[pl.ds(0, near_units // 2 + 2)], kv_send.at[which, 1])

            @pl.when(core == 1)
            def _(which=which, buf=buf):
                sent(buf.at[pl.ds(0, near_units // 2)], kv_send.at[which, 1])
                for here, amount in (
                    (line0 * by_chip0 == 0, remote_units),
                    ((y == 0) & by_chip0, remote_units - 2),
                    ((x == 0) & by_chip0, remote_units - 1),
                ):

                    @pl.when(here)
                    def _(which=which, buf=buf, amount=amount):
                        sent(buf.at[pl.ds(0, amount)], on_send.at[which])

        @pl.when(jnp.logical_not(late_stays))
        def _():
            sent(late_src, o1l_send)

    @pl.when(core == 0)
    def _():
        cache_gone()

        sent(qsrc.at[:, :, :, 0], q0_sem)
        sent(o1.at[0], o1_send)

    @pl.when(core == 1)
    def _():
        pl.semaphore_wait(side_row, jnp.where((y == 0) & (x != 0), side - 2, side - 1))
        for step in range(2):
            net = jnp.where(jnp.minimum(y, side - y) <= jnp.minimum(x, side - x), step, 1 - step)
            nu = jnp.where(net == 0, x, y)
            across = jnp.where(net == 0, y, x)
            line = net * side + nu

            def owner(along, pc, net=net):
                return chip(jnp.where(net == 0, along, x), jnp.where(net == 0, y, along), pc)

            def send_o2(src, device, line=line):
                remote(src, o2.at[line], o2_send, o2_recv, device).start()

            @pl.when(net == 0)
            def _():
                landed(o1.at[0], o1_recv.at[0])

            @pl.when(net == 1)
            def _():
                landed(o1.at[1, pl.ds(0, side - 1)], o1_recv.at[1])

            stats = []
            for b in range(2):
                vs = [(nu // 2 + b) % 2 + 2 * k for k in range(side // 2)]
                tiles = [o1[net, pv, width : width + EXTRA, :].astype(F32) for pv in vs]
                tops = [t[0:1] + t[1:2] + t[2:3] for t in tiles]
                dens = [t[3:4] + t[4:5] + t[5:6] for t in tiles]
                top = functools.reduce(jnp.maximum, tops)
                ws = [jnp.exp2((t - top) * exponent) for t in tops]
                stats += in_three(top) + in_three(sum(w * d for w, d in zip(ws, dens)))
                total = None
                for w, pv in zip(ws, vs):
                    part = o1[net, pv, 0:width, :].astype(F32) * w
                    total = part if total is None else total + part
                o2src[net, :, b] = total.T.reshape(toks, GROUP, width).astype(BF16)
            stat = jnp.concatenate(stats + [jnp.zeros((width - len(stats), piece), F32)]).T
            o2src[net, :, 2] = stat.reshape(toks, GROUP, width).astype(BF16)
            for d in far_first + [0]:
                along = (nu + d) % side

                @pl.when((along != 0) | (across != 0))
                def _(along=along):
                    send_o2(o2src.at[net, 2 * along], owner(along, 0))

                if d:
                    send_o2(o2src.at[net, 2 * along + 1], owner(along, 1))
            o2[line] = o2src[net, 2 * nu + 1]

            @pl.when((across == 0) & (me != 1))
            def _(net=net, nu=nu):
                @pl.when(net == 0)
                def _():
                    landed(o1l.at[0], o1l_recv.at[0])

                @pl.when(net == 1)
                def _():
                    landed(o1l.at[1, pl.ds(0, side - 1)], o1l_recv.at[1])

                merge_late(net, nu, o2l)
                send_o2(o2l, owner(0, 0))

        cache_gone()

        @pl.when(me == 1)
        def _():
            sent(q1.at[:, :, pl.ds(0, toks - 2)], q1_send)
            sent(q2.at[0, pl.ds(0, toks - 1)], q2l_send)

        @pl.when((me != 1) & (y == 0))
        def _():
            sent(q2.at[0, pl.ds(0, side)], q2l_send)

        @pl.when((me != 1) & (x == 0))
        def _():
            sent(q2.at[0, pl.ds(0, side - 1)], q2l_send)

        @pl.when(me > 1)
        def _():
            sent(q1.at[:, :, pl.ds(0, toks - 2)], q1_send)

        sent(q2, q2_send.at[0])
        sent(q2.at[pl.ds(0, side - 1)], q2_send.at[1])
        sent(o1.at[0, pl.ds(0, side - 1)], o1_send)
        landed(o2.at[pl.ds(0, toks - 2)], o2_recv)

    @pl.when(core == 0)
    def _():
        @pl.when(me != 0)
        def _():
            landed(o2, o2_recv)

        @pl.when(me == 0)
        def _():
            landed(o1l.at[0, pl.ds(0, side - 1)], o1l_recv.at[0])
            landed(o1l.at[1], o1l_recv.at[1])
            merge_late(0, 0, o2.at[0])
            merge_late(1, 0, o2.at[side])
            landed(o2.at[pl.ds(0, toks - 2)], o2_recv)

    tops, dens = [[], []], [[], []]
    for src in range(toks):
        tile = o2[src, 2].astype(F32)
        tile = tile + pltpu.roll(tile, width - 1, 1) + pltpu.roll(tile, width - 2, 1)
        for b in range(2):
            tops[b].append(jnp.broadcast_to(tile[:, 6 * b : 6 * b + 1], (GROUP, width)))
            dens[b].append(jnp.broadcast_to(tile[:, 6 * b + 3 : 6 * b + 4], (GROUP, width)))
    for net in range(2):
        for e in range(2):
            srcs = [net * side + e + 2 * k for k in range(side // 2)]
            for b in range(2):
                top = functools.reduce(jnp.maximum, [tops[b][s] for s in srcs])
                ws = [jnp.exp2((tops[b][s] - top) * exponent) for s in srcs]
                den = sum(w * dens[b][s] for w, s in zip(ws, srcs))
                num = sum(w * o2[s, b].astype(F32) for w, s in zip(ws, srcs))
                head = CLASSES * net + e + 2 * b
                out_ref[head * GROUP : (head + 1) * GROUP, :] = num / den

    @pl.when(me == 1)
    def _():
        sent(o2src.at[:, pl.ds(0, toks - 2)], o2_send)

    @pl.when((core == 1) & (me != 1))
    def _():
        sent(o2src.at[:, pl.ds(0, toks - 1)], o2_send)


def solution(mesh):
    seq = mesh.shape["seq"]
    side = math.isqrt(seq // 2)

    def body(
        queries, span_keys, span_values, cache_keys, cache_values, page_table, page_counts, span_start
    ):
        width = queries.shape[1] // H
        rows = cache_keys.shape[0]
        half = rows // 2
        toks = 2 * side
        piece = toks * GROUP
        table = jnp.asarray(rope_table(width, PAGE))
        units = 16
        vm = pltpu.VMEM
        dma = pltpu.SemaphoreType.DMA
        hbm = pl.BlockSpec(memory_space=pl.ANY)
        smem = pl.BlockSpec(memory_space=pltpu.SMEM)
        vmem = pl.BlockSpec(memory_space=pltpu.VMEM)
        scratch = [
            pltpu.SMEM(page_table.shape, jnp.int32),
            vm(table.shape, F32),
            vm((1, H * width), BF16),
            vm((1, KVH * width), BF16),
            vm((1, KVH * width), BF16),
            vm((rows, KVH * width), BF16),
            vm((H, width), F32),
            vm((rows, width), F32),
            vm((rows, width), F32),
            vm((KVH, 2, half + EXTRA, width), BF16),
            vm((KVH, 2, half, width), BF16),
            vm((units, half + EXTRA, width), BF16),
            vm((units, half, width), BF16),
            vm((units, half + EXTRA, width), BF16),
            vm((units, half, width), BF16),
            vm((width, units * half), BF16),
            vm((units * half, width), BF16),
            vm((3, 16, width), F32),
            vm((16, width), BF16),
            vm((width, width), BF16),
            vm((2, 2, 2, 2, GROUP, width), BF16),
            vm((2, 2, toks, GROUP, width), BF16),
            vm((side, toks, GROUP, width), BF16),
            vm((units * half, 2 * piece), F32),
            vm((units * half, 2 * piece), F32),
            vm((side, width + EXTRA, piece), BF16),
            vm((2, side, width + EXTRA, piece), BF16),
            vm((2, toks, 3, GROUP, width), BF16),
            vm((toks, 3, GROUP, width), BF16),
            vm((2, 2, GROUP, width), BF16),
            vm((GROUP, width), BF16),
            vm((2, GROUP, width), BF16),
            vm((2, side, 2, GROUP, width), BF16),
            vm((3, GROUP, width), BF16),
            dma((7,)),
            dma((2, 2)),
            dma((2, 2)),
            dma((2,)),
            dma(()),
            dma(()),
            dma((2,)),
            dma((2,)),
            dma((side,)),
            dma(()),
            dma((2,)),
            dma(()),
            dma(()),
            dma((2,)),
            dma(()),
            dma(()),
            dma(()),
            dma((2,)),
            pltpu.SemaphoreType.REGULAR,
            pltpu.SemaphoreType.REGULAR,
            pltpu.SemaphoreType.REGULAR,
            pltpu.SemaphoreType.REGULAR,
            vm((16, 2 * piece), F32),
            vm((16, 2 * piece), F32),
            vm((1, 2 * piece), F32),
            vm((1, 2 * piece), F32),
        ]
        out = pl.pallas_call(
            functools.partial(kernel, side),
            out_shape=pltpu.VMEM((H, width), F32),
            in_specs=[smem] * 2 + [hbm] * 7,
            out_specs=pl.BlockSpec(memory_space=pltpu.VMEM),
            scratch_shapes=scratch,
            compiler_params=pltpu.CompilerParams(collective_id=0, has_side_effects=True),
            name="paged_prefix",
        )(
            span_start,
            page_counts,
            page_table,
            table,
            queries,
            span_keys,
            span_values,
            cache_keys,
            cache_values,
        )
        return out.reshape(queries.shape).astype(BF16)

    in_specs = (
        P(("groups", "seq"), None),
        P(("groups", "seq"), None),
        P(("groups", "seq"), None),
        P(("groups", "seq"), None),
        P(("groups", "seq"), None),
        P(("groups", "seq")),
        P(("groups", "seq")),
        P("groups"),
    )
    out_specs = P(("groups", "seq"), None)
    return jax.shard_map(body, mesh=mesh, in_specs=in_specs, out_specs=out_specs, check_vma=False)
```

```python
import functools
import math

import jax
import jax.numpy as jnp
import numpy as np
from jax import lax
from jax.experimental import pallas as pl
from jax.experimental.pallas import tpu as pltpu
from jax.sharding import PartitionSpec as P

H = 64
KVH = 8
PAGE = 16
GROUP = H // KVH
ROPE_BASE = 1000000.0
DEAD = -1e30
FLOOR = -1e29
CLASSES = 4
MESH = pl.DeviceIdType.MESH
F32 = jnp.float32
BF16 = jnp.bfloat16
EXTRA = 8


def rope_table(width, rows):
    half = width // 2
    freq = ROPE_BASE ** (-(np.arange(half, dtype=np.float64) * 2.0 / width))
    turns = np.concatenate([freq, freq]) / (2.0 * np.pi)
    pieces, rest = [], turns
    for _ in range(2):
        scale = 2.0 ** (np.floor(np.log2(rest)) - 7.0)
        part = np.floor(rest / scale) * scale
        pieces.append(part)
        rest = rest - part
    pieces.append(rest)
    sign = np.concatenate([-np.ones(half), np.ones(half)])
    angle = np.arange(rows, dtype=np.float64)[:, None] * np.concatenate([freq, freq])[None, :]
    pad = np.zeros((8 - len(pieces) - 1, width))
    return np.concatenate(
        [np.stack(pieces), sign[None], pad, np.cos(angle), np.sin(angle) * sign[None]]
    ).astype(np.float32)


def cos_sin(position, table_ref):
    def part(k):
        turn = position * table_ref[k : k + 1, :]
        return turn - jnp.floor(turn)

    turn = part(0) + part(1) + part(2)
    turn = turn - jnp.floor(turn + 0.5)
    angle = turn * (2.0 * math.pi)
    return jnp.cos(angle), jnp.sin(angle) * table_ref[3:4, :]


def in_three(value):
    high = value.astype(BF16).astype(F32)
    middle = (value - high).astype(BF16).astype(F32)
    return [high, middle, value - high - middle]


def kernel(
    side,
    start_ref,
    count_ref,
    pages_hbm,
    table_hbm,
    q_hbm,
    sk_hbm,
    sv_hbm,
    k_hbm,
    v_hbm,
    out_ref,
    pages_ref,
    table_ref,
    q_raw,
    sk_raw,
    sv_raw,
    k_raw,
    q_rows,
    cos_ref,
    sin_ref,
    kx,
    vx,
    kall,
    vall,
    kall0,
    vall0,
    vturned,
    kbias,
    rows16,
    kspan,
    vspan,
    qsrc,
    q1,
    q2,
    scores_a,
    scores_b,
    o1src,
    o1,
    o2src,
    o2,
    qlate,
    q2l,
    late_src,
    o1l,
    o1d,
    o2l,
    local_sem,
    kv_send,
    kv_recv,
    on_send,
    q0_sem,
    q1_send,
    q1_recv,
    q2_send,
    q2_recv,
    o1_send,
    o1_recv,
    o2_send,
    o2_recv,
    ql_recv,
    q2l_send,
    q2l_recv,
    o1l_send,
    o1l_recv,
    o1d_recv,
    told,
    told_far,
    side_row,
    side_col,
    span_a,
    span_b,
    top_a,
    top_b,
):
    width = q_rows.shape[1]
    rows = k_hbm.shape[0]
    half_rows = rows // 2
    units = kall.shape[0]
    toks = 2 * side
    piece = toks * GROUP
    me = lax.axis_index("seq")
    core = me % 2
    x = (me // 2) % side
    y = me // (2 * side)
    u = jnp.where(core == 0, x, y)
    v = jnp.where(core == 0, y, x)
    other = 1 - core

    def chip(px, py, pc):
        return ((py % side) * side + px % side) * 2 + pc

    def dev(pu, pv, pc):
        return chip(jnp.where(core == 0, pu, pv), jnp.where(core == 0, pv, pu), pc)

    def remote(src, dst, send, recv, device):
        return pltpu.make_async_remote_copy(
            src_ref=src,
            dst_ref=dst,
            send_sem=send,
            recv_sem=recv,
            device_id={"seq": device},
            device_id_type=MESH,
        )

    def sent(ref, sem):
        remote(ref, ref, sem, sem, chip(x, y, other)).wait_send()

    def landed(ref, sem):
        remote(ref, ref, sem, sem, chip(x, y, other)).wait_recv()

    local = {
        name: pltpu.make_async_copy(src, dst, local_sem.at[k])
        for k, (name, src, dst) in enumerate(
            (
                ("pages", pages_hbm, pages_ref),
                ("table", table_hbm, table_ref),
                ("q", q_hbm, q_raw),
                ("sk", sk_hbm, sk_raw),
                ("sv", sv_hbm, sv_raw),
                ("k", k_hbm, k_raw),
            )
        )
    }
    for copy in local.values():
        copy.start()
    for h in range(KVH):
        for hf in range(2):
            pltpu.make_async_copy(
                v_hbm.at[pl.ds(hf * half_rows, half_rows), pl.ds(h * width, width)],
                vx.at[h, hf],
                local_sem.at[len(local)],
            ).start()

    barrier = pltpu.get_barrier_semaphore()

    def signal(sem, device):
        pl.semaphore_signal(sem, inc=1, device_id={"seq": device}, device_id_type=MESH)

    neighbours = ((1, 0), (side - 1, 0), (0, 1), (0, side - 1))
    line0 = jnp.where(y == 0, x, jnp.where(x == 0, y, 0))
    by_chip0 = (line0 == 1) | (line0 == side - 1)

    @pl.when((core == 0) & by_chip0)
    def _():
        signal(barrier, chip(0, 0, 0))

    @pl.when(core == 1)
    def _():
        signal(barrier, chip(x, y, 0))
        for dx, dy in neighbours:
            signal(barrier, chip(x + dx, y + dy, 0))
        for d in range(1, side):
            signal(barrier, chip(x + d, y, 1))
            signal(barrier, chip(x, y + d, 1))

    for name in ("pages", "table", "q"):
        local[name].wait()
    start = start_ref[0]
    count = count_ref[0]
    own_pos = (start + me).astype(F32)
    own_cos, own_sin = cos_sin(jnp.full((8, width), own_pos, F32), table_ref)
    q_all = q_raw[...].astype(F32)
    for r in range(H):
        q_rows[r : r + 1, :] = q_all[:, r * width : (r + 1) * width]
    for net in range(2):
        for e in range(2):
            for b in range(2):
                head = CLASSES * net + e + 2 * b
                part = q_rows[head * GROUP : (head + 1) * GROUP, :]
                turned = part * own_cos + pltpu.roll(part, width // 2, 1) * own_sin
                qsrc[net, e, b, core] = turned.astype(BF16)

    far_first = [side // 2]
    for step in range(side // 2 - 1, 0, -1):
        far_first += [step, side - step]

    def send_q1(toks_sent, landing, recv):
        for d in far_first:
            for net in range(2):
                place = x if net == 0 else y
                along = (place + d) % side
                remote(
                    qsrc.at[net, along % 2, :, toks_sent],
                    landing(net, place),
                    q1_send,
                    recv.at[net],
                    chip(along, y, 1) if net == 0 else chip(x, along, 1),
                ).start()

    @pl.when(core == 0)
    def _():
        pl.semaphore_wait(barrier, jnp.where(me == 0, 4 + 4 + 1, 4 + 1))
        signal(told, chip(x, y, 1))
        remote(qsrc.at[:, :, :, 0], qsrc.at[:, :, :, 0], q0_sem, q0_sem, chip(x, y, 1)).start()


    def send_cache(which):
        buf = (kx, vx)[which]

        def send_all(net, landing, target):
            def send(head, half, slot, device):
                src = buf.at[head] if half is None else buf.at[head, half]
                dst = landing.at[pl.ds(slot, 2)] if half is None else landing.at[slot]
                remote(src, dst, kv_send.at[which, net], kv_recv.at[which, net], device).start()

            nu, nv = (x, y) if net == 0 else (y, x)

            def at(pu, pv):
                return chip(pu, pv, target) if net == 0 else chip(pv, pu, target)

            base = nu + 2 * nv
            head = CLASSES * net + (base + 1) % CLASSES
            send(head, None, 4 + 2 * core, at(nu + 1, nv))
            head = CLASSES * net + (base + 3) % CLASSES
            send(head, None, 8 + 2 * core, at(nu + side - 1, nv))
            head = CLASSES * net + (base + 2) % CLASSES
            send(head, 0, 12 + core, at(nu, nv + 1))
            send(head, 1, 14 + core, at(nu, nv + side - 1))

        @pl.when(me != 0)
        def _():
            send_all(0, (kall0, vall0)[which], 1)

        @pl.when(me == 0)
        def _():
            send_all(0, (kall, vall)[which], 0)

        send_all(1, (kall, vall)[which], 1)
        own = ((kall, vall)[which], (kall0, vall0)[which])
        head0 = (x + 2 * y) % CLASSES
        head1 = CLASSES + (y + 2 * x) % CLASSES

        @pl.when(core == 0)
        def _():
            own[0][0:2] = buf[head0]
            remote(
                buf.at[head1],
                own[0].at[pl.ds(0, 2)],
                kv_send.at[which, 1],
                kv_recv.at[which, 1],
                chip(x, y, 1),
            ).start()

        @pl.when(core == 1)
        def _():
            own[0][2:4] = buf[head1]
            own[1][2:4] = buf[head0]

    pltpu.make_async_copy(vx, vx, local_sem.at[len(local)]).wait()

    @pl.when(core == 0)
    def _():
        send_cache(1)

    tile_row = lax.broadcasted_iota(jnp.int32, (EXTRA, width), 0)
    row16 = lax.broadcasted_iota(jnp.int32, (16, width), 0)
    lane = lax.broadcasted_iota(jnp.int32, (1, width), 1)
    half_pages = half_rows // PAGE
    biases = []
    for hf in range(2):
        page = jnp.zeros((1, width), jnp.int32)
        for j in range(half_pages):
            page = jnp.where(lane // PAGE == j, pages_ref[hf * half_pages + j], page)
        slot = hf * half_pages + lane // PAGE
        usable = (slot < count) & (page * PAGE + lane % PAGE < start)
        biases.append(jnp.where(usable, 0.0, DEAD).astype(F32))
    page_pos = jnp.zeros((16, width), jnp.int32)
    for j in range(rows // PAGE):
        page_pos = jnp.where(row16 == j, pages_ref[j] * PAGE, page_pos)
    page_cos, page_sin = cos_sin(page_pos.astype(F32), table_ref)
    row_cos = table_ref[8 : 8 + PAGE, :]
    row_sin = table_ref[8 + PAGE : 8 + 2 * PAGE, :]
    for j in range(rows // PAGE):
        pc_, ps_ = page_cos[j : j + 1, :], page_sin[j : j + 1, :]
        cos_ref[j * PAGE : (j + 1) * PAGE, :] = pc_ * row_cos - ps_ * row_sin
        sin_ref[j * PAGE : (j + 1) * PAGE, :] = ps_ * row_cos + pc_ * row_sin
    for name in ("sk", "sv", "k"):
        local[name].wait()
    sk_all = sk_raw[...].astype(F32)
    sv_all = sv_raw[...].astype(F32)
    for h in range(KVH):
        span = jnp.broadcast_to(sk_all[:, h * width : (h + 1) * width], (8, width))
        span = span * own_cos + pltpu.roll(span, width // 2, 1) * own_sin
        span = jnp.broadcast_to(span[0:1, :], (EXTRA, width))
        value = jnp.broadcast_to(sv_all[:, h * width : (h + 1) * width], (EXTRA, width))
        for hf in range(2):
            tile = jnp.where(tile_row == 0, span, jnp.where(tile_row == 2, value, 0.0))
            tile = jnp.where(tile_row == 1, biases[hf], tile)
            kx[h, hf, half_rows : half_rows + EXTRA, :] = tile.astype(BF16)

    @pl.loop(0, KVH // 2)
    def _(step):
        for h in (2 * step, 2 * step + 1):
            cols = pl.ds(pl.multiple_of(h * width, width), width)
            for hf in range(2):
                span_rows = slice(hf * half_rows, (hf + 1) * half_rows)
                part = k_raw[span_rows, cols].astype(F32)
                turned = part * cos_ref[span_rows, :]
                turned = turned + pltpu.roll(part, width // 2, 1) * sin_ref[span_rows, :]
                kx[h, hf, 0:half_rows, :] = turned.astype(BF16)

    @pl.when(core == 0)
    def _():
        send_cache(0)
        pl.semaphore_wait(told_far, 1)

        @pl.when(me != 0)
        def _():
            for d in far_first:
                signal(side_row, chip(x + d, y, 1))
                signal(side_col, chip(x, y + d, 1))

    @pl.when(core == 1)
    def _():
        @pl.when(me == 1)
        def _():
            pl.semaphore_wait(barrier, 2 * (side - 1))
            send_q1(1, lambda net, place: q1.at[net, :, 2 * place + 1], q1_recv)
            send_cache(1)
            send_cache(0)
            pl.semaphore_wait(told, 1)
            signal(told_far, chip(x, y, 0))
            landed(qsrc.at[:, :, :, 0], q0_sem)
            send_q1(0, lambda net, place: qlate.at[net], ql_recv)
            qlate[0] = qsrc[0, 0, :, 0]
            qlate[1] = qsrc[1, 0, :, 0]

        @pl.when(me > 1)
        def _():
            pl.semaphore_wait(told, 1)
            send_cache(1)
            pl.semaphore_wait(barrier, 2 * (side - 1))
            signal(told_far, chip(x, y, 0))
            landed(qsrc.at[:, :, :, 0], q0_sem)
            send_q1(pl.ds(0, 2), lambda net, place: q1.at[net, :, pl.ds(2 * place, 2)], q1_recv)
            send_cache(0)

    remote_units = units - 2
    near_units = units - 4

    @pl.when(core == 1)
    def _():
        for net, place in ((0, x), (1, y)):
            for b in range(2):
                q1[net, b, 2 * place + 1] = qsrc[net, place % 2, b, 1]

        @pl.when(me > 1)
        def _():
            for net, place in ((0, x), (1, y)):
                for b in range(2):
                    q1[net, b, 2 * place] = qsrc[net, place % 2, b, 0]

        for net, across in ((0, y), (1, x)):

            @pl.when(across == 0)
            def _(net=net):
                for b in range(2):
                    q1[net, b, 0] = jnp.zeros((GROUP, width), BF16)

        pl.semaphore_wait(side_col, jnp.where((x == 0) & (y != 0), side - 2, side - 1))

        def send_q2(net, pv):
            nu, nv = (x, y) if net == 0 else (y, x)
            remote(
                q1.at[net, (nu // 2 + pv) % 2],
                q2.at[nv],
                q2_send.at[net],
                q2_recv.at[nv],
                chip(x, pv, 0) if net == 0 else chip(pv, y, 1),
            ).start()

        def all_in(net, along, across):
            short = (across == 0) & (along != 0)

            @pl.when(short)
            def _():
                landed(q1.at[net, :, pl.ds(0, toks - 3)], q1_recv.at[net])

            @pl.when(jnp.logical_not(short))
            def _():
                landed(q1.at[net, :, pl.ds(0, toks - 2)], q1_recv.at[net])

        all_in(0, x, y)
        for d in far_first:
            pv = (y + d) % side

            @pl.when((x != 0) | (pv != 0))
            def _(pv=pv):
                send_q2(0, pv)

        send_q2(0, y)
        all_in(1, y, x)
        for d in far_first:
            send_q2(1, (x + d) % side)
        q2[x] = q1[1, (y // 2 + x) % 2]

        def hand_on():
            cases = [(jnp.logical_not(by_chip0), near_units, ((2, units),))]
            for here, slots in (
                ((y == 0) & (x == 1), (4, 6)),
                ((y == 0) & (x == side - 1), (8, 10)),
                ((x == 0) & (y == 1), (12, 13)),
                ((x == 0) & (y == side - 1), (14, 15)),
            ):
                spans = ((2, slots[0]), (slots[1], units))
                cases.append((here, near_units - slots[1] + slots[0], spans))
            for which, (src, dst) in ((1, (vall0, vall)), (0, (kall0, kall))):
                for here, amount, spans in cases:

                    @pl.when(here)
                    def _(which=which, src=src, dst=dst, amount=amount, spans=spans):
                        landed(src.at[pl.ds(0, amount)], kv_recv.at[which, 0])
                        for first, end in spans:
                            span = pl.ds(first, end - first)
                            remote(
                                src.at[span],
                                dst.at[span],
                                on_send.at[which],
                                kv_recv.at[which, 0],
                                chip(x, y, 0),
                            ).start()

        hand_on()

        @pl.when(y == 0)
        def _():
            @pl.when(x != 0)
            def _():
                landed(qlate.at[0], ql_recv.at[0])

            for d in far_first + [0]:
                remote(
                    qlate.at[0, (x // 2 + d) % 2], q2l, q2l_send, q2l_recv, chip(x, d, 0)
                ).start()

        @pl.when(x == 0)
        def _():
            @pl.when(y != 0)
            def _():
                landed(qlate.at[1], ql_recv.at[1])
                send_q2(0, 0)

            for d in far_first:
                remote(
                    qlate.at[1, (y // 2 + d) % 2], q2l, q2l_send, q2l_recv, chip(d, y, 1)
                ).start()
            q2l[...] = qlate[1, (y // 2) % 2]

        landed(vall.at[pl.ds(0, remote_units)], kv_recv.at[1, 1])

    @pl.when(core == 0)
    def _():
        landed(vall.at[pl.ds(0, remote_units)], kv_recv.at[1, 0])

    for unit in range(units):
        vturned[:, unit * half_rows : (unit + 1) * half_rows] = vall[unit].T

    @pl.when(core == 1)
    def _():
        landed(kall.at[pl.ds(0, remote_units)], kv_recv.at[0, 1])

    @pl.when(core == 0)
    def _():
        landed(kall.at[pl.ds(0, remote_units)], kv_recv.at[0, 0])

    span_units = [0, 2, 4, 6, 8, 10, 12, 13]
    span_toks = [
        dev(pu, pv, pc)
        for pu, pv in ((u, v), (u + side - 1, v), (u + 1, v), (u, v + side - 1))
        for pc in range(2)
    ]
    rows16[...] = jnp.zeros_like(rows16)
    for unit in range(units):
        tile = kall[unit, half_rows : half_rows + EXTRA, :].astype(F32)
        rows16[0, unit : unit + 1, :] = tile[1:2, :]
        if unit in span_units:
            k = span_units.index(unit)
            rows16[1, k : k + 1, :] = tile[0:1, :]
            rows16[2, k : k + 1, :] = tile[2:3, :]
    zeros = jnp.zeros((width - 16, width), F32)
    bias_cols = jnp.concatenate([rows16[0], zeros]).T
    for unit in range(units):
        turned = bias_cols if unit == 0 else pltpu.roll(bias_cols, width - unit, 1)
        kbias[unit * half_rows : (unit + 1) * half_rows, :] = turned.astype(BF16)
    kspan[...] = rows16[1].astype(BF16)
    vspan[...] = jnp.concatenate([rows16[2], zeros]).T.astype(BF16)
    span_tok = jnp.full((16, piece), 1 << 20, jnp.int32)
    for k, tok in enumerate(span_toks):
        span_tok = jnp.where(row16 == k, tok, span_tok)

    exponent = width**-0.5 / math.log(2.0)
    contract = (((1,), (1,)), ((), ()))
    chunk = 2 * half_rows
    cols = 2 * piece

    def send_o1(pv):
        remote(
            o1src.at[pv], o1.at[core, v], o1_send, o1_recv.at[core], dev(u, pv, 1)
        ).start()

    col_slot = lax.broadcasted_iota(jnp.int32, (1, piece), 1) // GROUP
    tok_along = jnp.where(core == 0, 2, 2 * side)
    tok_across = jnp.where(core == 0, 2 * side, 2)
    col_tok = (col_slot // 2) * tok_along + col_slot % 2
    one_hot = jnp.where(lax.broadcasted_iota(jnp.int32, (cols, width), 1) == 0, 1.0, 0.0).astype(BF16)

    scores, span_scores, tops = (scores_a, scores_b), (span_a, span_b), (top_a, top_b)
    half_units = units // 2
    half_cache = half_units * half_rows
    always = me < 4 * side * side

    def score(query, live, buf):
        n = query.shape[0]
        query = jnp.concatenate([query, one_hot[:n]], axis=1)
        s = lax.dot_general(kspan[...], query[:, :width], contract, preferred_element_type=F32)
        s_span = jnp.where(live, s, DEAD)
        span_scores[buf][:, :n] = s_span
        best = jnp.maximum(s_span[0:8], s_span[8:16])
        for p in range(2):
            span = slice(p * half_cache, (p + 1) * half_cache)
            keys = kall[p * half_units : (p + 1) * half_units, 0:half_rows, :]
            keys = jnp.concatenate([keys.reshape(half_cache, width), kbias[span, :]], axis=1)
            s = lax.dot_general(keys, query, contract, preferred_element_type=F32)
            scores[buf][span, :n] = s
            best = jnp.maximum(best, jnp.max(s.reshape(-1, 8, n), axis=0))
        tops[buf][:, :n] = jnp.maximum(jnp.max(best, axis=0, keepdims=True), FLOOR)

    def weigh(buf, n):
        top = tops[buf][:, :n]
        w = jnp.exp2((span_scores[buf][:, :n] - top) * exponent)
        total = w[0:8] + w[8:16]
        w = jnp.concatenate([w, jnp.zeros((width - 16, n), F32)])
        nums = [jnp.dot(vspan[...], w.astype(BF16), preferred_element_type=F32), None]
        for k in range(units // 2):
            w = jnp.exp2((scores[buf][k * chunk : (k + 1) * chunk, :n] - top) * exponent)
            total = total + jnp.sum(w.reshape(chunk // 8, 8, n), axis=0)
            part = jnp.dot(
                vturned[:, k * chunk : (k + 1) * chunk],
                w.astype(BF16),
                preferred_element_type=F32,
            )
            nums[k % 2] = part if nums[k % 2] is None else nums[k % 2] + part
        den = jnp.sum(total, axis=0, keepdims=True)
        stat = jnp.concatenate(in_three(top) + in_three(den) + [jnp.zeros((EXTRA - 6, n), F32)])
        return nums[0] + nums[1], stat

    def score_pair(pvs, buf):
        query = jnp.concatenate(
            [q2[pv].astype(F32).reshape(piece, width).astype(BF16) for pv in pvs]
        )
        live = jnp.concatenate([span_tok <= col_tok + pv * tok_across for pv in pvs], axis=1)
        score(query, live, buf)

    def weigh_pair(pvs, buf):
        num, stat = weigh(buf, cols)
        for k, pv in enumerate(pvs):
            lanes = slice(k * piece, (k + 1) * piece)
            o1src[pv, 0:width, :] = num[:, lanes].astype(BF16)
            o1src[pv, width : width + EXTRA, :] = stat[:, lanes].astype(BF16)

    def pair(k):
        late, away, half = (me <= 1) | by_chip0, jnp.where(v < side // 2, -1, 1), side // 2
        a, b = [(0, 1), (4, 3), (-3, 2), (-2, -1)][k]
        return [
            jnp.where(late, (side - k) % side, (v + away * a + side) % side),
            jnp.where(late, k + 1, (v + away * b + side) % side),
        ]

    def queries_in(pvs):
        for pv in pvs:

            @pl.when((pv != v) | (core == 0))
            def _(pv=pv):
                landed(q2.at[pv], q2_recv.at[pv])

    def results_out(pvs):
        for pv in pvs:

            @pl.when((pv != v) | (core == 0))
            def _(pv=pv):
                send_o1(pv)

            @pl.when((pv == v) & (core == 1))
            def _(pv=pv):
                o1[1, pv] = o1src[pv]

    pairs = side // 2
    queries_in(pair(0))
    score_pair(pair(0), 0)

    for k in range(pairs - 1):
        queries_in(pair(k + 1))

        @pl.when(always)
        def _(k=k):
            score_pair(pair(k + 1), (k + 1) % 2)
            weigh_pair(pair(k), k % 2)

        results_out(pair(k))

    @pl.when((core == 0) | (x != 0))
    def _():
        landed(q2l, q2l_recv)

    @pl.when(always)
    def _():
        query = jnp.concatenate([q2l[...].astype(F32), jnp.zeros((piece - GROUP, width), F32)])
        score(query.astype(BF16), span_tok <= 0, pairs % 2)
        weigh_pair(pair(pairs - 1), (pairs - 1) % 2)

    results_out(pair(pairs - 1))

    @pl.when(always)
    def _():
        num, stat = weigh(pairs % 2, piece)
        late_src[0] = num.T[0:GROUP].astype(BF16)
        wide = jnp.concatenate([stat, jnp.zeros((width - EXTRA, piece), F32)])
        late_src[1] = wide.T[0:GROUP].astype(BF16)

    far_lines = range(3, side - 2)

    def is_far(n):
        return (n >= far_lines[0]) & (n <= far_lines[-1])

    late_slot = jnp.where(core == 0, y, x)
    late_line = jnp.where(core == 0, x, y)
    late_far = is_far(late_line)
    late_to = jnp.where(
        core == 0,
        jnp.where(x == 0, 0, chip(x, 0, 1)),
        jnp.where(y == 0, 0, chip(0, y, 1)),
    )
    late_stays = (me == 0) | ((core == 1) & (x == 0) & (y != 0) & jnp.logical_not(late_far))

    @pl.when(late_far)
    def _():
        place = o1d.at[core, jnp.clip(late_line - far_lines[0], 0, len(far_lines) - 1), late_slot]
        remote(late_src, place, o1l_send, o1d_recv, chip(0, 0, 0)).start()

    @pl.when(jnp.logical_not(late_stays | late_far))
    def _():
        remote(late_src, o1l.at[core, late_slot], o1l_send, o1l_recv.at[core], late_to).start()

    @pl.when(late_stays)
    def _():
        o1l[core, late_slot] = late_src[...]

    def merge_late(parts, nu, out):
        stat = jnp.zeros((GROUP, width), F32)
        for b in range(2):
            vs = [(nu // 2 + b) % 2 + 2 * k for k in range(side // 2)]
            tops, dens = [], []
            for pv in vs:
                tile = parts[pv, 1].astype(F32)
                tile = tile + pltpu.roll(tile, width - 1, 1) + pltpu.roll(tile, width - 2, 1)
                tops.append(jnp.broadcast_to(tile[:, 0:1], (GROUP, width)))
                dens.append(jnp.broadcast_to(tile[:, 3:4], (GROUP, width)))
            top = functools.reduce(jnp.maximum, tops)
            ws = [jnp.exp2((t - top) * exponent) for t in tops]
            den = sum(w * d for w, d in zip(ws, dens))
            num = sum(w * parts[pv, 0].astype(F32) for w, pv in zip(ws, vs))
            out[b] = num.astype(BF16)
            for k, value in enumerate(in_three(top) + in_three(den)):
                stat = jnp.where(lane == 6 * b + k, value, stat)
        out[2] = stat.astype(BF16)

    def cache_gone():
        for which, buf in enumerate((kall, vall)):
            sent(buf.at[pl.ds(0, near_units // 2)], kv_send.at[which, 0])

            @pl.when(core == 0)
            def _(which=which, buf=buf):
                sent(buf.at[pl.ds(0, near_units // 2 + 2)], kv_send.at[which, 1])

            @pl.when(core == 1)
            def _(which=which, buf=buf):
                sent(buf.at[pl.ds(0, near_units // 2)], kv_send.at[which, 1])
                for here, amount in (
                    (line0 * by_chip0 == 0, remote_units),
                    ((y == 0) & by_chip0, remote_units - 2),
                    ((x == 0) & by_chip0, remote_units - 1),
                ):

                    @pl.when(here)
                    def _(which=which, buf=buf, amount=amount):
                        sent(buf.at[pl.ds(0, amount)], on_send.at[which])

        @pl.when(jnp.logical_not(late_stays))
        def _():
            sent(late_src, o1l_send)

    @pl.when(core == 0)
    def _():
        cache_gone()

        sent(qsrc.at[:, :, :, 0], q0_sem)
        sent(o1.at[0], o1_send)

    @pl.when(core == 1)
    def _():
        pl.semaphore_wait(side_row, jnp.where((y == 0) & (x != 0), side - 2, side - 1))
        for step in range(2):
            net = jnp.where(jnp.minimum(y, side - y) <= jnp.minimum(x, side - x), step, 1 - step)
            nu = jnp.where(net == 0, x, y)
            across = jnp.where(net == 0, y, x)
            line = net * side + nu

            def owner(along, pc, net=net):
                return chip(jnp.where(net == 0, along, x), jnp.where(net == 0, y, along), pc)

            def send_o2(src, device, net=net, line=line):
                remote(src, o2.at[line], o2_send.at[net], o2_recv, device).start()

            @pl.when(net == 0)
            def _():
                landed(o1.at[0], o1_recv.at[0])

            @pl.when(net == 1)
            def _():
                landed(o1.at[1, pl.ds(0, side - 1)], o1_recv.at[1])

            stats = []
            for b in range(2):
                vs = [(nu // 2 + b) % 2 + 2 * k for k in range(side // 2)]
                tiles = [o1[net, pv, width : width + EXTRA, :].astype(F32) for pv in vs]
                tops = [t[0:1] + t[1:2] + t[2:3] for t in tiles]
                dens = [t[3:4] + t[4:5] + t[5:6] for t in tiles]
                top = functools.reduce(jnp.maximum, tops)
                ws = [jnp.exp2((t - top) * exponent) for t in tops]
                stats += in_three(top) + in_three(sum(w * d for w, d in zip(ws, dens)))
                total = None
                for w, pv in zip(ws, vs):
                    part = o1[net, pv, 0:width, :].astype(F32) * w
                    total = part if total is None else total + part
                o2src[net, :, b] = total.T.reshape(toks, GROUP, width).astype(BF16)
            stat = jnp.concatenate(stats + [jnp.zeros((width - len(stats), piece), F32)]).T
            o2src[net, :, 2] = stat.reshape(toks, GROUP, width).astype(BF16)
            for along in [0] + far_first[::-1]:

                @pl.when(nu != along)
                def _(along=along):
                    send_o2(o2src.at[net, 2 * along + 1], owner(along, 1))

                if along:
                    send_o2(o2src.at[net, 2 * along], owner(along, 0))

            @pl.when(across != 0)
            def _():
                send_o2(o2src.at[net, 0], owner(0, 0))

            o2[line] = o2src[net, 2 * nu + 1]

            @pl.when((across == 0) & (me != 1) & jnp.logical_not(is_far(nu)))
            def _(net=net, nu=nu):
                @pl.when(net == 0)
                def _():
                    landed(o1l.at[0], o1l_recv.at[0])

                @pl.when(net == 1)
                def _():
                    landed(o1l.at[1, pl.ds(0, side - 1)], o1l_recv.at[1])

                merge_late(o1l.at[net], nu, o2l)
                send_o2(o2l, owner(0, 0))

        cache_gone()

        @pl.when(me == 1)
        def _():
            sent(q1.at[:, :, pl.ds(0, toks - 2)], q1_send)
            sent(q2.at[0, pl.ds(0, toks - 1)], q2l_send)

        @pl.when((me != 1) & (y == 0))
        def _():
            sent(q2.at[0, pl.ds(0, side)], q2l_send)

        @pl.when((me != 1) & (x == 0))
        def _():
            sent(q2.at[0, pl.ds(0, side - 1)], q2l_send)

        @pl.when(me > 1)
        def _():
            sent(q1.at[:, :, pl.ds(0, toks - 2)], q1_send)

        sent(q2, q2_send.at[0])
        sent(q2.at[pl.ds(0, side - 1)], q2_send.at[1])
        sent(o1.at[0, pl.ds(0, side - 1)], o1_send)
        landed(o2.at[pl.ds(0, toks - 2)], o2_recv)

    @pl.when(core == 0)
    def _():
        @pl.when(me != 0)
        def _():
            landed(o2, o2_recv)

        @pl.when(me == 0)
        def _():
            landed(o1l.at[0, pl.ds(0, side - 1)], o1l_recv.at[0])
            landed(o1l.at[1], o1l_recv.at[1])
            merge_late(o1l.at[0], 0, o2.at[0])
            merge_late(o1l.at[1], 0, o2.at[side])
            landed(o1d, o1d_recv)
            for net in range(2):
                for k, line in enumerate(far_lines):
                    merge_late(o1d.at[net, k], line, o2.at[net * side + line])
            landed(o2.at[pl.ds(0, toks - 2 - 2 * len(far_lines))], o2_recv)

    tops, dens = [[], []], [[], []]
    for src in range(toks):
        tile = o2[src, 2].astype(F32)
        tile = tile + pltpu.roll(tile, width - 1, 1) + pltpu.roll(tile, width - 2, 1)
        for b in range(2):
            tops[b].append(jnp.broadcast_to(tile[:, 6 * b : 6 * b + 1], (GROUP, width)))
            dens[b].append(jnp.broadcast_to(tile[:, 6 * b + 3 : 6 * b + 4], (GROUP, width)))
    for net in range(2):
        for e in range(2):
            srcs = [net * side + e + 2 * k for k in range(side // 2)]
            for b in range(2):
                top = functools.reduce(jnp.maximum, [tops[b][s] for s in srcs])
                ws = [jnp.exp2((tops[b][s] - top) * exponent) for s in srcs]
                den = sum(w * dens[b][s] for w, s in zip(ws, srcs))
                num = sum(w * o2[s, b].astype(F32) for w, s in zip(ws, srcs))
                head = CLASSES * net + e + 2 * b
                out_ref[head * GROUP : (head + 1) * GROUP, :] = num / den

    @pl.when(core == 1)
    def _():
        for net, nu, across in ((0, x, y), (1, y, x)):
            fewer = (across == 0) & ((me == 1) | is_far(nu))

            @pl.when(fewer)
            def _(net=net):
                sent(o2src.at[net, pl.ds(0, toks - 2)], o2_send.at[net])

            @pl.when(jnp.logical_not(fewer))
            def _(net=net):
                sent(o2src.at[net, pl.ds(0, toks - 1)], o2_send.at[net])


def solution(mesh):
    seq = mesh.shape["seq"]
    side = math.isqrt(seq // 2)

    def body(
        queries, span_keys, span_values, cache_keys, cache_values, page_table, page_counts, span_start
    ):
        width = queries.shape[1] // H
        rows = cache_keys.shape[0]
        half = rows // 2
        toks = 2 * side
        piece = toks * GROUP
        table = jnp.asarray(rope_table(width, PAGE))
        units = 16
        vm = pltpu.VMEM
        dma = pltpu.SemaphoreType.DMA
        hbm = pl.BlockSpec(memory_space=pl.ANY)
        smem = pl.BlockSpec(memory_space=pltpu.SMEM)
        vmem = pl.BlockSpec(memory_space=pltpu.VMEM)
        scratch = [
            pltpu.SMEM(page_table.shape, jnp.int32),
            vm(table.shape, F32),
            vm((1, H * width), BF16),
            vm((1, KVH * width), BF16),
            vm((1, KVH * width), BF16),
            vm((rows, KVH * width), BF16),
            vm((H, width), F32),
            vm((rows, width), F32),
            vm((rows, width), F32),
            vm((KVH, 2, half + EXTRA, width), BF16),
            vm((KVH, 2, half, width), BF16),
            vm((units, half + EXTRA, width), BF16),
            vm((units, half, width), BF16),
            vm((units, half + EXTRA, width), BF16),
            vm((units, half, width), BF16),
            vm((width, units * half), BF16),
            vm((units * half, width), BF16),
            vm((3, 16, width), F32),
            vm((16, width), BF16),
            vm((width, width), BF16),
            vm((2, 2, 2, 2, GROUP, width), BF16),
            vm((2, 2, toks, GROUP, width), BF16),
            vm((side, toks, GROUP, width), BF16),
            vm((units * half, 2 * piece), F32),
            vm((units * half, 2 * piece), F32),
            vm((side, width + EXTRA, piece), BF16),
            vm((2, side, width + EXTRA, piece), BF16),
            vm((2, toks, 3, GROUP, width), BF16),
            vm((toks, 3, GROUP, width), BF16),
            vm((2, 2, GROUP, width), BF16),
            vm((GROUP, width), BF16),
            vm((2, GROUP, width), BF16),
            vm((2, side, 2, GROUP, width), BF16),
            vm((2, side - 5, side, 2, GROUP, width), BF16),
            vm((3, GROUP, width), BF16),
            dma((7,)),
            dma((2, 2)),
            dma((2, 2)),
            dma((2,)),
            dma(()),
            dma(()),
            dma((2,)),
            dma((2,)),
            dma((side,)),
            dma(()),
            dma((2,)),
            dma((2,)),
            dma(()),
            dma((2,)),
            dma(()),
            dma(()),
            dma(()),
            dma((2,)),
            dma(()),
            pltpu.SemaphoreType.REGULAR,
            pltpu.SemaphoreType.REGULAR,
            pltpu.SemaphoreType.REGULAR,
            pltpu.SemaphoreType.REGULAR,
            vm((16, 2 * piece), F32),
            vm((16, 2 * piece), F32),
            vm((1, 2 * piece), F32),
            vm((1, 2 * piece), F32),
        ]
        out = pl.pallas_call(
            functools.partial(kernel, side),
            out_shape=pltpu.VMEM((H, width), F32),
            in_specs=[smem] * 2 + [hbm] * 7,
            out_specs=pl.BlockSpec(memory_space=pltpu.VMEM),
            scratch_shapes=scratch,
            compiler_params=pltpu.CompilerParams(collective_id=0, has_side_effects=True),
            name="paged_prefix",
        )(
            span_start,
            page_counts,
            page_table,
            table,
            queries,
            span_keys,
            span_values,
            cache_keys,
            cache_values,
        )
        return out.reshape(queries.shape).astype(BF16)

    in_specs = (
        P(("groups", "seq"), None),
        P(("groups", "seq"), None),
        P(("groups", "seq"), None),
        P(("groups", "seq"), None),
        P(("groups", "seq"), None),
        P(("groups", "seq")),
        P(("groups", "seq")),
        P("groups"),
    )
    out_specs = P(("groups", "seq"), None)
    return jax.shard_map(body, mesh=mesh, in_specs=in_specs, out_specs=out_specs, check_vma=False)
```

```python
import functools
import math

import jax
import jax.numpy as jnp
import numpy as np
from jax import lax
from jax.experimental import pallas as pl
from jax.experimental.pallas import tpu as pltpu
from jax.sharding import PartitionSpec as P

H = 64
KVH = 8
PAGE = 16
GROUP = H // KVH
ROPE_BASE = 1000000.0
DEAD = -1e30
FLOOR = -1e29
CLASSES = 4
MESH = pl.DeviceIdType.MESH
F32 = jnp.float32
BF16 = jnp.bfloat16
EXTRA = 8


def rope_table(width, rows):
    half = width // 2
    freq = ROPE_BASE ** (-(np.arange(half, dtype=np.float64) * 2.0 / width))
    turns = np.concatenate([freq, freq]) / (2.0 * np.pi)
    pieces, rest = [], turns
    for _ in range(2):
        scale = 2.0 ** (np.floor(np.log2(rest)) - 7.0)
        part = np.floor(rest / scale) * scale
        pieces.append(part)
        rest = rest - part
    pieces.append(rest)
    sign = np.concatenate([-np.ones(half), np.ones(half)])
    angle = np.arange(rows, dtype=np.float64)[:, None] * np.concatenate([freq, freq])[None, :]
    pad = np.zeros((8 - len(pieces) - 1, width))
    return np.concatenate(
        [np.stack(pieces), sign[None], pad, np.cos(angle), np.sin(angle) * sign[None]]
    ).astype(np.float32)


def cos_sin(position, table_ref):
    def part(k):
        turn = position * table_ref[k : k + 1, :]
        return turn - jnp.floor(turn)

    turn = part(0) + part(1) + part(2)
    turn = turn - jnp.floor(turn + 0.5)
    angle = turn * (2.0 * math.pi)
    return jnp.cos(angle), jnp.sin(angle) * table_ref[3:4, :]


def in_three(value):
    high = value.astype(BF16).astype(F32)
    middle = (value - high).astype(BF16).astype(F32)
    return [high, middle, value - high - middle]


def kernel(
    side,
    start_ref,
    count_ref,
    pages_hbm,
    table_hbm,
    q_hbm,
    sk_hbm,
    sv_hbm,
    k_hbm,
    v_hbm,
    out_ref,
    pages_ref,
    table_ref,
    q_raw,
    sk_raw,
    sv_raw,
    k_raw,
    q_rows,
    cos_ref,
    sin_ref,
    kx,
    vx,
    kall,
    vall,
    kall0,
    vall0,
    vturned,
    kbias,
    rows16,
    kspan,
    vspan,
    qsrc,
    q1,
    q2,
    scores_a,
    scores_b,
    o1src,
    o1,
    o2src,
    o2,
    qlate,
    q2l,
    late_src,
    o1l,
    o1d,
    o2l,
    local_sem,
    kv_send,
    kv_recv,
    on_send,
    q0_sem,
    q1_send,
    q1_recv,
    q2_send,
    q2_recv,
    o1_send,
    o1_recv,
    o2_send,
    o2_recv,
    ql_recv,
    q2l_send,
    q2l_recv,
    o1l_send,
    o1l_recv,
    o1d_recv,
    told,
    told_far,
    side_row,
    side_col,
    span_a,
    span_b,
    top_a,
    top_b,
):
    width = q_rows.shape[1]
    rows = k_hbm.shape[0]
    half_rows = rows // 2
    units = kall.shape[0]
    toks = 2 * side
    piece = toks * GROUP
    me = lax.axis_index("seq")
    core = me % 2
    x = (me // 2) % side
    y = me // (2 * side)
    u = jnp.where(core == 0, x, y)
    v = jnp.where(core == 0, y, x)
    other = 1 - core

    def chip(px, py, pc):
        return ((py % side) * side + px % side) * 2 + pc

    def dev(pu, pv, pc):
        return chip(jnp.where(core == 0, pu, pv), jnp.where(core == 0, pv, pu), pc)

    def remote(src, dst, send, recv, device):
        return pltpu.make_async_remote_copy(
            src_ref=src,
            dst_ref=dst,
            send_sem=send,
            recv_sem=recv,
            device_id={"seq": device},
            device_id_type=MESH,
        )

    def sent(ref, sem):
        remote(ref, ref, sem, sem, chip(x, y, other)).wait_send()

    def landed(ref, sem):
        remote(ref, ref, sem, sem, chip(x, y, other)).wait_recv()

    local = {
        name: pltpu.make_async_copy(src, dst, local_sem.at[k // 3])
        for k, (name, src, dst) in enumerate(
            (
                ("pages", pages_hbm, pages_ref),
                ("table", table_hbm, table_ref),
                ("q", q_hbm, q_raw),
                ("sk", sk_hbm, sk_raw),
                ("sv", sv_hbm, sv_raw),
                ("k", k_hbm, k_raw),
            )
        )
    }
    for copy in local.values():
        copy.start()
    for h in range(KVH):
        for hf in range(2):
            pltpu.make_async_copy(
                v_hbm.at[pl.ds(hf * half_rows, half_rows), pl.ds(h * width, width)],
                vx.at[h, hf],
                local_sem.at[2],
            ).start()

    barrier = pltpu.get_barrier_semaphore()

    def signal(sem, device):
        pl.semaphore_signal(sem, inc=1, device_id={"seq": device}, device_id_type=MESH)

    neighbours = ((1, 0), (side - 1, 0), (0, 1), (0, side - 1))
    line0 = jnp.where(y == 0, x, jnp.where(x == 0, y, 0))
    by_chip0 = (line0 == 1) | (line0 == side - 1)

    @pl.when((core == 0) & by_chip0)
    def _():
        signal(barrier, chip(0, 0, 0))

    @pl.when(core == 1)
    def _():
        signal(barrier, chip(x, y, 0))
        for dx, dy in neighbours:
            signal(barrier, chip(x + dx, y + dy, 0))
        for d in range(1, side):
            signal(barrier, chip(x + d, y, 1))
            signal(barrier, chip(x, y + d, 1))

    for name in ("pages", "table", "q"):
        local[name].wait()
    start = start_ref[0]
    count = count_ref[0]
    own_pos = (start + me).astype(F32)
    own_cos, own_sin = cos_sin(jnp.full((8, width), own_pos, F32), table_ref)
    q_all = q_raw[...].astype(F32)
    for r in range(H):
        q_rows[r : r + 1, :] = q_all[:, r * width : (r + 1) * width]
    for net in range(2):
        for e in range(2):
            for b in range(2):
                head = CLASSES * net + e + 2 * b
                part = q_rows[head * GROUP : (head + 1) * GROUP, :]
                turned = part * own_cos + pltpu.roll(part, width // 2, 1) * own_sin
                qsrc[net, e, b, core] = turned.astype(BF16)

    far_first = [side // 2]
    for step in range(side // 2 - 1, 0, -1):
        far_first += [step, side - step]

    def send_q1(toks_sent, landing, recv):
        for d in far_first:
            for net in range(2):
                place = x if net == 0 else y
                along = (place + d) % side
                remote(
                    qsrc.at[net, along % 2, :, toks_sent],
                    landing(net, place),
                    q1_send,
                    recv.at[net],
                    chip(along, y, 1) if net == 0 else chip(x, along, 1),
                ).start()

    @pl.when(core == 0)
    def _():
        pl.semaphore_wait(barrier, jnp.where(me == 0, 4 + 4 + 1, 4 + 1))
        signal(told, chip(x, y, 1))
        remote(qsrc.at[:, :, :, 0], qsrc.at[:, :, :, 0], q0_sem, q0_sem, chip(x, y, 1)).start()


    def send_cache(which):
        buf = (kx, vx)[which]

        def send_all(net, landing, target):
            def send(head, half, slot, device):
                src = buf.at[head] if half is None else buf.at[head, half]
                dst = landing.at[pl.ds(slot, 2)] if half is None else landing.at[slot]
                remote(src, dst, kv_send.at[which], kv_recv.at[which, net], device).start()

            nu, nv = (x, y) if net == 0 else (y, x)

            def at(pu, pv):
                return chip(pu, pv, target) if net == 0 else chip(pv, pu, target)

            base = nu + 2 * nv
            head = CLASSES * net + (base + 1) % CLASSES
            send(head, None, 4 + 2 * core, at(nu + 1, nv))
            head = CLASSES * net + (base + 3) % CLASSES
            send(head, None, 8 + 2 * core, at(nu + side - 1, nv))
            head = CLASSES * net + (base + 2) % CLASSES
            send(head, 0, 12 + core, at(nu, nv + 1))
            send(head, 1, 14 + core, at(nu, nv + side - 1))

        @pl.when(me != 0)
        def _():
            send_all(0, (kall0, vall0)[which], 1)

        @pl.when(me == 0)
        def _():
            send_all(0, (kall, vall)[which], 0)

        send_all(1, (kall, vall)[which], 1)
        own = ((kall, vall)[which], (kall0, vall0)[which])
        head0 = (x + 2 * y) % CLASSES
        head1 = CLASSES + (y + 2 * x) % CLASSES

        @pl.when(core == 0)
        def _():
            own[0][0:2] = buf[head0]
            remote(
                buf.at[head1],
                own[0].at[pl.ds(0, 2)],
                kv_send.at[which],
                kv_recv.at[which, 1],
                chip(x, y, 1),
            ).start()

        @pl.when(core == 1)
        def _():
            own[0][2:4] = buf[head1]
            own[1][2:4] = buf[head0]

    pltpu.make_async_copy(vx, vx, local_sem.at[2]).wait()

    @pl.when(core == 0)
    def _():
        send_cache(1)

    tile_row = lax.broadcasted_iota(jnp.int32, (EXTRA, width), 0)
    row16 = lax.broadcasted_iota(jnp.int32, (16, width), 0)
    lane = lax.broadcasted_iota(jnp.int32, (1, width), 1)
    half_pages = half_rows // PAGE
    biases = []
    for hf in range(2):
        page = jnp.zeros((1, width), jnp.int32)
        for j in range(half_pages):
            page = jnp.where(lane // PAGE == j, pages_ref[hf * half_pages + j], page)
        slot = hf * half_pages + lane // PAGE
        usable = (slot < count) & (page * PAGE + lane % PAGE < start)
        biases.append(jnp.where(usable, 0.0, DEAD).astype(F32))
    page_pos = jnp.zeros((16, width), jnp.int32)
    for j in range(rows // PAGE):
        page_pos = jnp.where(row16 == j, pages_ref[j] * PAGE, page_pos)
    page_cos, page_sin = cos_sin(page_pos.astype(F32), table_ref)
    row_cos = table_ref[8 : 8 + PAGE, :]
    row_sin = table_ref[8 + PAGE : 8 + 2 * PAGE, :]
    for j in range(rows // PAGE):
        pc_, ps_ = page_cos[j : j + 1, :], page_sin[j : j + 1, :]
        cos_ref[j * PAGE : (j + 1) * PAGE, :] = pc_ * row_cos - ps_ * row_sin
        sin_ref[j * PAGE : (j + 1) * PAGE, :] = ps_ * row_cos + pc_ * row_sin
    for name in ("sk", "sv", "k"):
        local[name].wait()
    sk_all = sk_raw[...].astype(F32)
    sv_all = sv_raw[...].astype(F32)
    for h in range(KVH):
        span = jnp.broadcast_to(sk_all[:, h * width : (h + 1) * width], (8, width))
        span = span * own_cos + pltpu.roll(span, width // 2, 1) * own_sin
        span = jnp.broadcast_to(span[0:1, :], (EXTRA, width))
        value = jnp.broadcast_to(sv_all[:, h * width : (h + 1) * width], (EXTRA, width))
        for hf in range(2):
            tile = jnp.where(tile_row == 0, span, jnp.where(tile_row == 2, value, 0.0))
            tile = jnp.where(tile_row == 1, biases[hf], tile)
            kx[h, hf, half_rows : half_rows + EXTRA, :] = tile.astype(BF16)

    @pl.loop(0, KVH // 2)
    def _(step):
        for h in (2 * step, 2 * step + 1):
            cols = pl.ds(pl.multiple_of(h * width, width), width)
            for hf in range(2):
                span_rows = slice(hf * half_rows, (hf + 1) * half_rows)
                part = k_raw[span_rows, cols].astype(F32)
                turned = part * cos_ref[span_rows, :]
                turned = turned + pltpu.roll(part, width // 2, 1) * sin_ref[span_rows, :]
                kx[h, hf, 0:half_rows, :] = turned.astype(BF16)

    @pl.when(core == 0)
    def _():
        send_cache(0)
        pl.semaphore_wait(told_far, 1)

        @pl.when(me != 0)
        def _():
            for d in far_first:
                signal(side_row, chip(x + d, y, 1))
                signal(side_col, chip(x, y + d, 1))

    @pl.when(core == 1)
    def _():
        @pl.when(me == 1)
        def _():
            pl.semaphore_wait(barrier, 2 * (side - 1))
            send_q1(1, lambda net, place: q1.at[net, :, 2 * place + 1], q1_recv)
            send_cache(1)
            send_cache(0)
            pl.semaphore_wait(told, 1)
            signal(told_far, chip(x, y, 0))
            landed(qsrc.at[:, :, :, 0], q0_sem)
            send_q1(0, lambda net, place: qlate.at[net], ql_recv)
            qlate[0] = qsrc[0, 0, :, 0]
            qlate[1] = qsrc[1, 0, :, 0]

        @pl.when(me > 1)
        def _():
            pl.semaphore_wait(told, 1)
            send_cache(1)
            pl.semaphore_wait(barrier, 2 * (side - 1))
            signal(told_far, chip(x, y, 0))
            landed(qsrc.at[:, :, :, 0], q0_sem)
            send_q1(pl.ds(0, 2), lambda net, place: q1.at[net, :, pl.ds(2 * place, 2)], q1_recv)
            send_cache(0)

    remote_units = units - 2
    near_units = units - 4

    @pl.when(core == 1)
    def _():
        for net, place in ((0, x), (1, y)):
            for b in range(2):
                q1[net, b, 2 * place + 1] = qsrc[net, place % 2, b, 1]

        @pl.when(me > 1)
        def _():
            for net, place in ((0, x), (1, y)):
                for b in range(2):
                    q1[net, b, 2 * place] = qsrc[net, place % 2, b, 0]

        for net, across in ((0, y), (1, x)):

            @pl.when(across == 0)
            def _(net=net):
                for b in range(2):
                    q1[net, b, 0] = jnp.zeros((GROUP, width), BF16)

        pl.semaphore_wait(side_col, jnp.where((x == 0) & (y != 0), side - 2, side - 1))

        def send_q2(net, pv):
            nu, nv = (x, y) if net == 0 else (y, x)
            remote(
                q1.at[net, (nu // 2 + pv) % 2],
                q2.at[nv],
                q2_send,
                q2_recv.at[nv],
                chip(x, pv, 0) if net == 0 else chip(pv, y, 1),
            ).start()

        def all_in(net, along, across):
            short = (across == 0) & (along != 0)

            @pl.when(short)
            def _():
                landed(q1.at[net, :, pl.ds(0, toks - 3)], q1_recv.at[net])

            @pl.when(jnp.logical_not(short))
            def _():
                landed(q1.at[net, :, pl.ds(0, toks - 2)], q1_recv.at[net])

        all_in(0, x, y)
        for d in far_first:
            pv = (y + d) % side

            @pl.when((x != 0) | (pv != 0))
            def _(pv=pv):
                send_q2(0, pv)

        send_q2(0, y)
        all_in(1, y, x)
        for d in far_first:
            send_q2(1, (x + d) % side)
        q2[x] = q1[1, (y // 2 + x) % 2]

        def hand_on():
            cases = [(jnp.logical_not(by_chip0), near_units, ((2, units),))]
            for here, slots in (
                ((y == 0) & (x == 1), (4, 6)),
                ((y == 0) & (x == side - 1), (8, 10)),
                ((x == 0) & (y == 1), (12, 13)),
                ((x == 0) & (y == side - 1), (14, 15)),
            ):
                spans = ((2, slots[0]), (slots[1], units))
                cases.append((here, near_units - slots[1] + slots[0], spans))
            for which, (src, dst) in ((1, (vall0, vall)), (0, (kall0, kall))):
                for here, amount, spans in cases:

                    @pl.when(here)
                    def _(which=which, src=src, dst=dst, amount=amount, spans=spans):
                        landed(src.at[pl.ds(0, amount)], kv_recv.at[which, 0])
                        for first, end in spans:
                            span = pl.ds(first, end - first)
                            remote(
                                src.at[span],
                                dst.at[span],
                                on_send.at[which],
                                kv_recv.at[which, 0],
                                chip(x, y, 0),
                            ).start()

        hand_on()

        @pl.when(y == 0)
        def _():
            @pl.when(x != 0)
            def _():
                landed(qlate.at[0], ql_recv.at[0])

            for d in far_first + [0]:
                remote(
                    qlate.at[0, (x // 2 + d) % 2], q2l, q2l_send, q2l_recv, chip(x, d, 0)
                ).start()

        @pl.when(x == 0)
        def _():
            @pl.when(y != 0)
            def _():
                landed(qlate.at[1], ql_recv.at[1])
                send_q2(0, 0)

            for d in far_first:
                remote(
                    qlate.at[1, (y // 2 + d) % 2], q2l, q2l_send, q2l_recv, chip(d, y, 1)
                ).start()
            q2l[...] = qlate[1, (y // 2) % 2]

        landed(vall.at[pl.ds(0, remote_units)], kv_recv.at[1, 1])

    @pl.when(core == 0)
    def _():
        landed(vall.at[pl.ds(0, remote_units)], kv_recv.at[1, 0])

    for unit in range(units):
        vturned[:, unit * half_rows : (unit + 1) * half_rows] = vall[unit].T

    @pl.when(core == 1)
    def _():
        landed(kall.at[pl.ds(0, remote_units)], kv_recv.at[0, 1])

    @pl.when(core == 0)
    def _():
        landed(kall.at[pl.ds(0, remote_units)], kv_recv.at[0, 0])

    span_units = [0, 2, 4, 6, 8, 10, 12, 13]
    span_toks = [
        dev(pu, pv, pc)
        for pu, pv in ((u, v), (u + side - 1, v), (u + 1, v), (u, v + side - 1))
        for pc in range(2)
    ]
    rows16[...] = jnp.zeros_like(rows16)
    for unit in range(units):
        tile = kall[unit, half_rows : half_rows + EXTRA, :].astype(F32)
        rows16[0, unit : unit + 1, :] = tile[1:2, :]
        if unit in span_units:
            k = span_units.index(unit)
            rows16[1, k : k + 1, :] = tile[0:1, :]
            rows16[2, k : k + 1, :] = tile[2:3, :]
    zeros = jnp.zeros((width - 16, width), F32)
    bias_cols = jnp.concatenate([rows16[0], zeros]).T
    for unit in range(units):
        turned = bias_cols if unit == 0 else pltpu.roll(bias_cols, width - unit, 1)
        kbias[unit * half_rows : (unit + 1) * half_rows, :] = turned.astype(BF16)
    kspan[...] = rows16[1].astype(BF16)
    vspan[...] = jnp.concatenate([rows16[2], zeros]).T.astype(BF16)
    span_tok = jnp.full((16, piece), 1 << 20, jnp.int32)
    for k, tok in enumerate(span_toks):
        span_tok = jnp.where(row16 == k, tok, span_tok)

    exponent = width**-0.5 / math.log(2.0)
    contract = (((1,), (1,)), ((), ()))
    chunk = 2 * half_rows
    cols = 2 * piece

    def send_o1(pv):
        remote(
            o1src.at[pv], o1.at[core, v], o1_send, o1_recv.at[core], dev(u, pv, 1)
        ).start()

    col_slot = lax.broadcasted_iota(jnp.int32, (1, piece), 1) // GROUP
    tok_along = jnp.where(core == 0, 2, 2 * side)
    tok_across = jnp.where(core == 0, 2 * side, 2)
    col_tok = (col_slot // 2) * tok_along + col_slot % 2
    one_hot = jnp.where(lax.broadcasted_iota(jnp.int32, (cols, width), 1) == 0, 1.0, 0.0).astype(BF16)

    scores, span_scores, tops = (scores_a, scores_b), (span_a, span_b), (top_a, top_b)
    half_units = units // 2
    half_cache = half_units * half_rows
    always = me < 4 * side * side

    def score(query, live, buf):
        n = query.shape[0]
        query = jnp.concatenate([query, one_hot[:n]], axis=1)
        s = lax.dot_general(kspan[...], query[:, :width], contract, preferred_element_type=F32)
        s_span = jnp.where(live, s, DEAD)
        span_scores[buf][:, :n] = s_span
        best = jnp.maximum(s_span[0:8], s_span[8:16])
        for p in range(2):
            span = slice(p * half_cache, (p + 1) * half_cache)
            keys = kall[p * half_units : (p + 1) * half_units, 0:half_rows, :]
            keys = jnp.concatenate([keys.reshape(half_cache, width), kbias[span, :]], axis=1)
            s = lax.dot_general(keys, query, contract, preferred_element_type=F32)
            scores[buf][span, :n] = s
            best = jnp.maximum(best, jnp.max(s.reshape(-1, 8, n), axis=0))
        tops[buf][:, :n] = jnp.maximum(jnp.max(best, axis=0, keepdims=True), FLOOR)

    def weigh(buf, n):
        top = tops[buf][:, :n]
        w = jnp.exp2((span_scores[buf][:, :n] - top) * exponent)
        total = w[0:8] + w[8:16]
        w = jnp.concatenate([w, jnp.zeros((width - 16, n), F32)])
        nums = [jnp.dot(vspan[...], w.astype(BF16), preferred_element_type=F32), None]
        for k in range(units // 2):
            w = jnp.exp2((scores[buf][k * chunk : (k + 1) * chunk, :n] - top) * exponent)
            total = total + jnp.sum(w.reshape(chunk // 8, 8, n), axis=0)
            part = jnp.dot(
                vturned[:, k * chunk : (k + 1) * chunk],
                w.astype(BF16),
                preferred_element_type=F32,
            )
            nums[k % 2] = part if nums[k % 2] is None else nums[k % 2] + part
        den = jnp.sum(total, axis=0, keepdims=True)
        stat = jnp.concatenate(in_three(top) + in_three(den) + [jnp.zeros((EXTRA - 6, n), F32)])
        return nums[0] + nums[1], stat

    def score_pair(pvs, buf):
        query = jnp.concatenate(
            [q2[pv].astype(F32).reshape(piece, width).astype(BF16) for pv in pvs]
        )
        live = jnp.concatenate([span_tok <= col_tok + pv * tok_across for pv in pvs], axis=1)
        score(query, live, buf)

    def weigh_pair(pvs, buf):
        num, stat = weigh(buf, cols)
        for k, pv in enumerate(pvs):
            lanes = slice(k * piece, (k + 1) * piece)
            o1src[pv, 0:width, :] = num[:, lanes].astype(BF16)
            o1src[pv, width : width + EXTRA, :] = stat[:, lanes].astype(BF16)

    def pair(k):
        late, away, half = (me <= 1) | by_chip0, jnp.where(v < side // 2, -1, 1), side // 2
        a, b = [(0, 1), (4, 3), (-3, 2), (-2, -1)][k]
        a, b = (v + away * a + side) % side, (v + away * b + side) % side
        a, b = jnp.where(b == 0, b, a), jnp.where(b == 0, a, b)
        return [jnp.where(late, (side - k) % side, a), jnp.where(late, k + 1, b)]

    def queries_in(pvs):
        for pv in pvs:

            @pl.when((pv != v) | (core == 0))
            def _(pv=pv):
                landed(q2.at[pv], q2_recv.at[pv])

    def results_out(pvs):
        for pv in pvs:

            @pl.when((pv != v) | (core == 0))
            def _(pv=pv):
                send_o1(pv)

            @pl.when((pv == v) & (core == 1))
            def _(pv=pv):
                o1[1, pv] = o1src[pv]

    pairs = side // 2
    queries_in(pair(0))
    score_pair(pair(0), 0)

    for k in range(pairs - 1):
        queries_in(pair(k + 1))

        @pl.when(always)
        def _(k=k):
            score_pair(pair(k + 1), (k + 1) % 2)
            weigh_pair(pair(k), k % 2)

        results_out(pair(k))

    @pl.when((core == 0) | (x != 0))
    def _():
        landed(q2l, q2l_recv)

    @pl.when(always)
    def _():
        query = jnp.concatenate([q2l[...].astype(F32), jnp.zeros((piece - GROUP, width), F32)])
        score(query.astype(BF16), span_tok <= 0, pairs % 2)
        weigh_pair(pair(pairs - 1), (pairs - 1) % 2)

    results_out(pair(pairs - 1))

    @pl.when(always)
    def _():
        num, stat = weigh(pairs % 2, piece)
        late_src[0] = num.T[0:GROUP].astype(BF16)
        wide = jnp.concatenate([stat, jnp.zeros((width - EXTRA, piece), F32)])
        late_src[1] = wide.T[0:GROUP].astype(BF16)

    far_lines = range(3, side - 2)

    def is_far(n):
        return (n >= far_lines[0]) & (n <= far_lines[-1])

    late_slot = jnp.where(core == 0, y, x)
    late_line = jnp.where(core == 0, x, y)
    late_far = is_far(late_line)
    late_to = jnp.where(
        core == 0,
        jnp.where(x == 0, 0, chip(x, 0, 1)),
        jnp.where(y == 0, 0, chip(0, y, 1)),
    )
    late_stays = (me == 0) | ((core == 1) & (x == 0) & (y != 0) & jnp.logical_not(late_far))

    @pl.when(late_far)
    def _():
        place = o1d.at[core, jnp.clip(late_line - far_lines[0], 0, len(far_lines) - 1), late_slot]
        remote(late_src, place, o1l_send, o1d_recv, chip(0, 0, 0)).start()

    @pl.when(jnp.logical_not(late_stays | late_far))
    def _():
        remote(late_src, o1l.at[core, late_slot], o1l_send, o1l_recv.at[core], late_to).start()

    @pl.when(late_stays)
    def _():
        o1l[core, late_slot] = late_src[...]

    def merge_late(parts, nu, out):
        stat = jnp.zeros((GROUP, width), F32)
        for b in range(2):
            vs = [(nu // 2 + b) % 2 + 2 * k for k in range(side // 2)]
            tops, dens = [], []
            for pv in vs:
                tile = parts[pv, 1].astype(F32)
                tile = tile + pltpu.roll(tile, width - 1, 1) + pltpu.roll(tile, width - 2, 1)
                tops.append(jnp.broadcast_to(tile[:, 0:1], (GROUP, width)))
                dens.append(jnp.broadcast_to(tile[:, 3:4], (GROUP, width)))
            top = functools.reduce(jnp.maximum, tops)
            ws = [jnp.exp2((t - top) * exponent) for t in tops]
            den = sum(w * d for w, d in zip(ws, dens))
            num = sum(w * parts[pv, 0].astype(F32) for w, pv in zip(ws, vs))
            out[b] = num.astype(BF16)
            for k, value in enumerate(in_three(top) + in_three(den)):
                stat = jnp.where(lane == 6 * b + k, value, stat)
        out[2] = stat.astype(BF16)

    def cache_gone():
        for which, buf in enumerate((kall, vall)):
            @pl.when(core == 0)
            def _(which=which, buf=buf):
                sent(buf.at[pl.ds(0, near_units + 2)], kv_send.at[which])

            @pl.when(core == 1)
            def _(which=which, buf=buf):
                sent(buf.at[pl.ds(0, near_units)], kv_send.at[which])
                for here, amount in (
                    (line0 * by_chip0 == 0, remote_units),
                    ((y == 0) & by_chip0, remote_units - 2),
                    ((x == 0) & by_chip0, remote_units - 1),
                ):

                    @pl.when(here)
                    def _(which=which, buf=buf, amount=amount):
                        sent(buf.at[pl.ds(0, amount)], on_send.at[which])

        @pl.when(jnp.logical_not(late_stays))
        def _():
            sent(late_src, o1l_send)

    @pl.when(core == 0)
    def _():
        cache_gone()

        sent(qsrc.at[:, :, :, 0], q0_sem)
        sent(o1.at[0], o1_send)

    @pl.when(core == 1)
    def _():
        pl.semaphore_wait(side_row, jnp.where((y == 0) & (x != 0), side - 2, side - 1))
        for step in range(2):
            net = jnp.where(jnp.minimum(y, side - y) <= jnp.minimum(x, side - x), step, 1 - step)
            nu = jnp.where(net == 0, x, y)
            across = jnp.where(net == 0, y, x)
            line = net * side + nu

            def owner(along, pc, net=net):
                return chip(jnp.where(net == 0, along, x), jnp.where(net == 0, y, along), pc)

            def send_o2(src, device, net=net, line=line):
                remote(src, o2.at[line], o2_send.at[net], o2_recv, device).start()

            @pl.when(net == 0)
            def _():
                landed(o1.at[0], o1_recv.at[0])

            @pl.when(net == 1)
            def _():
                landed(o1.at[1, pl.ds(0, side - 1)], o1_recv.at[1])

            stats = []
            for b in range(2):
                vs = [(nu // 2 + b) % 2 + 2 * k for k in range(side // 2)]
                tiles = [o1[net, pv, width : width + EXTRA, :].astype(F32) for pv in vs]
                tops = [t[0:1] + t[1:2] + t[2:3] for t in tiles]
                dens = [t[3:4] + t[4:5] + t[5:6] for t in tiles]
                top = functools.reduce(jnp.maximum, tops)
                ws = [jnp.exp2((t - top) * exponent) for t in tops]
                stats += in_three(top) + in_three(sum(w * d for w, d in zip(ws, dens)))
                total = None
                for w, pv in zip(ws, vs):
                    part = o1[net, pv, 0:width, :].astype(F32) * w
                    total = part if total is None else total + part
                o2src[net, :, b] = total.T.reshape(toks, GROUP, width).astype(BF16)
            stat = jnp.concatenate(stats + [jnp.zeros((width - len(stats), piece), F32)]).T
            o2src[net, :, 2] = stat.reshape(toks, GROUP, width).astype(BF16)
            for along in [0] + far_first[::-1]:

                @pl.when(nu != along)
                def _(along=along):
                    send_o2(o2src.at[net, 2 * along + 1], owner(along, 1))

                if along:
                    send_o2(o2src.at[net, 2 * along], owner(along, 0))

            @pl.when(across != 0)
            def _():
                send_o2(o2src.at[net, 0], owner(0, 0))

            o2[line] = o2src[net, 2 * nu + 1]

            @pl.when((across == 0) & (me != 1) & jnp.logical_not(is_far(nu)))
            def _(net=net, nu=nu):
                @pl.when(net == 0)
                def _():
                    landed(o1l.at[0], o1l_recv.at[0])

                @pl.when(net == 1)
                def _():
                    landed(o1l.at[1, pl.ds(0, side - 1)], o1l_recv.at[1])

                merge_late(o1l.at[net], nu, o2l)
                send_o2(o2l, owner(0, 0))

        cache_gone()

        @pl.when(me == 1)
        def _():
            sent(q1.at[:, :, pl.ds(0, toks - 2)], q1_send)
            sent(q2.at[0, pl.ds(0, toks - 1)], q2l_send)

        @pl.when((me != 1) & (y == 0))
        def _():
            sent(q2.at[0, pl.ds(0, side)], q2l_send)

        @pl.when((me != 1) & (x == 0))
        def _():
            sent(q2.at[0, pl.ds(0, side - 1)], q2l_send)

        @pl.when(me > 1)
        def _():
            sent(q1.at[:, :, pl.ds(0, toks - 2)], q1_send)

        sent(vall.at[pl.ds(0, toks - 1)], q2_send)
        sent(o1.at[0, pl.ds(0, side - 1)], o1_send)
        landed(o2.at[pl.ds(0, toks - 2)], o2_recv)

    @pl.when(core == 0)
    def _():
        @pl.when(me != 0)
        def _():
            landed(o2, o2_recv)

        @pl.when(me == 0)
        def _():
            landed(o1l.at[0, pl.ds(0, side - 1)], o1l_recv.at[0])
            landed(o1l.at[1], o1l_recv.at[1])
            merge_late(o1l.at[0], 0, o2.at[0])
            merge_late(o1l.at[1], 0, o2.at[side])
            landed(o1d, o1d_recv)
            for net in range(2):
                for k, line in enumerate(far_lines):
                    merge_late(o1d.at[net, k], line, o2.at[net * side + line])
            landed(o2.at[pl.ds(0, toks - 2 - 2 * len(far_lines))], o2_recv)

    tops, dens = [[], []], [[], []]
    for src in range(toks):
        tile = o2[src, 2].astype(F32)
        tile = tile + pltpu.roll(tile, width - 1, 1) + pltpu.roll(tile, width - 2, 1)
        for b in range(2):
            tops[b].append(jnp.broadcast_to(tile[:, 6 * b : 6 * b + 1], (GROUP, width)))
            dens[b].append(jnp.broadcast_to(tile[:, 6 * b + 3 : 6 * b + 4], (GROUP, width)))
    for net in range(2):
        for e in range(2):
            srcs = [net * side + e + 2 * k for k in range(side // 2)]
            for b in range(2):
                top = functools.reduce(jnp.maximum, [tops[b][s] for s in srcs])
                ws = [jnp.exp2((tops[b][s] - top) * exponent) for s in srcs]
                den = sum(w * dens[b][s] for w, s in zip(ws, srcs))
                num = sum(w * o2[s, b].astype(F32) for w, s in zip(ws, srcs))
                head = CLASSES * net + e + 2 * b
                out_ref[head * GROUP : (head + 1) * GROUP, :] = num / den

    @pl.when(core == 1)
    def _():
        for net, nu, across in ((0, x, y), (1, y, x)):
            fewer = (across == 0) & ((me == 1) | is_far(nu))

            @pl.when(fewer)
            def _(net=net):
                sent(o2src.at[net, pl.ds(0, toks - 2)], o2_send.at[net])

            @pl.when(jnp.logical_not(fewer))
            def _(net=net):
                sent(o2src.at[net, pl.ds(0, toks - 1)], o2_send.at[net])


def solution(mesh):
    seq = mesh.shape["seq"]
    side = math.isqrt(seq // 2)

    def body(
        queries, span_keys, span_values, cache_keys, cache_values, page_table, page_counts, span_start
    ):
        width = queries.shape[1] // H
        rows = cache_keys.shape[0]
        half = rows // 2
        toks = 2 * side
        piece = toks * GROUP
        table = jnp.asarray(rope_table(width, PAGE))
        units = 16
        vm = pltpu.VMEM
        dma = pltpu.SemaphoreType.DMA
        hbm = pl.BlockSpec(memory_space=pl.ANY)
        smem = pl.BlockSpec(memory_space=pltpu.SMEM)
        vmem = pl.BlockSpec(memory_space=pltpu.VMEM)
        scratch = [
            pltpu.SMEM(page_table.shape, jnp.int32),
            vm(table.shape, F32),
            vm((1, H * width), BF16),
            vm((1, KVH * width), BF16),
            vm((1, KVH * width), BF16),
            vm((rows, KVH * width), BF16),
            vm((H, width), F32),
            vm((rows, width), F32),
            vm((rows, width), F32),
            vm((KVH, 2, half + EXTRA, width), BF16),
            vm((KVH, 2, half, width), BF16),
            vm((units, half + EXTRA, width), BF16),
            vm((units, half, width), BF16),
            vm((units, half + EXTRA, width), BF16),
            vm((units, half, width), BF16),
            vm((width, units * half), BF16),
            vm((units * half, width), BF16),
            vm((3, 16, width), F32),
            vm((16, width), BF16),
            vm((width, width), BF16),
            vm((2, 2, 2, 2, GROUP, width), BF16),
            vm((2, 2, toks, GROUP, width), BF16),
            vm((side, toks, GROUP, width), BF16),
            vm((units * half, 2 * piece), F32),
            vm((units * half, 2 * piece), F32),
            vm((side, width + EXTRA, piece), BF16),
            vm((2, side, width + EXTRA, piece), BF16),
            vm((2, toks, 3, GROUP, width), BF16),
            vm((toks, 3, GROUP, width), BF16),
            vm((2, 2, GROUP, width), BF16),
            vm((GROUP, width), BF16),
            vm((2, GROUP, width), BF16),
            vm((2, side, 2, GROUP, width), BF16),
            vm((2, side - 5, side, 2, GROUP, width), BF16),
            vm((3, GROUP, width), BF16),
            dma((3,)),
            dma((2,)),
            dma((2, 2)),
            dma((2,)),
            dma(()),
            dma(()),
            dma((2,)),
            dma(()),
            dma((side,)),
            dma(()),
            dma((2,)),
            dma((2,)),
            dma(()),
            dma((2,)),
            dma(()),
            dma(()),
            dma(()),
            dma((2,)),
            dma(()),
            pltpu.SemaphoreType.REGULAR,
            pltpu.SemaphoreType.REGULAR,
            pltpu.SemaphoreType.REGULAR,
            pltpu.SemaphoreType.REGULAR,
            vm((16, 2 * piece), F32),
            vm((16, 2 * piece), F32),
            vm((1, 2 * piece), F32),
            vm((1, 2 * piece), F32),
        ]
        out = pl.pallas_call(
            functools.partial(kernel, side),
            out_shape=pltpu.VMEM((H, width), F32),
            in_specs=[smem] * 2 + [hbm] * 7,
            out_specs=pl.BlockSpec(memory_space=pltpu.VMEM),
            scratch_shapes=scratch,
            compiler_params=pltpu.CompilerParams(collective_id=0, has_side_effects=True),
            name="paged_prefix",
        )(
            span_start,
            page_counts,
            page_table,
            table,
            queries,
            span_keys,
            span_values,
            cache_keys,
            cache_values,
        )
        return out.reshape(queries.shape).astype(BF16)

    in_specs = (
        P(("groups", "seq"), None),
        P(("groups", "seq"), None),
        P(("groups", "seq"), None),
        P(("groups", "seq"), None),
        P(("groups", "seq"), None),
        P(("groups", "seq")),
        P(("groups", "seq")),
        P("groups"),
    )
    out_specs = P(("groups", "seq"), None)
    return jax.shard_map(body, mesh=mesh, in_specs=in_specs, out_specs=out_specs, check_vma=False)
```

```python
import functools
import math

import jax
import jax.numpy as jnp
import numpy as np
from jax import lax
from jax.experimental import pallas as pl
from jax.experimental.pallas import tpu as pltpu
from jax.sharding import PartitionSpec as P

H = 64
KVH = 8
PAGE = 16
GROUP = H // KVH
ROPE_BASE = 1000000.0
DEAD = -1e30
FLOOR = -1e29
CLASSES = 4
MESH = pl.DeviceIdType.MESH
F32 = jnp.float32
BF16 = jnp.bfloat16
EXTRA = 8


def rope_table(width, rows):
    half = width // 2
    freq = ROPE_BASE ** (-(np.arange(half, dtype=np.float64) * 2.0 / width))
    turns = np.concatenate([freq, freq]) / (2.0 * np.pi)
    pieces, rest = [], turns
    for _ in range(2):
        scale = 2.0 ** (np.floor(np.log2(rest)) - 7.0)
        part = np.floor(rest / scale) * scale
        pieces.append(part)
        rest = rest - part
    pieces.append(rest)
    sign = np.concatenate([-np.ones(half), np.ones(half)])
    angle = np.arange(rows, dtype=np.float64)[:, None] * np.concatenate([freq, freq])[None, :]
    pad = np.zeros((8 - len(pieces) - 1, width))
    return np.concatenate(
        [np.stack(pieces), sign[None], pad, np.cos(angle), np.sin(angle) * sign[None]]
    ).astype(np.float32)


def cos_sin(position, table_ref):
    def part(k):
        turn = position * table_ref[k : k + 1, :]
        return turn - jnp.floor(turn)

    turn = part(0) + part(1) + part(2)
    turn = turn - jnp.floor(turn + 0.5)
    angle = turn * (2.0 * math.pi)
    return jnp.cos(angle), jnp.sin(angle) * table_ref[3:4, :]


def in_three(value):
    high = value.astype(BF16).astype(F32)
    middle = (value - high).astype(BF16).astype(F32)
    return [high, middle, value - high - middle]


def kernel(
    side,
    start_ref,
    count_ref,
    pages_hbm,
    table_hbm,
    q_hbm,
    sk_hbm,
    sv_hbm,
    k_hbm,
    v_hbm,
    out_ref,
    pages_ref,
    table_ref,
    q_raw,
    sk_raw,
    sv_raw,
    k_raw,
    q_rows,
    cos_ref,
    sin_ref,
    kx,
    vx,
    kall,
    vall,
    kall0,
    vall0,
    vturned,
    kbias,
    rows16,
    kspan,
    vspan,
    qsrc,
    q1,
    q2,
    scores_a,
    scores_b,
    o1src,
    o1,
    o2src,
    o2,
    qlate,
    q2l,
    late_src,
    o1l,
    o1d,
    o2l,
    local_sem,
    kv_send,
    kv_recv,
    on_send,
    q0_sem,
    q1_send,
    q1_recv,
    q2_send,
    q2_recv,
    o1_send,
    o1_recv,
    o2_send,
    o2_recv,
    ql_recv,
    q2l_send,
    q2l_recv,
    o1l_send,
    o1l_recv,
    o1d_recv,
    told,
    told_far,
    side_row,
    side_col,
    span_a,
    span_b,
    top_a,
    top_b,
):
    width = q_rows.shape[1]
    rows = k_hbm.shape[0]
    half_rows = rows // 2
    units = kall.shape[0]
    toks = 2 * side
    piece = toks * GROUP
    me = lax.axis_index("seq")
    core = me % 2
    x = (me // 2) % side
    y = me // (2 * side)
    u = jnp.where(core == 0, x, y)
    v = jnp.where(core == 0, y, x)
    other = 1 - core

    def chip(px, py, pc):
        return ((py % side) * side + px % side) * 2 + pc

    def dev(pu, pv, pc):
        return chip(jnp.where(core == 0, pu, pv), jnp.where(core == 0, pv, pu), pc)

    def remote(src, dst, send, recv, device):
        return pltpu.make_async_remote_copy(
            src_ref=src,
            dst_ref=dst,
            send_sem=send,
            recv_sem=recv,
            device_id={"seq": device},
            device_id_type=MESH,
        )

    def sent(ref, sem):
        remote(ref, ref, sem, sem, chip(x, y, other)).wait_send()

    def landed(ref, sem):
        remote(ref, ref, sem, sem, chip(x, y, other)).wait_recv()

    local = {
        name: pltpu.make_async_copy(src, dst, local_sem.at[k // 3])
        for k, (name, src, dst) in enumerate(
            (
                ("pages", pages_hbm, pages_ref),
                ("table", table_hbm, table_ref),
                ("q", q_hbm, q_raw),
                ("sk", sk_hbm, sk_raw),
                ("sv", sv_hbm, sv_raw),
                ("k", k_hbm, k_raw),
            )
        )
    }
    for copy in local.values():
        copy.start()
    for h in range(KVH):
        for hf in range(2):
            pltpu.make_async_copy(
                v_hbm.at[pl.ds(hf * half_rows, half_rows), pl.ds(h * width, width)],
                vx.at[h, hf],
                local_sem.at[2],
            ).start()

    barrier = pltpu.get_barrier_semaphore()

    def signal(sem, device):
        pl.semaphore_signal(sem, inc=1, device_id={"seq": device}, device_id_type=MESH)

    neighbours = ((1, 0), (side - 1, 0), (0, 1), (0, side - 1))
    line0 = jnp.where(y == 0, x, jnp.where(x == 0, y, 0))
    by_chip0 = (line0 == 1) | (line0 == side - 1)

    @pl.when((core == 0) & by_chip0)
    def _():
        signal(barrier, chip(0, 0, 0))

    @pl.when(core == 1)
    def _():
        signal(barrier, chip(x, y, 0))
        for dx, dy in neighbours:
            signal(barrier, chip(x + dx, y + dy, 0))
        for d in range(1, side):
            signal(barrier, chip(x + d, y, 1))
            signal(barrier, chip(x, y + d, 1))

    for name in ("pages", "table", "q"):
        local[name].wait()
    start = start_ref[0]
    count = count_ref[0]
    own_pos = (start + me).astype(F32)
    own_cos, own_sin = cos_sin(jnp.full((8, width), own_pos, F32), table_ref)
    q_all = q_raw[...].astype(F32)
    for r in range(H):
        q_rows[r : r + 1, :] = q_all[:, r * width : (r + 1) * width]
    for net in range(2):
        for e in range(2):
            for b in range(2):
                head = CLASSES * net + e + 2 * b
                part = q_rows[head * GROUP : (head + 1) * GROUP, :]
                turned = part * own_cos + pltpu.roll(part, width // 2, 1) * own_sin
                qsrc[net, e, b, core] = turned.astype(BF16)

    far_first = [side // 2]
    for step in range(side // 2 - 1, 0, -1):
        far_first += [step, side - step]

    def send_q1(toks_sent, landing, recv):
        for d in far_first:
            for net in range(2):
                place = x if net == 0 else y
                along = (place + d) % side
                remote(
                    qsrc.at[net, along % 2, :, toks_sent],
                    landing(net, place),
                    q1_send,
                    recv.at[net],
                    chip(along, y, 1) if net == 0 else chip(x, along, 1),
                ).start()

    @pl.when(core == 0)
    def _():
        pl.semaphore_wait(barrier, jnp.where(me == 0, 4 + 4 + 1, 4 + 1))
        signal(told, chip(x, y, 1))
        remote(qsrc.at[:, :, :, 0], qsrc.at[:, :, :, 0], q0_sem, q0_sem, chip(x, y, 1)).start()


    def send_cache(which):
        buf = (kx, vx)[which]

        def send_all(net, landing, target):
            def send(head, half, slot, device):
                src = buf.at[head] if half is None else buf.at[head, half]
                dst = landing.at[pl.ds(slot, 2)] if half is None else landing.at[slot]
                remote(src, dst, kv_send.at[which], kv_recv.at[which, net], device).start()

            nu, nv = (x, y) if net == 0 else (y, x)

            def at(pu, pv):
                return chip(pu, pv, target) if net == 0 else chip(pv, pu, target)

            base = nu + 2 * nv
            head = CLASSES * net + (base + 1) % CLASSES
            send(head, None, 4 + 2 * core, at(nu + 1, nv))
            head = CLASSES * net + (base + 3) % CLASSES
            send(head, None, 8 + 2 * core, at(nu + side - 1, nv))
            head = CLASSES * net + (base + 2) % CLASSES
            send(head, 0, 12 + core, at(nu, nv + 1))
            send(head, 1, 14 + core, at(nu, nv + side - 1))

        @pl.when(me != 0)
        def _():
            send_all(0, (kall0, vall0)[which], 1)

        @pl.when(me == 0)
        def _():
            send_all(0, (kall, vall)[which], 0)

        send_all(1, (kall, vall)[which], 1)
        own = ((kall, vall)[which], (kall0, vall0)[which])
        head0 = (x + 2 * y) % CLASSES
        head1 = CLASSES + (y + 2 * x) % CLASSES

        @pl.when(core == 0)
        def _():
            own[0][0:2] = buf[head0]
            remote(
                buf.at[head1],
                own[0].at[pl.ds(0, 2)],
                kv_send.at[which],
                kv_recv.at[which, 1],
                chip(x, y, 1),
            ).start()

        @pl.when(core == 1)
        def _():
            own[0][2:4] = buf[head1]
            own[1][2:4] = buf[head0]

    pltpu.make_async_copy(vx, vx, local_sem.at[2]).wait()

    @pl.when(core == 0)
    def _():
        send_cache(1)

    tile_row = lax.broadcasted_iota(jnp.int32, (EXTRA, width), 0)
    row16 = lax.broadcasted_iota(jnp.int32, (16, width), 0)
    lane = lax.broadcasted_iota(jnp.int32, (1, width), 1)
    half_pages = half_rows // PAGE
    biases = []
    for hf in range(2):
        page = jnp.zeros((1, width), jnp.int32)
        for j in range(half_pages):
            page = jnp.where(lane // PAGE == j, pages_ref[hf * half_pages + j], page)
        slot = hf * half_pages + lane // PAGE
        usable = (slot < count) & (page * PAGE + lane % PAGE < start)
        biases.append(jnp.where(usable, 0.0, DEAD).astype(F32))
    page_pos = jnp.zeros((16, width), jnp.int32)
    for j in range(rows // PAGE):
        page_pos = jnp.where(row16 == j, pages_ref[j] * PAGE, page_pos)
    page_cos, page_sin = cos_sin(page_pos.astype(F32), table_ref)
    row_cos = table_ref[8 : 8 + PAGE, :]
    row_sin = table_ref[8 + PAGE : 8 + 2 * PAGE, :]
    for j in range(rows // PAGE):
        pc_, ps_ = page_cos[j : j + 1, :], page_sin[j : j + 1, :]
        cos_ref[j * PAGE : (j + 1) * PAGE, :] = pc_ * row_cos - ps_ * row_sin
        sin_ref[j * PAGE : (j + 1) * PAGE, :] = ps_ * row_cos + pc_ * row_sin
    for name in ("sk", "sv", "k"):
        local[name].wait()
    sk_all = sk_raw[...].astype(F32)
    sv_all = sv_raw[...].astype(F32)
    for h in range(KVH):
        span = jnp.broadcast_to(sk_all[:, h * width : (h + 1) * width], (8, width))
        span = span * own_cos + pltpu.roll(span, width // 2, 1) * own_sin
        span = jnp.broadcast_to(span[0:1, :], (EXTRA, width))
        value = jnp.broadcast_to(sv_all[:, h * width : (h + 1) * width], (EXTRA, width))
        for hf in range(2):
            tile = jnp.where(tile_row == 0, span, jnp.where(tile_row == 2, value, 0.0))
            tile = jnp.where(tile_row == 1, biases[hf], tile)
            kx[h, hf, half_rows : half_rows + EXTRA, :] = tile.astype(BF16)

    @pl.loop(0, KVH // 2)
    def _(step):
        for h in (2 * step, 2 * step + 1):
            cols = pl.ds(pl.multiple_of(h * width, width), width)
            for hf in range(2):
                span_rows = slice(hf * half_rows, (hf + 1) * half_rows)
                part = k_raw[span_rows, cols].astype(F32)
                turned = part * cos_ref[span_rows, :]
                turned = turned + pltpu.roll(part, width // 2, 1) * sin_ref[span_rows, :]
                kx[h, hf, 0:half_rows, :] = turned.astype(BF16)

    @pl.when(core == 0)
    def _():
        send_cache(0)
        pl.semaphore_wait(told_far, 1)

        @pl.when(me != 0)
        def _():
            for d in far_first:
                signal(side_row, chip(x + d, y, 1))
                signal(side_col, chip(x, y + d, 1))

    @pl.when(core == 1)
    def _():
        @pl.when(me == 1)
        def _():
            pl.semaphore_wait(barrier, 2 * (side - 1))
            send_q1(1, lambda net, place: q1.at[net, :, 2 * place + 1], q1_recv)
            send_cache(1)
            send_cache(0)
            pl.semaphore_wait(told, 1)
            signal(told_far, chip(x, y, 0))
            landed(qsrc.at[:, :, :, 0], q0_sem)
            send_q1(0, lambda net, place: qlate.at[net], ql_recv)
            qlate[0] = qsrc[0, 0, :, 0]
            qlate[1] = qsrc[1, 0, :, 0]

        @pl.when(me > 1)
        def _():
            pl.semaphore_wait(told, 1)
            send_cache(1)
            pl.semaphore_wait(barrier, 2 * (side - 1))
            signal(told_far, chip(x, y, 0))
            landed(qsrc.at[:, :, :, 0], q0_sem)
            send_q1(pl.ds(0, 2), lambda net, place: q1.at[net, :, pl.ds(2 * place, 2)], q1_recv)
            send_cache(0)

    remote_units = units - 2
    near_units = units - 4

    @pl.when(core == 1)
    def _():
        for net, place in ((0, x), (1, y)):
            for b in range(2):
                q1[net, b, 2 * place + 1] = qsrc[net, place % 2, b, 1]

        @pl.when(me > 1)
        def _():
            for net, place in ((0, x), (1, y)):
                for b in range(2):
                    q1[net, b, 2 * place] = qsrc[net, place % 2, b, 0]

        for net, across in ((0, y), (1, x)):

            @pl.when(across == 0)
            def _(net=net):
                for b in range(2):
                    q1[net, b, 0] = jnp.zeros((GROUP, width), BF16)

        pl.semaphore_wait(side_col, jnp.where((x == 0) & (y != 0), side - 2, side - 1))

        def send_q2(net, pv):
            nu, nv = (x, y) if net == 0 else (y, x)
            remote(
                q1.at[net, (nu // 2 + pv) % 2],
                q2.at[nv],
                q2_send,
                q2_recv.at[nv],
                chip(x, pv, 0) if net == 0 else chip(pv, y, 1),
            ).start()

        def all_in(net, along, across):
            short = (across == 0) & (along != 0)

            @pl.when(short)
            def _():
                landed(q1.at[net, :, pl.ds(0, toks - 3)], q1_recv.at[net])

            @pl.when(jnp.logical_not(short))
            def _():
                landed(q1.at[net, :, pl.ds(0, toks - 2)], q1_recv.at[net])

        all_in(0, x, y)
        for d in far_first:
            pv = (y + d) % side

            @pl.when((x != 0) | (pv != 0))
            def _(pv=pv):
                send_q2(0, pv)

        send_q2(0, y)
        all_in(1, y, x)
        for d in far_first:
            send_q2(1, (x + d) % side)
        q2[x] = q1[1, (y // 2 + x) % 2]

        def hand_on():
            cases = [(jnp.logical_not(by_chip0), near_units, ((2, units),))]
            for here, slots in (
                ((y == 0) & (x == 1), (4, 6)),
                ((y == 0) & (x == side - 1), (8, 10)),
                ((x == 0) & (y == 1), (12, 13)),
                ((x == 0) & (y == side - 1), (14, 15)),
            ):
                spans = ((2, slots[0]), (slots[1], units))
                cases.append((here, near_units - slots[1] + slots[0], spans))
            for which, (src, dst) in ((1, (vall0, vall)), (0, (kall0, kall))):
                for here, amount, spans in cases:

                    @pl.when(here)
                    def _(which=which, src=src, dst=dst, amount=amount, spans=spans):
                        landed(src.at[pl.ds(0, amount)], kv_recv.at[which, 0])
                        for first, end in spans:
                            span = pl.ds(first, end - first)
                            remote(
                                src.at[span],
                                dst.at[span],
                                on_send.at[which],
                                kv_recv.at[which, 0],
                                chip(x, y, 0),
                            ).start()

        hand_on()

        @pl.when(y == 0)
        def _():
            @pl.when(x != 0)
            def _():
                landed(qlate.at[0], ql_recv.at[0])

            for d in far_first + [0]:
                remote(
                    qlate.at[0, (x // 2 + d) % 2], q2l, q2l_send, q2l_recv, chip(x, d, 0)
                ).start()

        @pl.when(x == 0)
        def _():
            @pl.when(y != 0)
            def _():
                landed(qlate.at[1], ql_recv.at[1])
                send_q2(0, 0)

            for d in far_first:
                remote(
                    qlate.at[1, (y // 2 + d) % 2], q2l, q2l_send, q2l_recv, chip(d, y, 1)
                ).start()
            q2l[...] = qlate[1, (y // 2) % 2]

        landed(vall.at[pl.ds(0, remote_units)], kv_recv.at[1, 1])

    @pl.when(core == 0)
    def _():
        landed(vall.at[pl.ds(0, remote_units)], kv_recv.at[1, 0])

    for unit in range(units):
        vturned[:, unit * half_rows : (unit + 1) * half_rows] = vall[unit].T

    @pl.when(core == 1)
    def _():
        landed(kall.at[pl.ds(0, remote_units)], kv_recv.at[0, 1])

    @pl.when(core == 0)
    def _():
        landed(kall.at[pl.ds(0, remote_units)], kv_recv.at[0, 0])

    span_units = [0, 2, 4, 6, 8, 10, 12, 13]
    span_toks = [
        dev(pu, pv, pc)
        for pu, pv in ((u, v), (u + side - 1, v), (u + 1, v), (u, v + side - 1))
        for pc in range(2)
    ]
    rows16[...] = jnp.zeros_like(rows16)
    for unit in range(units):
        tile = kall[unit, half_rows : half_rows + EXTRA, :].astype(F32)
        rows16[0, unit : unit + 1, :] = tile[1:2, :]
        if unit in span_units:
            k = span_units.index(unit)
            rows16[1, k : k + 1, :] = tile[0:1, :]
            rows16[2, k : k + 1, :] = tile[2:3, :]
    zeros = jnp.zeros((width - 16, width), F32)
    bias_cols = jnp.concatenate([rows16[0], zeros]).T
    for unit in range(units):
        turned = bias_cols if unit == 0 else pltpu.roll(bias_cols, width - unit, 1)
        kbias[unit * half_rows : (unit + 1) * half_rows, :] = turned.astype(BF16)
    kspan[...] = rows16[1].astype(BF16)
    vspan[...] = jnp.concatenate([rows16[2], zeros]).T.astype(BF16)
    span_tok = jnp.full((16, piece), 1 << 20, jnp.int32)
    for k, tok in enumerate(span_toks):
        span_tok = jnp.where(row16 == k, tok, span_tok)

    exponent = width**-0.5 / math.log(2.0)
    contract = (((1,), (1,)), ((), ()))
    chunk = 2 * half_rows
    cols = 2 * piece

    def send_o1(pv):
        remote(
            o1src.at[pv], o1.at[core, v], o1_send, o1_recv.at[core], dev(u, pv, 1)
        ).start()

    col_slot = lax.broadcasted_iota(jnp.int32, (1, piece), 1) // GROUP
    tok_along = jnp.where(core == 0, 2, 2 * side)
    tok_across = jnp.where(core == 0, 2 * side, 2)
    col_tok = (col_slot // 2) * tok_along + col_slot % 2
    one_hot = jnp.where(lax.broadcasted_iota(jnp.int32, (cols, width), 1) == 0, 1.0, 0.0).astype(BF16)

    scores, span_scores, tops = (scores_a, scores_b), (span_a, span_b), (top_a, top_b)
    half_units = units // 2
    half_cache = half_units * half_rows
    always = me < 4 * side * side

    def score(query, live, buf):
        n = query.shape[0]
        query = jnp.concatenate([query, one_hot[:n]], axis=1)
        s = lax.dot_general(kspan[...], query[:, :width], contract, preferred_element_type=F32)
        s_span = jnp.where(live, s, DEAD)
        span_scores[buf][:, :n] = s_span
        best = jnp.maximum(s_span[0:8], s_span[8:16])
        for p in range(2):
            span = slice(p * half_cache, (p + 1) * half_cache)
            keys = kall[p * half_units : (p + 1) * half_units, 0:half_rows, :]
            keys = jnp.concatenate([keys.reshape(half_cache, width), kbias[span, :]], axis=1)
            s = lax.dot_general(keys, query, contract, preferred_element_type=F32)
            scores[buf][span, :n] = s
            best = jnp.maximum(best, jnp.max(s.reshape(-1, 8, n), axis=0))
        tops[buf][:, :n] = jnp.maximum(jnp.max(best, axis=0, keepdims=True), FLOOR)

    def weigh(buf, n):
        top = tops[buf][:, :n]
        w = jnp.exp2((span_scores[buf][:, :n] - top) * exponent)
        total = w[0:8] + w[8:16]
        w = jnp.concatenate([w, jnp.zeros((width - 16, n), F32)])
        nums = [jnp.dot(vspan[...], w.astype(BF16), preferred_element_type=F32), None]
        for k in range(units // 2):
            w = jnp.exp2((scores[buf][k * chunk : (k + 1) * chunk, :n] - top) * exponent)
            total = total + jnp.sum(w.reshape(chunk // 8, 8, n), axis=0)
            part = jnp.dot(
                vturned[:, k * chunk : (k + 1) * chunk],
                w.astype(BF16),
                preferred_element_type=F32,
            )
            nums[k % 2] = part if nums[k % 2] is None else nums[k % 2] + part
        den = jnp.sum(total, axis=0, keepdims=True)
        stat = jnp.concatenate(in_three(top) + in_three(den) + [jnp.zeros((EXTRA - 6, n), F32)])
        return nums[0] + nums[1], stat

    def score_pair(pvs, buf):
        query = jnp.concatenate(
            [q2[pv].astype(F32).reshape(piece, width).astype(BF16) for pv in pvs]
        )
        live = jnp.concatenate([span_tok <= col_tok + pv * tok_across for pv in pvs], axis=1)
        score(query, live, buf)

    def weigh_pair(pvs, buf):
        num, stat = weigh(buf, cols)
        for k, pv in enumerate(pvs):
            lanes = slice(k * piece, (k + 1) * piece)
            o1src[pv, 0:width, :] = num[:, lanes].astype(BF16)
            o1src[pv, width : width + EXTRA, :] = stat[:, lanes].astype(BF16)

    def pair(k):
        late, away, half = (me <= 1) | by_chip0, jnp.where(v < side // 2, -1, 1), side // 2
        a, b = [(0, 1), (4, 3), (-3, 2), (-2, -1)][k]
        a, b = (v + away * a + side) % side, (v + away * b + side) % side
        early, near = (u == side // 2), (v + away + side) % side
        if k == 0:
            b = jnp.where(early & (v != 0), 0, b)
        else:
            a, b = jnp.where(early & (a == 0), near, a), jnp.where(early & (b == 0), near, b)
        a, b = jnp.where(b == 0, b, a), jnp.where(b == 0, a, b)
        return [jnp.where(late, (side - k) % side, a), jnp.where(late, k + 1, b)]

    def queries_in(pvs):
        for pv in pvs:

            @pl.when((pv != v) | (core == 0))
            def _(pv=pv):
                landed(q2.at[pv], q2_recv.at[pv])

    def results_out(pvs):
        for pv in pvs:

            @pl.when((pv != v) | (core == 0))
            def _(pv=pv):
                send_o1(pv)

            @pl.when((pv == v) & (core == 1))
            def _(pv=pv):
                o1[1, pv] = o1src[pv]

    pairs = side // 2
    queries_in(pair(0))
    score_pair(pair(0), 0)

    for k in range(pairs - 1):
        queries_in(pair(k + 1))

        @pl.when(always)
        def _(k=k):
            score_pair(pair(k + 1), (k + 1) % 2)
            weigh_pair(pair(k), k % 2)

        results_out(pair(k))

    @pl.when((core == 0) | (x != 0))
    def _():
        landed(q2l, q2l_recv)

    @pl.when(always)
    def _():
        query = jnp.concatenate([q2l[...].astype(F32), jnp.zeros((piece - GROUP, width), F32)])
        score(query.astype(BF16), span_tok <= 0, pairs % 2)
        weigh_pair(pair(pairs - 1), (pairs - 1) % 2)

    results_out(pair(pairs - 1))

    @pl.when(always)
    def _():
        num, stat = weigh(pairs % 2, piece)
        late_src[0] = num.T[0:GROUP].astype(BF16)
        wide = jnp.concatenate([stat, jnp.zeros((width - EXTRA, piece), F32)])
        late_src[1] = wide.T[0:GROUP].astype(BF16)

    far_lines = range(3, side - 2)

    def is_far(n):
        return (n >= far_lines[0]) & (n <= far_lines[-1])

    late_slot = jnp.where(core == 0, y, x)
    late_line = jnp.where(core == 0, x, y)
    late_far = is_far(late_line)
    late_to = jnp.where(
        core == 0,
        jnp.where(x == 0, 0, chip(x, 0, 1)),
        jnp.where(y == 0, 0, chip(0, y, 1)),
    )
    late_stays = (me == 0) | ((core == 1) & (x == 0) & (y != 0) & jnp.logical_not(late_far))

    @pl.when(late_far)
    def _():
        place = o1d.at[core, jnp.clip(late_line - far_lines[0], 0, len(far_lines) - 1), late_slot]
        remote(late_src, place, o1l_send, o1d_recv, chip(0, 0, 0)).start()

    @pl.when(jnp.logical_not(late_stays | late_far))
    def _():
        remote(late_src, o1l.at[core, late_slot], o1l_send, o1l_recv.at[core], late_to).start()

    @pl.when(late_stays)
    def _():
        o1l[core, late_slot] = late_src[...]

    def merge_late(parts, nu, out):
        stat = jnp.zeros((GROUP, width), F32)
        for b in range(2):
            vs = [(nu // 2 + b) % 2 + 2 * k for k in range(side // 2)]
            tops, dens = [], []
            for pv in vs:
                tile = parts[pv, 1].astype(F32)
                tile = tile + pltpu.roll(tile, width - 1, 1) + pltpu.roll(tile, width - 2, 1)
                tops.append(jnp.broadcast_to(tile[:, 0:1], (GROUP, width)))
                dens.append(jnp.broadcast_to(tile[:, 3:4], (GROUP, width)))
            top = functools.reduce(jnp.maximum, tops)
            ws = [jnp.exp2((t - top) * exponent) for t in tops]
            den = sum(w * d for w, d in zip(ws, dens))
            num = sum(w * parts[pv, 0].astype(F32) for w, pv in zip(ws, vs))
            out[b] = num.astype(BF16)
            for k, value in enumerate(in_three(top) + in_three(den)):
                stat = jnp.where(lane == 6 * b + k, value, stat)
        out[2] = stat.astype(BF16)

    def cache_gone():
        for which, buf in enumerate((kall, vall)):
            @pl.when(core == 0)
            def _(which=which, buf=buf):
                sent(buf.at[pl.ds(0, near_units + 2)], kv_send.at[which])

            @pl.when(core == 1)
            def _(which=which, buf=buf):
                sent(buf.at[pl.ds(0, near_units)], kv_send.at[which])
                for here, amount in (
                    (line0 * by_chip0 == 0, remote_units),
                    ((y == 0) & by_chip0, remote_units - 2),
                    ((x == 0) & by_chip0, remote_units - 1),
                ):

                    @pl.when(here)
                    def _(which=which, buf=buf, amount=amount):
                        sent(buf.at[pl.ds(0, amount)], on_send.at[which])

        @pl.when(jnp.logical_not(late_stays))
        def _():
            sent(late_src, o1l_send)

    @pl.when(core == 0)
    def _():
        cache_gone()

        sent(qsrc.at[:, :, :, 0], q0_sem)
        sent(o1.at[0], o1_send)

    @pl.when(core == 1)
    def _():
        pl.semaphore_wait(side_row, jnp.where((y == 0) & (x != 0), side - 2, side - 1))
        for step in range(2):
            net = jnp.where(jnp.minimum(y, side - y) <= jnp.minimum(x, side - x), step, 1 - step)
            nu = jnp.where(net == 0, x, y)
            across = jnp.where(net == 0, y, x)
            line = net * side + nu

            def owner(along, pc, net=net):
                return chip(jnp.where(net == 0, along, x), jnp.where(net == 0, y, along), pc)

            def send_o2(src, device, net=net, line=line):
                remote(src, o2.at[line], o2_send.at[net], o2_recv, device).start()

            @pl.when(net == 0)
            def _():
                landed(o1.at[0], o1_recv.at[0])

            @pl.when(net == 1)
            def _():
                landed(o1.at[1, pl.ds(0, side - 1)], o1_recv.at[1])

            stats = []
            for b in range(2):
                vs = [(nu // 2 + b) % 2 + 2 * k for k in range(side // 2)]
                tiles = [o1[net, pv, width : width + EXTRA, :].astype(F32) for pv in vs]
                tops = [t[0:1] + t[1:2] + t[2:3] for t in tiles]
                dens = [t[3:4] + t[4:5] + t[5:6] for t in tiles]
                top = functools.reduce(jnp.maximum, tops)
                ws = [jnp.exp2((t - top) * exponent) for t in tops]
                stats += in_three(top) + in_three(sum(w * d for w, d in zip(ws, dens)))
                total = None
                for w, pv in zip(ws, vs):
                    part = o1[net, pv, 0:width, :].astype(F32) * w
                    total = part if total is None else total + part
                o2src[net, :, b] = total.T.reshape(toks, GROUP, width).astype(BF16)
            stat = jnp.concatenate(stats + [jnp.zeros((width - len(stats), piece), F32)]).T
            o2src[net, :, 2] = stat.reshape(toks, GROUP, width).astype(BF16)
            for along in [0] + far_first[::-1]:

                @pl.when(nu != along)
                def _(along=along):
                    send_o2(o2src.at[net, 2 * along + 1], owner(along, 1))

                if along:
                    send_o2(o2src.at[net, 2 * along], owner(along, 0))

            @pl.when(across != 0)
            def _():
                send_o2(o2src.at[net, 0], owner(0, 0))

            o2[line] = o2src[net, 2 * nu + 1]

            @pl.when((across == 0) & (me != 1) & jnp.logical_not(is_far(nu)))
            def _(net=net, nu=nu):
                @pl.when(net == 0)
                def _():
                    landed(o1l.at[0], o1l_recv.at[0])

                @pl.when(net == 1)
                def _():
                    landed(o1l.at[1, pl.ds(0, side - 1)], o1l_recv.at[1])

                merge_late(o1l.at[net], nu, o2l)
                send_o2(o2l, owner(0, 0))

        cache_gone()

        @pl.when(me == 1)
        def _():
            sent(q1.at[:, :, pl.ds(0, toks - 2)], q1_send)
            sent(q2.at[0, pl.ds(0, toks - 1)], q2l_send)

        @pl.when((me != 1) & (y == 0))
        def _():
            sent(q2.at[0, pl.ds(0, side)], q2l_send)

        @pl.when((me != 1) & (x == 0))
        def _():
            sent(q2.at[0, pl.ds(0, side - 1)], q2l_send)

        @pl.when(me > 1)
        def _():
            sent(q1.at[:, :, pl.ds(0, toks - 2)], q1_send)

        sent(vall.at[pl.ds(0, toks - 1)], q2_send)
        sent(o1.at[0, pl.ds(0, side - 1)], o1_send)
        landed(o2.at[pl.ds(0, toks - 2)], o2_recv)

    @pl.when(core == 0)
    def _():
        @pl.when(me != 0)
        def _():
            landed(o2, o2_recv)

        @pl.when(me == 0)
        def _():
            landed(o1l.at[0, pl.ds(0, side - 1)], o1l_recv.at[0])
            landed(o1l.at[1], o1l_recv.at[1])
            merge_late(o1l.at[0], 0, o2.at[0])
            merge_late(o1l.at[1], 0, o2.at[side])
            landed(o1d, o1d_recv)
            for net in range(2):
                for k, line in enumerate(far_lines):
                    merge_late(o1d.at[net, k], line, o2.at[net * side + line])
            landed(o2.at[pl.ds(0, toks - 2 - 2 * len(far_lines))], o2_recv)

    tops, dens = [[], []], [[], []]
    for src in range(toks):
        tile = o2[src, 2].astype(F32)
        tile = tile + pltpu.roll(tile, width - 1, 1) + pltpu.roll(tile, width - 2, 1)
        for b in range(2):
            tops[b].append(jnp.broadcast_to(tile[:, 6 * b : 6 * b + 1], (GROUP, width)))
            dens[b].append(jnp.broadcast_to(tile[:, 6 * b + 3 : 6 * b + 4], (GROUP, width)))
    for net in range(2):
        for e in range(2):
            srcs = [net * side + e + 2 * k for k in range(side // 2)]
            for b in range(2):
                top = functools.reduce(jnp.maximum, [tops[b][s] for s in srcs])
                ws = [jnp.exp2((tops[b][s] - top) * exponent) for s in srcs]
                den = sum(w * dens[b][s] for w, s in zip(ws, srcs))
                num = sum(w * o2[s, b].astype(F32) for w, s in zip(ws, srcs))
                head = CLASSES * net + e + 2 * b
                out_ref[head * GROUP : (head + 1) * GROUP, :] = num / den

    @pl.when(core == 1)
    def _():
        for net, nu, across in ((0, x, y), (1, y, x)):
            fewer = (across == 0) & ((me == 1) | is_far(nu))

            @pl.when(fewer)
            def _(net=net):
                sent(o2src.at[net, pl.ds(0, toks - 2)], o2_send.at[net])

            @pl.when(jnp.logical_not(fewer))
            def _(net=net):
                sent(o2src.at[net, pl.ds(0, toks - 1)], o2_send.at[net])


def solution(mesh):
    seq = mesh.shape["seq"]
    side = math.isqrt(seq // 2)

    def body(
        queries, span_keys, span_values, cache_keys, cache_values, page_table, page_counts, span_start
    ):
        width = queries.shape[1] // H
        rows = cache_keys.shape[0]
        half = rows // 2
        toks = 2 * side
        piece = toks * GROUP
        table = jnp.asarray(rope_table(width, PAGE))
        units = 16
        vm = pltpu.VMEM
        dma = pltpu.SemaphoreType.DMA
        hbm = pl.BlockSpec(memory_space=pl.ANY)
        smem = pl.BlockSpec(memory_space=pltpu.SMEM)
        vmem = pl.BlockSpec(memory_space=pltpu.VMEM)
        scratch = [
            pltpu.SMEM(page_table.shape, jnp.int32),
            vm(table.shape, F32),
            vm((1, H * width), BF16),
            vm((1, KVH * width), BF16),
            vm((1, KVH * width), BF16),
            vm((rows, KVH * width), BF16),
            vm((H, width), F32),
            vm((rows, width), F32),
            vm((rows, width), F32),
            vm((KVH, 2, half + EXTRA, width), BF16),
            vm((KVH, 2, half, width), BF16),
            vm((units, half + EXTRA, width), BF16),
            vm((units, half, width), BF16),
            vm((units, half + EXTRA, width), BF16),
            vm((units, half, width), BF16),
            vm((width, units * half), BF16),
            vm((units * half, width), BF16),
            vm((3, 16, width), F32),
            vm((16, width), BF16),
            vm((width, width), BF16),
            vm((2, 2, 2, 2, GROUP, width), BF16),
            vm((2, 2, toks, GROUP, width), BF16),
            vm((side, toks, GROUP, width), BF16),
            vm((units * half, 2 * piece), F32),
            vm((units * half, 2 * piece), F32),
            vm((side, width + EXTRA, piece), BF16),
            vm((2, side, width + EXTRA, piece), BF16),
            vm((2, toks, 3, GROUP, width), BF16),
            vm((toks, 3, GROUP, width), BF16),
            vm((2, 2, GROUP, width), BF16),
            vm((GROUP, width), BF16),
            vm((2, GROUP, width), BF16),
            vm((2, side, 2, GROUP, width), BF16),
            vm((2, side - 5, side, 2, GROUP, width), BF16),
            vm((3, GROUP, width), BF16),
            dma((3,)),
            dma((2,)),
            dma((2, 2)),
            dma((2,)),
            dma(()),
            dma(()),
            dma((2,)),
            dma(()),
            dma((side,)),
            dma(()),
            dma((2,)),
            dma((2,)),
            dma(()),
            dma((2,)),
            dma(()),
            dma(()),
            dma(()),
            dma((2,)),
            dma(()),
            pltpu.SemaphoreType.REGULAR,
            pltpu.SemaphoreType.REGULAR,
            pltpu.SemaphoreType.REGULAR,
            pltpu.SemaphoreType.REGULAR,
            vm((16, 2 * piece), F32),
            vm((16, 2 * piece), F32),
            vm((1, 2 * piece), F32),
            vm((1, 2 * piece), F32),
        ]
        out = pl.pallas_call(
            functools.partial(kernel, side),
            out_shape=pltpu.VMEM((H, width), F32),
            in_specs=[smem] * 2 + [hbm] * 7,
            out_specs=pl.BlockSpec(memory_space=pltpu.VMEM),
            scratch_shapes=scratch,
            compiler_params=pltpu.CompilerParams(collective_id=0, has_side_effects=True),
            name="paged_prefix",
        )(
            span_start,
            page_counts,
            page_table,
            table,
            queries,
            span_keys,
            span_values,
            cache_keys,
            cache_values,
        )
        return out.reshape(queries.shape).astype(BF16)

    in_specs = (
        P(("groups", "seq"), None),
        P(("groups", "seq"), None),
        P(("groups", "seq"), None),
        P(("groups", "seq"), None),
        P(("groups", "seq"), None),
        P(("groups", "seq")),
        P(("groups", "seq")),
        P("groups"),
    )
    out_specs = P(("groups", "seq"), None)
    return jax.shard_map(body, mesh=mesh, in_specs=in_specs, out_specs=out_specs, check_vma=False)
```

```python
import functools
import math

import jax
import jax.numpy as jnp
import numpy as np
from jax import lax
from jax.experimental import pallas as pl
from jax.experimental.pallas import tpu as pltpu
from jax.sharding import PartitionSpec as P

H = 64
KVH = 8
PAGE = 16
GROUP = H // KVH
ROPE_BASE = 1000000.0
DEAD = -1e30
FLOOR = -1e29
CLASSES = 4
MESH = pl.DeviceIdType.MESH
F32 = jnp.float32
BF16 = jnp.bfloat16
EXTRA = 8


def rope_table(width, rows):
    half = width // 2
    freq = ROPE_BASE ** (-(np.arange(half, dtype=np.float64) * 2.0 / width))
    turns = np.concatenate([freq, freq]) / (2.0 * np.pi)
    pieces, rest = [], turns
    for _ in range(2):
        scale = 2.0 ** (np.floor(np.log2(rest)) - 7.0)
        part = np.floor(rest / scale) * scale
        pieces.append(part)
        rest = rest - part
    pieces.append(rest)
    sign = np.concatenate([-np.ones(half), np.ones(half)])
    angle = np.arange(rows, dtype=np.float64)[:, None] * np.concatenate([freq, freq])[None, :]
    pad = np.zeros((8 - len(pieces) - 1, width))
    return np.concatenate(
        [np.stack(pieces), sign[None], pad, np.cos(angle), np.sin(angle) * sign[None]]
    ).astype(np.float32)


def cos_sin(position, table_ref):
    def part(k):
        turn = position * table_ref[k : k + 1, :]
        return turn - jnp.floor(turn)

    turn = part(0) + part(1) + part(2)
    turn = turn - jnp.floor(turn + 0.5)
    angle = turn * (2.0 * math.pi)
    return jnp.cos(angle), jnp.sin(angle) * table_ref[3:4, :]


def in_three(value):
    high = value.astype(BF16).astype(F32)
    middle = (value - high).astype(BF16).astype(F32)
    return [high, middle, value - high - middle]


def kernel(
    side,
    start_ref,
    count_ref,
    pages_hbm,
    table_hbm,
    q_hbm,
    sk_hbm,
    sv_hbm,
    k_hbm,
    v_hbm,
    out_ref,
    pages_ref,
    table_ref,
    q_raw,
    sk_raw,
    sv_raw,
    k_raw,
    q_rows,
    cos_ref,
    sin_ref,
    kx,
    vx,
    kall,
    vall,
    kall0,
    vall0,
    vturned,
    kbias,
    rows16,
    kspan,
    vspan,
    qsrc,
    q1,
    q2,
    scores_a,
    scores_b,
    o1src,
    o1,
    o2src,
    o2,
    qlate,
    q2l,
    late_src,
    o1l,
    o1d,
    o2l,
    local_sem,
    kv_send,
    kv_recv,
    on_send,
    q0_sem,
    q1_send,
    q1_recv,
    q2_send,
    q2_recv,
    o1_send,
    o1_recv,
    o2_send,
    o2_recv,
    ql_recv,
    q2l_send,
    q2l_recv,
    o1l_send,
    o1l_recv,
    o1d_recv,
    told,
    told_far,
    side_row,
    side_col,
    span_a,
    span_b,
    top_a,
    top_b,
):
    width = q_rows.shape[1]
    rows = k_hbm.shape[0]
    half_rows = rows // 2
    units = kall.shape[0]
    toks = 2 * side
    piece = toks * GROUP
    me = lax.axis_index("seq")
    core = me % 2
    x = (me // 2) % side
    y = me // (2 * side)
    u = jnp.where(core == 0, x, y)
    v = jnp.where(core == 0, y, x)
    other = 1 - core

    def chip(px, py, pc):
        return ((py % side) * side + px % side) * 2 + pc

    def dev(pu, pv, pc):
        return chip(jnp.where(core == 0, pu, pv), jnp.where(core == 0, pv, pu), pc)

    def remote(src, dst, send, recv, device):
        return pltpu.make_async_remote_copy(
            src_ref=src,
            dst_ref=dst,
            send_sem=send,
            recv_sem=recv,
            device_id={"seq": device},
            device_id_type=MESH,
        )

    def sent(ref, sem):
        remote(ref, ref, sem, sem, chip(x, y, other)).wait_send()

    def landed(ref, sem):
        remote(ref, ref, sem, sem, chip(x, y, other)).wait_recv()

    local = {
        name: pltpu.make_async_copy(src, dst, local_sem.at[k // 3])
        for k, (name, src, dst) in enumerate(
            (
                ("pages", pages_hbm, pages_ref),
                ("table", table_hbm, table_ref),
                ("q", q_hbm, q_raw),
                ("sk", sk_hbm, sk_raw),
                ("sv", sv_hbm, sv_raw),
                ("k", k_hbm, k_raw),
            )
        )
    }
    for copy in local.values():
        copy.start()
    for h in range(KVH):
        for hf in range(2):
            pltpu.make_async_copy(
                v_hbm.at[pl.ds(hf * half_rows, half_rows), pl.ds(h * width, width)],
                vx.at[h, hf],
                local_sem.at[2],
            ).start()

    barrier = pltpu.get_barrier_semaphore()

    def signal(sem, device):
        pl.semaphore_signal(sem, inc=1, device_id={"seq": device}, device_id_type=MESH)

    neighbours = ((1, 0), (side - 1, 0), (0, 1), (0, side - 1))
    line0 = jnp.where(y == 0, x, jnp.where(x == 0, y, 0))
    by_chip0 = (line0 == 1) | (line0 == side - 1)

    @pl.when((core == 0) & by_chip0)
    def _():
        signal(barrier, chip(0, 0, 0))

    @pl.when(core == 1)
    def _():
        signal(barrier, chip(x, y, 0))
        for dx, dy in neighbours:
            signal(barrier, chip(x + dx, y + dy, 0))
        for d in range(1, side):
            signal(barrier, chip(x + d, y, 1))
            signal(barrier, chip(x, y + d, 1))

    for name in ("pages", "table", "q"):
        local[name].wait()
    start = start_ref[0]
    count = count_ref[0]
    own_pos = (start + me).astype(F32)
    own_cos, own_sin = cos_sin(jnp.full((8, width), own_pos, F32), table_ref)
    q_all = q_raw[...].astype(F32)
    for r in range(H):
        q_rows[r : r + 1, :] = q_all[:, r * width : (r + 1) * width]
    for net in range(2):
        for e in range(2):
            for b in range(2):
                head = CLASSES * net + e + 2 * b
                part = q_rows[head * GROUP : (head + 1) * GROUP, :]
                turned = part * own_cos + pltpu.roll(part, width // 2, 1) * own_sin
                qsrc[net, e, b, core] = turned.astype(BF16)

    far_first = [side // 2]
    for step in range(side // 2 - 1, 0, -1):
        far_first += [step, side - step]

    def send_q1(toks_sent, landing, recv):
        for d in far_first:
            for net in range(2):
                place = x if net == 0 else y
                along = (place + d) % side
                remote(
                    qsrc.at[net, along % 2, :, toks_sent],
                    landing(net, place),
                    q1_send,
                    recv.at[net],
                    chip(along, y, 1) if net == 0 else chip(x, along, 1),
                ).start()

    @pl.when(core == 0)
    def _():
        pl.semaphore_wait(barrier, jnp.where(me == 0, 4 + 4 + 1, 4 + 1))
        signal(told, chip(x, y, 1))
        remote(qsrc.at[:, :, :, 0], qsrc.at[:, :, :, 0], q0_sem, q0_sem, chip(x, y, 1)).start()


    def send_cache(which):
        buf = (kx, vx)[which]

        def send_all(net, landing, target):
            def send(head, half, slot, device):
                src = buf.at[head] if half is None else buf.at[head, half]
                dst = landing.at[pl.ds(slot, 2)] if half is None else landing.at[slot]
                remote(src, dst, kv_send.at[which], kv_recv.at[which, net], device).start()

            nu, nv = (x, y) if net == 0 else (y, x)

            def at(pu, pv):
                return chip(pu, pv, target) if net == 0 else chip(pv, pu, target)

            base = nu + 2 * nv
            head = CLASSES * net + (base + 1) % CLASSES
            send(head, None, 4 + 2 * core, at(nu + 1, nv))
            head = CLASSES * net + (base + 3) % CLASSES
            send(head, None, 8 + 2 * core, at(nu + side - 1, nv))
            head = CLASSES * net + (base + 2) % CLASSES
            send(head, 0, 12 + core, at(nu, nv + 1))
            send(head, 1, 14 + core, at(nu, nv + side - 1))

        @pl.when(me != 0)
        def _():
            send_all(0, (kall0, vall0)[which], 1)

        @pl.when(me == 0)
        def _():
            send_all(0, (kall, vall)[which], 0)

        send_all(1, (kall, vall)[which], 1)
        own = ((kall, vall)[which], (kall0, vall0)[which])
        head0 = (x + 2 * y) % CLASSES
        head1 = CLASSES + (y + 2 * x) % CLASSES

        @pl.when(core == 0)
        def _():
            own[0][0:2] = buf[head0]
            remote(
                buf.at[head1],
                own[0].at[pl.ds(0, 2)],
                kv_send.at[which],
                kv_recv.at[which, 1],
                chip(x, y, 1),
            ).start()

        @pl.when(core == 1)
        def _():
            own[0][2:4] = buf[head1]
            own[1][2:4] = buf[head0]

    pltpu.make_async_copy(vx, vx, local_sem.at[2]).wait()

    @pl.when(core == 0)
    def _():
        send_cache(1)

    tile_row = lax.broadcasted_iota(jnp.int32, (EXTRA, width), 0)
    row16 = lax.broadcasted_iota(jnp.int32, (16, width), 0)
    lane = lax.broadcasted_iota(jnp.int32, (1, width), 1)
    half_pages = half_rows // PAGE
    biases = []
    for hf in range(2):
        page = jnp.zeros((1, width), jnp.int32)
        for j in range(half_pages):
            page = jnp.where(lane // PAGE == j, pages_ref[hf * half_pages + j], page)
        slot = hf * half_pages + lane // PAGE
        usable = (slot < count) & (page * PAGE + lane % PAGE < start)
        biases.append(jnp.where(usable, 0.0, DEAD).astype(F32))
    page_pos = jnp.zeros((16, width), jnp.int32)
    for j in range(rows // PAGE):
        page_pos = jnp.where(row16 == j, pages_ref[j] * PAGE, page_pos)
    page_cos, page_sin = cos_sin(page_pos.astype(F32), table_ref)
    row_cos = table_ref[8 : 8 + PAGE, :]
    row_sin = table_ref[8 + PAGE : 8 + 2 * PAGE, :]
    for j in range(rows // PAGE):
        pc_, ps_ = page_cos[j : j + 1, :], page_sin[j : j + 1, :]
        cos_ref[j * PAGE : (j + 1) * PAGE, :] = pc_ * row_cos - ps_ * row_sin
        sin_ref[j * PAGE : (j + 1) * PAGE, :] = ps_ * row_cos + pc_ * row_sin
    for name in ("sk", "sv", "k"):
        local[name].wait()
    sk_all = sk_raw[...].astype(F32)
    sv_all = sv_raw[...].astype(F32)
    for h in range(KVH):
        span = jnp.broadcast_to(sk_all[:, h * width : (h + 1) * width], (8, width))
        span = span * own_cos + pltpu.roll(span, width // 2, 1) * own_sin
        span = jnp.broadcast_to(span[0:1, :], (EXTRA, width))
        value = jnp.broadcast_to(sv_all[:, h * width : (h + 1) * width], (EXTRA, width))
        for hf in range(2):
            tile = jnp.where(tile_row == 0, span, jnp.where(tile_row == 2, value, 0.0))
            tile = jnp.where(tile_row == 1, biases[hf], tile)
            kx[h, hf, half_rows : half_rows + EXTRA, :] = tile.astype(BF16)

    @pl.loop(0, KVH // 2)
    def _(step):
        for h in (2 * step, 2 * step + 1):
            cols = pl.ds(pl.multiple_of(h * width, width), width)
            for hf in range(2):
                span_rows = slice(hf * half_rows, (hf + 1) * half_rows)
                part = k_raw[span_rows, cols].astype(F32)
                turned = part * cos_ref[span_rows, :]
                turned = turned + pltpu.roll(part, width // 2, 1) * sin_ref[span_rows, :]
                kx[h, hf, 0:half_rows, :] = turned.astype(BF16)

    @pl.when(core == 0)
    def _():
        send_cache(0)
        pl.semaphore_wait(told_far, 1)

        @pl.when(me != 0)
        def _():
            for d in far_first:
                signal(side_row, chip(x + d, y, 1))
                signal(side_col, chip(x, y + d, 1))

    @pl.when(core == 1)
    def _():
        @pl.when(me == 1)
        def _():
            pl.semaphore_wait(barrier, 2 * (side - 1))
            send_q1(1, lambda net, place: q1.at[net, :, 2 * place + 1], q1_recv)
            send_cache(1)
            send_cache(0)
            pl.semaphore_wait(told, 1)
            signal(told_far, chip(x, y, 0))
            landed(qsrc.at[:, :, :, 0], q0_sem)
            send_q1(0, lambda net, place: qlate.at[net], ql_recv)
            qlate[0] = qsrc[0, 0, :, 0]
            qlate[1] = qsrc[1, 0, :, 0]

        @pl.when(me > 1)
        def _():
            pl.semaphore_wait(told, 1)
            send_cache(1)
            pl.semaphore_wait(barrier, 2 * (side - 1))
            signal(told_far, chip(x, y, 0))
            landed(qsrc.at[:, :, :, 0], q0_sem)
            send_q1(pl.ds(0, 2), lambda net, place: q1.at[net, :, pl.ds(2 * place, 2)], q1_recv)
            send_cache(0)

    remote_units = units - 2
    near_units = units - 4

    @pl.when(core == 1)
    def _():
        for net, place in ((0, x), (1, y)):
            for b in range(2):
                q1[net, b, 2 * place + 1] = qsrc[net, place % 2, b, 1]

        @pl.when(me > 1)
        def _():
            for net, place in ((0, x), (1, y)):
                for b in range(2):
                    q1[net, b, 2 * place] = qsrc[net, place % 2, b, 0]

        for net, across in ((0, y), (1, x)):

            @pl.when(across == 0)
            def _(net=net):
                for b in range(2):
                    q1[net, b, 0] = jnp.zeros((GROUP, width), BF16)

        pl.semaphore_wait(side_col, jnp.where((x == 0) & (y != 0), side - 2, side - 1))

        def send_q2(net, pv):
            nu, nv = (x, y) if net == 0 else (y, x)
            remote(
                q1.at[net, (nu // 2 + pv) % 2],
                q2.at[nv],
                q2_send,
                q2_recv.at[nv],
                chip(x, pv, 0) if net == 0 else chip(pv, y, 1),
            ).start()

        def all_in(net, along, across):
            short = (across == 0) & (along != 0)

            @pl.when(short)
            def _():
                landed(q1.at[net, :, pl.ds(0, toks - 3)], q1_recv.at[net])

            @pl.when(jnp.logical_not(short))
            def _():
                landed(q1.at[net, :, pl.ds(0, toks - 2)], q1_recv.at[net])

        all_in(0, x, y)
        for d in far_first:
            pv = (y + d) % side

            @pl.when((x != 0) | (pv != 0))
            def _(pv=pv):
                send_q2(0, pv)

        send_q2(0, y)
        all_in(1, y, x)
        for d in far_first:
            send_q2(1, (x + d) % side)
        q2[x] = q1[1, (y // 2 + x) % 2]

        def hand_on():
            cases = [(jnp.logical_not(by_chip0), near_units, ((2, units),))]
            for here, slots in (
                ((y == 0) & (x == 1), (4, 6)),
                ((y == 0) & (x == side - 1), (8, 10)),
                ((x == 0) & (y == 1), (12, 13)),
                ((x == 0) & (y == side - 1), (14, 15)),
            ):
                spans = ((2, slots[0]), (slots[1], units))
                cases.append((here, near_units - slots[1] + slots[0], spans))
            for which, (src, dst) in ((1, (vall0, vall)), (0, (kall0, kall))):
                for here, amount, spans in cases:

                    @pl.when(here)
                    def _(which=which, src=src, dst=dst, amount=amount, spans=spans):
                        landed(src.at[pl.ds(0, amount)], kv_recv.at[which, 0])
                        for first, end in spans:
                            span = pl.ds(first, end - first)
                            remote(
                                src.at[span],
                                dst.at[span],
                                on_send.at[which],
                                kv_recv.at[which, 0],
                                chip(x, y, 0),
                            ).start()

        hand_on()

        @pl.when(y == 0)
        def _():
            @pl.when(x != 0)
            def _():
                landed(qlate.at[0], ql_recv.at[0])

            for d in far_first + [0]:
                remote(
                    qlate.at[0, (x // 2 + d) % 2], q2l, q2l_send, q2l_recv, chip(x, d, 0)
                ).start()

        @pl.when(x == 0)
        def _():
            @pl.when(y != 0)
            def _():
                landed(qlate.at[1], ql_recv.at[1])
                send_q2(0, 0)

            for d in far_first:
                remote(
                    qlate.at[1, (y // 2 + d) % 2], q2l, q2l_send, q2l_recv, chip(d, y, 1)
                ).start()
            q2l[...] = qlate[1, (y // 2) % 2]

        landed(vall.at[pl.ds(0, remote_units)], kv_recv.at[1, 1])

    @pl.when(core == 0)
    def _():
        landed(vall.at[pl.ds(0, remote_units)], kv_recv.at[1, 0])

    for unit in range(units):
        vturned[:, unit * half_rows : (unit + 1) * half_rows] = vall[unit].T

    @pl.when(core == 1)
    def _():
        landed(kall.at[pl.ds(0, remote_units)], kv_recv.at[0, 1])

    @pl.when(core == 0)
    def _():
        landed(kall.at[pl.ds(0, remote_units)], kv_recv.at[0, 0])

    span_units = [0, 2, 4, 6, 8, 10, 12, 13]
    span_toks = [
        dev(pu, pv, pc)
        for pu, pv in ((u, v), (u + side - 1, v), (u + 1, v), (u, v + side - 1))
        for pc in range(2)
    ]
    rows16[...] = jnp.zeros_like(rows16)
    for unit in range(units):
        tile = kall[unit, half_rows : half_rows + EXTRA, :].astype(F32)
        rows16[0, unit : unit + 1, :] = tile[1:2, :]
        if unit in span_units:
            k = span_units.index(unit)
            rows16[1, k : k + 1, :] = tile[0:1, :]
            rows16[2, k : k + 1, :] = tile[2:3, :]
    zeros = jnp.zeros((width - 16, width), F32)
    bias_cols = jnp.concatenate([rows16[0], zeros]).T
    for unit in range(units):
        turned = bias_cols if unit == 0 else pltpu.roll(bias_cols, width - unit, 1)
        kbias[unit * half_rows : (unit + 1) * half_rows, :] = turned.astype(BF16)
    kspan[...] = rows16[1].astype(BF16)
    vspan[...] = jnp.concatenate([rows16[2], zeros]).T.astype(BF16)
    span_tok = jnp.full((16, piece), 1 << 20, jnp.int32)
    for k, tok in enumerate(span_toks):
        span_tok = jnp.where(row16 == k, tok, span_tok)

    exponent = width**-0.5 / math.log(2.0)
    contract = (((1,), (1,)), ((), ()))
    chunk = 2 * half_rows
    cols = 2 * piece

    def send_o1(pv):
        remote(
            o1src.at[pv], o1.at[core, v], o1_send, o1_recv.at[core], dev(u, pv, 1)
        ).start()

    col_slot = lax.broadcasted_iota(jnp.int32, (1, piece), 1) // GROUP
    tok_along = jnp.where(core == 0, 2, 2 * side)
    tok_across = jnp.where(core == 0, 2 * side, 2)
    col_tok = (col_slot // 2) * tok_along + col_slot % 2
    one_hot = jnp.where(lax.broadcasted_iota(jnp.int32, (cols, width), 1) == 0, 1.0, 0.0).astype(BF16)

    scores, span_scores, tops = (scores_a, scores_b), (span_a, span_b), (top_a, top_b)
    half_units = units // 2
    half_cache = half_units * half_rows
    always = me < 4 * side * side

    def score(query, live, buf):
        n = query.shape[0]
        query = jnp.concatenate([query, one_hot[:n]], axis=1)
        s = lax.dot_general(kspan[...], query[:, :width], contract, preferred_element_type=F32)
        s_span = jnp.where(live, s, DEAD)
        span_scores[buf][:, :n] = s_span
        best = jnp.maximum(s_span[0:8], s_span[8:16])
        for p in range(2):
            span = slice(p * half_cache, (p + 1) * half_cache)
            keys = kall[p * half_units : (p + 1) * half_units, 0:half_rows, :]
            keys = jnp.concatenate([keys.reshape(half_cache, width), kbias[span, :]], axis=1)
            s = lax.dot_general(keys, query, contract, preferred_element_type=F32)
            scores[buf][span, :n] = s
            best = jnp.maximum(best, jnp.max(s.reshape(-1, 8, n), axis=0))
        tops[buf][:, :n] = jnp.maximum(jnp.max(best, axis=0, keepdims=True), FLOOR)

    def weigh(buf, n):
        top = tops[buf][:, :n]
        w = jnp.exp2((span_scores[buf][:, :n] - top) * exponent)
        total = w[0:8] + w[8:16]
        w = jnp.concatenate([w, jnp.zeros((width - 16, n), F32)])
        nums = [jnp.dot(vspan[...], w.astype(BF16), preferred_element_type=F32), None]
        for k in range(units // 2):
            w = jnp.exp2((scores[buf][k * chunk : (k + 1) * chunk, :n] - top) * exponent)
            total = total + jnp.sum(w.reshape(chunk // 8, 8, n), axis=0)
            part = jnp.dot(
                vturned[:, k * chunk : (k + 1) * chunk],
                w.astype(BF16),
                preferred_element_type=F32,
            )
            nums[k % 2] = part if nums[k % 2] is None else nums[k % 2] + part
        den = jnp.sum(total, axis=0, keepdims=True)
        stat = jnp.concatenate(in_three(top) + in_three(den) + [jnp.zeros((EXTRA - 6, n), F32)])
        return nums[0] + nums[1], stat

    def score_pair(pvs, buf):
        query = jnp.concatenate(
            [q2[pv].astype(F32).reshape(piece, width).astype(BF16) for pv in pvs]
        )
        live = jnp.concatenate([span_tok <= col_tok + pv * tok_across for pv in pvs], axis=1)
        score(query, live, buf)

    def weigh_pair(pvs, buf):
        num, stat = weigh(buf, cols)
        for k, pv in enumerate(pvs):
            lanes = slice(k * piece, (k + 1) * piece)
            o1src[pv, 0:width, :] = num[:, lanes].astype(BF16)
            o1src[pv, width : width + EXTRA, :] = stat[:, lanes].astype(BF16)

    def pair(k):
        late, away, half = (me <= 1) | by_chip0, jnp.where(v < side // 2, -1, 1), side // 2
        a, b = [(0, 1), (4, 3), (-3, 2), (-2, -1)][k]
        a, b = (v + away * a + side) % side, (v + away * b + side) % side
        early, near = (u == side // 2), (v + away + side) % side
        if k == 0:
            b = jnp.where(early & (v != 0), 0, b)
        else:
            a, b = jnp.where(early & (a == 0), near, a), jnp.where(early & (b == 0), near, b)
        a, b = jnp.where(b == 0, b, a), jnp.where(b == 0, a, b)
        return [jnp.where(late, (side - k) % side, a), jnp.where(late, k + 1, b)]

    def queries_in(pvs):
        for pv in pvs:

            @pl.when((pv != v) | (core == 0))
            def _(pv=pv):
                landed(q2.at[pv], q2_recv.at[pv])

    def results_out(pvs):
        for pv in pvs:

            @pl.when((pv != v) | (core == 0))
            def _(pv=pv):
                send_o1(pv)

            @pl.when((pv == v) & (core == 1))
            def _(pv=pv):
                o1[1, pv] = o1src[pv]

    pairs = side // 2
    queries_in(pair(0))
    score_pair(pair(0), 0)

    for k in range(pairs - 1):
        queries_in(pair(k + 1))

        @pl.when(always)
        def _(k=k):
            score_pair(pair(k + 1), (k + 1) % 2)
            weigh_pair(pair(k), k % 2)

        results_out(pair(k))

    @pl.when((core == 0) | (x != 0))
    def _():
        landed(q2l, q2l_recv)

    @pl.when(always)
    def _():
        query = jnp.concatenate([q2l[...].astype(F32), jnp.zeros((piece - GROUP, width), F32)])
        score(query.astype(BF16), span_tok <= 0, pairs % 2)
        weigh_pair(pair(pairs - 1), (pairs - 1) % 2)

    results_out(pair(pairs - 1))

    @pl.when(always)
    def _():
        num, stat = weigh(pairs % 2, piece)
        late_src[0] = num.T[0:GROUP].astype(BF16)
        wide = jnp.concatenate([stat, jnp.zeros((width - EXTRA, piece), F32)])
        late_src[1] = wide.T[0:GROUP].astype(BF16)

    far_lines = range(4, side - 3)

    def is_far(n):
        return (n >= far_lines[0]) & (n <= far_lines[-1])

    late_slot = jnp.where(core == 0, y, x)
    late_line = jnp.where(core == 0, x, y)
    late_far = is_far(late_line)
    late_to = jnp.where(
        core == 0,
        jnp.where(x == 0, 0, chip(x, 0, 1)),
        jnp.where(y == 0, 0, chip(0, y, 1)),
    )
    late_stays = (me == 0) | ((core == 1) & (x == 0) & (y != 0) & jnp.logical_not(late_far))

    @pl.when(late_far)
    def _():
        place = o1d.at[core, jnp.clip(late_line - far_lines[0], 0, len(far_lines) - 1), late_slot]
        remote(late_src, place, o1l_send, o1d_recv, chip(0, 0, 0)).start()

    @pl.when(jnp.logical_not(late_stays | late_far))
    def _():
        remote(late_src, o1l.at[core, late_slot], o1l_send, o1l_recv.at[core], late_to).start()

    @pl.when(late_stays)
    def _():
        o1l[core, late_slot] = late_src[...]

    def merge_late(parts, nu, out):
        stat = jnp.zeros((GROUP, width), F32)
        for b in range(2):
            vs = [(nu // 2 + b) % 2 + 2 * k for k in range(side // 2)]
            tops, dens = [], []
            for pv in vs:
                tile = parts[pv, 1].astype(F32)
                tile = tile + pltpu.roll(tile, width - 1, 1) + pltpu.roll(tile, width - 2, 1)
                tops.append(jnp.broadcast_to(tile[:, 0:1], (GROUP, width)))
                dens.append(jnp.broadcast_to(tile[:, 3:4], (GROUP, width)))
            top = functools.reduce(jnp.maximum, tops)
            ws = [jnp.exp2((t - top) * exponent) for t in tops]
            den = sum(w * d for w, d in zip(ws, dens))
            num = sum(w * parts[pv, 0].astype(F32) for w, pv in zip(ws, vs))
            out[b] = num.astype(BF16)
            for k, value in enumerate(in_three(top) + in_three(den)):
                stat = jnp.where(lane == 6 * b + k, value, stat)
        out[2] = stat.astype(BF16)

    def cache_gone():
        for which, buf in enumerate((kall, vall)):
            @pl.when(core == 0)
            def _(which=which, buf=buf):
                sent(buf.at[pl.ds(0, near_units + 2)], kv_send.at[which])

            @pl.when(core == 1)
            def _(which=which, buf=buf):
                sent(buf.at[pl.ds(0, near_units)], kv_send.at[which])
                for here, amount in (
                    (line0 * by_chip0 == 0, remote_units),
                    ((y == 0) & by_chip0, remote_units - 2),
                    ((x == 0) & by_chip0, remote_units - 1),
                ):

                    @pl.when(here)
                    def _(which=which, buf=buf, amount=amount):
                        sent(buf.at[pl.ds(0, amount)], on_send.at[which])

        @pl.when(jnp.logical_not(late_stays))
        def _():
            sent(late_src, o1l_send)

    @pl.when(core == 0)
    def _():
        cache_gone()

        sent(qsrc.at[:, :, :, 0], q0_sem)
        sent(o1.at[0], o1_send)

    @pl.when(core == 1)
    def _():
        pl.semaphore_wait(side_row, jnp.where((y == 0) & (x != 0), side - 2, side - 1))
        for step in range(2):
            net = jnp.where(jnp.minimum(y, side - y) <= jnp.minimum(x, side - x), step, 1 - step)
            nu = jnp.where(net == 0, x, y)
            across = jnp.where(net == 0, y, x)
            line = net * side + nu

            def owner(along, pc, net=net):
                return chip(jnp.where(net == 0, along, x), jnp.where(net == 0, y, along), pc)

            def send_o2(src, device, net=net, line=line):
                remote(src, o2.at[line], o2_send.at[net], o2_recv, device).start()

            @pl.when(net == 0)
            def _():
                landed(o1.at[0], o1_recv.at[0])

            @pl.when(net == 1)
            def _():
                landed(o1.at[1, pl.ds(0, side - 1)], o1_recv.at[1])

            stats = []
            for b in range(2):
                vs = [(nu // 2 + b) % 2 + 2 * k for k in range(side // 2)]
                tiles = [o1[net, pv, width : width + EXTRA, :].astype(F32) for pv in vs]
                tops = [t[0:1] + t[1:2] + t[2:3] for t in tiles]
                dens = [t[3:4] + t[4:5] + t[5:6] for t in tiles]
                top = functools.reduce(jnp.maximum, tops)
                ws = [jnp.exp2((t - top) * exponent) for t in tops]
                stats += in_three(top) + in_three(sum(w * d for w, d in zip(ws, dens)))
                total = None
                for w, pv in zip(ws, vs):
                    part = o1[net, pv, 0:width, :].astype(F32) * w
                    total = part if total is None else total + part
                o2src[net, :, b] = total.T.reshape(toks, GROUP, width).astype(BF16)
            stat = jnp.concatenate(stats + [jnp.zeros((width - len(stats), piece), F32)]).T
            o2src[net, :, 2] = stat.reshape(toks, GROUP, width).astype(BF16)
            for along in [0] + far_first[::-1]:

                @pl.when(nu != along)
                def _(along=along):
                    send_o2(o2src.at[net, 2 * along + 1], owner(along, 1))

                if along:
                    send_o2(o2src.at[net, 2 * along], owner(along, 0))

            @pl.when(across != 0)
            def _():
                send_o2(o2src.at[net, 0], owner(0, 0))

            o2[line] = o2src[net, 2 * nu + 1]

            @pl.when((across == 0) & (me != 1) & jnp.logical_not(is_far(nu)))
            def _(net=net, nu=nu):
                @pl.when(net == 0)
                def _():
                    landed(o1l.at[0], o1l_recv.at[0])

                @pl.when(net == 1)
                def _():
                    landed(o1l.at[1, pl.ds(0, side - 1)], o1l_recv.at[1])

                merge_late(o1l.at[net], nu, o2l)
                send_o2(o2l, owner(0, 0))

        cache_gone()

        @pl.when(me == 1)
        def _():
            sent(q1.at[:, :, pl.ds(0, toks - 2)], q1_send)
            sent(q2.at[0, pl.ds(0, toks - 1)], q2l_send)

        @pl.when((me != 1) & (y == 0))
        def _():
            sent(q2.at[0, pl.ds(0, side)], q2l_send)

        @pl.when((me != 1) & (x == 0))
        def _():
            sent(q2.at[0, pl.ds(0, side - 1)], q2l_send)

        @pl.when(me > 1)
        def _():
            sent(q1.at[:, :, pl.ds(0, toks - 2)], q1_send)

        sent(vall.at[pl.ds(0, toks - 1)], q2_send)
        sent(o1.at[0, pl.ds(0, side - 1)], o1_send)
        landed(o2.at[pl.ds(0, toks - 2)], o2_recv)

    @pl.when(core == 0)
    def _():
        @pl.when(me != 0)
        def _():
            landed(o2, o2_recv)

        @pl.when(me == 0)
        def _():
            landed(o1l.at[0, pl.ds(0, side - 1)], o1l_recv.at[0])
            landed(o1l.at[1], o1l_recv.at[1])
            merge_late(o1l.at[0], 0, o2.at[0])
            merge_late(o1l.at[1], 0, o2.at[side])
            landed(o1d, o1d_recv)
            for net in range(2):
                for k, line in enumerate(far_lines):
                    merge_late(o1d.at[net, k], line, o2.at[net * side + line])
            landed(o2.at[pl.ds(0, toks - 2 - 2 * len(far_lines))], o2_recv)

    tops, dens = [[], []], [[], []]
    for src in range(toks):
        tile = o2[src, 2].astype(F32)
        tile = tile + pltpu.roll(tile, width - 1, 1) + pltpu.roll(tile, width - 2, 1)
        for b in range(2):
            tops[b].append(jnp.broadcast_to(tile[:, 6 * b : 6 * b + 1], (GROUP, width)))
            dens[b].append(jnp.broadcast_to(tile[:, 6 * b + 3 : 6 * b + 4], (GROUP, width)))
    for net in range(2):
        for e in range(2):
            srcs = [net * side + e + 2 * k for k in range(side // 2)]
            for b in range(2):
                top = functools.reduce(jnp.maximum, [tops[b][s] for s in srcs])
                ws = [jnp.exp2((tops[b][s] - top) * exponent) for s in srcs]
                den = sum(w * dens[b][s] for w, s in zip(ws, srcs))
                num = sum(w * o2[s, b].astype(F32) for w, s in zip(ws, srcs))
                head = CLASSES * net + e + 2 * b
                out_ref[head * GROUP : (head + 1) * GROUP, :] = num / den

    @pl.when(core == 1)
    def _():
        for net, nu, across in ((0, x, y), (1, y, x)):
            fewer = (across == 0) & ((me == 1) | is_far(nu))

            @pl.when(fewer)
            def _(net=net):
                sent(o2src.at[net, pl.ds(0, toks - 2)], o2_send.at[net])

            @pl.when(jnp.logical_not(fewer))
            def _(net=net):
                sent(o2src.at[net, pl.ds(0, toks - 1)], o2_send.at[net])


def solution(mesh):
    seq = mesh.shape["seq"]
    side = math.isqrt(seq // 2)

    def body(
        queries, span_keys, span_values, cache_keys, cache_values, page_table, page_counts, span_start
    ):
        width = queries.shape[1] // H
        rows = cache_keys.shape[0]
        half = rows // 2
        toks = 2 * side
        piece = toks * GROUP
        table = jnp.asarray(rope_table(width, PAGE))
        units = 16
        vm = pltpu.VMEM
        dma = pltpu.SemaphoreType.DMA
        hbm = pl.BlockSpec(memory_space=pl.ANY)
        smem = pl.BlockSpec(memory_space=pltpu.SMEM)
        vmem = pl.BlockSpec(memory_space=pltpu.VMEM)
        scratch = [
            pltpu.SMEM(page_table.shape, jnp.int32),
            vm(table.shape, F32),
            vm((1, H * width), BF16),
            vm((1, KVH * width), BF16),
            vm((1, KVH * width), BF16),
            vm((rows, KVH * width), BF16),
            vm((H, width), F32),
            vm((rows, width), F32),
            vm((rows, width), F32),
            vm((KVH, 2, half + EXTRA, width), BF16),
            vm((KVH, 2, half, width), BF16),
            vm((units, half + EXTRA, width), BF16),
            vm((units, half, width), BF16),
            vm((units, half + EXTRA, width), BF16),
            vm((units, half, width), BF16),
            vm((width, units * half), BF16),
            vm((units * half, width), BF16),
            vm((3, 16, width), F32),
            vm((16, width), BF16),
            vm((width, width), BF16),
            vm((2, 2, 2, 2, GROUP, width), BF16),
            vm((2, 2, toks, GROUP, width), BF16),
            vm((side, toks, GROUP, width), BF16),
            vm((units * half, 2 * piece), F32),
            vm((units * half, 2 * piece), F32),
            vm((side, width + EXTRA, piece), BF16),
            vm((2, side, width + EXTRA, piece), BF16),
            vm((2, toks, 3, GROUP, width), BF16),
            vm((toks, 3, GROUP, width), BF16),
            vm((2, 2, GROUP, width), BF16),
            vm((GROUP, width), BF16),
            vm((2, GROUP, width), BF16),
            vm((2, side, 2, GROUP, width), BF16),
            vm((2, side - 7, side, 2, GROUP, width), BF16),
            vm((3, GROUP, width), BF16),
            dma((3,)),
            dma((2,)),
            dma((2, 2)),
            dma((2,)),
            dma(()),
            dma(()),
            dma((2,)),
            dma(()),
            dma((side,)),
            dma(()),
            dma((2,)),
            dma((2,)),
            dma(()),
            dma((2,)),
            dma(()),
            dma(()),
            dma(()),
            dma((2,)),
            dma(()),
            pltpu.SemaphoreType.REGULAR,
            pltpu.SemaphoreType.REGULAR,
            pltpu.SemaphoreType.REGULAR,
            pltpu.SemaphoreType.REGULAR,
            vm((16, 2 * piece), F32),
            vm((16, 2 * piece), F32),
            vm((1, 2 * piece), F32),
            vm((1, 2 * piece), F32),
        ]
        out = pl.pallas_call(
            functools.partial(kernel, side),
            out_shape=pltpu.VMEM((H, width), F32),
            in_specs=[smem] * 2 + [hbm] * 7,
            out_specs=pl.BlockSpec(memory_space=pltpu.VMEM),
            scratch_shapes=scratch,
            compiler_params=pltpu.CompilerParams(collective_id=0, has_side_effects=True),
            name="paged_prefix",
        )(
            span_start,
            page_counts,
            page_table,
            table,
            queries,
            span_keys,
            span_values,
            cache_keys,
            cache_values,
        )
        return out.reshape(queries.shape).astype(BF16)

    in_specs = (
        P(("groups", "seq"), None),
        P(("groups", "seq"), None),
        P(("groups", "seq"), None),
        P(("groups", "seq"), None),
        P(("groups", "seq"), None),
        P(("groups", "seq")),
        P(("groups", "seq")),
        P("groups"),
    )
    out_specs = P(("groups", "seq"), None)
    return jax.shard_map(body, mesh=mesh, in_specs=in_specs, out_specs=out_specs, check_vma=False)
```

```python
import functools
import math

import jax
import jax.numpy as jnp
import numpy as np
from jax import lax
from jax.experimental import pallas as pl
from jax.experimental.pallas import tpu as pltpu
from jax.sharding import PartitionSpec as P

H = 64
KVH = 8
PAGE = 16
GROUP = H // KVH
ROPE_BASE = 1000000.0
DEAD = -1e30
FLOOR = -1e29
CLASSES = 4
MESH = pl.DeviceIdType.MESH
F32 = jnp.float32
BF16 = jnp.bfloat16
EXTRA = 8


def rope_table(width, rows):
    half = width // 2
    freq = ROPE_BASE ** (-(np.arange(half, dtype=np.float64) * 2.0 / width))
    turns = np.concatenate([freq, freq]) / (2.0 * np.pi)
    pieces, rest = [], turns
    for _ in range(2):
        scale = 2.0 ** (np.floor(np.log2(rest)) - 7.0)
        part = np.floor(rest / scale) * scale
        pieces.append(part)
        rest = rest - part
    pieces.append(rest)
    sign = np.concatenate([-np.ones(half), np.ones(half)])
    angle = np.arange(rows, dtype=np.float64)[:, None] * np.concatenate([freq, freq])[None, :]
    pad = np.zeros((8 - len(pieces) - 1, width))
    return np.concatenate(
        [np.stack(pieces), sign[None], pad, np.cos(angle), np.sin(angle) * sign[None]]
    ).astype(np.float32)


def cos_sin(position, table_ref):
    def part(k):
        turn = position * table_ref[k : k + 1, :]
        return turn - jnp.floor(turn)

    turn = part(0) + part(1) + part(2)
    turn = turn - jnp.floor(turn + 0.5)
    angle = turn * (2.0 * math.pi)
    return jnp.cos(angle), jnp.sin(angle) * table_ref[3:4, :]


def in_three(value):
    high = value.astype(BF16).astype(F32)
    middle = (value - high).astype(BF16).astype(F32)
    return [high, middle, value - high - middle]


def kernel(
    side,
    start_ref,
    count_ref,
    pages_hbm,
    table_hbm,
    q_hbm,
    sk_hbm,
    sv_hbm,
    k_hbm,
    v_hbm,
    out_ref,
    pages_ref,
    table_ref,
    q_raw,
    sk_raw,
    sv_raw,
    k_raw,
    q_rows,
    cos_ref,
    sin_ref,
    kx,
    vx,
    kall,
    vall,
    kall0,
    vall0,
    vturned,
    kbias,
    rows16,
    kspan,
    vspan,
    qsrc,
    q1,
    q2,
    scores_a,
    scores_b,
    o1src,
    o1,
    o2src,
    o2,
    qlate,
    q2l,
    late_src,
    o1l,
    o1d,
    o2l,
    local_sem,
    kv_send,
    kv_recv,
    on_send,
    q0_sem,
    q1_send,
    q1_recv,
    q2_send,
    q2_recv,
    o1_send,
    o1_recv,
    o2_send,
    o2_recv,
    ql_recv,
    q2l_send,
    q2l_recv,
    o1l_send,
    o1l_recv,
    o1d_recv,
    told,
    told_far,
    side_row,
    side_col,
    span_a,
    span_b,
    top_a,
    top_b,
):
    width = q_rows.shape[1]
    rows = k_hbm.shape[0]
    half_rows = rows // 2
    units = kall.shape[0]
    toks = 2 * side
    piece = toks * GROUP
    me = lax.axis_index("seq")
    core = me % 2
    x = (me // 2) % side
    y = me // (2 * side)
    u = jnp.where(core == 0, x, y)
    v = jnp.where(core == 0, y, x)
    other = 1 - core

    def chip(px, py, pc):
        return ((py % side) * side + px % side) * 2 + pc

    def dev(pu, pv, pc):
        return chip(jnp.where(core == 0, pu, pv), jnp.where(core == 0, pv, pu), pc)

    def remote(src, dst, send, recv, device):
        return pltpu.make_async_remote_copy(
            src_ref=src,
            dst_ref=dst,
            send_sem=send,
            recv_sem=recv,
            device_id={"seq": device},
            device_id_type=MESH,
        )

    def sent(ref, sem):
        remote(ref, ref, sem, sem, chip(x, y, other)).wait_send()

    def landed(ref, sem):
        remote(ref, ref, sem, sem, chip(x, y, other)).wait_recv()

    local = {
        name: pltpu.make_async_copy(src, dst, local_sem.at[k // 3])
        for k, (name, src, dst) in enumerate(
            (
                ("pages", pages_hbm, pages_ref),
                ("table", table_hbm, table_ref),
                ("q", q_hbm, q_raw),
                ("sk", sk_hbm, sk_raw),
                ("sv", sv_hbm, sv_raw),
                ("k", k_hbm, k_raw),
            )
        )
    }
    for copy in local.values():
        copy.start()
    for h in range(KVH):
        for hf in range(2):
            pltpu.make_async_copy(
                v_hbm.at[pl.ds(hf * half_rows, half_rows), pl.ds(h * width, width)],
                vx.at[h, hf],
                local_sem.at[2],
            ).start()

    barrier = pltpu.get_barrier_semaphore()

    def signal(sem, device):
        pl.semaphore_signal(sem, inc=1, device_id={"seq": device}, device_id_type=MESH)

    neighbours = ((1, 0), (side - 1, 0), (0, 1), (0, side - 1))
    line0 = jnp.where(y == 0, x, jnp.where(x == 0, y, 0))
    by_chip0 = (line0 == 1) | (line0 == side - 1)

    @pl.when((core == 0) & by_chip0)
    def _():
        signal(barrier, chip(0, 0, 0))

    @pl.when(core == 1)
    def _():
        signal(barrier, chip(x, y, 0))
        for dx, dy in neighbours:
            signal(barrier, chip(x + dx, y + dy, 0))
        for d in range(1, side):
            signal(barrier, chip(x + d, y, 1))
            signal(barrier, chip(x, y + d, 1))

    for name in ("pages", "table", "q"):
        local[name].wait()
    start = start_ref[0]
    count = count_ref[0]
    own_pos = (start + me).astype(F32)
    own_cos, own_sin = cos_sin(jnp.full((8, width), own_pos, F32), table_ref)
    q_all = q_raw[...].astype(F32)
    for r in range(H):
        q_rows[r : r + 1, :] = q_all[:, r * width : (r + 1) * width]
    for net in range(2):
        for e in range(2):
            for b in range(2):
                head = CLASSES * net + e + 2 * b
                part = q_rows[head * GROUP : (head + 1) * GROUP, :]
                turned = part * own_cos + pltpu.roll(part, width // 2, 1) * own_sin
                qsrc[net, e, b, core] = turned.astype(BF16)

    far_first = [side // 2]
    for step in range(side // 2 - 1, 0, -1):
        far_first += [step, side - step]

    def send_q1(toks_sent, landing, recv):
        for d in far_first:
            for net in range(2):
                place = x if net == 0 else y
                along = (place + d) % side
                remote(
                    qsrc.at[net, along % 2, :, toks_sent],
                    landing(net, place),
                    q1_send,
                    recv.at[net],
                    chip(along, y, 1) if net == 0 else chip(x, along, 1),
                ).start()

    @pl.when(core == 0)
    def _():
        pl.semaphore_wait(barrier, jnp.where(me == 0, 4 + 4 + 1, 4 + 1))
        signal(told, chip(x, y, 1))
        remote(qsrc.at[:, :, :, 0], qsrc.at[:, :, :, 0], q0_sem, q0_sem, chip(x, y, 1)).start()


    def send_cache(which):
        buf = (kx, vx)[which]

        def send_all(net, landing, target):
            def send(head, half, slot, device):
                src = buf.at[head] if half is None else buf.at[head, half]
                dst = landing.at[pl.ds(slot, 2)] if half is None else landing.at[slot]
                remote(src, dst, kv_send.at[which], kv_recv.at[which, net], device).start()

            nu, nv = (x, y) if net == 0 else (y, x)

            def at(pu, pv):
                return chip(pu, pv, target) if net == 0 else chip(pv, pu, target)

            base = nu + 2 * nv
            head = CLASSES * net + (base + 1) % CLASSES
            send(head, None, 4 + 2 * core, at(nu + 1, nv))
            head = CLASSES * net + (base + 3) % CLASSES
            send(head, None, 8 + 2 * core, at(nu + side - 1, nv))
            head = CLASSES * net + (base + 2) % CLASSES
            send(head, 0, 12 + core, at(nu, nv + 1))
            send(head, 1, 14 + core, at(nu, nv + side - 1))

        @pl.when(me != 0)
        def _():
            send_all(0, (kall0, vall0)[which], 1)

        @pl.when(me == 0)
        def _():
            send_all(0, (kall, vall)[which], 0)

        send_all(1, (kall, vall)[which], 1)
        own = ((kall, vall)[which], (kall0, vall0)[which])
        head0 = (x + 2 * y) % CLASSES
        head1 = CLASSES + (y + 2 * x) % CLASSES

        @pl.when(core == 0)
        def _():
            own[0][0:2] = buf[head0]
            remote(
                buf.at[head1],
                own[0].at[pl.ds(0, 2)],
                kv_send.at[which],
                kv_recv.at[which, 1],
                chip(x, y, 1),
            ).start()

        @pl.when(core == 1)
        def _():
            own[0][2:4] = buf[head1]
            own[1][2:4] = buf[head0]

    pltpu.make_async_copy(vx, vx, local_sem.at[2]).wait()

    @pl.when(core == 0)
    def _():
        send_cache(1)

    tile_row = lax.broadcasted_iota(jnp.int32, (EXTRA, width), 0)
    row16 = lax.broadcasted_iota(jnp.int32, (16, width), 0)
    lane = lax.broadcasted_iota(jnp.int32, (1, width), 1)
    half_pages = half_rows // PAGE
    biases = []
    for hf in range(2):
        page = jnp.zeros((1, width), jnp.int32)
        for j in range(half_pages):
            page = jnp.where(lane // PAGE == j, pages_ref[hf * half_pages + j], page)
        slot = hf * half_pages + lane // PAGE
        usable = (slot < count) & (page * PAGE + lane % PAGE < start)
        biases.append(jnp.where(usable, 0.0, DEAD).astype(F32))
    page_pos = jnp.zeros((16, width), jnp.int32)
    for j in range(rows // PAGE):
        page_pos = jnp.where(row16 == j, pages_ref[j] * PAGE, page_pos)
    page_cos, page_sin = cos_sin(page_pos.astype(F32), table_ref)
    row_cos = table_ref[8 : 8 + PAGE, :]
    row_sin = table_ref[8 + PAGE : 8 + 2 * PAGE, :]
    for j in range(rows // PAGE):
        pc_, ps_ = page_cos[j : j + 1, :], page_sin[j : j + 1, :]
        cos_ref[j * PAGE : (j + 1) * PAGE, :] = pc_ * row_cos - ps_ * row_sin
        sin_ref[j * PAGE : (j + 1) * PAGE, :] = ps_ * row_cos + pc_ * row_sin
    for name in ("sk", "sv", "k"):
        local[name].wait()
    sk_all = sk_raw[...].astype(F32)
    sv_all = sv_raw[...].astype(F32)
    for h in range(KVH):
        span = jnp.broadcast_to(sk_all[:, h * width : (h + 1) * width], (8, width))
        span = span * own_cos + pltpu.roll(span, width // 2, 1) * own_sin
        span = jnp.broadcast_to(span[0:1, :], (EXTRA, width))
        value = jnp.broadcast_to(sv_all[:, h * width : (h + 1) * width], (EXTRA, width))
        for hf in range(2):
            tile = jnp.where(tile_row == 0, span, jnp.where(tile_row == 2, value, 0.0))
            tile = jnp.where(tile_row == 1, biases[hf], tile)
            kx[h, hf, half_rows : half_rows + EXTRA, :] = tile.astype(BF16)

    @pl.loop(0, KVH // 2)
    def _(step):
        for h in (2 * step, 2 * step + 1):
            cols = pl.ds(pl.multiple_of(h * width, width), width)
            for hf in range(2):
                span_rows = slice(hf * half_rows, (hf + 1) * half_rows)
                part = k_raw[span_rows, cols].astype(F32)
                turned = part * cos_ref[span_rows, :]
                turned = turned + pltpu.roll(part, width // 2, 1) * sin_ref[span_rows, :]
                kx[h, hf, 0:half_rows, :] = turned.astype(BF16)

    @pl.when(core == 0)
    def _():
        send_cache(0)
        pl.semaphore_wait(told_far, 1)

        @pl.when(me != 0)
        def _():
            for d in far_first:
                signal(side_row, chip(x + d, y, 1))
                signal(side_col, chip(x, y + d, 1))

    @pl.when(core == 1)
    def _():
        @pl.when(me == 1)
        def _():
            pl.semaphore_wait(barrier, 2 * (side - 1))
            send_q1(1, lambda net, place: q1.at[net, :, 2 * place + 1], q1_recv)
            send_cache(1)
            send_cache(0)
            pl.semaphore_wait(told, 1)
            signal(told_far, chip(x, y, 0))
            landed(qsrc.at[:, :, :, 0], q0_sem)
            send_q1(0, lambda net, place: qlate.at[net], ql_recv)
            qlate[0] = qsrc[0, 0, :, 0]
            qlate[1] = qsrc[1, 0, :, 0]

        @pl.when(me > 1)
        def _():
            pl.semaphore_wait(told, 1)
            send_cache(1)
            pl.semaphore_wait(barrier, 2 * (side - 1))
            signal(told_far, chip(x, y, 0))
            landed(qsrc.at[:, :, :, 0], q0_sem)
            send_q1(pl.ds(0, 2), lambda net, place: q1.at[net, :, pl.ds(2 * place, 2)], q1_recv)
            send_cache(0)

    remote_units = units - 2
    near_units = units - 4

    @pl.when(core == 1)
    def _():
        for net, place in ((0, x), (1, y)):
            for b in range(2):
                q1[net, b, 2 * place + 1] = qsrc[net, place % 2, b, 1]

        @pl.when(me > 1)
        def _():
            for net, place in ((0, x), (1, y)):
                for b in range(2):
                    q1[net, b, 2 * place] = qsrc[net, place % 2, b, 0]

        for net, across in ((0, y), (1, x)):

            @pl.when(across == 0)
            def _(net=net):
                for b in range(2):
                    q1[net, b, 0] = jnp.zeros((GROUP, width), BF16)

        pl.semaphore_wait(side_col, jnp.where((x == 0) & (y != 0), side - 2, side - 1))

        def send_q2(net, pv):
            nu, nv = (x, y) if net == 0 else (y, x)
            remote(
                q1.at[net, (nu // 2 + pv) % 2],
                q2.at[nv],
                q2_send,
                q2_recv.at[nv],
                chip(x, pv, 0) if net == 0 else chip(pv, y, 1),
            ).start()

        def all_in(net, along, across):
            short = (across == 0) & (along != 0)

            @pl.when(short)
            def _():
                landed(q1.at[net, :, pl.ds(0, toks - 3)], q1_recv.at[net])

            @pl.when(jnp.logical_not(short))
            def _():
                landed(q1.at[net, :, pl.ds(0, toks - 2)], q1_recv.at[net])

        all_in(0, x, y)
        for d in far_first:
            pv = (y + d) % side

            @pl.when((x != 0) | (pv != 0))
            def _(pv=pv):
                send_q2(0, pv)

        send_q2(0, y)
        all_in(1, y, x)
        for d in far_first:
            send_q2(1, (x + d) % side)
        q2[x] = q1[1, (y // 2 + x) % 2]

        def hand_on():
            cases = [(jnp.logical_not(by_chip0), near_units, ((2, units),))]
            for here, slots in (
                ((y == 0) & (x == 1), (4, 6)),
                ((y == 0) & (x == side - 1), (8, 10)),
                ((x == 0) & (y == 1), (12, 13)),
                ((x == 0) & (y == side - 1), (14, 15)),
            ):
                spans = ((2, slots[0]), (slots[1], units))
                cases.append((here, near_units - slots[1] + slots[0], spans))
            for which, (src, dst) in ((1, (vall0, vall)), (0, (kall0, kall))):
                for here, amount, spans in cases:

                    @pl.when(here)
                    def _(which=which, src=src, dst=dst, amount=amount, spans=spans):
                        landed(src.at[pl.ds(0, amount)], kv_recv.at[which, 0])
                        for first, end in spans:
                            span = pl.ds(first, end - first)
                            remote(
                                src.at[span],
                                dst.at[span],
                                on_send.at[which],
                                kv_recv.at[which, 0],
                                chip(x, y, 0),
                            ).start()

        hand_on()

        @pl.when(y == 0)
        def _():
            @pl.when(x != 0)
            def _():
                landed(qlate.at[0], ql_recv.at[0])

            for d in far_first + [0]:
                remote(
                    qlate.at[0, (x // 2 + d) % 2], q2l, q2l_send, q2l_recv, chip(x, d, 0)
                ).start()

        @pl.when(x == 0)
        def _():
            @pl.when(y != 0)
            def _():
                landed(qlate.at[1], ql_recv.at[1])
                send_q2(0, 0)

            for d in far_first:
                remote(
                    qlate.at[1, (y // 2 + d) % 2], q2l, q2l_send, q2l_recv, chip(d, y, 1)
                ).start()
            q2l[...] = qlate[1, (y // 2) % 2]

        landed(vall.at[pl.ds(0, remote_units)], kv_recv.at[1, 1])

    @pl.when(core == 0)
    def _():
        landed(vall.at[pl.ds(0, remote_units)], kv_recv.at[1, 0])

    for unit in range(units):
        vturned[:, unit * half_rows : (unit + 1) * half_rows] = vall[unit].T

    @pl.when(core == 1)
    def _():
        landed(kall.at[pl.ds(0, remote_units)], kv_recv.at[0, 1])

    @pl.when(core == 0)
    def _():
        landed(kall.at[pl.ds(0, remote_units)], kv_recv.at[0, 0])

    span_units = [0, 2, 4, 6, 8, 10, 12, 13]
    span_toks = [
        dev(pu, pv, pc)
        for pu, pv in ((u, v), (u + side - 1, v), (u + 1, v), (u, v + side - 1))
        for pc in range(2)
    ]
    rows16[...] = jnp.zeros_like(rows16)
    for unit in range(units):
        tile = kall[unit, half_rows : half_rows + EXTRA, :].astype(F32)
        rows16[0, unit : unit + 1, :] = tile[1:2, :]
        if unit in span_units:
            k = span_units.index(unit)
            rows16[1, k : k + 1, :] = tile[0:1, :]
            rows16[2, k : k + 1, :] = tile[2:3, :]
    zeros = jnp.zeros((width - 16, width), F32)
    bias_cols = jnp.concatenate([rows16[0], zeros]).T
    for unit in range(units):
        turned = bias_cols if unit == 0 else pltpu.roll(bias_cols, width - unit, 1)
        kbias[unit * half_rows : (unit + 1) * half_rows, :] = turned.astype(BF16)
    kspan[...] = rows16[1].astype(BF16)
    vspan[...] = jnp.concatenate([rows16[2], zeros]).T.astype(BF16)
    span_tok = jnp.full((16, piece), 1 << 20, jnp.int32)
    for k, tok in enumerate(span_toks):
        span_tok = jnp.where(row16 == k, tok, span_tok)

    exponent = width**-0.5 / math.log(2.0)
    contract = (((1,), (1,)), ((), ()))
    chunk = 2 * half_rows
    cols = 2 * piece

    def send_o1(pv):
        remote(
            o1src.at[pv], o1.at[core, v], o1_send, o1_recv.at[core], dev(u, pv, 1)
        ).start()

    col_slot = lax.broadcasted_iota(jnp.int32, (1, piece), 1) // GROUP
    tok_along = jnp.where(core == 0, 2, 2 * side)
    tok_across = jnp.where(core == 0, 2 * side, 2)
    col_tok = (col_slot // 2) * tok_along + col_slot % 2
    one_hot = jnp.where(lax.broadcasted_iota(jnp.int32, (cols, width), 1) == 0, 1.0, 0.0).astype(BF16)

    scores, span_scores, tops = (scores_a, scores_b), (span_a, span_b), (top_a, top_b)
    half_units = units // 2
    half_cache = half_units * half_rows
    always = me < 4 * side * side

    def score(query, live, buf):
        n = query.shape[0]
        query = jnp.concatenate([query, one_hot[:n]], axis=1)
        s = lax.dot_general(kspan[...], query[:, :width], contract, preferred_element_type=F32)
        s_span = jnp.where(live, s, DEAD)
        span_scores[buf][:, :n] = s_span
        best = jnp.maximum(s_span[0:8], s_span[8:16])
        for p in range(2):
            span = slice(p * half_cache, (p + 1) * half_cache)
            keys = kall[p * half_units : (p + 1) * half_units, 0:half_rows, :]
            keys = jnp.concatenate([keys.reshape(half_cache, width), kbias[span, :]], axis=1)
            s = lax.dot_general(keys, query, contract, preferred_element_type=F32)
            scores[buf][span, :n] = s
            best = jnp.maximum(best, jnp.max(s.reshape(-1, 8, n), axis=0))
        tops[buf][:, :n] = jnp.maximum(jnp.max(best, axis=0, keepdims=True), FLOOR)

    def weigh(buf, n):
        top = tops[buf][:, :n]
        w = jnp.exp2((span_scores[buf][:, :n] - top) * exponent)
        total = w[0:8] + w[8:16]
        w = jnp.concatenate([w, jnp.zeros((width - 16, n), F32)])
        nums = [jnp.dot(vspan[...], w.astype(BF16), preferred_element_type=F32), None]
        for k in range(units // 2):
            w = jnp.exp2((scores[buf][k * chunk : (k + 1) * chunk, :n] - top) * exponent)
            total = total + jnp.sum(w.reshape(chunk // 8, 8, n), axis=0)
            part = jnp.dot(
                vturned[:, k * chunk : (k + 1) * chunk],
                w.astype(BF16),
                preferred_element_type=F32,
            )
            nums[k % 2] = part if nums[k % 2] is None else nums[k % 2] + part
        den = jnp.sum(total, axis=0, keepdims=True)
        stat = jnp.concatenate(in_three(top) + in_three(den) + [jnp.zeros((EXTRA - 6, n), F32)])
        return nums[0] + nums[1], stat

    def score_pair(pvs, buf):
        query = jnp.concatenate(
            [q2[pv].astype(F32).reshape(piece, width).astype(BF16) for pv in pvs]
        )
        live = jnp.concatenate([span_tok <= col_tok + pv * tok_across for pv in pvs], axis=1)
        score(query, live, buf)

    def weigh_pair(pvs, buf):
        num, stat = weigh(buf, cols)
        for k, pv in enumerate(pvs):
            lanes = slice(k * piece, (k + 1) * piece)
            o1src[pv, 0:width, :] = num[:, lanes].astype(BF16)
            o1src[pv, width : width + EXTRA, :] = stat[:, lanes].astype(BF16)

    def pair(k):
        late, away, half = (me <= 1) | by_chip0, jnp.where(v < side // 2, -1, 1), side // 2
        a, b = [(0, 1), (4, 3), (-3, 2), (-2, -1)][k]
        a, b = (v + away * a + side) % side, (v + away * b + side) % side
        early, near = ((u >= 3) & (u <= side - 3)), (v + away + side) % side
        if k == 0:
            b = jnp.where(early & (v != 0), 0, b)
        else:
            a, b = jnp.where(early & (a == 0), near, a), jnp.where(early & (b == 0), near, b)
        a, b = jnp.where(b == 0, b, a), jnp.where(b == 0, a, b)
        return [jnp.where(late, (side - k) % side, a), jnp.where(late, k + 1, b)]

    def queries_in(pvs):
        for pv in pvs:

            @pl.when((pv != v) | (core == 0))
            def _(pv=pv):
                landed(q2.at[pv], q2_recv.at[pv])

    def results_out(pvs):
        for pv in pvs:

            @pl.when((pv != v) | (core == 0))
            def _(pv=pv):
                send_o1(pv)

            @pl.when((pv == v) & (core == 1))
            def _(pv=pv):
                o1[1, pv] = o1src[pv]

    pairs = side // 2
    queries_in(pair(0))
    score_pair(pair(0), 0)

    for k in range(pairs - 1):
        queries_in(pair(k + 1))

        @pl.when(always)
        def _(k=k):
            score_pair(pair(k + 1), (k + 1) % 2)
            weigh_pair(pair(k), k % 2)

        results_out(pair(k))

    @pl.when((core == 0) | (x != 0))
    def _():
        landed(q2l, q2l_recv)

    @pl.when(always)
    def _():
        query = jnp.concatenate([q2l[...].astype(F32), jnp.zeros((piece - GROUP, width), F32)])
        score(query.astype(BF16), span_tok <= 0, pairs % 2)
        weigh_pair(pair(pairs - 1), (pairs - 1) % 2)

    results_out(pair(pairs - 1))

    @pl.when(always)
    def _():
        num, stat = weigh(pairs % 2, piece)
        late_src[0] = num.T[0:GROUP].astype(BF16)
        wide = jnp.concatenate([stat, jnp.zeros((width - EXTRA, piece), F32)])
        late_src[1] = wide.T[0:GROUP].astype(BF16)

    far_lines = range(4, side - 3)

    def is_far(n):
        return (n >= far_lines[0]) & (n <= far_lines[-1])

    late_slot = jnp.where(core == 0, y, x)
    late_line = jnp.where(core == 0, x, y)
    late_far = is_far(late_line)
    late_to = jnp.where(
        core == 0,
        jnp.where(x == 0, 0, chip(x, 0, 1)),
        jnp.where(y == 0, 0, chip(0, y, 1)),
    )
    late_stays = (me == 0) | ((core == 1) & (x == 0) & (y != 0) & jnp.logical_not(late_far))

    @pl.when(late_far)
    def _():
        place = o1d.at[core, jnp.clip(late_line - far_lines[0], 0, len(far_lines) - 1), late_slot]
        remote(late_src, place, o1l_send, o1d_recv, chip(0, 0, 0)).start()

    @pl.when(jnp.logical_not(late_stays | late_far))
    def _():
        remote(late_src, o1l.at[core, late_slot], o1l_send, o1l_recv.at[core], late_to).start()

    @pl.when(late_stays)
    def _():
        o1l[core, late_slot] = late_src[...]

    def merge_late(parts, nu, out):
        stat = jnp.zeros((GROUP, width), F32)
        for b in range(2):
            vs = [(nu // 2 + b) % 2 + 2 * k for k in range(side // 2)]
            tops, dens = [], []
            for pv in vs:
                tile = parts[pv, 1].astype(F32)
                tile = tile + pltpu.roll(tile, width - 1, 1) + pltpu.roll(tile, width - 2, 1)
                tops.append(jnp.broadcast_to(tile[:, 0:1], (GROUP, width)))
                dens.append(jnp.broadcast_to(tile[:, 3:4], (GROUP, width)))
            top = functools.reduce(jnp.maximum, tops)
            ws = [jnp.exp2((t - top) * exponent) for t in tops]
            den = sum(w * d for w, d in zip(ws, dens))
            num = sum(w * parts[pv, 0].astype(F32) for w, pv in zip(ws, vs))
            out[b] = num.astype(BF16)
            for k, value in enumerate(in_three(top) + in_three(den)):
                stat = jnp.where(lane == 6 * b + k, value, stat)
        out[2] = stat.astype(BF16)

    def cache_gone():
        for which, buf in enumerate((kall, vall)):
            @pl.when(core == 0)
            def _(which=which, buf=buf):
                sent(buf.at[pl.ds(0, near_units + 2)], kv_send.at[which])

            @pl.when(core == 1)
            def _(which=which, buf=buf):
                sent(buf.at[pl.ds(0, near_units)], kv_send.at[which])
                for here, amount in (
                    (line0 * by_chip0 == 0, remote_units),
                    ((y == 0) & by_chip0, remote_units - 2),
                    ((x == 0) & by_chip0, remote_units - 1),
                ):

                    @pl.when(here)
                    def _(which=which, buf=buf, amount=amount):
                        sent(buf.at[pl.ds(0, amount)], on_send.at[which])

        @pl.when(jnp.logical_not(late_stays))
        def _():
            sent(late_src, o1l_send)

    @pl.when(core == 0)
    def _():
        cache_gone()

        sent(qsrc.at[:, :, :, 0], q0_sem)
        sent(o1.at[0], o1_send)

    @pl.when(core == 1)
    def _():
        pl.semaphore_wait(side_row, jnp.where((y == 0) & (x != 0), side - 2, side - 1))
        for step in range(2):
            net = jnp.where(jnp.minimum(y, side - y) <= jnp.minimum(x, side - x), step, 1 - step)
            nu = jnp.where(net == 0, x, y)
            across = jnp.where(net == 0, y, x)
            line = net * side + nu

            def owner(along, pc, net=net):
                return chip(jnp.where(net == 0, along, x), jnp.where(net == 0, y, along), pc)

            def send_o2(src, device, net=net, line=line):
                remote(src, o2.at[line], o2_send.at[net], o2_recv, device).start()

            @pl.when(net == 0)
            def _():
                landed(o1.at[0], o1_recv.at[0])

            @pl.when(net == 1)
            def _():
                landed(o1.at[1, pl.ds(0, side - 1)], o1_recv.at[1])

            stats = []
            for b in range(2):
                vs = [(nu // 2 + b) % 2 + 2 * k for k in range(side // 2)]
                tiles = [o1[net, pv, width : width + EXTRA, :].astype(F32) for pv in vs]
                tops = [t[0:1] + t[1:2] + t[2:3] for t in tiles]
                dens = [t[3:4] + t[4:5] + t[5:6] for t in tiles]
                top = functools.reduce(jnp.maximum, tops)
                ws = [jnp.exp2((t - top) * exponent) for t in tops]
                stats += in_three(top) + in_three(sum(w * d for w, d in zip(ws, dens)))
                total = None
                for w, pv in zip(ws, vs):
                    part = o1[net, pv, 0:width, :].astype(F32) * w
                    total = part if total is None else total + part
                o2src[net, :, b] = total.T.reshape(toks, GROUP, width).astype(BF16)
            stat = jnp.concatenate(stats + [jnp.zeros((width - len(stats), piece), F32)]).T
            o2src[net, :, 2] = stat.reshape(toks, GROUP, width).astype(BF16)
            for along in [0] + far_first[::-1]:

                @pl.when(nu != along)
                def _(along=along):
                    send_o2(o2src.at[net, 2 * along + 1], owner(along, 1))

                if along:
                    send_o2(o2src.at[net, 2 * along], owner(along, 0))

            @pl.when(across != 0)
            def _():
                send_o2(o2src.at[net, 0], owner(0, 0))

            o2[line] = o2src[net, 2 * nu + 1]

            @pl.when((across == 0) & (me != 1) & jnp.logical_not(is_far(nu)))
            def _(net=net, nu=nu):
                @pl.when(net == 0)
                def _():
                    landed(o1l.at[0], o1l_recv.at[0])

                @pl.when(net == 1)
                def _():
                    landed(o1l.at[1, pl.ds(0, side - 1)], o1l_recv.at[1])

                merge_late(o1l.at[net], nu, o2l)
                send_o2(o2l, owner(0, 0))

        cache_gone()

        @pl.when(me == 1)
        def _():
            sent(q1.at[:, :, pl.ds(0, toks - 2)], q1_send)
            sent(q2.at[0, pl.ds(0, toks - 1)], q2l_send)

        @pl.when((me != 1) & (y == 0))
        def _():
            sent(q2.at[0, pl.ds(0, side)], q2l_send)

        @pl.when((me != 1) & (x == 0))
        def _():
            sent(q2.at[0, pl.ds(0, side - 1)], q2l_send)

        @pl.when(me > 1)
        def _():
            sent(q1.at[:, :, pl.ds(0, toks - 2)], q1_send)

        sent(vall.at[pl.ds(0, toks - 1)], q2_send)
        sent(o1.at[0, pl.ds(0, side - 1)], o1_send)
        landed(o2.at[pl.ds(0, toks - 2)], o2_recv)

    @pl.when(core == 0)
    def _():
        @pl.when(me != 0)
        def _():
            landed(o2, o2_recv)

        @pl.when(me == 0)
        def _():
            landed(o1l.at[0, pl.ds(0, side - 1)], o1l_recv.at[0])
            landed(o1l.at[1], o1l_recv.at[1])
            merge_late(o1l.at[0], 0, o2.at[0])
            merge_late(o1l.at[1], 0, o2.at[side])
            landed(o1d, o1d_recv)
            for net in range(2):
                for k, line in enumerate(far_lines):
                    merge_late(o1d.at[net, k], line, o2.at[net * side + line])
            landed(o2.at[pl.ds(0, toks - 2 - 2 * len(far_lines))], o2_recv)

    tops, dens = [[], []], [[], []]
    for src in range(toks):
        tile = o2[src, 2].astype(F32)
        tile = tile + pltpu.roll(tile, width - 1, 1) + pltpu.roll(tile, width - 2, 1)
        for b in range(2):
            tops[b].append(jnp.broadcast_to(tile[:, 6 * b : 6 * b + 1], (GROUP, width)))
            dens[b].append(jnp.broadcast_to(tile[:, 6 * b + 3 : 6 * b + 4], (GROUP, width)))
    for net in range(2):
        for e in range(2):
            srcs = [net * side + e + 2 * k for k in range(side // 2)]
            for b in range(2):
                top = functools.reduce(jnp.maximum, [tops[b][s] for s in srcs])
                ws = [jnp.exp2((tops[b][s] - top) * exponent) for s in srcs]
                den = sum(w * dens[b][s] for w, s in zip(ws, srcs))
                num = sum(w * o2[s, b].astype(F32) for w, s in zip(ws, srcs))
                head = CLASSES * net + e + 2 * b
                out_ref[head * GROUP : (head + 1) * GROUP, :] = num / den

    @pl.when(core == 1)
    def _():
        for net, nu, across in ((0, x, y), (1, y, x)):
            fewer = (across == 0) & ((me == 1) | is_far(nu))

            @pl.when(fewer)
            def _(net=net):
                sent(o2src.at[net, pl.ds(0, toks - 2)], o2_send.at[net])

            @pl.when(jnp.logical_not(fewer))
            def _(net=net):
                sent(o2src.at[net, pl.ds(0, toks - 1)], o2_send.at[net])


def solution(mesh):
    seq = mesh.shape["seq"]
    side = math.isqrt(seq // 2)

    def body(
        queries, span_keys, span_values, cache_keys, cache_values, page_table, page_counts, span_start
    ):
        width = queries.shape[1] // H
        rows = cache_keys.shape[0]
        half = rows // 2
        toks = 2 * side
        piece = toks * GROUP
        table = jnp.asarray(rope_table(width, PAGE))
        units = 16
        vm = pltpu.VMEM
        dma = pltpu.SemaphoreType.DMA
        hbm = pl.BlockSpec(memory_space=pl.ANY)
        smem = pl.BlockSpec(memory_space=pltpu.SMEM)
        vmem = pl.BlockSpec(memory_space=pltpu.VMEM)
        scratch = [
            pltpu.SMEM(page_table.shape, jnp.int32),
            vm(table.shape, F32),
            vm((1, H * width), BF16),
            vm((1, KVH * width), BF16),
            vm((1, KVH * width), BF16),
            vm((rows, KVH * width), BF16),
            vm((H, width), F32),
            vm((rows, width), F32),
            vm((rows, width), F32),
            vm((KVH, 2, half + EXTRA, width), BF16),
            vm((KVH, 2, half, width), BF16),
            vm((units, half + EXTRA, width), BF16),
            vm((units, half, width), BF16),
            vm((units, half + EXTRA, width), BF16),
            vm((units, half, width), BF16),
            vm((width, units * half), BF16),
            vm((units * half, width), BF16),
            vm((3, 16, width), F32),
            vm((16, width), BF16),
            vm((width, width), BF16),
            vm((2, 2, 2, 2, GROUP, width), BF16),
            vm((2, 2, toks, GROUP, width), BF16),
            vm((side, toks, GROUP, width), BF16),
            vm((units * half, 2 * piece), F32),
            vm((units * half, 2 * piece), F32),
            vm((side, width + EXTRA, piece), BF16),
            vm((2, side, width + EXTRA, piece), BF16),
            vm((2, toks, 3, GROUP, width), BF16),
            vm((toks, 3, GROUP, width), BF16),
            vm((2, 2, GROUP, width), BF16),
            vm((GROUP, width), BF16),
            vm((2, GROUP, width), BF16),
            vm((2, side, 2, GROUP, width), BF16),
            vm((2, side - 7, side, 2, GROUP, width), BF16),
            vm((3, GROUP, width), BF16),
            dma((3,)),
            dma((2,)),
            dma((2, 2)),
            dma((2,)),
            dma(()),
            dma(()),
            dma((2,)),
            dma(()),
            dma((side,)),
            dma(()),
            dma((2,)),
            dma((2,)),
            dma(()),
            dma((2,)),
            dma(()),
            dma(()),
            dma(()),
            dma((2,)),
            dma(()),
            pltpu.SemaphoreType.REGULAR,
            pltpu.SemaphoreType.REGULAR,
            pltpu.SemaphoreType.REGULAR,
            pltpu.SemaphoreType.REGULAR,
            vm((16, 2 * piece), F32),
            vm((16, 2 * piece), F32),
            vm((1, 2 * piece), F32),
            vm((1, 2 * piece), F32),
        ]
        out = pl.pallas_call(
            functools.partial(kernel, side),
            out_shape=pltpu.VMEM((H, width), F32),
            in_specs=[smem] * 2 + [hbm] * 7,
            out_specs=pl.BlockSpec(memory_space=pltpu.VMEM),
            scratch_shapes=scratch,
            compiler_params=pltpu.CompilerParams(collective_id=0, has_side_effects=True),
            name="paged_prefix",
        )(
            span_start,
            page_counts,
            page_table,
            table,
            queries,
            span_keys,
            span_values,
            cache_keys,
            cache_values,
        )
        return out.reshape(queries.shape).astype(BF16)

    in_specs = (
        P(("groups", "seq"), None),
        P(("groups", "seq"), None),
        P(("groups", "seq"), None),
        P(("groups", "seq"), None),
        P(("groups", "seq"), None),
        P(("groups", "seq")),
        P(("groups", "seq")),
        P("groups"),
    )
    out_specs = P(("groups", "seq"), None)
    return jax.shard_map(body, mesh=mesh, in_specs=in_specs, out_specs=out_specs, check_vma=False)
```
